8 devices in a mesh: replica: 1 (over z), model: 8 (over y, x, core).
Axes of the slice: x: 2, y: 2, z: 1, core: 2. Of those that a mesh axis runs over, the one named last changes fastest.
Arguments:
- prompt: bfloat16 [8, 1024, 4096], P('replica', 'model')
- lengths: int32 [8], P('replica')
- new_tok: bfloat16 [8, 4096], P('replica')
- norm_attn: bfloat16 [1, 4096], replicated
- w_q: bfloat16 [1, 4096, 4096], P(None, None, 'model')
- w_k: bfloat16 [1, 4096, 4096], P(None, None, 'model')
- w_v: bfloat16 [1, 4096, 4096], P(None, None, 'model')
- w_o: bfloat16 [1, 4096, 4096], P(None, 'model')
- norm_mlp: bfloat16 [1, 4096], replicated
- w_gate: bfloat16 [1, 4096, 11008], P(None, None, 'model')
- w_up: bfloat16 [1, 4096, 11008], P(None, None, 'model')
- w_down: bfloat16 [1, 11008, 4096], P(None, 'model')
Outputs:
- output 1: bfloat16 [8, 4096], P('replica')
- output 2: bfloat16 [8, 4096], P('replica')
- output 3: bfloat16 [1, 8, 1025, 32, 128], P(None, 'replica', None, 'model')
- output 4: bfloat16 [1, 8, 1025, 32, 128], P(None, 'replica', None, 'model')
All inputs are finite; a program needn't handle non-finite values.
Results may differ from the reference program's by a relative error of at most 0.0108766.
Values are sent between devices in bfloat16 or wider.
A program may use at most 1 GiB of HBM per device.

```python
import jax
import jax.numpy as jnp
from jax import lax

BATCH_SIZE = 8
SEQ_LEN = 1024
Q_BLOCK = 128
D_MODEL = 4096
NUM_HEADS = 32
KV_HEADS = 32
HEAD_DIM = 128
FF_DIM = 11008
N_LAYERS = 1

Q_WIDTH = NUM_HEADS * HEAD_DIM
KV_WIDTH = KV_HEADS * HEAD_DIM
GROUP_SIZE = NUM_HEADS // KV_HEADS
N_QBLOCKS = SEQ_LEN // Q_BLOCK
N_TOKENS = BATCH_SIZE * SEQ_LEN


def setup_inputs(seed: int = 0, part: int = 0) -> dict:
    part_keys = jax.random.split(jax.random.fold_in(jax.random.key(seed), part), 4)
    shared_keys = jax.random.split(jax.random.key(seed + 1), 9)
    qk_scale = (2.0 / D_MODEL) ** 0.5
    in_scale = D_MODEL ** -0.5

    def normal_bf16(rng_key, dims, scale_val):
        return (jax.random.normal(rng_key, dims, jnp.float32) * scale_val).astype(jnp.bfloat16)

    def gain_bf16(rng_key):
        return jax.random.uniform(rng_key, (N_LAYERS, D_MODEL), jnp.float32, 0.6, 1.4).astype(jnp.bfloat16)

    lengths = jax.random.randint(part_keys[1], (BATCH_SIZE,), SEQ_LEN // 2 + 1, SEQ_LEN + 1)
    full_row = jax.random.randint(part_keys[2], (), 0, BATCH_SIZE)
    lengths = jnp.where(jnp.arange(BATCH_SIZE) == full_row, SEQ_LEN, lengths).astype(jnp.int32)
    return {
        'prompt': normal_bf16(part_keys[0], (BATCH_SIZE, SEQ_LEN, D_MODEL), 1.0),
        'lengths': lengths,
        'new_tok': normal_bf16(part_keys[3], (BATCH_SIZE, D_MODEL), 1.0),
        'norm_attn': gain_bf16(shared_keys[0]),
        'w_q': normal_bf16(shared_keys[1], (N_LAYERS, D_MODEL, Q_WIDTH), qk_scale),
        'w_k': normal_bf16(shared_keys[2], (N_LAYERS, D_MODEL, KV_WIDTH), qk_scale),
        'w_v': normal_bf16(shared_keys[3], (N_LAYERS, D_MODEL, KV_WIDTH), in_scale),
        'w_o': normal_bf16(shared_keys[4], (N_LAYERS, Q_WIDTH, D_MODEL), Q_WIDTH ** -0.5),
        'norm_mlp': gain_bf16(shared_keys[5]),
        'w_gate': normal_bf16(shared_keys[6], (N_LAYERS, D_MODEL, FF_DIM), in_scale),
        'w_up': normal_bf16(shared_keys[7], (N_LAYERS, D_MODEL, FF_DIM), in_scale),
        'w_down': normal_bf16(shared_keys[8], (N_LAYERS, FF_DIM, D_MODEL), FF_DIM ** -0.5),
    }


def rms_norm(hidden, gain_vec):
    hid_f32 = hidden.astype(jnp.float32)
    inv_rms = lax.rsqrt(jnp.mean(hid_f32 * hid_f32, axis=-1, keepdims=True) + 1e-5)
    return (hid_f32 * inv_rms * gain_vec.astype(jnp.float32)).astype(jnp.bfloat16)


def rotary(heads_f32, positions):
    half_dim = HEAD_DIM // 2
    inv_freq = 10000.0 ** (-2.0 * jnp.arange(half_dim, dtype=jnp.float32) / HEAD_DIM)
    angles = positions.astype(jnp.float32)[..., None] * inv_freq
    cos_tab = jnp.cos(angles)[..., None, :]
    sin_tab = jnp.sin(angles)[..., None, :]
    lo_half = heads_f32[..., :half_dim]
    hi_half = heads_f32[..., half_dim:]
    return jnp.concatenate([lo_half * cos_tab - hi_half * sin_tab, hi_half * cos_tab + lo_half * sin_tab], axis=-1)


def prefill_attention(queries, key_rot, val_proj, lengths):
    q_blocks = jnp.moveaxis(queries.astype(jnp.float32).reshape(BATCH_SIZE, N_QBLOCKS, Q_BLOCK, KV_HEADS, GROUP_SIZE, HEAD_DIM), 1, 0)
    key_f32 = key_rot.astype(jnp.float32)
    val_f32 = val_proj.astype(jnp.float32)
    key_pos = jnp.arange(SEQ_LEN)
    key_valid = key_pos[None, :] < lengths[:, None]

    def one_block(block_args):
        q_blk, blk_idx = block_args
        q_pos = blk_idx * Q_BLOCK + jnp.arange(Q_BLOCK)
        scores = jnp.einsum('bqhgd,bkhd->bqhgk', q_blk, key_f32) * (HEAD_DIM ** -0.5)
        visible = (key_pos[None, None, :] <= q_pos[None, :, None]) & key_valid[:, None, :]
        scores = jnp.where(visible[:, :, None, None, :], scores, -1e30)
        attn_prob = jax.nn.softmax(scores, axis=-1)
        return jnp.einsum('bqhgk,bkhd->bqhgd', attn_prob, val_f32)

    blocks_out = lax.map(one_block, (q_blocks, jnp.arange(N_QBLOCKS)))
    return jnp.moveaxis(blocks_out, 0, 1).reshape(BATCH_SIZE, SEQ_LEN, Q_WIDTH).astype(jnp.bfloat16)


def decode_attention(q_new, key_cache, value_cache, lengths):
    q_f32 = q_new.astype(jnp.float32).reshape(BATCH_SIZE, KV_HEADS, GROUP_SIZE, HEAD_DIM)
    scores = jnp.einsum('bhgd,bkhd->bhgk', q_f32, key_cache.astype(jnp.float32)) * (HEAD_DIM ** -0.5)
    cache_pos = jnp.arange(SEQ_LEN + 1)
    visible = (cache_pos[None, :] < lengths[:, None]) | (cache_pos[None, :] == SEQ_LEN)
    scores = jnp.where(visible[:, None, None, :], scores, -1e30)
    attn_prob = jax.nn.softmax(scores, axis=-1)
    out_f32 = jnp.einsum('bhgk,bkhd->bhgd', attn_prob, value_cache.astype(jnp.float32))
    return out_f32.reshape(BATCH_SIZE, Q_WIDTH).astype(jnp.bfloat16)


def reference(prompt, lengths, new_tok, norm_attn, w_q, w_k, w_v, w_o, norm_mlp, w_gate, w_up, w_down):
    seq_pos = jnp.arange(SEQ_LEN)

    def layer_step(loop_state, layer_w):
        hidden, dec_hidden = loop_state
        g_attn, wq_l, wk_l, wv_l, wo_l, g_mlp, wg_l, wu_l, wd_l = layer_w
        normed = rms_norm(hidden, g_attn).reshape(N_TOKENS, D_MODEL)
        q_rot = rotary(jnp.dot(normed, wq_l, preferred_element_type=jnp.float32).reshape(BATCH_SIZE, SEQ_LEN, NUM_HEADS, HEAD_DIM), seq_pos).astype(jnp.bfloat16)
        k_rot = rotary(jnp.dot(normed, wk_l, preferred_element_type=jnp.float32).reshape(BATCH_SIZE, SEQ_LEN, KV_HEADS, HEAD_DIM), seq_pos).astype(jnp.bfloat16)
        v_proj = jnp.dot(normed, wv_l, preferred_element_type=jnp.float32).astype(jnp.bfloat16).reshape(BATCH_SIZE, SEQ_LEN, KV_HEADS, HEAD_DIM)
        attn_out = prefill_attention(q_rot, k_rot, v_proj, lengths).reshape(N_TOKENS, Q_WIDTH)
        hidden = (hidden.astype(jnp.float32) + jnp.dot(attn_out, wo_l, preferred_element_type=jnp.float32).reshape(BATCH_SIZE, SEQ_LEN, D_MODEL)).astype(jnp.bfloat16)
        normed = rms_norm(hidden, g_mlp).reshape(N_TOKENS, D_MODEL)
        mlp_mid = (jax.nn.silu(jnp.dot(normed, wg_l, preferred_element_type=jnp.float32)) * jnp.dot(normed, wu_l, preferred_element_type=jnp.float32)).astype(jnp.bfloat16)
        hidden = (hidden.astype(jnp.float32) + jnp.dot(mlp_mid, wd_l, preferred_element_type=jnp.float32).reshape(BATCH_SIZE, SEQ_LEN, D_MODEL)).astype(jnp.bfloat16)

        tok_norm = rms_norm(dec_hidden, g_attn)
        q_new = rotary(jnp.dot(tok_norm, wq_l, preferred_element_type=jnp.float32).reshape(BATCH_SIZE, NUM_HEADS, HEAD_DIM), lengths).astype(jnp.bfloat16)
        k_new = rotary(jnp.dot(tok_norm, wk_l, preferred_element_type=jnp.float32).reshape(BATCH_SIZE, KV_HEADS, HEAD_DIM), lengths).astype(jnp.bfloat16)
        v_new = jnp.dot(tok_norm, wv_l, preferred_element_type=jnp.float32).astype(jnp.bfloat16).reshape(BATCH_SIZE, KV_HEADS, HEAD_DIM)
        key_cache = jnp.concatenate([k_rot, k_new[:, None]], axis=1)
        value_cache = jnp.concatenate([v_proj, v_new[:, None]], axis=1)
        tok_attn = decode_attention(q_new, key_cache, value_cache, lengths)
        dec_hidden = (dec_hidden.astype(jnp.float32) + jnp.dot(tok_attn, wo_l, preferred_element_type=jnp.float32)).astype(jnp.bfloat16)
        tok_norm = rms_norm(dec_hidden, g_mlp)
        tok_mid = (jax.nn.silu(jnp.dot(tok_norm, wg_l, preferred_element_type=jnp.float32)) * jnp.dot(tok_norm, wu_l, preferred_element_type=jnp.float32)).astype(jnp.bfloat16)
        dec_hidden = (dec_hidden.astype(jnp.float32) + jnp.dot(tok_mid, wd_l, preferred_element_type=jnp.float32)).astype(jnp.bfloat16)
        return (hidden, dec_hidden), (key_cache, value_cache)

    (hidden, dec_hidden), (key_cache, value_cache) = lax.scan(layer_step, (prompt, new_tok), (norm_attn, w_q, w_k, w_v, w_o, norm_mlp, w_gate, w_up, w_down))
    last_sel = seq_pos[None, :] == (lengths - 1)[:, None]
    last_hidden = jnp.sum(jnp.where(last_sel[:, :, None], hidden.astype(jnp.float32), 0.0), axis=1).astype(jnp.bfloat16)
    return dec_hidden, last_hidden, key_cache, value_cache
```

```python
import functools

import jax
import jax.numpy as jnp
from jax import lax
from jax.experimental import pallas as pl
from jax.experimental.pallas import tpu as pltpu
from jax.sharding import PartitionSpec as P


HEAD_DIM = 128
NEG_BIG = -1e30
STAT_ROWS = 8
MESH = pl.DeviceIdType.MESH


def rms_norm(hidden, gain_vec):
    hid_f32 = hidden.astype(jnp.float32)
    inv_rms = lax.rsqrt(jnp.mean(hid_f32 * hid_f32, axis=-1, keepdims=True) + 1e-5)
    return (hid_f32 * inv_rms * gain_vec.astype(jnp.float32)).astype(jnp.bfloat16)


def rotary_tables(positions):
    half_dim = HEAD_DIM // 2
    inv_freq = 10000.0 ** (-2.0 * jnp.arange(half_dim, dtype=jnp.float32) / HEAD_DIM)
    angles = positions.astype(jnp.float32)[..., None] * inv_freq
    cos_tab = jnp.cos(angles)
    sin_tab = jnp.sin(angles)
    return jnp.concatenate([cos_tab, cos_tab], axis=-1), jnp.concatenate([-sin_tab, sin_tab], axis=-1)


def rotate(heads_f32, cos_tab, sin_tab):
    half_dim = HEAD_DIM // 2
    swapped = jnp.concatenate([heads_f32[..., half_dim:], heads_f32[..., :half_dim]], axis=-1)
    return heads_f32 * cos_tab + swapped * sin_tab


def kv_kernel(n_in, with_new, sc_ref, *refs):
    x_refs = refs[:n_in]
    cos_refs = refs[n_in:2 * n_in]
    sin_refs = refs[2 * n_in:3 * n_in]
    rest = refs[3 * n_in:]
    wk_ref, wv_ref, gain_ref, q_ref = rest[:4]
    rest = rest[4:]
    if with_new:
        knew_ref, vnew_ref, _ = rest[:3]
        rest = rest[3:]
    else:
        rest = rest[3:]
    kc_ref, vc_ref, st_ref, n_buf, k_buf, v_buf, k_out, v_out, s_out, sems, new_sem = rest
    step = pl.program_id(0)
    n_steps = pl.num_programs(0)
    slot = lax.rem(step, 2)
    blk = x_refs[0].shape[1]
    width = wk_ref.shape[1]
    heads = width // HEAD_DIM

    def out_copies(which, at_step):
        copies = []
        for i in range(n_in):
            shard = sc_ref[i]
            bat = sc_ref[n_in + i] + at_step
            rows = pl.ds(shard * blk, blk)
            copies.append(pltpu.make_async_copy(k_out.at[which, i], kc_ref.at[bat, rows], sems.at[which, i, 0]))
            copies.append(pltpu.make_async_copy(v_out.at[which, i], vc_ref.at[bat, rows], sems.at[which, i, 1]))
            copies.append(pltpu.make_async_copy(s_out.at[which, i], st_ref.at[shard, bat], sems.at[which, i, 2]))
        return copies

    if with_new:
        @pl.when(step == 0)
        def _():
            for idx, (src, dst) in enumerate(((knew_ref, kc_ref), (vnew_ref, vc_ref))):
                for b in range(src.shape[0]):
                    pltpu.make_async_copy(src.at[b], dst.at[b, pl.ds(dst.shape[1] - 1, 1)], new_sem.at[idx, b]).start()

    @pl.when(step >= 2)
    def _():
        for copy in out_copies(slot, step - 2):
            copy.wait()

    gain = gain_ref[...]
    for i in range(n_in):
        def norm_rows(r, carry, i=i):
            rows = pl.ds(pl.multiple_of(r * 16, 16), 16)
            xf = x_refs[i][0, rows, :].astype(jnp.float32)
            inv_rms = lax.rsqrt(jnp.mean(xf * xf, axis=-1, keepdims=True) + 1e-5)
            n_buf[pl.ds(pl.multiple_of(i * blk + r * 16, 16), 16), :] = (xf * inv_rms * gain).astype(jnp.bfloat16)
            return carry

        lax.fori_loop(0, blk // 16, norm_rows, 0)

    def col_tile(c, carry):
        cols = pl.ds(pl.multiple_of(c * 256, 256), 256)
        kf = jnp.dot(n_buf[...], wk_ref[:, cols], preferred_element_type=jnp.float32)
        parts = []
        for i in range(n_in):
            cos_tab = cos_refs[i][0]
            sin_tab = sin_refs[i][0]
            halves = []
            for h in range(2):
                kh = kf[i * blk:(i + 1) * blk, h * HEAD_DIM:(h + 1) * HEAD_DIM]
                halves.append(kh * cos_tab + pltpu.roll(kh, HEAD_DIM // 2, 1) * sin_tab)
            parts.append(jnp.concatenate(halves, axis=1))
        k_buf[:, cols] = jnp.concatenate(parts, axis=0).astype(jnp.bfloat16)
        vf = jnp.dot(n_buf[...], wv_ref[:, cols], preferred_element_type=jnp.float32)
        v_buf[:, cols] = vf.astype(jnp.bfloat16)
        return carry

    lax.fori_loop(0, width // 256, col_tile, 0)

    head_of_row = lax.broadcasted_iota(jnp.int32, (STAT_ROWS, HEAD_DIM), 0) // (STAT_ROWS // heads)
    for i in range(n_in):
        shard = sc_ref[i]
        bat = sc_ref[n_in + i] + step
        seq_len = sc_ref[2 * n_in + bat]
        k_blk = k_buf[i * blk:(i + 1) * blk, :]
        v_blk = v_buf[i * blk:(i + 1) * blk, :]
        k_out[slot, i] = k_blk.reshape(blk, heads, HEAD_DIM)
        v_out[slot, i] = v_blk.reshape(blk, heads, HEAD_DIM)
        scores = lax.dot_general(q_ref[bat], k_blk, (((1,), (1,)), ((), ())), preferred_element_type=jnp.float32) * (HEAD_DIM ** -0.5)
        pos = shard * blk + lax.broadcasted_iota(jnp.int32, scores.shape, 1)
        visible = pos < seq_len
        scores = jnp.where(visible, scores, NEG_BIG)
        blk_max = jnp.max(scores, axis=-1, keepdims=True)
        prob = jnp.where(visible, jnp.exp(scores - blk_max), 0.0)
        blk_sum = jnp.sum(prob, axis=-1, keepdims=True)
        full = jnp.dot(prob.astype(jnp.bfloat16), v_blk, preferred_element_type=jnp.float32)
        acc = jnp.zeros((STAT_ROWS, HEAD_DIM), jnp.float32)
        for h in range(heads):
            acc = jnp.where(head_of_row == h, full[:, h * HEAD_DIM:(h + 1) * HEAD_DIM], acc)
        s_out[slot, i, 0] = acc
        s_out[slot, i, 1] = jnp.broadcast_to(blk_max, (STAT_ROWS, HEAD_DIM))
        s_out[slot, i, 2] = jnp.broadcast_to(blk_sum, (STAT_ROWS, HEAD_DIM))

    for copy in out_copies(slot, step):
        copy.start()

    @pl.when(step == n_steps - 1)
    def _():
        for copy in out_copies(slot, step):
            copy.wait()
        if with_new:
            for idx, (src, dst) in enumerate(((knew_ref, kc_ref), (vnew_ref, vc_ref))):
                for b in range(src.shape[0]):
                    pltpu.make_async_copy(src.at[b], dst.at[b, pl.ds(dst.shape[1] - 1, 1)], new_sem.at[idx, b]).wait()

    @pl.when((step == n_steps - 1) & (n_steps >= 2))
    def _():
        for copy in out_copies(1 - slot, step - 1):
            copy.wait()


def kv_call(inputs, shards, batches, lengths, tabs, w_k, w_v, gain, q_diag, caches, new_rows=None):
    n_in = len(inputs)
    n_steps = inputs[0][2]
    cos_tab, sin_tab = tabs
    blk, d_model = inputs[0][0].shape[1:]
    width = w_k.shape[1]
    heads = width // HEAD_DIM
    scalars = jnp.concatenate([jnp.stack([jnp.int32(s) for s in shards]), jnp.array(batches, jnp.int32), lengths])
    in_specs = []
    operands = []
    for arr, first, _ in inputs:
        in_specs.append(pl.BlockSpec((1, blk, d_model), lambda g, sc, first=first: (first + g, 0, 0)))
        operands.append(arr)
    for tab in (cos_tab, sin_tab):
        for i in range(n_in):
            in_specs.append(pl.BlockSpec((1, blk, HEAD_DIM), lambda g, sc, i=i: (sc[i], 0, 0)))
            operands.append(tab)
    once = pl.Buffered(1)
    in_specs += [
        pl.BlockSpec((d_model, width), lambda g, sc: (0, 0), pipeline_mode=once),
        pl.BlockSpec((d_model, width), lambda g, sc: (0, 0), pipeline_mode=once),
        pl.BlockSpec((1, d_model), lambda g, sc: (0, 0)),
        pl.BlockSpec(q_diag.shape, lambda g, sc: (0, 0, 0)),
    ]
    operands += [w_k, w_v, gain, q_diag]
    any_spec = pl.BlockSpec(memory_space=pl.ANY)
    with_new = new_rows is not None
    if with_new:
        operands += [*new_rows, caches[2]]
        in_specs += [any_spec] * 3
        aliases = {len(operands): 2}
    else:
        operands += list(caches)
        in_specs += [any_spec] * 3
        aliases = {len(operands) - 2: 0, len(operands) - 1: 1, len(operands): 2}
    cache_shape = caches[0].shape
    tokens = n_in * blk
    flops = 2 * n_steps * tokens * d_model * 2 * width
    return pl.pallas_call(
        functools.partial(kv_kernel, n_in, with_new),
        grid_spec=pltpu.PrefetchScalarGridSpec(
            num_scalar_prefetch=1,
            grid=(n_steps,),
            in_specs=in_specs,
            out_specs=[any_spec] * 3,
            scratch_shapes=[
                pltpu.VMEM((tokens, d_model), jnp.bfloat16),
                pltpu.VMEM((tokens, width), jnp.bfloat16),
                pltpu.VMEM((tokens, width), jnp.bfloat16),
                pltpu.VMEM((2, n_in, blk, heads, HEAD_DIM), jnp.bfloat16),
                pltpu.VMEM((2, n_in, blk, heads, HEAD_DIM), jnp.bfloat16),
                pltpu.VMEM((2, n_in, 3, STAT_ROWS, HEAD_DIM), jnp.float32),
                pltpu.SemaphoreType.DMA((2, n_in, 3)),
                pltpu.SemaphoreType.DMA((2, cache_shape[0])),
            ],
        ),
        out_shape=[
            jax.ShapeDtypeStruct(cache_shape, jnp.bfloat16),
            jax.ShapeDtypeStruct(cache_shape, jnp.bfloat16),
            jax.ShapeDtypeStruct(caches[2].shape, jnp.float32),
        ],
        input_output_aliases=aliases,
        compiler_params=pltpu.CompilerParams(vmem_limit_bytes=28 * 2 ** 20),
        cost_estimate=pl.CostEstimate(flops=flops, bytes_accessed=2 * 2 * d_model * width + 2 * n_steps * tokens * (d_model + 2 * width), transcendentals=0),
        name="kv_chunk",
    )(scalars, *operands)


def tail_kernel(n_dev, n_part, st_ref, xs_ref, gain_ref, wo_hbm, wg_hbm, wu_hbm, wd_hbm, dec_ref, last_ref,
                wo, wg, wu, wd, stv, rows, a_buf, n_buf, ps1, pr1, ps2, pr2, xo1, xg1, xo2, xg2,
                w_sem, send_sem, recv_sem):
    me = lax.axis_index("model")
    n_batch = dec_ref.shape[0]
    n_rows = 2 * n_batch
    d_model = dec_ref.shape[1]
    cols = d_model // n_dev
    heads = STAT_ROWS // 2
    loads = [pltpu.make_async_copy(src, dst, w_sem.at[i]) for i, (src, dst) in enumerate(
        ((st_ref, stv), (wo_hbm, wo), (wg_hbm, wg), (wu_hbm, wu), (wd_hbm, wd)))]
    for load in loads:
        load.start()
    barrier = pltpu.get_barrier_semaphore()
    for k in range(1, n_dev):
        peer = lax.rem(me + k, n_dev)
        pl.semaphore_signal(barrier, inc=1, device_id={"model": peer}, device_id_type=MESH)
    pl.semaphore_wait(barrier, n_dev - 1)

    def send(phase, k, src, dst):
        peer = lax.rem(me + k, n_dev)
        return pltpu.make_async_remote_copy(
            src_ref=src, dst_ref=dst, send_sem=send_sem.at[phase, k - 1], recv_sem=recv_sem.at[phase, k - 1],
            device_id={"model": peer}, device_id_type=MESH)

    loads[0].wait()
    for b in range(n_batch):
        top = stv[0, b, 1]
        for j in range(1, n_part):
            top = jnp.maximum(top, stv[j, b, 1])
        den = jnp.zeros((STAT_ROWS, HEAD_DIM), jnp.float32)
        num = jnp.zeros((STAT_ROWS, HEAD_DIM), jnp.float32)
        for j in range(n_part):
            scale = jnp.exp(stv[j, b, 1] - top)
            den += scale * stv[j, b, 2]
            num += scale * stv[j, b, 0]
        rows[:, b, :] = num / den
    for h in range(heads):
        for t in range(2):
            a_buf[t * n_batch:(t + 1) * n_batch, h * HEAD_DIM:(h + 1) * HEAD_DIM] = rows[2 * h + t]
    att = a_buf[...].astype(jnp.bfloat16)

    def all_reduce(phase, partial, base, ps, pr, xo, xg):
        copies = []
        for k in range(1, n_dev):
            peer = lax.rem(me + k, n_dev)
            ps[k - 1] = partial(peer)
            copies.append(send(phase, k, ps.at[k - 1], pr.at[k - 1]))
            copies[-1].start()
        total = base + partial(me)
        for k in range(1, n_dev):
            copies[k - 1].wait_recv()
            total = total + pr[k - 1]
        xo[...] = total.astype(jnp.bfloat16)
        outs = []
        for k in range(1, n_dev):
            outs.append(send(phase + 1, k, xo, xg.at[me]))
            outs[-1].start()
        xg[me] = xo[...]
        for k in range(1, n_dev):
            outs[k - 1].wait_recv()
        return copies + outs

    def col_block(p):
        return pl.ds(pl.multiple_of(p * cols, cols), cols)

    loads[1].wait()
    sent = all_reduce(0, lambda p: jnp.dot(att, wo[:, col_block(p)], preferred_element_type=jnp.float32),
                      xs_ref[...].astype(jnp.float32), ps1, pr1, xo1, xg1)
    sq = jnp.zeros((n_rows, 1), jnp.float32)
    for j in range(n_dev):
        xf = xg1[j].astype(jnp.float32)
        sq += jnp.sum(xf * xf, axis=-1, keepdims=True)
    inv_rms = lax.rsqrt(sq / d_model + 1e-5)
    for j in range(n_dev):
        xf = xg1[j].astype(jnp.float32)
        n_buf[:, j * cols:(j + 1) * cols] = (xf * inv_rms * gain_ref[:, j * cols:(j + 1) * cols]).astype(jnp.bfloat16)
    loads[2].wait()
    nt = (((1,), (1,)), ((), ()))
    gate = lax.dot_general(wg[...], n_buf[...], nt, preferred_element_type=jnp.float32)
    loads[3].wait()
    up = lax.dot_general(wu[...], n_buf[...], nt, preferred_element_type=jnp.float32)
    mid_t = gate * (1.0 / (1.0 + jnp.exp(-gate))) * up
    mid = mid_t.T.astype(jnp.bfloat16)
    loads[4].wait()
    sent += all_reduce(2, lambda p: jnp.dot(mid, wd[:, col_block(p)], preferred_element_type=jnp.float32),
                       xo1[...].astype(jnp.float32), ps2, pr2, xo2, xg2)
    for j in range(n_dev):
        dec_ref[:, j * cols:(j + 1) * cols] = xg2[j, :n_batch]
        last_ref[:, j * cols:(j + 1) * cols] = xg2[j, n_batch:]
    for copy in sent:
        copy.wait_send()


def tail_call(n_dev, stats, x_mine, gain, w_o, w_gate_t, w_up_t, w_down, n_batch):
    n_rows, cols = x_mine.shape
    d_model = w_o.shape[1]
    n_part = stats.shape[0]
    vmem = pl.BlockSpec(memory_space=pltpu.VMEM)
    hbm = pl.BlockSpec(memory_space=pl.ANY)
    return pl.pallas_call(
        functools.partial(tail_kernel, n_dev, n_part),
        out_shape=[jax.ShapeDtypeStruct((n_batch, d_model), jnp.bfloat16)] * 2,
        in_specs=[hbm, vmem, vmem, hbm, hbm, hbm, hbm],
        out_specs=[vmem, vmem],
        scratch_shapes=[
            pltpu.VMEM(w_o.shape, jnp.bfloat16),
            pltpu.VMEM(w_gate_t.shape, jnp.bfloat16),
            pltpu.VMEM(w_up_t.shape, jnp.bfloat16),
            pltpu.VMEM(w_down.shape, jnp.bfloat16),
            pltpu.VMEM(stats.shape, jnp.float32),
            pltpu.VMEM((STAT_ROWS, n_batch, HEAD_DIM), jnp.float32),
            pltpu.VMEM((n_rows, w_o.shape[0]), jnp.float32),
            pltpu.VMEM((n_rows, d_model), jnp.bfloat16),
            pltpu.VMEM((n_dev - 1, n_rows, cols), jnp.float32),
            pltpu.VMEM((n_dev - 1, n_rows, cols), jnp.float32),
            pltpu.VMEM((n_dev - 1, n_rows, cols), jnp.float32),
            pltpu.VMEM((n_dev - 1, n_rows, cols), jnp.float32),
            pltpu.VMEM((n_rows, cols), jnp.bfloat16),
            pltpu.VMEM((n_dev, n_rows, cols), jnp.bfloat16),
            pltpu.VMEM((n_rows, cols), jnp.bfloat16),
            pltpu.VMEM((n_dev, n_rows, cols), jnp.bfloat16),
            pltpu.SemaphoreType.DMA((5,)),
            pltpu.SemaphoreType.DMA((4, n_dev - 1)),
            pltpu.SemaphoreType.DMA((4, n_dev - 1)),
        ],
        compiler_params=pltpu.CompilerParams(collective_id=0, has_side_effects=True, vmem_limit_bytes=52 * 2 ** 20),
        name="tail",
    )(stats, x_mine, gain, w_o, w_gate_t, w_up_t, w_down)


def solution(mesh):
    n_dev = mesh.shape['model']
    seq_spec = P('replica', 'model', None)
    col_spec = P(None, None, 'model')
    row_spec = P(None, 'model', None)
    gain_spec = P(None, None)
    tok_spec = P('replica', None)
    cache_spec = P(None, 'replica', None, 'model', None)
    in_specs = (seq_spec, P('replica'), tok_spec, gain_spec, col_spec, col_spec, col_spec, row_spec, gain_spec, col_spec, col_spec, row_spec)
    out_specs = (tok_spec, tok_spec, cache_spec, cache_spec)

    def swap(arr, bit):
        return lax.ppermute(arr, 'model', [(i, i ^ bit) for i in range(n_dev)])

    def per_device(prompt, lengths, new_tok, norm_attn, w_q, w_k, w_v, w_o, norm_mlp, w_gate, w_up, w_down):
        my_idx = lax.axis_index('model')
        n_batch, blk, d_model = prompt.shape
        seq_len = blk * n_dev
        width = w_k.shape[2]
        heads = width // HEAD_DIM
        half = n_batch // 2
        wq, wk, wv = w_q[0], w_k[0], w_v[0]

        y_parts = [(0, 1), (1, half), (half, n_batch)]
        x_parts = [(half, half + 1), (half + 1, n_batch), (0, half)]
        seq_pos = my_idx * blk + jnp.arange(blk)
        sel = (seq_pos[None, :] == (lengths - 1)[:, None]).astype(jnp.bfloat16)
        from_y, from_x = {}, {}
        from_y[y_parts[0]] = swap(prompt[0:1], 4)
        from_x[x_parts[0]] = swap(prompt[half:half + 1], 2)
        last_x = jnp.einsum('bs,bsd->bd', sel, prompt, preferred_element_type=jnp.float32).astype(jnp.bfloat16)
        last_x = last_x + swap(last_x, 1)
        rest, last_x = lax.optimization_barrier((prompt, last_x))
        last_x = (last_x + swap(last_x, 2)) + (swap(last_x, 4) + swap(last_x, 6))
        for y_part, x_part in zip(y_parts[1:], x_parts[1:]):
            from_y[y_part] = swap(rest[y_part[0]:y_part[1]], 4)
            from_x[x_part] = swap(rest[x_part[0]:x_part[1]], 2)
        core_all = swap(rest, 1)
        x_rows = jnp.concatenate([new_tok, last_x], axis=0)
        n_rows = rms_norm(x_rows, norm_attn[0])
        row_cos, row_sin = rotary_tables(jnp.stack([lengths, lengths - 1]))
        q_rows = jnp.dot(n_rows, wq, preferred_element_type=jnp.float32).reshape(2, n_batch, heads, HEAD_DIM)
        q_rows = rotate(q_rows, row_cos[:, :, None], row_sin[:, :, None]).astype(jnp.bfloat16)
        k_new = jnp.dot(n_rows[:n_batch], wk, preferred_element_type=jnp.float32).reshape(n_batch, heads, HEAD_DIM)
        k_new = rotate(k_new, row_cos[0][:, None], row_sin[0][:, None]).astype(jnp.bfloat16)
        v_new = jnp.dot(n_rows[:n_batch], wv, preferred_element_type=jnp.float32).astype(jnp.bfloat16).reshape(n_batch, heads, HEAD_DIM)

        q_bht = jnp.moveaxis(q_rows, 0, 2)
        q_diag = (q_bht[:, :, :, None, :] * jnp.eye(heads, dtype=jnp.bfloat16)[None, :, None, :, None]).reshape(n_batch, STAT_ROWS, width)
        self_score = jnp.sum(q_rows[0].astype(jnp.float32) * k_new.astype(jnp.float32), axis=-1) * (HEAD_DIM ** -0.5)
        is_new = (jnp.arange(2) == 0)[None, None, :, None]
        full = (n_batch, heads, 2, HEAD_DIM)
        self_max = jnp.where(is_new, jnp.broadcast_to(self_score[:, :, None, None], full), NEG_BIG)
        self_sum = jnp.broadcast_to(jnp.where(is_new, 1.0, 0.0), full)
        self_acc = jnp.where(is_new, v_new.astype(jnp.float32)[:, :, None, :], 0.0)
        self_stat = jnp.stack([a.reshape(n_batch, STAT_ROWS, HEAD_DIM) for a in (self_acc, self_max, self_sum)], axis=1)
        stats = jnp.zeros((n_dev + 1, n_batch, 3, STAT_ROWS, HEAD_DIM), jnp.float32).at[n_dev].set(self_stat)

        tabs = tuple(tab.reshape(n_dev, blk, HEAD_DIM) for tab in rotary_tables(jnp.arange(seq_len)))
        gain = norm_attn.astype(jnp.float32)
        cache_shape = jax.ShapeDtypeStruct((n_batch, seq_len + 1, heads, HEAD_DIM), jnp.bfloat16)
        caches = (cache_shape, cache_shape, stats)

        def run(streams, shards, batches, caches, new_rows=None):
            return kv_call(streams, shards, batches, lengths, tabs, wk, wv, gain, q_diag, caches, new_rows)

        def shard_of(bits):
            idx = my_idx
            for bit in (1, 2, 4):
                if bits & bit:
                    idx = idx + jnp.where((my_idx // bit) % 2 == 0, bit, -bit)
            return idx

        def after(caches, *arrays):
            out = lax.optimization_barrier((caches[2], *arrays))
            return (caches[0], caches[1], out[0]), out[1:]

        s_own, s_core = my_idx, shard_of(1)
        caches = run([(prompt, 0, half), (prompt, half, half)], [s_own] * 2, [0, half], caches,
                     (k_new[:, None], v_new[:, None]))
        caches, (core_all,) = after(caches, core_all)
        caches = run([(core_all, 0, half), (core_all, half, half)], [s_core] * 2, [0, half], caches)
        diag = {}
        for step, (y_part, x_part) in enumerate(zip(y_parts, x_parts)):
            n = y_part[1] - y_part[0]
            caches, (got_y, got_x) = after(caches, from_y[y_part], from_x[x_part])
            other_y, other_x = swap(got_y, 1), swap(got_x, 1)
            if step < 2:
                diag[step] = (swap(got_y, 2), swap(got_x, 4))
            caches = run([(got_y, 0, n), (got_x, 0, n)], [shard_of(4), shard_of(2)], [y_part[0], x_part[0]], caches)
            caches, (other_y, other_x) = after(caches, other_y, other_x)
            caches = run([(other_y, 0, n), (other_x, 0, n)], [shard_of(5), shard_of(3)], [y_part[0], x_part[0]], caches)
        for step in (1, 0):
            y_part, x_part = y_parts[step], x_parts[step]
            n = y_part[1] - y_part[0]
            caches, (via_x, via_y) = after(caches, *diag[step])
            other_x, other_y = swap(via_x, 1), swap(via_y, 1)
            caches = run([(via_x, 0, n), (via_y, 0, n)], [shard_of(6)] * 2, [y_part[0], x_part[0]], caches)
            caches, (other_x, other_y) = after(caches, other_x, other_y)
            caches = run([(other_x, 0, n), (other_y, 0, n)], [shard_of(7)] * 2, [y_part[0], x_part[0]], caches)

        k_cache, v_cache, stats = caches
        x_mine = lax.dynamic_slice_in_dim(x_rows, my_idx * (d_model // n_dev), d_model // n_dev, axis=1)
        dec_hidden, last_hidden = tail_call(n_dev, stats, x_mine, norm_mlp.astype(jnp.float32), w_o[0],
                                            w_gate[0].T, w_up[0].T, w_down[0], n_batch)
        return dec_hidden, last_hidden, k_cache[None], v_cache[None]

    return jax.shard_map(per_device, mesh=mesh, in_specs=in_specs, out_specs=out_specs, check_vma=False)
```

```python
import functools

import jax
import jax.numpy as jnp
from jax import lax
from jax.experimental import pallas as pl
from jax.experimental.pallas import tpu as pltpu
from jax.sharding import PartitionSpec as P


HEAD_DIM = 128
NEG_BIG = -1e30
STAT_ROWS = 8
NORM_ROWS = 32
COL_TILE = 256
MESH = pl.DeviceIdType.MESH


def rms_norm(hidden, gain_vec):
    hid_f32 = hidden.astype(jnp.float32)
    inv_rms = lax.rsqrt(jnp.mean(hid_f32 * hid_f32, axis=-1, keepdims=True) + 1e-5)
    return (hid_f32 * inv_rms * gain_vec.astype(jnp.float32)).astype(jnp.bfloat16)


def rotary_tables(positions):
    half_dim = HEAD_DIM // 2
    inv_freq = 10000.0 ** (-2.0 * jnp.arange(half_dim, dtype=jnp.float32) / HEAD_DIM)
    angles = positions.astype(jnp.float32)[..., None] * inv_freq
    cos_tab = jnp.cos(angles)
    sin_tab = jnp.sin(angles)
    return jnp.concatenate([cos_tab, cos_tab], axis=-1), jnp.concatenate([-sin_tab, sin_tab], axis=-1)


def rotate(heads_f32, cos_tab, sin_tab):
    half_dim = HEAD_DIM // 2
    swapped = jnp.concatenate([heads_f32[..., half_dim:], heads_f32[..., :half_dim]], axis=-1)
    return heads_f32 * cos_tab + swapped * sin_tab


def kv_kernel(n_in, n_groups, with_new, sc_ref, *refs):
    n_arr = n_in * n_groups
    x_refs = refs[:n_arr]
    cos_refs = refs[n_arr:n_arr + n_in]
    sin_refs = refs[n_arr + n_in:n_arr + 2 * n_in]
    wk_hbm, wv_hbm, gain_ref, q_ref = refs[n_arr + 2 * n_in:n_arr + 2 * n_in + 4]
    rest = refs[n_arr + 2 * n_in + 4:]
    if with_new:
        new_refs = rest[:2]
    (kc_ref, vc_ref, st_ref, wk, wv, n_buf, ss_buf, k_buf, v_buf, k_out, v_out, s_out, w_sem, sems, new_sem) = rest[3:]
    step = pl.program_id(0)
    n_steps = pl.num_programs(0)
    slot = lax.rem(step, 2)
    per_group = n_steps // n_groups
    blk = x_refs[0].shape[1]
    d_model = n_buf.shape[1]
    width = wk.shape[1]
    heads = width // HEAD_DIM
    n_tok = n_in * blk

    def w_copy(c, which):
        cols = pl.ds(pl.multiple_of(c * COL_TILE, COL_TILE), COL_TILE)
        src, dst = ((wk_hbm, wk), (wv_hbm, wv))[which]
        return pltpu.make_async_copy(src.at[:, cols], dst.at[:, cols], w_sem.at[c, which])

    def place(i, at_step):
        group = at_step // per_group
        return sc_ref[group * n_in + i], sc_ref[n_arr + group * n_in + i] + lax.rem(at_step, per_group)

    def out_copies(which, at_step):
        copies = []
        for i in range(n_in):
            shard, bat = place(i, at_step)
            rows = pl.ds(shard * blk, blk)
            copies.append(pltpu.make_async_copy(k_out.at[which, i], kc_ref.at[bat, rows], sems.at[which, i, 0]))
            copies.append(pltpu.make_async_copy(v_out.at[which, i], vc_ref.at[bat, rows], sems.at[which, i, 1]))
            copies.append(pltpu.make_async_copy(s_out.at[which, i], st_ref.at[shard, bat], sems.at[which, i, 2]))
        return copies

    def new_copies():
        return [pltpu.make_async_copy(src.at[b], dst.at[b, pl.ds(dst.shape[1] - 1, 1)], new_sem.at[idx, b])
                for idx, (src, dst) in enumerate(zip(new_refs, (kc_ref, vc_ref))) for b in range(src.shape[0])]

    @pl.when(step == 0)
    def _():
        for c in range(width // COL_TILE):
            for which in range(2):
                w_copy(c, which).start()
        if with_new:
            for copy in new_copies():
                copy.start()

    @pl.when(step >= 2)
    def _():
        for copy in out_copies(slot, step - 2):
            copy.wait()

    lanes = [slice(c * HEAD_DIM, (c + 1) * HEAD_DIM) for c in range(d_model // HEAD_DIM)]
    for group in range(n_groups):
        @pl.when(step // per_group == group)
        def _(group=group):
            for i in range(n_in):
                x_ref = x_refs[group * n_in + i]

                def square_rows(r, carry):
                    rows = pl.ds(pl.multiple_of(r * NORM_ROWS, NORM_ROWS), NORM_ROWS)
                    acc = [jnp.zeros((NORM_ROWS, HEAD_DIM), jnp.float32) for _ in range(2)]
                    for c, lane in enumerate(lanes):
                        xf = x_ref[0, rows, lane].astype(jnp.float32)
                        acc[c % 2] += xf * xf
                    ss_buf[pl.ds(pl.multiple_of(i * blk + r * NORM_ROWS, NORM_ROWS), NORM_ROWS), :] = acc[0] + acc[1]
                    return carry

                lax.fori_loop(0, blk // NORM_ROWS, square_rows, 0)
            total = jnp.sum(ss_buf[...], axis=-1, keepdims=True)
            ss_buf[...] = jnp.broadcast_to(lax.rsqrt(total / d_model + 1e-5), (n_tok, HEAD_DIM))
            for i in range(n_in):
                x_ref = x_refs[group * n_in + i]

                def norm_rows(r, carry):
                    rows = pl.ds(pl.multiple_of(r * NORM_ROWS, NORM_ROWS), NORM_ROWS)
                    out_rows = pl.ds(pl.multiple_of(i * blk + r * NORM_ROWS, NORM_ROWS), NORM_ROWS)
                    inv_rms = ss_buf[out_rows, :]
                    for lane in lanes:
                        xf = x_ref[0, rows, lane].astype(jnp.float32)
                        n_buf[out_rows, lane] = (xf * inv_rms * gain_ref[:, lane]).astype(jnp.bfloat16)
                    return carry

                lax.fori_loop(0, blk // NORM_ROWS, norm_rows, 0)

    def col_tile(c, carry):
        @pl.when(step == 0)
        def _():
            w_copy(c, 0).wait()
            w_copy(c, 1).wait()

        cols = pl.ds(pl.multiple_of(c * COL_TILE, COL_TILE), COL_TILE)
        kf = jnp.dot(n_buf[...], wk[:, cols], preferred_element_type=jnp.float32)
        vf = jnp.dot(n_buf[...], wv[:, cols], preferred_element_type=jnp.float32)
        v_buf[:, cols] = vf.astype(jnp.bfloat16)
        parts = []
        for i in range(n_in):
            cos_tab = cos_refs[i][0]
            sin_tab = sin_refs[i][0]
            halves = []
            for h in range(COL_TILE // HEAD_DIM):
                kh = kf[i * blk:(i + 1) * blk, h * HEAD_DIM:(h + 1) * HEAD_DIM]
                halves.append(kh * cos_tab + pltpu.roll(kh, HEAD_DIM // 2, 1) * sin_tab)
            parts.append(jnp.concatenate(halves, axis=1))
        k_buf[:, cols] = jnp.concatenate(parts, axis=0).astype(jnp.bfloat16)
        return carry

    lax.fori_loop(0, width // COL_TILE, col_tile, 0)

    head_of_row = lax.broadcasted_iota(jnp.int32, (STAT_ROWS, HEAD_DIM), 0) // (STAT_ROWS // heads)
    probs = []
    for i in range(n_in):
        shard, bat = place(i, step)
        scores = lax.dot_general(q_ref[bat], k_buf[i * blk:(i + 1) * blk, :], (((1,), (1,)), ((), ())),
                                 preferred_element_type=jnp.float32) * (HEAD_DIM ** -0.5)
        pos = shard * blk + lax.broadcasted_iota(jnp.int32, scores.shape, 1)
        visible = pos < sc_ref[2 * n_arr + bat]
        scores = jnp.where(visible, scores, NEG_BIG)
        blk_max = jnp.max(scores, axis=-1, keepdims=True)
        prob = jnp.where(visible, jnp.exp(scores - blk_max), 0.0)
        probs.append((blk_max, prob))
    stats = []
    for i, (blk_max, prob) in enumerate(probs):
        full = jnp.dot(prob.astype(jnp.bfloat16), v_buf[i * blk:(i + 1) * blk, :], preferred_element_type=jnp.float32)
        acc = jnp.zeros((STAT_ROWS, HEAD_DIM), jnp.float32)
        for h in range(heads):
            acc = jnp.where(head_of_row == h, full[:, h * HEAD_DIM:(h + 1) * HEAD_DIM], acc)
        stats.append((acc, blk_max, jnp.sum(prob, axis=-1, keepdims=True)))
    for i in range(n_in):
        k_out[slot, i] = k_buf[i * blk:(i + 1) * blk, :].reshape(blk, heads, HEAD_DIM)
        v_out[slot, i] = v_buf[i * blk:(i + 1) * blk, :].reshape(blk, heads, HEAD_DIM)
        for k, stat in enumerate(stats[i]):
            s_out[slot, i, k] = jnp.broadcast_to(stat, (STAT_ROWS, HEAD_DIM))

    for copy in out_copies(slot, step):
        copy.start()

    @pl.when(step == n_steps - 1)
    def _():
        for copy in out_copies(slot, step):
            copy.wait()
        if with_new:
            for copy in new_copies():
                copy.wait()

    @pl.when((step == n_steps - 1) & (n_steps >= 2))
    def _():
        for copy in out_copies(1 - slot, step - 1):
            copy.wait()


def kv_call(groups, per_group, shards, batches, lengths, tabs, w_k, w_v, gain, q_diag, caches, new_rows=None):
    n_groups = len(groups)
    n_in = len(groups[0])
    n_steps = n_groups * per_group
    cos_tab, sin_tab = tabs
    blk, d_model = groups[0][0][0].shape[1:]
    width = w_k.shape[1]
    heads = width // HEAD_DIM
    scalars = jnp.concatenate([jnp.stack([jnp.int32(s) for group in shards for s in group]),
                               jnp.array([b for group in batches for b in group], jnp.int32), lengths])
    in_specs = []
    operands = []
    for p, group in enumerate(groups):
        for arr, first in group:
            in_specs.append(pl.BlockSpec((1, blk, d_model), lambda g, sc, p=p, first=first: (
                first + jnp.clip(g - p * per_group, 0, per_group - 1), 0, 0)))
            operands.append(arr)
    for tab in (cos_tab, sin_tab):
        for i in range(n_in):
            in_specs.append(pl.BlockSpec((1, blk, HEAD_DIM), lambda g, sc, i=i: (sc[g // per_group * n_in + i], 0, 0)))
            operands.append(tab)
    hbm_spec = pl.BlockSpec(memory_space=pltpu.HBM)
    in_specs += [
        hbm_spec,
        hbm_spec,
        pl.BlockSpec((1, d_model), lambda g, sc: (0, 0)),
        pl.BlockSpec(q_diag.shape, lambda g, sc: (0, 0, 0)),
    ]
    operands += [pltpu.with_memory_space_constraint(w, pltpu.HBM) for w in (w_k, w_v)] + [gain, q_diag]
    any_spec = pl.BlockSpec(memory_space=pl.ANY)
    with_new = new_rows is not None
    if with_new:
        operands += [*new_rows, caches[2]]
        in_specs += [any_spec] * 3
        aliases = {len(operands): 2}
    else:
        operands += list(caches)
        in_specs += [any_spec] * 3
        aliases = {len(operands) - 2: 0, len(operands) - 1: 1, len(operands): 2}
    cache_shape = caches[0].shape
    tokens = n_in * blk
    flops = 2 * n_steps * tokens * d_model * 2 * width
    return pl.pallas_call(
        functools.partial(kv_kernel, n_in, n_groups, with_new),
        grid_spec=pltpu.PrefetchScalarGridSpec(
            num_scalar_prefetch=1,
            grid=(n_steps,),
            in_specs=in_specs,
            out_specs=[any_spec] * 3,
            scratch_shapes=[
                pltpu.VMEM((d_model, width), jnp.bfloat16),
                pltpu.VMEM((d_model, width), jnp.bfloat16),
                pltpu.VMEM((tokens, d_model), jnp.bfloat16),
                pltpu.VMEM((tokens, HEAD_DIM), jnp.float32),
                pltpu.VMEM((tokens, width), jnp.bfloat16),
                pltpu.VMEM((tokens, width), jnp.bfloat16),
                pltpu.VMEM((2, n_in, blk, heads, HEAD_DIM), jnp.bfloat16),
                pltpu.VMEM((2, n_in, blk, heads, HEAD_DIM), jnp.bfloat16),
                pltpu.VMEM((2, n_in, 3, STAT_ROWS, HEAD_DIM), jnp.float32),
                pltpu.SemaphoreType.DMA((width // COL_TILE, 2)),
                pltpu.SemaphoreType.DMA((2, n_in, 3)),
                pltpu.SemaphoreType.DMA((2, cache_shape[0])),
            ],
        ),
        out_shape=[
            jax.ShapeDtypeStruct(cache_shape, jnp.bfloat16),
            jax.ShapeDtypeStruct(cache_shape, jnp.bfloat16),
            jax.ShapeDtypeStruct(caches[2].shape, jnp.float32),
        ],
        input_output_aliases=aliases,
        compiler_params=pltpu.CompilerParams(vmem_limit_bytes=30 * 2 ** 20),
        cost_estimate=pl.CostEstimate(flops=flops, bytes_accessed=2 * 2 * d_model * width + 2 * n_steps * tokens * (d_model + 2 * width), transcendentals=0),
        name="kv_chunk",
    )(scalars, *operands)


def tail_kernel(n_dev, n_part, st_ref, xs_ref, gain_ref, wo_hbm, wg_hbm, wu_hbm, wd_hbm, dec_ref, last_ref,
                wo, wg, wu, wd, stv, rows, a_buf, n_buf, mid_buf, ps1, pr1, ps2, pr2, xo1, xg1, xo2, xg2,
                w_sem, send_sem, recv_sem):
    me = lax.axis_index("model")
    n_batch = dec_ref.shape[0]
    n_rows = 2 * n_batch
    d_model = dec_ref.shape[1]
    cols = d_model // n_dev
    heads = STAT_ROWS // 2
    loads = [pltpu.make_async_copy(src, dst, w_sem.at[i]) for i, (src, dst) in enumerate(
        ((st_ref, stv), (wo_hbm, wo), (wg_hbm, wg), (wu_hbm, wu), (wd_hbm, wd)))]
    loads[0].start()
    loads[1].start()
    barrier = pltpu.get_barrier_semaphore()
    for k in range(1, n_dev):
        peer = lax.rem(me + k, n_dev)
        pl.semaphore_signal(barrier, inc=1, device_id={"model": peer}, device_id_type=MESH)

    def send(phase, k, src, dst):
        peer = lax.rem(me + k, n_dev)
        return pltpu.make_async_remote_copy(
            src_ref=src, dst_ref=dst, send_sem=send_sem.at[phase, k - 1], recv_sem=recv_sem.at[phase, k - 1],
            device_id={"model": peer}, device_id_type=MESH)

    loads[0].wait()
    for load in loads[2:]:
        load.start()
    for b in range(n_batch):
        top = stv[0, b, 1]
        for j in range(1, n_part):
            top = jnp.maximum(top, stv[j, b, 1])
        den = jnp.zeros((STAT_ROWS, HEAD_DIM), jnp.float32)
        num = jnp.zeros((STAT_ROWS, HEAD_DIM), jnp.float32)
        for j in range(n_part):
            scale = jnp.exp(stv[j, b, 1] - top)
            den += scale * stv[j, b, 2]
            num += scale * stv[j, b, 0]
        rows[:, b, :] = num / den
    for h in range(heads):
        for t in range(2):
            a_buf[t * n_batch:(t + 1) * n_batch, h * HEAD_DIM:(h + 1) * HEAD_DIM] = rows[2 * h + t]
    att = a_buf[...].astype(jnp.bfloat16)

    def all_reduce(phase, partial, base, ps, pr, xo, xg):
        copies = []
        for k in range(1, n_dev):
            peer = lax.rem(me + k, n_dev)
            ps[k - 1] = partial(peer)
            copies.append(send(phase, k, ps.at[k - 1], pr.at[k - 1]))
            copies[-1].start()
        total = base + partial(me)
        for k in range(1, n_dev):
            copies[k - 1].wait_recv()
            total = total + pr[k - 1]
        xo[...] = total.astype(jnp.bfloat16)
        outs = []
        for k in range(1, n_dev):
            outs.append(send(phase + 1, k, xo, xg.at[me]))
            outs[-1].start()
        xg[me] = xo[...]
        for k in range(1, n_dev):
            outs[k - 1].wait_recv()
        return copies + outs

    def col_block(p):
        return pl.ds(pl.multiple_of(p * cols, cols), cols)

    loads[1].wait()
    pl.semaphore_wait(barrier, n_dev - 1)
    sent = all_reduce(0, lambda p: jnp.dot(att, wo[:, col_block(p)], preferred_element_type=jnp.float32),
                      xs_ref[...].astype(jnp.float32), ps1, pr1, xo1, xg1)
    sq = jnp.zeros((n_rows, 1), jnp.float32)
    for j in range(n_dev):
        xf = xg1[j].astype(jnp.float32)
        sq += jnp.sum(xf * xf, axis=-1, keepdims=True)
    inv_rms = lax.rsqrt(sq / d_model + 1e-5)
    for j in range(n_dev):
        xf = xg1[j].astype(jnp.float32)
        n_buf[:, j * cols:(j + 1) * cols] = (xf * inv_rms * gain_ref[:, j * cols:(j + 1) * cols]).astype(jnp.bfloat16)
    loads[2].wait()
    loads[3].wait()
    nt = (((1,), (1,)), ((), ()))
    n_hid = wg.shape[0]
    rows_per = n_hid // 2

    def hidden_rows(r, carry):
        at = pl.ds(pl.multiple_of(r * rows_per, 8), rows_per)
        gate = lax.dot_general(wg[at, :], n_buf[...], nt, preferred_element_type=jnp.float32)
        up = lax.dot_general(wu[at, :], n_buf[...], nt, preferred_element_type=jnp.float32)
        mid_buf[at, :] = gate * (1.0 / (1.0 + jnp.exp(-gate))) * up
        return carry

    lax.fori_loop(0, 2, hidden_rows, 0)
    mid = mid_buf[...].T.astype(jnp.bfloat16)
    loads[4].wait()
    sent += all_reduce(2, lambda p: jnp.dot(mid, wd[:, col_block(p)], preferred_element_type=jnp.float32),
                       xo1[...].astype(jnp.float32), ps2, pr2, xo2, xg2)
    for j in range(n_dev):
        dec_ref[:, j * cols:(j + 1) * cols] = xg2[j, :n_batch]
        last_ref[:, j * cols:(j + 1) * cols] = xg2[j, n_batch:]
    for copy in sent:
        copy.wait_send()


def tail_call(n_dev, stats, x_mine, gain, w_o, w_gate_t, w_up_t, w_down, n_batch):
    n_rows, cols = x_mine.shape
    d_model = w_o.shape[1]
    n_part = stats.shape[0]
    vmem = pl.BlockSpec(memory_space=pltpu.VMEM)
    hbm = pl.BlockSpec(memory_space=pltpu.HBM)
    return pl.pallas_call(
        functools.partial(tail_kernel, n_dev, n_part),
        out_shape=[jax.ShapeDtypeStruct((n_batch, d_model), jnp.bfloat16)] * 2,
        in_specs=[pl.BlockSpec(memory_space=pl.ANY), vmem, vmem, hbm, hbm, hbm, hbm],
        out_specs=[vmem, vmem],
        scratch_shapes=[
            pltpu.VMEM(w_o.shape, jnp.bfloat16),
            pltpu.VMEM(w_gate_t.shape, jnp.bfloat16),
            pltpu.VMEM(w_up_t.shape, jnp.bfloat16),
            pltpu.VMEM(w_down.shape, jnp.bfloat16),
            pltpu.VMEM(stats.shape, jnp.float32),
            pltpu.VMEM((STAT_ROWS, n_batch, HEAD_DIM), jnp.float32),
            pltpu.VMEM((n_rows, w_o.shape[0]), jnp.float32),
            pltpu.VMEM((n_rows, d_model), jnp.bfloat16),
            pltpu.VMEM((w_gate_t.shape[0], n_rows), jnp.float32),
            pltpu.VMEM((n_dev - 1, n_rows, cols), jnp.float32),
            pltpu.VMEM((n_dev - 1, n_rows, cols), jnp.float32),
            pltpu.VMEM((n_dev - 1, n_rows, cols), jnp.float32),
            pltpu.VMEM((n_dev - 1, n_rows, cols), jnp.float32),
            pltpu.VMEM((n_rows, cols), jnp.bfloat16),
            pltpu.VMEM((n_dev, n_rows, cols), jnp.bfloat16),
            pltpu.VMEM((n_rows, cols), jnp.bfloat16),
            pltpu.VMEM((n_dev, n_rows, cols), jnp.bfloat16),
            pltpu.SemaphoreType.DMA((5,)),
            pltpu.SemaphoreType.DMA((4, n_dev - 1)),
            pltpu.SemaphoreType.DMA((4, n_dev - 1)),
        ],
        compiler_params=pltpu.CompilerParams(collective_id=0, has_side_effects=True, vmem_limit_bytes=52 * 2 ** 20),
        name="tail",
    )(stats, x_mine, gain, *(pltpu.with_memory_space_constraint(w, pltpu.HBM) for w in (w_o, w_gate_t, w_up_t, w_down)))


def solution(mesh):
    n_dev = mesh.shape['model']
    seq_spec = P('replica', 'model', None)
    col_spec = P(None, None, 'model')
    row_spec = P(None, 'model', None)
    gain_spec = P(None, None)
    tok_spec = P('replica', None)
    cache_spec = P(None, 'replica', None, 'model', None)
    in_specs = (seq_spec, P('replica'), tok_spec, gain_spec, col_spec, col_spec, col_spec, row_spec, gain_spec, col_spec, col_spec, row_spec)
    out_specs = (tok_spec, tok_spec, cache_spec, cache_spec)

    def swap(arr, bit):
        return lax.ppermute(arr, 'model', [(i, i ^ bit) for i in range(n_dev)])

    def per_device(prompt, lengths, new_tok, norm_attn, w_q, w_k, w_v, w_o, norm_mlp, w_gate, w_up, w_down):
        my_idx = lax.axis_index('model')
        n_batch, blk, d_model = prompt.shape
        seq_len = blk * n_dev
        width = w_k.shape[2]
        heads = width // HEAD_DIM
        half = n_batch // 2
        wq, wk, wv = w_q[0], w_k[0], w_v[0]

        q1, q2 = n_batch // 8, n_batch // 4
        y_parts = [(0, q1), (q1, q2), (q2, half), (half, n_batch)]
        x_parts = [(half, half + q1), (half + q1, half + q2), (half + q2, n_batch), (0, half)]
        from_y, from_x = {}, {}

        def send_part(step, source):
            y_part, x_part = y_parts[step], x_parts[step]
            from_y[y_part] = swap(source[y_part[0]:y_part[1]], 4)
            from_x[x_part] = swap(source[x_part[0]:x_part[1]], 2)

        send_part(0, prompt)
        seq_pos = my_idx * blk + jnp.arange(blk)
        sel = (seq_pos[None, :] == (lengths - 1)[:, None]).astype(jnp.bfloat16)
        last_x = jnp.einsum('bs,bsd->bd', sel, prompt, preferred_element_type=jnp.float32).astype(jnp.bfloat16)
        last_x = last_x + swap(last_x, 1)
        last_x = (last_x + swap(last_x, 2)) + (swap(last_x, 4) + swap(last_x, 6))
        for step in range(1, len(y_parts)):
            send_part(step, prompt)
        core_all = swap(prompt, 1)
        x_rows = jnp.concatenate([new_tok, last_x], axis=0)
        n_rows = rms_norm(x_rows, norm_attn[0])
        row_cos, row_sin = rotary_tables(jnp.stack([lengths, lengths - 1]))
        q_rows = jnp.dot(n_rows, wq, preferred_element_type=jnp.float32).reshape(2, n_batch, heads, HEAD_DIM)
        q_rows = rotate(q_rows, row_cos[:, :, None], row_sin[:, :, None]).astype(jnp.bfloat16)
        k_new = jnp.dot(n_rows[:n_batch], wk, preferred_element_type=jnp.float32).reshape(n_batch, heads, HEAD_DIM)
        k_new = rotate(k_new, row_cos[0][:, None], row_sin[0][:, None]).astype(jnp.bfloat16)
        v_new = jnp.dot(n_rows[:n_batch], wv, preferred_element_type=jnp.float32).astype(jnp.bfloat16).reshape(n_batch, heads, HEAD_DIM)

        q_bht = jnp.moveaxis(q_rows, 0, 2)
        q_diag = (q_bht[:, :, :, None, :] * jnp.eye(heads, dtype=jnp.bfloat16)[None, :, None, :, None]).reshape(n_batch, STAT_ROWS, width)
        self_score = jnp.sum(q_rows[0].astype(jnp.float32) * k_new.astype(jnp.float32), axis=-1) * (HEAD_DIM ** -0.5)
        is_new = (jnp.arange(2) == 0)[None, None, :, None]
        full = (n_batch, heads, 2, HEAD_DIM)
        self_max = jnp.where(is_new, jnp.broadcast_to(self_score[:, :, None, None], full), NEG_BIG)
        self_sum = jnp.broadcast_to(jnp.where(is_new, 1.0, 0.0), full)
        self_acc = jnp.where(is_new, v_new.astype(jnp.float32)[:, :, None, :], 0.0)
        self_stat = jnp.stack([a.reshape(n_batch, STAT_ROWS, HEAD_DIM) for a in (self_acc, self_max, self_sum)], axis=1)
        stats = jnp.zeros((n_dev + 1, n_batch, 3, STAT_ROWS, HEAD_DIM), jnp.float32).at[n_dev].set(self_stat)

        tabs = tuple(tab.reshape(n_dev, blk, HEAD_DIM) for tab in rotary_tables(jnp.arange(seq_len)))
        gain = norm_attn.astype(jnp.float32)
        cache_shape = jax.ShapeDtypeStruct((n_batch, seq_len + 1, heads, HEAD_DIM), jnp.bfloat16)
        caches = (cache_shape, cache_shape, stats)

        def run(groups, per_group, shards, batches, caches, new_rows=None):
            return kv_call(groups, per_group, shards, batches, lengths, tabs, wk, wv, gain, q_diag, caches, new_rows)

        def shard_of(bits):
            idx = my_idx
            for bit in (1, 2, 4):
                if bits & bit:
                    idx = idx + jnp.where((my_idx // bit) % 2 == 0, bit, -bit)
            return idx

        def after(caches, *arrays):
            out = lax.optimization_barrier((caches[2], *arrays))
            return (caches[0], caches[1], out[0]), out[1:]

        caches = run([[(arr, 0), (arr, half)] for arr in (prompt, core_all)], half,
                     [[my_idx] * 2, [shard_of(1)] * 2], [[0, half]] * 2, caches, (k_new[:, None], v_new[:, None]))
        diag = {}
        n_fwd = len(y_parts) - 1
        for step, (y_part, x_part) in enumerate(zip(y_parts, x_parts)):
            caches, (got_y, got_x) = after(caches, from_y[y_part], from_x[x_part])
            other_y, other_x = swap(got_y, 1), swap(got_x, 1)
            if step < n_fwd:
                diag[step] = (swap(got_y, 2), swap(got_x, 4))
            caches = run([[(got_y, 0), (got_x, 0)], [(other_y, 0), (other_x, 0)]], y_part[1] - y_part[0],
                         [[shard_of(4), shard_of(2)], [shard_of(5), shard_of(3)]], [[y_part[0], x_part[0]]] * 2, caches)
        for step in reversed(range(n_fwd)):
            y_part, x_part = y_parts[step], x_parts[step]
            caches, (via_x, via_y) = after(caches, *diag[step])
            other_x, other_y = swap(via_x, 1), swap(via_y, 1)
            caches = run([[(via_x, 0), (via_y, 0)], [(other_x, 0), (other_y, 0)]], y_part[1] - y_part[0],
                         [[shard_of(6)] * 2, [shard_of(7)] * 2], [[y_part[0], x_part[0]]] * 2, caches)

        k_cache, v_cache, stats = caches
        x_mine = lax.dynamic_slice_in_dim(x_rows, my_idx * (d_model // n_dev), d_model // n_dev, axis=1)
        dec_hidden, last_hidden = tail_call(n_dev, stats, x_mine, norm_mlp.astype(jnp.float32), w_o[0],
                                            w_gate[0].T, w_up[0].T, w_down[0], n_batch)
        return dec_hidden, last_hidden, k_cache[None], v_cache[None]

    return jax.shard_map(per_device, mesh=mesh, in_specs=in_specs, out_specs=out_specs, check_vma=False)
```

```python
import functools

import jax
import jax.numpy as jnp
from jax import lax
from jax.experimental import pallas as pl
from jax.experimental.pallas import tpu as pltpu
from jax.sharding import PartitionSpec as P


HEAD_DIM = 128
NEG_BIG = -1e30
STAT_ROWS = 8
NORM_ROWS = 32
COL_TILE = 256
N_MASKS = 8
MESH = pl.DeviceIdType.MESH


def rotary_tables(positions):
    half_dim = HEAD_DIM // 2
    inv_freq = 10000.0 ** (-2.0 * jnp.arange(half_dim, dtype=jnp.float32) / HEAD_DIM)
    angles = positions.astype(jnp.float32)[..., None] * inv_freq
    cos_tab = jnp.cos(angles)
    sin_tab = jnp.sin(angles)
    return jnp.concatenate([cos_tab, cos_tab], axis=-1), jnp.concatenate([-sin_tab, sin_tab], axis=-1)


def load_kernel(*refs):
    n = len(refs) // 2
    sem = refs[-1]
    copies = [pltpu.make_async_copy(refs[i], refs[n + i], sem.at[i]) for i in range(n)]
    for copy in copies:
        copy.start()
    for copy in copies:
        copy.wait()


def keep_in_vmem(*arrays):
    return pl.pallas_call(
        load_kernel,
        out_shape=[pltpu.VMEM(arr.shape, arr.dtype) for arr in arrays],
        in_specs=[pl.BlockSpec(memory_space=pl.ANY)] * len(arrays),
        out_specs=[pl.BlockSpec(memory_space=pltpu.VMEM)] * len(arrays),
        scratch_shapes=[pltpu.SemaphoreType.DMA((len(arrays),))],
        compiler_params=pltpu.CompilerParams(vmem_limit_bytes=24 * 2 ** 20),
        name="keep",
    )(*(pltpu.with_memory_space_constraint(arr, pltpu.HBM) for arr in arrays))


def norm_kernel(outs_of, x_ref, gain_ref, *refs):
    n_out = len(refs) - 3
    out_refs = refs[:n_out]
    ss_buf, n_buf, sems = refs[n_out:]
    step = pl.program_id(0)
    blk, d_model = x_ref.shape[1:]
    lanes = [slice(c * HEAD_DIM, (c + 1) * HEAD_DIM) for c in range(d_model // HEAD_DIM)]

    def copies(at_step):
        return [pltpu.make_async_copy(n_buf.at[at_step % 2], out_refs[o].at[i], sems.at[at_step % 2, k])
                for k, (o, i) in enumerate(outs_of[at_step])]

    for at_step in range(2, len(outs_of)):
        @pl.when(step == at_step)
        def _():
            for copy in copies(at_step - 2):
                copy.wait()

    def square_rows(r, carry):
        rows = pl.ds(pl.multiple_of(r * NORM_ROWS, NORM_ROWS), NORM_ROWS)
        acc = [jnp.zeros((NORM_ROWS, HEAD_DIM), jnp.float32) for _ in range(2)]
        for c, lane in enumerate(lanes):
            xf = x_ref[0, rows, lane].astype(jnp.float32)
            acc[c % 2] += xf * xf
        ss_buf[rows, :] = acc[0] + acc[1]
        return carry

    lax.fori_loop(0, blk // NORM_ROWS, square_rows, 0)
    total = jnp.sum(ss_buf[...], axis=-1, keepdims=True)
    ss_buf[...] = jnp.broadcast_to(lax.rsqrt(total / d_model + 1e-5), (blk, HEAD_DIM))
    slot = lax.rem(step, 2)

    def norm_rows(r, carry):
        rows = pl.ds(pl.multiple_of(r * NORM_ROWS, NORM_ROWS), NORM_ROWS)
        inv_rms = ss_buf[rows, :]
        for lane in lanes:
            xf = x_ref[0, rows, lane].astype(jnp.float32)
            n_buf[slot, rows, lane] = (xf * inv_rms * gain_ref[:, lane]).astype(jnp.bfloat16)
        return carry

    lax.fori_loop(0, blk // NORM_ROWS, norm_rows, 0)
    for at_step in range(len(outs_of)):
        @pl.when(step == at_step)
        def _():
            for copy in copies(at_step):
                copy.start()
            if at_step == len(outs_of) - 1:
                for copy in copies(at_step):
                    copy.wait()
                if at_step >= 1:
                    for copy in copies(at_step - 1):
                        copy.wait()


def norm_call(x, gain, order, outs_of, sizes):
    blk, d_model = x.shape[1:]

    def prompt_of(g):
        idx = jnp.int32(order[-1])
        for k in range(len(order) - 1):
            idx = jnp.where(g == k, order[k], idx)
        return idx

    return pl.pallas_call(
        functools.partial(norm_kernel, outs_of),
        grid=(len(order),),
        in_specs=[pl.BlockSpec((1, blk, d_model), lambda g: (prompt_of(g), 0, 0)),
                  pl.BlockSpec((1, d_model), lambda g: (0, 0))],
        out_specs=[pl.BlockSpec(memory_space=pl.ANY)] * len(sizes),
        out_shape=[jax.ShapeDtypeStruct((size, blk, d_model), jnp.bfloat16) for size in sizes],
        scratch_shapes=[
            pltpu.VMEM((blk, HEAD_DIM), jnp.float32),
            pltpu.VMEM((2, blk, d_model), jnp.bfloat16),
            pltpu.SemaphoreType.DMA((2, max(len(o) for o in outs_of))),
        ],
        compiler_params=pltpu.CompilerParams(vmem_limit_bytes=24 * 2 ** 20),
        cost_estimate=pl.CostEstimate(flops=len(order) * blk * d_model * 8, bytes_accessed=len(order) * blk * d_model * 6, transcendentals=0),
        name="norm_rows",
    )(x, gain)


def rows_kernel(new_ref, last_ref, gain_ref, cos_ref, sin_ref, wq_hbm, wk, wv, q_ref, k_ref, v_ref, st_ref, wq, q_buf, sem):
    load = pltpu.make_async_copy(wq_hbm, wq, sem)
    load.start()
    n_batch = new_ref.shape[0]
    heads = wk.shape[1] // HEAD_DIM
    xf = jnp.concatenate([new_ref[...].astype(jnp.float32), last_ref[...].astype(jnp.float32)], axis=0)
    inv_rms = lax.rsqrt(jnp.mean(xf * xf, axis=-1, keepdims=True) + 1e-5)
    normed = (xf * inv_rms * gain_ref[...]).astype(jnp.bfloat16)
    k_all = jnp.dot(normed, wk[...], preferred_element_type=jnp.float32)[:n_batch]
    v_all = jnp.dot(normed, wv[...], preferred_element_type=jnp.float32)[:n_batch].astype(jnp.bfloat16)
    load.wait()
    q_all = jnp.dot(normed, wq[...], preferred_element_type=jnp.float32)
    q_buf[...] = jnp.zeros_like(q_buf)
    k_rot = []
    for h in range(heads):
        cols = slice(h * HEAD_DIM, (h + 1) * HEAD_DIM)
        qh = q_all[:, cols]
        qh = (qh * cos_ref[...] + pltpu.roll(qh, HEAD_DIM // 2, 1) * sin_ref[...]).astype(jnp.bfloat16).astype(jnp.float32)
        kh = k_all[:, cols]
        kh = (kh * cos_ref[:n_batch, :] + pltpu.roll(kh, HEAD_DIM // 2, 1) * sin_ref[:n_batch, :]).astype(jnp.bfloat16)
        k_rot.append(kh)
        score = jnp.sum(qh[:n_batch] * kh.astype(jnp.float32), axis=-1, keepdims=True) * (HEAD_DIM ** -0.5)
        zero = jnp.zeros((n_batch, HEAD_DIM), jnp.float32)
        for t in range(2):
            row = 2 * h + t
            q_buf[:, row, cols] = qh[t * n_batch:(t + 1) * n_batch]
            st_ref[0, :, row, :] = v_all[:, cols].astype(jnp.float32) if t == 0 else zero
            st_ref[1, :, row, :] = zero + score if t == 0 else zero + NEG_BIG
            st_ref[2, :, row, :] = zero + 1.0 if t == 0 else zero
    q_ref[...] = q_buf[...].astype(jnp.bfloat16)
    k_ref[...] = jnp.concatenate(k_rot, axis=1).reshape(n_batch, heads, HEAD_DIM)
    v_ref[...] = v_all.reshape(n_batch, heads, HEAD_DIM)


def rows_call(new_tok, last_x, gain, row_tabs, w_q, w_k, w_v):
    n_batch = new_tok.shape[0]
    width = w_q.shape[1]
    heads = width // HEAD_DIM
    vmem = pl.BlockSpec(memory_space=pltpu.VMEM)
    return pl.pallas_call(
        rows_kernel,
        out_shape=[
            jax.ShapeDtypeStruct((n_batch, STAT_ROWS, width), jnp.bfloat16),
            jax.ShapeDtypeStruct((n_batch, heads, HEAD_DIM), jnp.bfloat16),
            jax.ShapeDtypeStruct((n_batch, heads, HEAD_DIM), jnp.bfloat16),
            jax.ShapeDtypeStruct((3, n_batch, STAT_ROWS, HEAD_DIM), jnp.float32),
        ],
        in_specs=[vmem] * 5 + [pl.BlockSpec(memory_space=pl.ANY)] + [vmem] * 2,
        out_specs=[vmem] * 4,
        scratch_shapes=[
            pltpu.VMEM(w_q.shape, jnp.bfloat16),
            pltpu.VMEM((n_batch, STAT_ROWS, width), jnp.float32),
            pltpu.SemaphoreType.DMA,
        ],
        compiler_params=pltpu.CompilerParams(vmem_limit_bytes=24 * 2 ** 20),
        cost_estimate=pl.CostEstimate(flops=2 * 2 * n_batch * 3 * w_q.shape[0] * width, bytes_accessed=2 * w_q.size, transcendentals=0),
        name="query_rows",
    )(new_tok, last_x, gain, *row_tabs, pltpu.with_memory_space_constraint(w_q, pltpu.HBM), w_k, w_v)


def by_group(group, values):
    out = values[-1]
    for p in range(len(values) - 1):
        out = jnp.where(group == p, values[p], out)
    return out


def kv_kernel(n_in, masks, batches, firsts, with_new, sc_ref, *refs):
    n_groups = len(masks)
    n_arr = n_in * n_groups
    x_refs = refs[:n_arr]
    cos_refs = refs[n_arr:n_arr + n_in]
    sin_refs = refs[n_arr + n_in:n_arr + 2 * n_in]
    wk, wv, q_ref = refs[n_arr + 2 * n_in:n_arr + 2 * n_in + 3]
    rest = refs[n_arr + 2 * n_in + 3:]
    if with_new:
        new_refs = rest[:2]
        rest = rest[2:]
    else:
        rest = rest[3:]
    kc_ref, vc_ref, st_ref, x_buf, k_buf, v_buf, k_out, v_out, s_out, x_sem, sems, new_sem = rest
    step = pl.program_id(0)
    n_steps = pl.num_programs(0)
    slot = lax.rem(step, 2)
    per_group = n_steps // n_groups
    blk = x_buf.shape[2]
    width = wk.shape[1]
    heads = width // HEAD_DIM
    n_tok = n_in * blk

    def x_copies(at_step, which, group):
        local = at_step - group * per_group
        return [pltpu.make_async_copy(x_refs[group * n_in + i].at[firsts[group][i] + local],
                                      x_buf.at[which, i], x_sem.at[which, i]) for i in range(n_in)]

    def start_x(at_step, which):
        for group in range(n_groups):
            @pl.when(at_step // per_group == group)
            def _(group=group):
                for copy in x_copies(at_step, which, group):
                    copy.start()

    def place(i, at_step):
        group = at_step // per_group
        shard = sc_ref[by_group(group, [mask[i] for mask in masks])]
        return shard, by_group(group, [batch[i] for batch in batches]) + lax.rem(at_step, per_group)

    def out_copies(which, at_step):
        copies = []
        for i in range(n_in):
            shard, bat = place(i, at_step)
            rows = pl.ds(shard * blk, blk)
            copies.append(pltpu.make_async_copy(k_out.at[which, i], kc_ref.at[bat, rows], sems.at[which, i, 0]))
            copies.append(pltpu.make_async_copy(v_out.at[which, i], vc_ref.at[bat, rows], sems.at[which, i, 1]))
            copies.append(pltpu.make_async_copy(s_out.at[which, i], st_ref.at[shard, bat], sems.at[which, i, 2]))
        return copies

    def new_copies():
        return [pltpu.make_async_copy(src.at[pl.ds(b, 1)], dst.at[b, pl.ds(dst.shape[1] - 1, 1)], new_sem.at[idx, b])
                for idx, (src, dst) in enumerate(zip(new_refs, (kc_ref, vc_ref))) for b in range(src.shape[0])]

    @pl.when(step == 0)
    def _():
        start_x(step, slot)
        if with_new:
            for copy in new_copies():
                copy.start()

    @pl.when(step + 1 < n_steps)
    def _():
        start_x(step + 1, 1 - slot)

    @pl.when(step >= 2)
    def _():
        for copy in out_copies(slot, step - 2):
            copy.wait()

    for copy in x_copies(0, slot, 0):
        copy.wait()
    x_rows = x_buf.at[slot]

    def col_tile(c, carry):
        cols = pl.ds(pl.multiple_of(c * COL_TILE, COL_TILE), COL_TILE)
        normed = x_rows[...].reshape(n_tok, x_buf.shape[3])
        kf = jnp.dot(normed, wk[:, cols], preferred_element_type=jnp.float32)
        vf = jnp.dot(normed, wv[:, cols], preferred_element_type=jnp.float32)
        v_buf[:, cols] = vf.astype(jnp.bfloat16)
        parts = []
        for i in range(n_in):
            cos_tab = cos_refs[i][0]
            sin_tab = sin_refs[i][0]
            halves = []
            for h in range(COL_TILE // HEAD_DIM):
                kh = kf[i * blk:(i + 1) * blk, h * HEAD_DIM:(h + 1) * HEAD_DIM]
                halves.append(kh * cos_tab + pltpu.roll(kh, HEAD_DIM // 2, 1) * sin_tab)
            parts.append(jnp.concatenate(halves, axis=1))
        k_buf[:, cols] = jnp.concatenate(parts, axis=0).astype(jnp.bfloat16)
        return carry

    lax.fori_loop(0, width // COL_TILE, col_tile, 0)

    head_of_row = lax.broadcasted_iota(jnp.int32, (STAT_ROWS, HEAD_DIM), 0) // (STAT_ROWS // heads)
    probs = []
    for i in range(n_in):
        shard, bat = place(i, step)
        scores = lax.dot_general(q_ref[bat], k_buf[i * blk:(i + 1) * blk, :], (((1,), (1,)), ((), ())),
                                 preferred_element_type=jnp.float32) * (HEAD_DIM ** -0.5)
        pos = shard * blk + lax.broadcasted_iota(jnp.int32, scores.shape, 1)
        visible = pos < sc_ref[N_MASKS + bat]
        scores = jnp.where(visible, scores, NEG_BIG)
        blk_max = jnp.max(scores, axis=-1, keepdims=True)
        prob = jnp.where(visible, jnp.exp(scores - blk_max), 0.0)
        probs.append((blk_max, prob))
    stats = []
    for i, (blk_max, prob) in enumerate(probs):
        full = jnp.dot(prob.astype(jnp.bfloat16), v_buf[i * blk:(i + 1) * blk, :], preferred_element_type=jnp.float32)
        acc = jnp.zeros((STAT_ROWS, HEAD_DIM), jnp.float32)
        for h in range(heads):
            acc = jnp.where(head_of_row == h, full[:, h * HEAD_DIM:(h + 1) * HEAD_DIM], acc)
        stats.append((acc, blk_max, jnp.sum(prob, axis=-1, keepdims=True)))
    for i in range(n_in):
        k_out[slot, i] = k_buf[i * blk:(i + 1) * blk, :].reshape(blk, heads, HEAD_DIM)
        v_out[slot, i] = v_buf[i * blk:(i + 1) * blk, :].reshape(blk, heads, HEAD_DIM)
        for k, stat in enumerate(stats[i]):
            s_out[slot, i, k] = jnp.broadcast_to(stat, (STAT_ROWS, HEAD_DIM))

    for copy in out_copies(slot, step):
        copy.start()

    @pl.when(step == n_steps - 1)
    def _():
        for copy in out_copies(slot, step):
            copy.wait()
        if with_new:
            for copy in new_copies():
                copy.wait()

    @pl.when((step == n_steps - 1) & (n_steps >= 2))
    def _():
        for copy in out_copies(1 - slot, step - 1):
            copy.wait()


def kv_call(groups, per_group, masks, batches, scalars, tabs, w_k, w_v, q_diag, caches, new_rows=None):
    n_groups = len(groups)
    n_in = len(groups[0])
    n_steps = n_groups * per_group
    cos_tab, sin_tab = tabs
    blk, d_model = groups[0][0][0].shape[1:]
    width = w_k.shape[1]
    heads = width // HEAD_DIM
    any_spec = pl.BlockSpec(memory_space=pl.ANY)
    operands = [arr for group in groups for arr, _ in group]
    in_specs = [any_spec] * len(operands)
    for tab in (cos_tab, sin_tab):
        for i in range(n_in):
            in_specs.append(pl.BlockSpec((1, blk, HEAD_DIM), lambda g, sc, i=i: (
                sc[by_group(g // per_group, [mask[i] for mask in masks])], 0, 0)))
            operands.append(tab)
    in_specs += [pl.BlockSpec(memory_space=pltpu.VMEM)] * 2 + [pl.BlockSpec(q_diag.shape, lambda g, sc: (0, 0, 0))]
    operands += [w_k, w_v, q_diag]
    with_new = new_rows is not None
    if with_new:
        operands += new_rows
        in_specs += [any_spec] * 2
        aliases = {}
    else:
        operands += caches
        in_specs += [any_spec] * 3
        aliases = {len(operands) - 2: 0, len(operands) - 1: 1, len(operands): 2}
    tokens = n_in * blk
    n_batch = q_diag.shape[0]
    return pl.pallas_call(
        functools.partial(kv_kernel, n_in, masks, batches, [[first for _, first in group] for group in groups], with_new),
        grid_spec=pltpu.PrefetchScalarGridSpec(
            num_scalar_prefetch=1,
            grid=(n_steps,),
            in_specs=in_specs,
            out_specs=[any_spec] * 3,
            scratch_shapes=[
                pltpu.VMEM((2, n_in, blk, d_model), jnp.bfloat16),
                pltpu.VMEM((tokens, width), jnp.bfloat16),
                pltpu.VMEM((tokens, width), jnp.bfloat16),
                pltpu.VMEM((2, n_in, blk, heads, HEAD_DIM), jnp.bfloat16),
                pltpu.VMEM((2, n_in, blk, heads, HEAD_DIM), jnp.bfloat16),
                pltpu.VMEM((2, n_in, 3, STAT_ROWS, HEAD_DIM), jnp.float32),
                pltpu.SemaphoreType.DMA((2, n_in)),
                pltpu.SemaphoreType.DMA((2, n_in, 3)),
                pltpu.SemaphoreType.DMA((2, n_batch)),
            ],
        ),
        out_shape=[jax.ShapeDtypeStruct(c.shape, c.dtype) for c in caches],
        input_output_aliases=aliases,
        compiler_params=pltpu.CompilerParams(vmem_limit_bytes=20 * 2 ** 20),
        cost_estimate=pl.CostEstimate(flops=4 * n_steps * tokens * d_model * width, bytes_accessed=2 * n_steps * tokens * (d_model + 2 * width), transcendentals=0),
        name="kv_chunk",
    )(scalars, *operands)


def tail_kernel(n_dev, n_part, st_ref, self_ref, xs_ref, gain_ref, wo_hbm, wg_hbm, wu_hbm, wd_hbm, dec_ref, last_ref,
                wo, wg, wu, wd, stv, rows, a_buf, n_buf, mid_buf, ps1, pr1, ps2, pr2, xo1, xg1, xo2, xg2,
                w_sem, send_sem, recv_sem):
    me = lax.axis_index("model")
    n_batch = dec_ref.shape[0]
    n_rows = 2 * n_batch
    d_model = dec_ref.shape[1]
    cols = d_model // n_dev
    heads = STAT_ROWS // 2
    loads = [pltpu.make_async_copy(src, dst, w_sem.at[i]) for i, (src, dst) in enumerate(
        ((st_ref, stv), (wo_hbm, wo), (wg_hbm, wg), (wu_hbm, wu), (wd_hbm, wd)))]
    loads[0].start()
    loads[1].start()
    barrier = pltpu.get_barrier_semaphore()
    for k in range(1, n_dev):
        peer = lax.rem(me + k, n_dev)
        pl.semaphore_signal(barrier, inc=1, device_id={"model": peer}, device_id_type=MESH)

    def send(phase, k, src, dst):
        peer = lax.rem(me + k, n_dev)
        return pltpu.make_async_remote_copy(
            src_ref=src, dst_ref=dst, send_sem=send_sem.at[phase, k - 1], recv_sem=recv_sem.at[phase, k - 1],
            device_id={"model": peer}, device_id_type=MESH)

    loads[0].wait()
    for load in loads[2:]:
        load.start()
    for b in range(n_batch):
        top = self_ref[1, b]
        for j in range(n_part):
            top = jnp.maximum(top, stv[j, b, 1])
        scale = jnp.exp(self_ref[1, b] - top)
        den = scale * self_ref[2, b]
        num = scale * self_ref[0, b]
        for j in range(n_part):
            scale = jnp.exp(stv[j, b, 1] - top)
            den += scale * stv[j, b, 2]
            num += scale * stv[j, b, 0]
        rows[:, b, :] = num / den
    for h in range(heads):
        for t in range(2):
            a_buf[t * n_batch:(t + 1) * n_batch, h * HEAD_DIM:(h + 1) * HEAD_DIM] = rows[2 * h + t]
    att = a_buf[...].astype(jnp.bfloat16)

    def all_reduce(phase, partial, base, ps, pr, xo, xg):
        copies = []
        for k in range(1, n_dev):
            peer = lax.rem(me + k, n_dev)
            ps[k - 1] = partial(peer)
            copies.append(send(phase, k, ps.at[k - 1], pr.at[k - 1]))
            copies[-1].start()
        total = base + partial(me)
        for k in range(1, n_dev):
            copies[k - 1].wait_recv()
            total = total + pr[k - 1]
        xo[...] = total.astype(jnp.bfloat16)
        outs = []
        for k in range(1, n_dev):
            outs.append(send(phase + 1, k, xo, xg.at[me]))
            outs[-1].start()
        xg[me] = xo[...]
        for k in range(1, n_dev):
            outs[k - 1].wait_recv()
        return copies + outs

    def col_block(p):
        return pl.ds(pl.multiple_of(p * cols, cols), cols)

    loads[1].wait()
    pl.semaphore_wait(barrier, n_dev - 1)
    sent = all_reduce(0, lambda p: jnp.dot(att, wo[:, col_block(p)], preferred_element_type=jnp.float32),
                      xs_ref[...].astype(jnp.float32), ps1, pr1, xo1, xg1)
    sq = jnp.zeros((n_rows, 1), jnp.float32)
    for j in range(n_dev):
        xf = xg1[j].astype(jnp.float32)
        sq += jnp.sum(xf * xf, axis=-1, keepdims=True)
    inv_rms = lax.rsqrt(sq / d_model + 1e-5)
    for j in range(n_dev):
        xf = xg1[j].astype(jnp.float32)
        n_buf[:, j * cols:(j + 1) * cols] = (xf * inv_rms * gain_ref[:, j * cols:(j + 1) * cols]).astype(jnp.bfloat16)
    loads[2].wait()
    loads[3].wait()
    nt = (((1,), (1,)), ((), ()))
    n_hid = wg.shape[0]
    rows_per = n_hid // 2

    def hidden_rows(r, carry):
        at = pl.ds(pl.multiple_of(r * rows_per, 8), rows_per)
        gate = lax.dot_general(wg[at, :], n_buf[...], nt, preferred_element_type=jnp.float32)
        up = lax.dot_general(wu[at, :], n_buf[...], nt, preferred_element_type=jnp.float32)
        mid_buf[at, :] = gate * (1.0 / (1.0 + jnp.exp(-gate))) * up
        return carry

    lax.fori_loop(0, 2, hidden_rows, 0)
    mid = mid_buf[...].T.astype(jnp.bfloat16)
    loads[4].wait()
    sent += all_reduce(2, lambda p: jnp.dot(mid, wd[:, col_block(p)], preferred_element_type=jnp.float32),
                       xo1[...].astype(jnp.float32), ps2, pr2, xo2, xg2)
    for j in range(n_dev):
        dec_ref[:, j * cols:(j + 1) * cols] = xg2[j, :n_batch]
        last_ref[:, j * cols:(j + 1) * cols] = xg2[j, n_batch:]
    for copy in sent:
        copy.wait_send()


def tail_call(n_dev, stats, self_stat, x_mine, gain, w_o, w_gate_t, w_up_t, w_down, n_batch):
    n_rows, cols = x_mine.shape
    d_model = w_o.shape[1]
    n_part = stats.shape[0]
    vmem = pl.BlockSpec(memory_space=pltpu.VMEM)
    hbm = pl.BlockSpec(memory_space=pltpu.HBM)
    return pl.pallas_call(
        functools.partial(tail_kernel, n_dev, n_part),
        out_shape=[jax.ShapeDtypeStruct((n_batch, d_model), jnp.bfloat16)] * 2,
        in_specs=[pl.BlockSpec(memory_space=pl.ANY), vmem, vmem, vmem, hbm, hbm, hbm, hbm],
        out_specs=[vmem, vmem],
        scratch_shapes=[
            pltpu.VMEM(w_o.shape, jnp.bfloat16),
            pltpu.VMEM(w_gate_t.shape, jnp.bfloat16),
            pltpu.VMEM(w_up_t.shape, jnp.bfloat16),
            pltpu.VMEM(w_down.shape, jnp.bfloat16),
            pltpu.VMEM(stats.shape, jnp.float32),
            pltpu.VMEM((STAT_ROWS, n_batch, HEAD_DIM), jnp.float32),
            pltpu.VMEM((n_rows, w_o.shape[0]), jnp.float32),
            pltpu.VMEM((n_rows, d_model), jnp.bfloat16),
            pltpu.VMEM((w_gate_t.shape[0], n_rows), jnp.float32),
            pltpu.VMEM((n_dev - 1, n_rows, cols), jnp.float32),
            pltpu.VMEM((n_dev - 1, n_rows, cols), jnp.float32),
            pltpu.VMEM((n_dev - 1, n_rows, cols), jnp.float32),
            pltpu.VMEM((n_dev - 1, n_rows, cols), jnp.float32),
            pltpu.VMEM((n_rows, cols), jnp.bfloat16),
            pltpu.VMEM((n_dev, n_rows, cols), jnp.bfloat16),
            pltpu.VMEM((n_rows, cols), jnp.bfloat16),
            pltpu.VMEM((n_dev, n_rows, cols), jnp.bfloat16),
            pltpu.SemaphoreType.DMA((5,)),
            pltpu.SemaphoreType.DMA((4, n_dev - 1)),
            pltpu.SemaphoreType.DMA((4, n_dev - 1)),
        ],
        compiler_params=pltpu.CompilerParams(collective_id=0, has_side_effects=True, vmem_limit_bytes=52 * 2 ** 20),
        name="tail",
    )(stats, self_stat, x_mine, gain, *(pltpu.with_memory_space_constraint(w, pltpu.HBM) for w in (w_o, w_gate_t, w_up_t, w_down)))


def solution(mesh):
    n_dev = mesh.shape['model']
    seq_spec = P('replica', 'model', None)
    col_spec = P(None, None, 'model')
    row_spec = P(None, 'model', None)
    gain_spec = P(None, None)
    tok_spec = P('replica', None)
    cache_spec = P(None, 'replica', None, 'model', None)
    in_specs = (seq_spec, P('replica'), tok_spec, gain_spec, col_spec, col_spec, col_spec, row_spec, gain_spec, col_spec, col_spec, row_spec)
    out_specs = (tok_spec, tok_spec, cache_spec, cache_spec)

    def swap(arr, bit):
        return lax.ppermute(arr, 'model', [(i, i ^ bit) for i in range(n_dev)])

    def per_device(prompt, lengths, new_tok, norm_attn, w_q, w_k, w_v, w_o, norm_mlp, w_gate, w_up, w_down):
        my_idx = lax.axis_index('model')
        n_batch, blk, d_model = prompt.shape
        seq_len = blk * n_dev
        width = w_k.shape[2]
        heads = width // HEAD_DIM
        half = n_batch // 2
        wq = w_q[0]
        gain = norm_attn.astype(jnp.float32)

        q1, q2 = n_batch // 8, n_batch // 4
        bounds = [(0, q1), (q1, q2), (q2, half)]
        a_parts, b_parts = {}, {}
        first = [*range(q1), *range(half, half + q1)]
        a_parts[0], b_parts[0] = norm_call(prompt, gain, first, [[(k // q1, k % q1)] for k in range(2 * q1)], [q1, q1])
        from_y, from_x = {}, {}

        def send_part(step, along_y, along_x):
            from_y[step] = swap(along_y, 4)
            from_x[step] = swap(along_x, 2)

        send_part(0, a_parts[0], b_parts[0])
        seq_pos = my_idx * blk + jnp.arange(blk)
        sel = (seq_pos[None, :] == (lengths - 1)[:, None]).astype(jnp.bfloat16)
        last_x = jnp.einsum('bs,bsd->bd', sel, prompt, preferred_element_type=jnp.float32).astype(jnp.bfloat16)
        last_x = last_x + swap(last_x, 1)
        last_x = (last_x + swap(last_x, 2)) + (swap(last_x, 4) + swap(last_x, 6))
        order, outs_of = [], []
        for part in (1, 2, 0):
            lo, hi = bounds[part]
            for side in range(2):
                for k in range(lo, hi):
                    order.append(side * half + k)
                    outs_of.append([(4, side * half + k)] + ([(2 * part - 2 + side, k - lo)] if part else []))
        a_parts[1], b_parts[1], a_parts[2], b_parts[2], normed = norm_call(
            prompt, gain, order, outs_of, [q2 - q1, q2 - q1, half - q2, half - q2, n_batch])
        send_part(1, a_parts[1], b_parts[1])
        send_part(2, a_parts[2], b_parts[2])
        send_part(3, b_parts[2], a_parts[2])
        send_part(4, normed[half:half + q2], normed[:q2])
        core_all = swap(normed, 1)

        bits = jnp.arange(N_MASKS)
        scalars = jnp.concatenate([sum(((my_idx // bit + bits // bit) % 2) * bit for bit in (1, 2, 4)), lengths]).astype(jnp.int32)
        row_tabs = rotary_tables(jnp.concatenate([lengths, lengths - 1]))
        tabs = tuple(tab.reshape(n_dev, blk, HEAD_DIM) for tab in rotary_tables(jnp.arange(seq_len)))
        x_rows = jnp.concatenate([new_tok, last_x], axis=0)
        x_mine = lax.dynamic_slice_in_dim(x_rows, my_idx * (d_model // n_dev), d_model // n_dev, axis=1)
        wk, wv, last_x, scalars, row_tabs, tabs, x_mine, gain_mlp = lax.optimization_barrier(
            (w_k[0], w_v[0], last_x, scalars, row_tabs, tabs, x_mine, norm_mlp.astype(jnp.float32)))
        wk, wv = keep_in_vmem(wk, wv)
        q_diag, k_new, v_new, self_stat = rows_call(new_tok, last_x, gain, row_tabs, wq, wk, wv)
        cache_shape = jax.ShapeDtypeStruct((n_batch, seq_len + 1, heads, HEAD_DIM), jnp.bfloat16)
        caches = [cache_shape, cache_shape, jax.ShapeDtypeStruct((n_dev, n_batch, 3, STAT_ROWS, HEAD_DIM), jnp.float32)]

        def run(groups, per_group, masks, batches, caches, new_rows=None):
            return kv_call(groups, per_group, masks, batches, scalars, tabs, wk, wv, q_diag, caches, new_rows)

        def after(caches, *arrays):
            out = lax.optimization_barrier((caches[2], *arrays))
            return [caches[0], caches[1], out[0]], out[1:]

        caches = run([[(arr, 0), (arr, half)] for arr in (normed, core_all)], half,
                     [[0] * 2, [1] * 2], [[0, half]] * 2, caches, [k_new, v_new])
        diag = {}
        starts = [(lo, half + lo) for lo, _ in bounds] + [(half + q2, q2), (half, 0)]
        for step, start in enumerate(starts):
            caches, (got_y, got_x) = after(caches, from_y[step], from_x[step])
            other_y, other_x = swap(got_y, 1), swap(got_x, 1)
            if step < 3:
                diag[step] = (swap(got_y, 2), swap(got_x, 4))
            caches = run([[(got_y, 0), (got_x, 0)], [(other_y, 0), (other_x, 0)]], got_y.shape[0],
                         [[4, 2], [5, 3]], [list(start)] * 2, caches)
        for step in (2, 1, 0):
            caches, (via_x, via_y) = after(caches, *diag[step])
            other_x, other_y = swap(via_x, 1), swap(via_y, 1)
            caches = run([[(via_x, 0), (via_y, 0)], [(other_x, 0), (other_y, 0)]], via_x.shape[0],
                         [[6] * 2, [7] * 2], [list(starts[step])] * 2, caches)

        k_cache, v_cache, stats = caches
        dec_hidden, last_hidden = tail_call(n_dev, stats, self_stat, x_mine, gain_mlp, w_o[0],
                                            w_gate[0].T, w_up[0].T, w_down[0], n_batch)
        return dec_hidden, last_hidden, k_cache[None], v_cache[None]

    return jax.shard_map(per_device, mesh=mesh, in_specs=in_specs, out_specs=out_specs, check_vma=False)
```

```python
import functools

import jax
import jax.numpy as jnp
from jax import lax
from jax.experimental import pallas as pl
from jax.experimental.pallas import tpu as pltpu
from jax.sharding import PartitionSpec as P


HEAD_DIM = 128
NEG_BIG = -1e30
STAT_ROWS = 8
NORM_ROWS = 32
COL_TILE = 256
N_MASKS = 8
MESH = pl.DeviceIdType.MESH


def rotary_tables(positions):
    half_dim = HEAD_DIM // 2
    inv_freq = 10000.0 ** (-2.0 * jnp.arange(half_dim, dtype=jnp.float32) / HEAD_DIM)
    angles = positions.astype(jnp.float32)[..., None] * inv_freq
    cos_tab = jnp.cos(angles)
    sin_tab = jnp.sin(angles)
    return jnp.concatenate([cos_tab, cos_tab], axis=-1), jnp.concatenate([-sin_tab, sin_tab], axis=-1)


def load_kernel(*refs):
    n = len(refs) // 2
    sem = refs[-1]
    copies = [pltpu.make_async_copy(refs[i], refs[n + i], sem.at[i]) for i in range(n)]
    for copy in copies:
        copy.start()
    for copy in copies:
        copy.wait()


def keep_in_vmem(*arrays):
    return pl.pallas_call(
        load_kernel,
        out_shape=[pltpu.VMEM(arr.shape, arr.dtype) for arr in arrays],
        in_specs=[pl.BlockSpec(memory_space=pl.ANY)] * len(arrays),
        out_specs=[pl.BlockSpec(memory_space=pltpu.VMEM)] * len(arrays),
        scratch_shapes=[pltpu.SemaphoreType.DMA((len(arrays),))],
        compiler_params=pltpu.CompilerParams(vmem_limit_bytes=24 * 2 ** 20),
        name="keep",
    )(*(pltpu.with_memory_space_constraint(arr, pltpu.HBM) for arr in arrays))


def norm_kernel(outs_of, x_ref, gain_ref, *refs):
    n_out = len(refs) - 3
    out_refs = refs[:n_out]
    ss_buf, n_buf, sems = refs[n_out:]
    step = pl.program_id(0)
    blk, d_model = x_ref.shape[1:]
    lanes = [slice(c * HEAD_DIM, (c + 1) * HEAD_DIM) for c in range(d_model // HEAD_DIM)]

    def copies(at_step):
        return [pltpu.make_async_copy(n_buf.at[at_step % 2, pl.ds(lo, rows)], out_refs[o].at[i], sems.at[at_step % 2, k])
                for k, (o, i, lo, rows) in enumerate(outs_of[at_step])]

    for at_step in range(2, len(outs_of)):
        @pl.when(step == at_step)
        def _():
            for copy in copies(at_step - 2):
                copy.wait()

    def square_rows(r, carry):
        rows = pl.ds(pl.multiple_of(r * NORM_ROWS, NORM_ROWS), NORM_ROWS)
        acc = [jnp.zeros((NORM_ROWS, HEAD_DIM), jnp.float32) for _ in range(2)]
        for c, lane in enumerate(lanes):
            xf = x_ref[0, rows, lane].astype(jnp.float32)
            acc[c % 2] += xf * xf
        ss_buf[rows, :] = acc[0] + acc[1]
        return carry

    lax.fori_loop(0, blk // NORM_ROWS, square_rows, 0)
    total = jnp.sum(ss_buf[...], axis=-1, keepdims=True)
    ss_buf[...] = jnp.broadcast_to(lax.rsqrt(total / d_model + 1e-5), (blk, HEAD_DIM))
    slot = lax.rem(step, 2)

    def norm_rows(r, carry):
        rows = pl.ds(pl.multiple_of(r * NORM_ROWS, NORM_ROWS), NORM_ROWS)
        inv_rms = ss_buf[rows, :]
        for lane in lanes:
            xf = x_ref[0, rows, lane].astype(jnp.float32)
            n_buf[slot, rows, lane] = (xf * inv_rms * gain_ref[:, lane]).astype(jnp.bfloat16)
        return carry

    lax.fori_loop(0, blk // NORM_ROWS, norm_rows, 0)
    for at_step in range(len(outs_of)):
        @pl.when(step == at_step)
        def _():
            for copy in copies(at_step):
                copy.start()
            if at_step == len(outs_of) - 1:
                for copy in copies(at_step):
                    copy.wait()
                if at_step >= 1:
                    for copy in copies(at_step - 1):
                        copy.wait()


def norm_call(x, gain, order, outs_of, shapes):
    blk, d_model = x.shape[1:]

    def prompt_of(g):
        idx = jnp.int32(order[-1])
        for k in range(len(order) - 1):
            idx = jnp.where(g == k, order[k], idx)
        return idx

    return pl.pallas_call(
        functools.partial(norm_kernel, outs_of),
        grid=(len(order),),
        in_specs=[pl.BlockSpec((1, blk, d_model), lambda g: (prompt_of(g), 0, 0)),
                  pl.BlockSpec((1, d_model), lambda g: (0, 0))],
        out_specs=[pl.BlockSpec(memory_space=pl.ANY)] * len(shapes),
        out_shape=[jax.ShapeDtypeStruct((*shape, d_model), jnp.bfloat16) for shape in shapes],
        scratch_shapes=[
            pltpu.VMEM((blk, HEAD_DIM), jnp.float32),
            pltpu.VMEM((2, blk, d_model), jnp.bfloat16),
            pltpu.SemaphoreType.DMA((2, max(len(o) for o in outs_of))),
        ],
        compiler_params=pltpu.CompilerParams(vmem_limit_bytes=24 * 2 ** 20),
        cost_estimate=pl.CostEstimate(flops=len(order) * blk * d_model * 8, bytes_accessed=len(order) * blk * d_model * 6, transcendentals=0),
        name="norm_rows",
    )(pltpu.with_memory_space_constraint(x, pltpu.HBM), gain)


def rows_kernel(new_ref, last_ref, gain_ref, cos_ref, sin_ref, wq_hbm, wk, wv, q_ref, k_ref, v_ref, st_ref, wq, q_buf, sem):
    load = pltpu.make_async_copy(wq_hbm, wq, sem)
    load.start()
    n_batch = new_ref.shape[0]
    heads = wk.shape[1] // HEAD_DIM
    xf = jnp.concatenate([new_ref[...].astype(jnp.float32), last_ref[...].astype(jnp.float32)], axis=0)
    inv_rms = lax.rsqrt(jnp.mean(xf * xf, axis=-1, keepdims=True) + 1e-5)
    normed = (xf * inv_rms * gain_ref[...]).astype(jnp.bfloat16)
    k_all = jnp.dot(normed, wk[...], preferred_element_type=jnp.float32)[:n_batch]
    v_all = jnp.dot(normed, wv[...], preferred_element_type=jnp.float32)[:n_batch].astype(jnp.bfloat16)
    load.wait()
    q_all = jnp.dot(normed, wq[...], preferred_element_type=jnp.float32)
    q_buf[...] = jnp.zeros_like(q_buf)
    k_rot = []
    for h in range(heads):
        cols = slice(h * HEAD_DIM, (h + 1) * HEAD_DIM)
        qh = q_all[:, cols]
        qh = (qh * cos_ref[...] + pltpu.roll(qh, HEAD_DIM // 2, 1) * sin_ref[...]).astype(jnp.bfloat16).astype(jnp.float32)
        kh = k_all[:, cols]
        kh = (kh * cos_ref[:n_batch, :] + pltpu.roll(kh, HEAD_DIM // 2, 1) * sin_ref[:n_batch, :]).astype(jnp.bfloat16)
        k_rot.append(kh)
        score = jnp.sum(qh[:n_batch] * kh.astype(jnp.float32), axis=-1, keepdims=True) * (HEAD_DIM ** -0.5)
        zero = jnp.zeros((n_batch, HEAD_DIM), jnp.float32)
        for t in range(2):
            row = 2 * h + t
            q_buf[:, row, cols] = qh[t * n_batch:(t + 1) * n_batch]
            st_ref[0, :, row, :] = v_all[:, cols].astype(jnp.float32) if t == 0 else zero
            st_ref[1, :, row, :] = zero + score if t == 0 else zero + NEG_BIG
            st_ref[2, :, row, :] = zero + 1.0 if t == 0 else zero
    q_ref[...] = q_buf[...].astype(jnp.bfloat16)
    k_ref[...] = jnp.concatenate(k_rot, axis=1).reshape(n_batch, heads, HEAD_DIM)
    v_ref[...] = v_all.reshape(n_batch, heads, HEAD_DIM)


def rows_call(new_tok, last_x, gain, row_tabs, w_q, w_k, w_v):
    n_batch = new_tok.shape[0]
    width = w_q.shape[1]
    heads = width // HEAD_DIM
    vmem = pl.BlockSpec(memory_space=pltpu.VMEM)
    return pl.pallas_call(
        rows_kernel,
        out_shape=[
            jax.ShapeDtypeStruct((n_batch, STAT_ROWS, width), jnp.bfloat16),
            jax.ShapeDtypeStruct((n_batch, heads, HEAD_DIM), jnp.bfloat16),
            jax.ShapeDtypeStruct((n_batch, heads, HEAD_DIM), jnp.bfloat16),
            jax.ShapeDtypeStruct((3, n_batch, STAT_ROWS, HEAD_DIM), jnp.float32),
        ],
        in_specs=[vmem] * 5 + [pl.BlockSpec(memory_space=pl.ANY)] + [vmem] * 2,
        out_specs=[vmem] * 4,
        scratch_shapes=[
            pltpu.VMEM(w_q.shape, jnp.bfloat16),
            pltpu.VMEM((n_batch, STAT_ROWS, width), jnp.float32),
            pltpu.SemaphoreType.DMA,
        ],
        compiler_params=pltpu.CompilerParams(vmem_limit_bytes=24 * 2 ** 20),
        cost_estimate=pl.CostEstimate(flops=2 * 2 * n_batch * 3 * w_q.shape[0] * width, bytes_accessed=2 * w_q.size, transcendentals=0),
        name="query_rows",
    )(new_tok, last_x, gain, *row_tabs, pltpu.with_memory_space_constraint(w_q, pltpu.HBM), w_k, w_v)


def by_group(group, values):
    out = values[-1]
    for p in range(len(values) - 1):
        out = jnp.where(group == p, values[p], out)
    return out


def kv_kernel(n_in, masks, batches, firsts, row0, stat_of, with_new, sc_ref, *refs):
    n_groups = len(masks)
    n_arr = n_in * n_groups
    x_refs = refs[:n_arr]
    cos_ref, sin_ref, wk, wv, q_ref = refs[n_arr:n_arr + 5]
    rest = refs[n_arr + 5:]
    if with_new:
        new_refs = rest[:2]
        rest = rest[2:]
    else:
        rest = rest[3:]
    kc_ref, vc_ref, st_ref, x_buf, k_buf, v_buf, k_out, v_out, s_out, x_sem, sems, new_sem = rest
    step = pl.program_id(0)
    n_steps = pl.num_programs(0)
    slot = lax.rem(step, 2)
    per_group = n_steps // n_groups
    blk = x_buf.shape[2]
    shard_rows = cos_ref.shape[1]
    width = wk.shape[1]
    heads = width // HEAD_DIM
    n_tok = n_in * blk

    def x_copies(at_step, which, group):
        local = at_step - group * per_group
        return [pltpu.make_async_copy(x_refs[group * n_in + i].at[firsts[group][i] + local],
                                      x_buf.at[which, i], x_sem.at[which, i]) for i in range(n_in)]

    def start_x(at_step, which):
        for group in range(n_groups):
            @pl.when(at_step // per_group == group)
            def _(group=group):
                for copy in x_copies(at_step, which, group):
                    copy.start()

    def place(i, at_step):
        group = at_step // per_group
        mask = by_group(group, [m[i] for m in masks])
        return sc_ref[mask], by_group(group, [b[i] for b in batches]) + lax.rem(at_step, per_group), mask

    def out_copies(which, at_step):
        copies = []
        for i in range(n_in):
            shard, bat, mask = place(i, at_step)
            rows = pl.ds(shard * shard_rows + row0, blk)
            copies.append(pltpu.make_async_copy(k_out.at[which, i], kc_ref.at[bat, rows], sems.at[which, i, 0]))
            copies.append(pltpu.make_async_copy(v_out.at[which, i], vc_ref.at[bat, rows], sems.at[which, i, 1]))
            copies.append(pltpu.make_async_copy(s_out.at[which, i], st_ref.at[mask + stat_of, bat], sems.at[which, i, 2]))
        return copies

    def new_copies():
        return [pltpu.make_async_copy(src.at[pl.ds(b, 1)], dst.at[b, pl.ds(dst.shape[1] - 1, 1)], new_sem.at[idx, b])
                for idx, (src, dst) in enumerate(zip(new_refs, (kc_ref, vc_ref))) for b in range(src.shape[0])]

    @pl.when(step == 0)
    def _():
        start_x(step, slot)
        if with_new:
            for copy in new_copies():
                copy.start()

    @pl.when(step + 1 < n_steps)
    def _():
        start_x(step + 1, 1 - slot)

    @pl.when(step >= 2)
    def _():
        for copy in out_copies(slot, step - 2):
            copy.wait()

    for copy in x_copies(0, slot, 0):
        copy.wait()
    x_rows = x_buf.at[slot]

    def col_tile(c, carry):
        cols = pl.ds(pl.multiple_of(c * COL_TILE, COL_TILE), COL_TILE)
        normed = x_rows[...].reshape(n_tok, x_buf.shape[3])
        kf = jnp.dot(normed, wk[:, cols], preferred_element_type=jnp.float32)
        vf = jnp.dot(normed, wv[:, cols], preferred_element_type=jnp.float32)
        v_buf[:, cols] = vf.astype(jnp.bfloat16)
        parts = []
        for i in range(n_in):
            shard = place(i, step)[0]
            cos_tab = cos_ref[shard, row0:row0 + blk]
            sin_tab = sin_ref[shard, row0:row0 + blk]
            halves = []
            for h in range(COL_TILE // HEAD_DIM):
                kh = kf[i * blk:(i + 1) * blk, h * HEAD_DIM:(h + 1) * HEAD_DIM]
                halves.append(kh * cos_tab + pltpu.roll(kh, HEAD_DIM // 2, 1) * sin_tab)
            parts.append(jnp.concatenate(halves, axis=1))
        k_buf[:, cols] = jnp.concatenate(parts, axis=0).astype(jnp.bfloat16)
        return carry

    lax.fori_loop(0, width // COL_TILE, col_tile, 0)

    head_of_row = lax.broadcasted_iota(jnp.int32, (STAT_ROWS, HEAD_DIM), 0) // (STAT_ROWS // heads)
    probs = []
    for i in range(n_in):
        shard, bat, _ = place(i, step)
        scores = lax.dot_general(q_ref[bat], k_buf[i * blk:(i + 1) * blk, :], (((1,), (1,)), ((), ())),
                                 preferred_element_type=jnp.float32) * (HEAD_DIM ** -0.5)
        pos = shard * shard_rows + row0 + lax.broadcasted_iota(jnp.int32, scores.shape, 1)
        visible = pos < sc_ref[N_MASKS + bat]
        scores = jnp.where(visible, scores, NEG_BIG)
        blk_max = jnp.max(scores, axis=-1, keepdims=True)
        prob = jnp.where(visible, jnp.exp(scores - blk_max), 0.0)
        probs.append((blk_max, prob))
    stats = []
    for i, (blk_max, prob) in enumerate(probs):
        full = jnp.dot(prob.astype(jnp.bfloat16), v_buf[i * blk:(i + 1) * blk, :], preferred_element_type=jnp.float32)
        acc = jnp.zeros((STAT_ROWS, HEAD_DIM), jnp.float32)
        for h in range(heads):
            acc = jnp.where(head_of_row == h, full[:, h * HEAD_DIM:(h + 1) * HEAD_DIM], acc)
        stats.append((acc, blk_max, jnp.sum(prob, axis=-1, keepdims=True)))
    for i in range(n_in):
        k_out[slot, i] = k_buf[i * blk:(i + 1) * blk, :].reshape(blk, heads, HEAD_DIM)
        v_out[slot, i] = v_buf[i * blk:(i + 1) * blk, :].reshape(blk, heads, HEAD_DIM)
        for k, stat in enumerate(stats[i]):
            s_out[slot, i, k] = jnp.broadcast_to(stat, (STAT_ROWS, HEAD_DIM))

    for copy in out_copies(slot, step):
        copy.start()

    @pl.when(step == n_steps - 1)
    def _():
        for copy in out_copies(slot, step):
            copy.wait()
        if with_new:
            for copy in new_copies():
                copy.wait()

    @pl.when((step == n_steps - 1) & (n_steps >= 2))
    def _():
        for copy in out_copies(1 - slot, step - 1):
            copy.wait()


def kv_call(groups, per_group, masks, batches, scalars, tabs, w_k, w_v, q_diag, caches, new_rows=None, row0=0, stat_of=0):
    n_groups = len(groups)
    n_in = len(groups[0])
    n_steps = n_groups * per_group
    cos_tab, sin_tab = tabs
    blk, d_model = groups[0][0][0].shape[1:]
    width = w_k.shape[1]
    heads = width // HEAD_DIM
    any_spec = pl.BlockSpec(memory_space=pl.ANY)
    operands = [arr for group in groups for arr, _ in group]
    in_specs = [any_spec] * len(operands) + [pl.BlockSpec(memory_space=pltpu.VMEM)] * 5
    operands += [cos_tab, sin_tab, w_k, w_v, q_diag]
    with_new = new_rows is not None
    if with_new:
        operands += new_rows
        in_specs += [any_spec] * 2
        aliases = {}
    else:
        operands += caches
        in_specs += [any_spec] * 3
        aliases = {len(operands) - 2: 0, len(operands) - 1: 1, len(operands): 2}
    tokens = n_in * blk
    n_batch = q_diag.shape[0]
    return pl.pallas_call(
        functools.partial(kv_kernel, n_in, masks, batches, [[first for _, first in group] for group in groups], row0, stat_of, with_new),
        grid_spec=pltpu.PrefetchScalarGridSpec(
            num_scalar_prefetch=1,
            grid=(n_steps,),
            in_specs=in_specs,
            out_specs=[any_spec] * 3,
            scratch_shapes=[
                pltpu.VMEM((2, n_in, blk, d_model), jnp.bfloat16),
                pltpu.VMEM((tokens, width), jnp.bfloat16),
                pltpu.VMEM((tokens, width), jnp.bfloat16),
                pltpu.VMEM((2, n_in, blk, heads, HEAD_DIM), jnp.bfloat16),
                pltpu.VMEM((2, n_in, blk, heads, HEAD_DIM), jnp.bfloat16),
                pltpu.VMEM((2, n_in, 3, STAT_ROWS, HEAD_DIM), jnp.float32),
                pltpu.SemaphoreType.DMA((2, n_in)),
                pltpu.SemaphoreType.DMA((2, n_in, 3)),
                pltpu.SemaphoreType.DMA((2, n_batch)),
            ],
        ),
        out_shape=[jax.ShapeDtypeStruct(c.shape, c.dtype) for c in caches],
        input_output_aliases=aliases,
        compiler_params=pltpu.CompilerParams(vmem_limit_bytes=20 * 2 ** 20),
        cost_estimate=pl.CostEstimate(flops=4 * n_steps * tokens * d_model * width, bytes_accessed=2 * n_steps * tokens * (d_model + 2 * width), transcendentals=0),
        name="kv_chunk",
    )(scalars, *operands)


def tail_kernel(n_dev, parts_of, st_ref, self_ref, xs_ref, gain_ref, wo_hbm, wg_hbm, wu_hbm, wd_hbm, dec_ref, last_ref,
                wo, wg, wu, wd, stv, rows, a_buf, n_buf, mid_buf, ps1, pr1, ps2, pr2, xo1, xg1, xo2, xg2,
                w_sem, send_sem, recv_sem):
    me = lax.axis_index("model")
    n_batch = dec_ref.shape[0]
    n_rows = 2 * n_batch
    d_model = dec_ref.shape[1]
    cols = d_model // n_dev
    heads = STAT_ROWS // 2
    loads = [pltpu.make_async_copy(src, dst, w_sem.at[i]) for i, (src, dst) in enumerate(
        ((st_ref, stv), (wo_hbm, wo), (wg_hbm, wg), (wu_hbm, wu), (wd_hbm, wd)))]
    loads[0].start()
    loads[1].start()
    barrier = pltpu.get_barrier_semaphore()

    def peer_of(mask):
        return sum(lax.rem(me // bit + mask // bit, 2) * bit for bit in (1, 2, 4))

    far_first = sorted(range(1, n_dev), key=lambda mask: (-(mask & 2) - (mask & 4) // 2, mask))
    for mask in far_first:
        pl.semaphore_signal(barrier, inc=1, device_id={"model": peer_of(mask)}, device_id_type=MESH)

    def send(phase, mask, src, dst):
        return pltpu.make_async_remote_copy(
            src_ref=src, dst_ref=dst, send_sem=send_sem.at[phase, mask - 1], recv_sem=recv_sem.at[phase, mask - 1],
            device_id={"model": peer_of(mask)}, device_id_type=MESH)

    loads[0].wait()
    for load in loads[2:]:
        load.start()
    for b in range(n_batch):
        top = self_ref[1, b]
        for j in range(parts_of[b]):
            top = jnp.maximum(top, stv[j, b, 1])
        scale = jnp.exp(self_ref[1, b] - top)
        den = scale * self_ref[2, b]
        num = scale * self_ref[0, b]
        for j in range(parts_of[b]):
            scale = jnp.exp(stv[j, b, 1] - top)
            den += scale * stv[j, b, 2]
            num += scale * stv[j, b, 0]
        rows[:, b, :] = num / den
    for h in range(heads):
        for t in range(2):
            a_buf[t * n_batch:(t + 1) * n_batch, h * HEAD_DIM:(h + 1) * HEAD_DIM] = rows[2 * h + t]
    att = a_buf[...].astype(jnp.bfloat16)

    def all_reduce(phase, partial, base, ps, pr, xo, xg):
        copies = []
        for mask in far_first:
            ps[mask - 1] = partial(peer_of(mask))
            copies.append(send(phase, mask, ps.at[mask - 1], pr.at[mask - 1]))
            copies[-1].start()
        total = base + partial(me)
        for copy, mask in zip(reversed(copies), reversed(far_first)):
            copy.wait_recv()
            total = total + pr[mask - 1]
        xo[...] = total.astype(jnp.bfloat16)
        outs = []
        for mask in far_first:
            outs.append(send(phase + 1, mask, xo, xg.at[me]))
            outs[-1].start()
        xg[me] = xo[...]
        for out in outs:
            out.wait_recv()
        return copies + outs

    def col_block(p):
        return pl.ds(pl.multiple_of(p * cols, cols), cols)

    loads[1].wait()
    pl.semaphore_wait(barrier, n_dev - 1)
    sent = all_reduce(0, lambda p: jnp.dot(att, wo[:, col_block(p)], preferred_element_type=jnp.float32),
                      xs_ref[...].astype(jnp.float32), ps1, pr1, xo1, xg1)
    sq = jnp.zeros((n_rows, 1), jnp.float32)
    for j in range(n_dev):
        xf = xg1[j].astype(jnp.float32)
        sq += jnp.sum(xf * xf, axis=-1, keepdims=True)
    inv_rms = lax.rsqrt(sq / d_model + 1e-5)
    for j in range(n_dev):
        xf = xg1[j].astype(jnp.float32)
        n_buf[:, j * cols:(j + 1) * cols] = (xf * inv_rms * gain_ref[:, j * cols:(j + 1) * cols]).astype(jnp.bfloat16)
    loads[2].wait()
    loads[3].wait()
    nt = (((1,), (1,)), ((), ()))
    n_hid = wg.shape[0]
    rows_per = n_hid // 2

    def hidden_rows(r, carry):
        at = pl.ds(pl.multiple_of(r * rows_per, 8), rows_per)
        gate = lax.dot_general(wg[at, :], n_buf[...], nt, preferred_element_type=jnp.float32)
        up = lax.dot_general(wu[at, :], n_buf[...], nt, preferred_element_type=jnp.float32)
        mid_buf[at, :] = gate * (1.0 / (1.0 + jnp.exp(-gate))) * up
        return carry

    lax.fori_loop(0, 2, hidden_rows, 0)
    mid = mid_buf[...].T.astype(jnp.bfloat16)
    loads[4].wait()
    sent += all_reduce(2, lambda p: jnp.dot(mid, wd[:, col_block(p)], preferred_element_type=jnp.float32),
                       xo1[...].astype(jnp.float32), ps2, pr2, xo2, xg2)
    for j in range(n_dev):
        dec_ref[:, j * cols:(j + 1) * cols] = xg2[j, :n_batch]
        last_ref[:, j * cols:(j + 1) * cols] = xg2[j, n_batch:]
    for copy in sent:
        copy.wait_send()


def tail_call(n_dev, parts_of, stats, self_stat, x_mine, gain, w_o, w_gate_t, w_up_t, w_down, n_batch):
    n_rows, cols = x_mine.shape
    d_model = w_o.shape[1]
    vmem = pl.BlockSpec(memory_space=pltpu.VMEM)
    hbm = pl.BlockSpec(memory_space=pltpu.HBM)
    return pl.pallas_call(
        functools.partial(tail_kernel, n_dev, parts_of),
        out_shape=[jax.ShapeDtypeStruct((n_batch, d_model), jnp.bfloat16)] * 2,
        in_specs=[pl.BlockSpec(memory_space=pl.ANY), vmem, vmem, vmem, hbm, hbm, hbm, hbm],
        out_specs=[vmem, vmem],
        scratch_shapes=[
            pltpu.VMEM(w_o.shape, jnp.bfloat16),
            pltpu.VMEM(w_gate_t.shape, jnp.bfloat16),
            pltpu.VMEM(w_up_t.shape, jnp.bfloat16),
            pltpu.VMEM(w_down.shape, jnp.bfloat16),
            pltpu.VMEM(stats.shape, jnp.float32),
            pltpu.VMEM((STAT_ROWS, n_batch, HEAD_DIM), jnp.float32),
            pltpu.VMEM((n_rows, w_o.shape[0]), jnp.float32),
            pltpu.VMEM((n_rows, d_model), jnp.bfloat16),
            pltpu.VMEM((w_gate_t.shape[0], n_rows), jnp.float32),
            pltpu.VMEM((n_dev - 1, n_rows, cols), jnp.float32),
            pltpu.VMEM((n_dev - 1, n_rows, cols), jnp.float32),
            pltpu.VMEM((n_dev - 1, n_rows, cols), jnp.float32),
            pltpu.VMEM((n_dev - 1, n_rows, cols), jnp.float32),
            pltpu.VMEM((n_rows, cols), jnp.bfloat16),
            pltpu.VMEM((n_dev, n_rows, cols), jnp.bfloat16),
            pltpu.VMEM((n_rows, cols), jnp.bfloat16),
            pltpu.VMEM((n_dev, n_rows, cols), jnp.bfloat16),
            pltpu.SemaphoreType.DMA((5,)),
            pltpu.SemaphoreType.DMA((4, n_dev - 1)),
            pltpu.SemaphoreType.DMA((4, n_dev - 1)),
        ],
        compiler_params=pltpu.CompilerParams(collective_id=0, has_side_effects=True, vmem_limit_bytes=52 * 2 ** 20),
        name="tail",
    )(stats, self_stat, x_mine, gain, *(pltpu.with_memory_space_constraint(w, pltpu.HBM) for w in (w_o, w_gate_t, w_up_t, w_down)))


def solution(mesh):
    n_dev = mesh.shape['model']
    seq_spec = P('replica', 'model', None)
    col_spec = P(None, None, 'model')
    row_spec = P(None, 'model', None)
    gain_spec = P(None, None)
    tok_spec = P('replica', None)
    cache_spec = P(None, 'replica', None, 'model', None)
    in_specs = (seq_spec, P('replica'), tok_spec, gain_spec, col_spec, col_spec, col_spec, row_spec, gain_spec, col_spec, col_spec, row_spec)
    out_specs = (tok_spec, tok_spec, cache_spec, cache_spec)

    def swap(arr, bit):
        return lax.ppermute(arr, 'model', [(i, i ^ bit) for i in range(n_dev)])

    def per_device(prompt, lengths, new_tok, norm_attn, w_q, w_k, w_v, w_o, norm_mlp, w_gate, w_up, w_down):
        my_idx = lax.axis_index('model')
        n_batch, blk, d_model = prompt.shape
        seq_len = blk * n_dev
        width = w_k.shape[2]
        heads = width // HEAD_DIM
        half = n_batch // 2
        wq = w_q[0]
        gain = norm_attn.astype(jnp.float32)

        q1, q2, rows_h = n_batch // 8, n_batch // 4, blk // 2
        a_parts, b_parts = {}, {}
        order = [side * half + k for k in range(q1) for side in range(2)]
        outs_of = [[(2 * h + side, k, h * rows_h, rows_h) for h in range(2)] for k in range(q1) for side in range(2)]
        a_parts["0a"], b_parts["0a"], a_parts["0b"], b_parts["0b"] = norm_call(prompt, gain, order, outs_of, [(q1, rows_h)] * 4)
        from_y, from_x = {}, {}

        def send_part(step, along_y, along_x):
            from_y[step] = swap(along_y, 4)
            from_x[step] = swap(along_x, 2)

        send_part("0a", a_parts["0a"], b_parts["0a"])
        send_part("0b", a_parts["0b"], b_parts["0b"])
        order, outs_of = [], []
        for part, (lo, hi) in ((1, (q1, q2)), (2, (q2, half)), (0, (0, q1))):
            for k in range(lo, hi):
                for side in range(2):
                    order.append(side * half + k)
                    outs_of.append([(4, side * half + k, 0, blk)] + ([(2 * part - 2 + side, k - lo, 0, blk)] if part else []))
        a_parts["1"], b_parts["1"], a_parts["2"], b_parts["2"], normed = norm_call(
            prompt, gain, order, outs_of, [(q2 - q1, blk)] * 2 + [(half - q2, blk)] * 2 + [(n_batch, blk)])
        send_part("1", a_parts["1"], b_parts["1"])
        seq_pos = my_idx * blk + jnp.arange(blk)
        sel = (seq_pos[None, :] == (lengths - 1)[:, None]).astype(jnp.bfloat16)
        last_x = jnp.einsum('bs,bsd->bd', sel, prompt, preferred_element_type=jnp.float32).astype(jnp.bfloat16)
        last_x = last_x + swap(last_x, 1)
        last_x = (last_x + swap(last_x, 2)) + (swap(last_x, 4) + swap(last_x, 6))
        send_part("2", a_parts["2"], b_parts["2"])
        send_part("3", b_parts["2"], a_parts["2"])
        send_part("4", normed[half:half + q2], normed[:q2])
        core_all = swap(normed, 1)

        bits = jnp.arange(N_MASKS)
        scalars = jnp.concatenate([sum(((my_idx // bit + bits // bit) % 2) * bit for bit in (1, 2, 4)), lengths]).astype(jnp.int32)
        row_tabs = rotary_tables(jnp.concatenate([lengths, lengths - 1]))
        tabs = tuple(tab.reshape(n_dev, blk, HEAD_DIM) for tab in rotary_tables(jnp.arange(seq_len)))
        x_rows = jnp.concatenate([new_tok, last_x], axis=0)
        x_mine = lax.dynamic_slice_in_dim(x_rows, my_idx * (d_model // n_dev), d_model // n_dev, axis=1)
        wk, wv, last_x, scalars, row_tabs, tabs, x_mine, gain_mlp = lax.optimization_barrier(
            (w_k[0], w_v[0], last_x, scalars, row_tabs, tabs, x_mine, norm_mlp.astype(jnp.float32)))
        wk, wv = keep_in_vmem(wk, wv)
        q_diag, k_new, v_new, self_stat = rows_call(new_tok, last_x, gain, row_tabs, wq, wk, wv)
        cache_shape = jax.ShapeDtypeStruct((n_batch, seq_len + 1, heads, HEAD_DIM), jnp.bfloat16)
        caches = [cache_shape, cache_shape, jax.ShapeDtypeStruct((2 * n_dev - 2, n_batch, 3, STAT_ROWS, HEAD_DIM), jnp.float32)]

        def run(groups, per_group, masks, batches, caches, **kw):
            return kv_call(groups, per_group, masks, batches, scalars, tabs, wk, wv, q_diag, caches, **kw)

        def half_rows(step):
            return {"row0": rows_h * (step == "0b"), "stat_of": (n_dev - 2) * (step == "0b")}

        def after(caches, *arrays):
            out = lax.optimization_barrier((caches[2], *arrays))
            return [caches[0], caches[1], out[0]], out[1:]

        caches = run([[(arr, 0), (arr, half)] for arr in (normed, core_all)], half,
                     [[0] * 2, [1] * 2], [[0, half]] * 2, caches, new_rows=[k_new, v_new])
        diag = {}
        starts = {"0a": (0, half), "0b": (0, half), "1": (q1, half + q1), "2": (q2, half + q2), "3": (half + q2, q2), "4": (half, 0)}
        for step, start in starts.items():
            caches, (got_y, got_x) = after(caches, from_y[step], from_x[step])
            other_y, other_x = swap(got_y, 1), swap(got_x, 1)
            if step not in "34":
                diag[step] = (swap(got_y, 2), swap(got_x, 4))
            streams = [[(got_y, 0), (got_x, 0)], [(other_y, 0), (other_x, 0)]]
            if step in ("0a", "0b"):
                caches = run([streams[0] + streams[1]], q1, [[4, 2, 5, 3]], [[*start, *start]], caches, **half_rows(step))
            else:
                caches = run(streams, got_y.shape[0], [[4, 2], [5, 3]], [list(start)] * 2, caches)
        for step in ("2", "1", "0a", "0b"):
            caches, (via_x, via_y) = after(caches, *diag[step])
            other_x, other_y = swap(via_x, 1), swap(via_y, 1)
            start = starts[step]
            streams = [[(via_x, 0), (via_y, 0)], [(other_x, 0), (other_y, 0)]]
            if step in ("0a", "0b"):
                caches = run([streams[0] + streams[1]], q1, [[6, 6, 7, 7]], [[*start, *start]], caches, **half_rows(step))
            else:
                caches = run(streams, via_x.shape[0], [[6] * 2, [7] * 2], [list(start)] * 2, caches)

        k_cache, v_cache, stats = caches
        parts_of = [2 * n_dev - 2 if b % half < q1 else n_dev for b in range(n_batch)]
        dec_hidden, last_hidden = tail_call(n_dev, parts_of, stats, self_stat, x_mine, gain_mlp, w_o[0],
                                            w_gate[0].T, w_up[0].T, w_down[0], n_batch)
        return dec_hidden, last_hidden, k_cache[None], v_cache[None]

    return jax.shard_map(per_device, mesh=mesh, in_specs=in_specs, out_specs=out_specs, check_vma=False)
```

```python
import functools

import jax
import jax.numpy as jnp
from jax import lax
from jax.experimental import pallas as pl
from jax.experimental.pallas import tpu as pltpu
from jax.sharding import PartitionSpec as P


HEAD_DIM = 128
NEG_BIG = -1e30
STAT_ROWS = 8
NORM_ROWS = 32
COL_TILE = 256
N_MASKS = 8
MESH = pl.DeviceIdType.MESH


def rotary_tables(positions):
    half_dim = HEAD_DIM // 2
    inv_freq = 10000.0 ** (-2.0 * jnp.arange(half_dim, dtype=jnp.float32) / HEAD_DIM)
    angles = positions.astype(jnp.float32)[..., None] * inv_freq
    cos_tab = jnp.cos(angles)
    sin_tab = jnp.sin(angles)
    return jnp.concatenate([cos_tab, cos_tab], axis=-1), jnp.concatenate([-sin_tab, sin_tab], axis=-1)


def load_kernel(*refs):
    n = len(refs) // 2
    sem = refs[-1]
    copies = [pltpu.make_async_copy(refs[i], refs[n + i], sem.at[i]) for i in range(n)]
    for copy in copies:
        copy.start()
    for copy in copies:
        copy.wait()


def keep_in_vmem(*arrays):
    return pl.pallas_call(
        load_kernel,
        out_shape=[pltpu.VMEM(arr.shape, arr.dtype) for arr in arrays],
        in_specs=[pl.BlockSpec(memory_space=pl.ANY)] * len(arrays),
        out_specs=[pl.BlockSpec(memory_space=pltpu.VMEM)] * len(arrays),
        scratch_shapes=[pltpu.SemaphoreType.DMA((len(arrays),))],
        compiler_params=pltpu.CompilerParams(vmem_limit_bytes=24 * 2 ** 20),
        name="keep",
    )(*(pltpu.with_memory_space_constraint(arr, pltpu.HBM) for arr in arrays))


def turn_kernel(w_ref, out_ref):
    out_ref[...] = w_ref[...].T


def turn_call(w_t):
    n, d = w_t.shape
    cols = 512
    return pl.pallas_call(
        turn_kernel,
        grid=(d // cols,),
        in_specs=[pl.BlockSpec((n, cols), lambda g: (0, g))],
        out_specs=pl.BlockSpec((cols, n), lambda g: (g, 0)),
        out_shape=jax.ShapeDtypeStruct((d, n), w_t.dtype),
        compiler_params=pltpu.CompilerParams(vmem_limit_bytes=12 * 2 ** 20),
        cost_estimate=pl.CostEstimate(flops=2 * d * n * 128, bytes_accessed=4 * d * n, transcendentals=0),
        name="turn",
    )(pltpu.with_memory_space_constraint(w_t, pltpu.HBM))


def norm_kernel(outs_of, x_ref, gain_ref, *refs):
    n_out = len(refs) - 3
    out_refs = refs[:n_out]
    ss_buf, n_buf, sems = refs[n_out:]
    step = pl.program_id(0)
    blk, d_model = x_ref.shape[1:]
    lanes = [slice(c * HEAD_DIM, (c + 1) * HEAD_DIM) for c in range(d_model // HEAD_DIM)]

    def copies(at_step):
        return [pltpu.make_async_copy(n_buf.at[at_step % 2, pl.ds(lo, rows)], out_refs[o].at[i], sems.at[at_step % 2, k])
                for k, (o, i, lo, rows) in enumerate(outs_of[at_step])]

    for at_step in range(2, len(outs_of)):
        @pl.when(step == at_step)
        def _():
            for copy in copies(at_step - 2):
                copy.wait()

    def square_rows(r, carry):
        rows = pl.ds(pl.multiple_of(r * NORM_ROWS, NORM_ROWS), NORM_ROWS)
        acc = [jnp.zeros((NORM_ROWS, HEAD_DIM), jnp.float32) for _ in range(2)]
        for c, lane in enumerate(lanes):
            xf = x_ref[0, rows, lane].astype(jnp.float32)
            acc[c % 2] += xf * xf
        ss_buf[rows, :] = acc[0] + acc[1]
        return carry

    lax.fori_loop(0, blk // NORM_ROWS, square_rows, 0)
    total = jnp.sum(ss_buf[...], axis=-1, keepdims=True)
    ss_buf[...] = jnp.broadcast_to(lax.rsqrt(total / d_model + 1e-5), (blk, HEAD_DIM))
    slot = lax.rem(step, 2)

    def norm_rows(r, carry):
        rows = pl.ds(pl.multiple_of(r * NORM_ROWS, NORM_ROWS), NORM_ROWS)
        inv_rms = ss_buf[rows, :]
        for lane in lanes:
            xf = x_ref[0, rows, lane].astype(jnp.float32)
            n_buf[slot, rows, lane] = (xf * inv_rms * gain_ref[:, lane].astype(jnp.float32)).astype(jnp.bfloat16)
        return carry

    lax.fori_loop(0, blk // NORM_ROWS, norm_rows, 0)
    for at_step in range(len(outs_of)):
        @pl.when(step == at_step)
        def _():
            for copy in copies(at_step):
                copy.start()
            if at_step == len(outs_of) - 1:
                for copy in copies(at_step):
                    copy.wait()
                if at_step >= 1:
                    for copy in copies(at_step - 1):
                        copy.wait()


def norm_call(x, gain, order, outs_of, shapes, blk=None, row_block=0):
    d_model = x.shape[2]
    blk = blk or x.shape[1]

    def prompt_of(g):
        idx = jnp.int32(order[-1])
        for k in range(len(order) - 1):
            idx = jnp.where(g == k, order[k], idx)
        return idx

    return pl.pallas_call(
        functools.partial(norm_kernel, outs_of),
        grid=(len(order),),
        in_specs=[pl.BlockSpec((1, blk, d_model), lambda g: (prompt_of(g), row_block, 0)),
                  pl.BlockSpec((1, d_model), lambda g: (0, 0))],
        out_specs=[pl.BlockSpec(memory_space=pl.ANY)] * len(shapes),
        out_shape=[jax.ShapeDtypeStruct((*shape, d_model), jnp.bfloat16) for shape in shapes],
        scratch_shapes=[
            pltpu.VMEM((blk, HEAD_DIM), jnp.float32),
            pltpu.VMEM((2, blk, d_model), jnp.bfloat16),
            pltpu.SemaphoreType.DMA((2, max(len(o) for o in outs_of))),
        ],
        compiler_params=pltpu.CompilerParams(vmem_limit_bytes=24 * 2 ** 20),
        cost_estimate=pl.CostEstimate(flops=len(order) * blk * d_model * 8, bytes_accessed=len(order) * blk * d_model * 6, transcendentals=0),
        name="norm_rows",
    )(pltpu.with_memory_space_constraint(x, pltpu.HBM), gain)


def rows_kernel(new_ref, last_ref, gain_ref, cos_ref, sin_ref, wq_hbm, wk, wv, q_ref, k_ref, v_ref, st_ref, wq, q_buf, sem):
    load = pltpu.make_async_copy(wq_hbm, wq, sem)
    load.start()
    n_batch = new_ref.shape[0]
    heads = wk.shape[1] // HEAD_DIM
    xf = jnp.concatenate([new_ref[...].astype(jnp.float32), last_ref[...].astype(jnp.float32)], axis=0)
    inv_rms = lax.rsqrt(jnp.mean(xf * xf, axis=-1, keepdims=True) + 1e-5)
    normed = (xf * inv_rms * gain_ref[...].astype(jnp.float32)).astype(jnp.bfloat16)
    k_all = jnp.dot(normed, wk[...], preferred_element_type=jnp.float32)[:n_batch]
    v_all = jnp.dot(normed, wv[...], preferred_element_type=jnp.float32)[:n_batch].astype(jnp.bfloat16)
    load.wait()
    q_all = jnp.dot(normed, wq[...], preferred_element_type=jnp.float32)
    q_buf[...] = jnp.zeros_like(q_buf)
    k_rot = []
    for h in range(heads):
        cols = slice(h * HEAD_DIM, (h + 1) * HEAD_DIM)
        qh = q_all[:, cols]
        qh = (qh * cos_ref[...] + pltpu.roll(qh, HEAD_DIM // 2, 1) * sin_ref[...]).astype(jnp.bfloat16).astype(jnp.float32)
        kh = k_all[:, cols]
        kh = (kh * cos_ref[:n_batch, :] + pltpu.roll(kh, HEAD_DIM // 2, 1) * sin_ref[:n_batch, :]).astype(jnp.bfloat16)
        k_rot.append(kh)
        score = jnp.sum(qh[:n_batch] * kh.astype(jnp.float32), axis=-1, keepdims=True) * (HEAD_DIM ** -0.5)
        zero = jnp.zeros((n_batch, HEAD_DIM), jnp.float32)
        for t in range(2):
            row = 2 * h + t
            q_buf[:, row, cols] = qh[t * n_batch:(t + 1) * n_batch]
            st_ref[0, :, row, :] = v_all[:, cols].astype(jnp.float32) if t == 0 else zero
            st_ref[1, :, row, :] = zero + score if t == 0 else zero + NEG_BIG
            st_ref[2, :, row, :] = zero + 1.0 if t == 0 else zero
    q_ref[...] = q_buf[...].astype(jnp.bfloat16)
    k_ref[...] = jnp.concatenate(k_rot, axis=1).reshape(n_batch, heads, HEAD_DIM)
    v_ref[...] = v_all.reshape(n_batch, heads, HEAD_DIM)


def rows_call(new_tok, last_x, gain, row_tabs, w_q, w_k, w_v):
    n_batch = new_tok.shape[0]
    width = w_q.shape[1]
    heads = width // HEAD_DIM
    vmem = pl.BlockSpec(memory_space=pltpu.VMEM)
    return pl.pallas_call(
        rows_kernel,
        out_shape=[
            jax.ShapeDtypeStruct((n_batch, STAT_ROWS, width), jnp.bfloat16),
            jax.ShapeDtypeStruct((n_batch, heads, HEAD_DIM), jnp.bfloat16),
            jax.ShapeDtypeStruct((n_batch, heads, HEAD_DIM), jnp.bfloat16),
            jax.ShapeDtypeStruct((3, n_batch, STAT_ROWS, HEAD_DIM), jnp.float32),
        ],
        in_specs=[vmem] * 5 + [pl.BlockSpec(memory_space=pl.ANY)] + [vmem] * 2,
        out_specs=[vmem] * 4,
        scratch_shapes=[
            pltpu.VMEM(w_q.shape, jnp.bfloat16),
            pltpu.VMEM((n_batch, STAT_ROWS, width), jnp.float32),
            pltpu.SemaphoreType.DMA,
        ],
        compiler_params=pltpu.CompilerParams(vmem_limit_bytes=24 * 2 ** 20),
        cost_estimate=pl.CostEstimate(flops=2 * 2 * n_batch * 3 * w_q.shape[0] * width, bytes_accessed=2 * w_q.size, transcendentals=0),
        name="query_rows",
    )(new_tok, last_x, gain, *row_tabs, pltpu.with_memory_space_constraint(w_q, pltpu.HBM), w_k, w_v)


def by_group(group, values):
    out = values[-1]
    for p in range(len(values) - 1):
        out = jnp.where(group == p, values[p], out)
    return out


def kv_kernel(n_in, masks, batches, firsts, row0, stat_of, with_new, sc_ref, *refs):
    n_groups = len(masks)
    n_arr = n_in * n_groups
    x_refs = refs[:n_arr]
    cos_ref, sin_ref, wk, wv, q_ref = refs[n_arr:n_arr + 5]
    rest = refs[n_arr + 5:]
    if with_new:
        new_refs = rest[:2]
        rest = rest[2:]
    else:
        rest = rest[3:]
    kc_ref, vc_ref, st_ref, x_buf, k_buf, v_buf, k_out, v_out, s_out, x_sem, sems, s_sem, new_sem = rest
    step = pl.program_id(0)
    n_steps = pl.num_programs(0)
    slot = lax.rem(step, 2)
    per_group = n_steps // n_groups
    blk = x_buf.shape[2]
    shard_rows = cos_ref.shape[1]
    width = wk.shape[1]
    heads = width // HEAD_DIM
    n_tok = n_in * blk

    def x_copies(at_step, which, group):
        local = at_step - group * per_group
        return [pltpu.make_async_copy(x_refs[group * n_in + i].at[firsts[group][i] + local],
                                      x_buf.at[which, i], x_sem.at[which, i]) for i in range(n_in)]

    def start_x(at_step, which):
        for group in range(n_groups):
            @pl.when(at_step // per_group == group)
            def _(group=group):
                for copy in x_copies(at_step, which, group):
                    copy.start()

    def place(i, at_step):
        group = at_step // per_group
        mask = by_group(group, [m[i] for m in masks])
        return sc_ref[mask], by_group(group, [b[i] for b in batches]) + lax.rem(at_step, per_group), mask

    def out_copies(which, at_step):
        copies = []
        for i in range(n_in):
            shard, bat, _ = place(i, at_step)
            rows = pl.ds(shard * shard_rows + row0, blk)
            copies.append(pltpu.make_async_copy(k_out.at[which, i], kc_ref.at[bat, rows], sems.at[which, i, 0]))
            copies.append(pltpu.make_async_copy(v_out.at[which, i], vc_ref.at[bat, rows], sems.at[which, i, 1]))
        return copies

    def new_copies():
        return [pltpu.make_async_copy(src.at[pl.ds(b, 1)], dst.at[b, pl.ds(dst.shape[1] - 1, 1)], new_sem.at[idx, b])
                for idx, (src, dst) in enumerate(zip(new_refs, (kc_ref, vc_ref))) for b in range(src.shape[0])]

    @pl.when(step == 0)
    def _():
        start_x(step, slot)
        if with_new:
            for copy in new_copies():
                copy.start()

    @pl.when(step + 1 < n_steps)
    def _():
        start_x(step + 1, 1 - slot)

    @pl.when(step >= 2)
    def _():
        for copy in out_copies(slot, step - 2):
            copy.wait()

    for copy in x_copies(0, slot, 0):
        copy.wait()
    x_rows = x_buf.at[slot]

    def col_tile(c, carry):
        cols = pl.ds(pl.multiple_of(c * COL_TILE, COL_TILE), COL_TILE)
        normed = x_rows[...].reshape(n_tok, x_buf.shape[3])
        kf = jnp.dot(normed, wk[:, cols], preferred_element_type=jnp.float32)
        vf = jnp.dot(normed, wv[:, cols], preferred_element_type=jnp.float32)
        v_buf[:, cols] = vf.astype(jnp.bfloat16)
        parts = []
        for i in range(n_in):
            shard = place(i, step)[0]
            cos_tab = cos_ref[shard, row0:row0 + blk]
            sin_tab = sin_ref[shard, row0:row0 + blk]
            halves = []
            for h in range(COL_TILE // HEAD_DIM):
                kh = kf[i * blk:(i + 1) * blk, h * HEAD_DIM:(h + 1) * HEAD_DIM]
                halves.append(kh * cos_tab + pltpu.roll(kh, HEAD_DIM // 2, 1) * sin_tab)
            parts.append(jnp.concatenate(halves, axis=1))
        k_buf[:, cols] = jnp.concatenate(parts, axis=0).astype(jnp.bfloat16)
        return carry

    lax.fori_loop(0, width // COL_TILE, col_tile, 0)

    for i in range(n_in):
        k_out[slot, i] = k_buf[i * blk:(i + 1) * blk, :].reshape(blk, heads, HEAD_DIM)
        v_out[slot, i] = v_buf[i * blk:(i + 1) * blk, :].reshape(blk, heads, HEAD_DIM)
    for copy in out_copies(slot, step):
        copy.start()

    head_of_row = lax.broadcasted_iota(jnp.int32, (STAT_ROWS, HEAD_DIM), 0) // (STAT_ROWS // heads)
    probs = []
    for i in range(n_in):
        shard, bat, _ = place(i, step)
        scores = lax.dot_general(q_ref[bat], k_buf[i * blk:(i + 1) * blk, :], (((1,), (1,)), ((), ())),
                                 preferred_element_type=jnp.float32) * (HEAD_DIM ** -0.5)
        pos = shard * shard_rows + row0 + lax.broadcasted_iota(jnp.int32, scores.shape, 1)
        visible = pos < sc_ref[N_MASKS + bat]
        scores = jnp.where(visible, scores, NEG_BIG)
        blk_max = jnp.max(scores, axis=-1, keepdims=True)
        prob = jnp.where(visible, jnp.exp(scores - blk_max), 0.0)
        probs.append((blk_max, prob))
    for i, (blk_max, prob) in enumerate(probs):
        full = jnp.dot(prob.astype(jnp.bfloat16), v_buf[i * blk:(i + 1) * blk, :], preferred_element_type=jnp.float32)
        acc = jnp.zeros((STAT_ROWS, HEAD_DIM), jnp.float32)
        for h in range(heads):
            acc = jnp.where(head_of_row == h, full[:, h * HEAD_DIM:(h + 1) * HEAD_DIM], acc)
        s_out[i, 0] = acc
        s_out[i, 1] = jnp.broadcast_to(blk_max, (STAT_ROWS, HEAD_DIM))
        s_out[i, 2] = jnp.broadcast_to(jnp.sum(prob, axis=-1, keepdims=True), (STAT_ROWS, HEAD_DIM))
    stat_copies = []
    for i in range(n_in):
        _, bat, mask = place(i, step)
        stat_copies.append(pltpu.make_async_copy(s_out.at[i], st_ref.at[mask + stat_of, bat], s_sem.at[i]))
        stat_copies[-1].start()
    for copy in stat_copies:
        copy.wait()

    @pl.when(step == n_steps - 1)
    def _():
        for copy in out_copies(slot, step):
            copy.wait()
        if with_new:
            for copy in new_copies():
                copy.wait()

    @pl.when((step == n_steps - 1) & (n_steps >= 2))
    def _():
        for copy in out_copies(1 - slot, step - 1):
            copy.wait()


def kv_call(groups, per_group, masks, batches, scalars, tabs, w_k, w_v, q_diag, caches, new_rows=None, row0=0, stat_of=0):
    n_groups = len(groups)
    n_in = len(groups[0])
    n_steps = n_groups * per_group
    cos_tab, sin_tab = tabs
    blk, d_model = groups[0][0][0].shape[1:]
    width = w_k.shape[1]
    heads = width // HEAD_DIM
    any_spec = pl.BlockSpec(memory_space=pl.ANY)
    operands = [arr for group in groups for arr, _ in group]
    in_specs = [any_spec] * len(operands) + [pl.BlockSpec(memory_space=pltpu.VMEM)] * 5
    operands += [cos_tab, sin_tab, w_k, w_v, q_diag]
    with_new = new_rows is not None
    if with_new:
        operands += new_rows
        in_specs += [any_spec] * 2
        aliases = {}
    else:
        operands += [*caches[:2], pltpu.with_memory_space_constraint(caches[2], pltpu.VMEM)]
        in_specs += [any_spec] * 3
        aliases = {len(operands) - 2: 0, len(operands) - 1: 1, len(operands): 2}
    tokens = n_in * blk
    n_batch = q_diag.shape[0]
    return pl.pallas_call(
        functools.partial(kv_kernel, n_in, masks, batches, [[first for _, first in group] for group in groups], row0, stat_of, with_new),
        grid_spec=pltpu.PrefetchScalarGridSpec(
            num_scalar_prefetch=1,
            grid=(n_steps,),
            in_specs=in_specs,
            out_specs=[any_spec] * 3,
            scratch_shapes=[
                pltpu.VMEM((2, n_in, blk, d_model), jnp.bfloat16),
                pltpu.VMEM((tokens, width), jnp.bfloat16),
                pltpu.VMEM((tokens, width), jnp.bfloat16),
                pltpu.VMEM((2, n_in, blk, heads, HEAD_DIM), jnp.bfloat16),
                pltpu.VMEM((2, n_in, blk, heads, HEAD_DIM), jnp.bfloat16),
                pltpu.VMEM((n_in, 3, STAT_ROWS, HEAD_DIM), jnp.float32),
                pltpu.SemaphoreType.DMA((2, n_in)),
                pltpu.SemaphoreType.DMA((2, n_in, 2)),
                pltpu.SemaphoreType.DMA((n_in,)),
                pltpu.SemaphoreType.DMA((2, n_batch)),
            ],
        ),
        out_shape=[*(jax.ShapeDtypeStruct(c.shape, c.dtype) for c in caches[:2]), pltpu.VMEM(caches[2].shape, caches[2].dtype)],
        input_output_aliases=aliases,
        compiler_params=pltpu.CompilerParams(vmem_limit_bytes=20 * 2 ** 20),
        cost_estimate=pl.CostEstimate(flops=4 * n_steps * tokens * d_model * width, bytes_accessed=2 * n_steps * tokens * (d_model + 2 * width), transcendentals=0),
        name="kv_chunk",
    )(scalars, *operands)


def tail_kernel(n_dev, parts_of, stv, self_ref, xs_ref, gain_ref, wo, wg_hbm, wu_hbm, wd_hbm, out_ref,
                wg, wu, wd, rows, a_buf, n_buf, ps1, pr1, ps2, pr2, xo1, xg1, xo2, xg2, w_sem, send_sem, recv_sem):
    me = lax.axis_index("model")
    n_batch = out_ref.shape[1]
    n_rows = 2 * n_batch
    d_model = out_ref.shape[2]
    cols = d_model // n_dev
    heads = STAT_ROWS // 2
    loads = [pltpu.make_async_copy(src, dst, w_sem.at[i]) for i, (src, dst) in enumerate(((wg_hbm, wg), (wu_hbm, wu), (wd_hbm, wd)))]
    for load in loads:
        load.start()
    barrier = pltpu.get_barrier_semaphore()

    def peer_of(mask):
        return sum(lax.rem(me // bit + mask // bit, 2) * bit for bit in (1, 2, 4))

    far_first = ((6, 7), (2, 3, 4, 5), (1,))
    for mask in sum(far_first, ()):
        pl.semaphore_signal(barrier, inc=1, device_id={"model": peer_of(mask)}, device_id_type=MESH)

    def send(phase, mask, src, dst):
        return pltpu.make_async_remote_copy(
            src_ref=src, dst_ref=dst, send_sem=send_sem.at[phase, mask - 1], recv_sem=recv_sem.at[phase, mask - 1],
            device_id={"model": peer_of(mask)}, device_id_type=MESH)

    for b in range(n_batch):
        top = self_ref[1, b]
        for j in range(parts_of[b]):
            top = jnp.maximum(top, stv[j, b, 1])
        scale = jnp.exp(self_ref[1, b] - top)
        den = scale * self_ref[2, b]
        num = scale * self_ref[0, b]
        for j in range(parts_of[b]):
            scale = jnp.exp(stv[j, b, 1] - top)
            den += scale * stv[j, b, 2]
            num += scale * stv[j, b, 0]
        rows[:, b, :] = num / den
    for h in range(heads):
        for t in range(2):
            a_buf[t * n_batch:(t + 1) * n_batch, h * HEAD_DIM:(h + 1) * HEAD_DIM] = rows[2 * h + t]
    att = a_buf[...].astype(jnp.bfloat16)

    def exchange(phase, base, copies, pr, xo, xg):
        total = base
        for copy, mask in reversed(copies):
            copy.wait_recv()
            total = total + pr[mask - 1]
        xo[...] = total.astype(jnp.bfloat16)
        outs = []
        for mask in sum(far_first, ()):
            outs.append(send(phase + 1, mask, xo, xg.at[me]))
            outs[-1].start()
        xg[me] = xo[...]
        for out in outs:
            out.wait_recv()
        return [copy for copy, _ in copies] + outs

    def col_block(p):
        return pl.ds(pl.multiple_of(p * cols, cols), cols)

    part = jnp.dot(att, wo[...], preferred_element_type=jnp.float32)
    for j in range(n_dev):
        ps1[j] = part[:, j * cols:(j + 1) * cols]
    pl.semaphore_wait(barrier, n_dev - 1)
    copies = []
    for mask in sum(far_first, ()):
        copies.append((send(0, mask, ps1.at[peer_of(mask)], pr1.at[mask - 1]), mask))
        copies[-1][0].start()
    sent = exchange(0, xs_ref[...].astype(jnp.float32) + ps1[me], copies, pr1, xo1, xg1)
    sq = jnp.zeros((n_rows, 1), jnp.float32)
    for j in range(n_dev):
        xf = xg1[j].astype(jnp.float32)
        sq += jnp.sum(xf * xf, axis=-1, keepdims=True)
    inv_rms = lax.rsqrt(sq / d_model + 1e-5)
    for j in range(n_dev):
        at = slice(j * cols, (j + 1) * cols)
        n_buf[:, at] = (xg1[j].astype(jnp.float32) * inv_rms * gain_ref[:, at].astype(jnp.float32)).astype(jnp.bfloat16)
    loads[0].wait()
    loads[1].wait()
    gate = jnp.dot(n_buf[...], wg[...], preferred_element_type=jnp.float32)
    up = jnp.dot(n_buf[...], wu[...], preferred_element_type=jnp.float32)
    mid = (gate * (1.0 / (1.0 + jnp.exp(-gate))) * up).astype(jnp.bfloat16)
    loads[2].wait()
    copies = []
    for group in far_first:
        for mask in group:
            ps2[mask] = jnp.dot(mid, wd[:, col_block(peer_of(mask))], preferred_element_type=jnp.float32)
        if group == far_first[-1]:
            ps2[0] = jnp.dot(mid, wd[:, col_block(me)], preferred_element_type=jnp.float32)
        for mask in group:
            copies.append((send(2, mask, ps2.at[mask], pr2.at[mask - 1]), mask))
            copies[-1][0].start()
    sent += exchange(2, xo1[...].astype(jnp.float32) + ps2[0], copies, pr2, xo2, xg2)
    for j in range(n_dev):
        at = slice(j * cols, (j + 1) * cols)
        out_ref[0, :, at] = xg2[j, :n_batch]
        out_ref[1, :, at] = xg2[j, n_batch:]
    for copy in sent:
        copy.wait_send()


def tail_call(n_dev, parts_of, stats, self_stat, x_mine, gain, w_o, w_gate, w_up, w_down, n_batch):
    n_rows, cols = x_mine.shape
    d_model = w_o.shape[1]
    vmem = pl.BlockSpec(memory_space=pltpu.VMEM)
    any_spec = pl.BlockSpec(memory_space=pl.ANY)
    exchanged = [pltpu.VMEM((n_dev, n_rows, cols), jnp.float32), pltpu.VMEM((n_dev - 1, n_rows, cols), jnp.float32)]
    summed = [pltpu.VMEM((n_rows, cols), jnp.bfloat16), pltpu.VMEM((n_dev, n_rows, cols), jnp.bfloat16)]
    return pl.pallas_call(
        functools.partial(tail_kernel, n_dev, parts_of),
        out_shape=jax.ShapeDtypeStruct((2, n_batch, d_model), jnp.bfloat16),
        in_specs=[vmem] * 5 + [any_spec] * 3,
        out_specs=vmem,
        scratch_shapes=[
            pltpu.VMEM(w_gate.shape, jnp.bfloat16),
            pltpu.VMEM(w_up.shape, jnp.bfloat16),
            pltpu.VMEM(w_down.shape, jnp.bfloat16),
            pltpu.VMEM((STAT_ROWS, n_batch, HEAD_DIM), jnp.float32),
            pltpu.VMEM((n_rows, w_o.shape[0]), jnp.float32),
            pltpu.VMEM((n_rows, d_model), jnp.bfloat16),
            *exchanged, *exchanged, *summed, *summed,
            pltpu.SemaphoreType.DMA((3,)),
            pltpu.SemaphoreType.DMA((4, n_dev - 1)),
            pltpu.SemaphoreType.DMA((4, n_dev - 1)),
        ],
        compiler_params=pltpu.CompilerParams(collective_id=0, has_side_effects=True, vmem_limit_bytes=46 * 2 ** 20),
        name="tail",
    )(pltpu.with_memory_space_constraint(stats, pltpu.VMEM), self_stat, x_mine, gain, w_o,
      *(pltpu.with_memory_space_constraint(w, pltpu.HBM) for w in (w_gate, w_up, w_down)))


def solution(mesh):
    n_dev = mesh.shape['model']
    seq_spec = P('replica', 'model', None)
    col_spec = P(None, None, 'model')
    row_spec = P(None, 'model', None)
    gain_spec = P(None, None)
    tok_spec = P('replica', None)
    cache_spec = P(None, 'replica', None, 'model', None)
    in_specs = (seq_spec, P('replica'), tok_spec, gain_spec, col_spec, col_spec, col_spec, row_spec, gain_spec, col_spec, col_spec, row_spec)
    out_specs = (tok_spec, tok_spec, cache_spec, cache_spec)

    def swap(arr, bit):
        return lax.ppermute(arr, 'model', [(i, i ^ bit) for i in range(n_dev)])

    def per_device(prompt, lengths, new_tok, norm_attn, w_q, w_k, w_v, w_o, norm_mlp, w_gate, w_up, w_down):
        my_idx = lax.axis_index('model')
        n_batch, blk, d_model = prompt.shape
        seq_len = blk * n_dev
        width = w_k.shape[2]
        heads = width // HEAD_DIM
        half = n_batch // 2
        wq = w_q[0]
        gain = norm_attn

        q1, q2, rows_h = n_batch // 8, n_batch // 4, blk // 2
        a_parts, b_parts = {}, {}
        order = [side * half + k for k in range(q1) for side in range(2)]
        outs_of = [[(side, k, 0, rows_h)] for k in range(q1) for side in range(2)]
        for h, name in enumerate(("0a", "0b")):
            a_parts[name], b_parts[name] = norm_call(prompt, gain, order, outs_of, [(q1, rows_h)] * 2, rows_h, h)
        from_y, from_x = {}, {}

        def send_part(step, along_y, along_x):
            from_y[step] = swap(along_y, 4)
            from_x[step] = swap(along_x, 2)

        send_part("0a", a_parts["0a"], b_parts["0a"])
        send_part("0b", a_parts["0b"], b_parts["0b"])
        order, outs_of = [], []
        for part, (lo, hi) in ((1, (q1, q2)), (2, (q2, half)), (0, (0, q1))):
            for k in range(lo, hi):
                for side in range(2):
                    order.append(side * half + k)
                    outs_of.append([(4, side * half + k, 0, blk)] + ([(2 * part - 2 + side, k - lo, 0, blk)] if part else []))
        a_parts["1"], b_parts["1"], a_parts["2"], b_parts["2"], normed = norm_call(
            prompt, gain, order, outs_of, [(q2 - q1, blk)] * 2 + [(half - q2, blk)] * 2 + [(n_batch, blk)])
        send_part("1", a_parts["1"], b_parts["1"])
        seq_pos = my_idx * blk + jnp.arange(blk)
        sel = (seq_pos[None, :] == (lengths - 1)[:, None]).astype(jnp.bfloat16)
        last_x = jnp.einsum('bs,bsd->bd', sel, prompt, preferred_element_type=jnp.float32).astype(jnp.bfloat16)
        last_x = last_x + swap(last_x, 1)
        last_x = (last_x + swap(last_x, 2)) + (swap(last_x, 4) + swap(last_x, 6))
        send_part("2", a_parts["2"], b_parts["2"])
        send_part("3", b_parts["2"], a_parts["2"])
        send_part("4", normed[half:half + q2], normed[:q2])
        core_all = swap(normed, 1)

        bits = jnp.arange(N_MASKS)
        scalars = jnp.concatenate([sum(((my_idx // bit + bits // bit) % 2) * bit for bit in (1, 2, 4)), lengths]).astype(jnp.int32)
        row_tabs = rotary_tables(jnp.concatenate([lengths, lengths - 1]))
        tabs = tuple(tab.reshape(n_dev, blk, HEAD_DIM) for tab in rotary_tables(jnp.arange(seq_len)))
        x_rows = jnp.concatenate([new_tok, last_x], axis=0)
        x_mine = lax.dynamic_slice_in_dim(x_rows, my_idx * (d_model // n_dev), d_model // n_dev, axis=1)
        wk, wv, wo, last_x, scalars, row_tabs, tabs, x_mine = lax.optimization_barrier(
            (w_k[0], w_v[0], w_o[0], last_x, scalars, row_tabs, tabs, x_mine))
        wk, wv, wo = keep_in_vmem(wk, wv, wo)
        q_diag, k_new, v_new, self_stat = rows_call(new_tok, last_x, gain, row_tabs, wq, wk, wv)
        cache_shape = jax.ShapeDtypeStruct((n_batch, seq_len + 1, heads, HEAD_DIM), jnp.bfloat16)
        caches = [cache_shape, cache_shape, jax.ShapeDtypeStruct((2 * n_dev - 2, n_batch, 3, STAT_ROWS, HEAD_DIM), jnp.float32)]

        def run(groups, per_group, masks, batches, caches, **kw):
            return kv_call(groups, per_group, masks, batches, scalars, tabs, wk, wv, q_diag, caches, **kw)

        def half_rows(step):
            return {"row0": rows_h * (step == "0b"), "stat_of": (n_dev - 2) * (step == "0b")}

        def after(caches, *arrays):
            out = lax.optimization_barrier((caches[2], *arrays))
            return [caches[0], caches[1], out[0]], out[1:]

        caches = run([[(arr, 0), (arr, half)] for arr in (normed, core_all)], half,
                     [[0] * 2, [1] * 2], [[0, half]] * 2, caches, new_rows=[k_new, v_new])
        diag, turned = {}, {}
        starts = {"0a": (0, half), "0b": (0, half), "1": (q1, half + q1), "2": (q2, half + q2), "3": (half + q2, q2), "4": (half, 0)}
        for step, start in starts.items():
            caches, (got_y, got_x) = after(caches, from_y[step], from_x[step])
            other_y, other_x = swap(got_y, 1), swap(got_x, 1)
            if step not in "34":
                diag[step] = (swap(got_y, 2), swap(got_x, 4))
            streams = [[(got_y, 0), (got_x, 0)], [(other_y, 0), (other_x, 0)]]
            if step in ("0a", "0b"):
                caches = run([streams[0] + streams[1]], q1, [[4, 2, 5, 3]], [[*start, *start]], caches, **half_rows(step))
            else:
                caches = run(streams, got_y.shape[0], [[4, 2], [5, 3]], [list(start)] * 2, caches)
            if step in "34":
                caches, (w_t,) = after(caches, (w_gate if step == "3" else w_up)[0].T)
                turned[step] = turn_call(w_t)
                caches, (turned[step],) = after(caches, turned[step])
        for step in ("2", "1", "0a", "0b"):
            caches, (via_x, via_y) = after(caches, *diag[step])
            other_x, other_y = swap(via_x, 1), swap(via_y, 1)
            start = starts[step]
            streams = [[(via_x, 0), (via_y, 0)], [(other_x, 0), (other_y, 0)]]
            if step in ("0a", "0b"):
                caches = run([streams[0] + streams[1]], q1, [[6, 6, 7, 7]], [[*start, *start]], caches, **half_rows(step))
            else:
                caches = run(streams, via_x.shape[0], [[6] * 2, [7] * 2], [list(start)] * 2, caches)

        k_cache, v_cache, stats = caches
        parts_of = [2 * n_dev - 2 if b % half < q1 else n_dev for b in range(n_batch)]
        both = tail_call(n_dev, parts_of, stats, self_stat, x_mine, norm_mlp, wo, turned["3"], turned["4"], w_down[0], n_batch)
        return both[0], both[1], k_cache[None], v_cache[None]

    return jax.shard_map(per_device, mesh=mesh, in_specs=in_specs, out_specs=out_specs, check_vma=False)
```

```python
import jax
import jax.numpy as jnp
from jax import lax
from jax.sharding import PartitionSpec as P

HEAD_DIM = 128
NEG_BIG = -1e30


def rms_norm(hidden, gain_vec):
    hid_f32 = hidden.astype(jnp.float32)
    inv_rms = lax.rsqrt(jnp.mean(hid_f32 * hid_f32, axis=-1, keepdims=True) + 1e-5)
    return (hid_f32 * inv_rms * gain_vec.astype(jnp.float32)).astype(jnp.bfloat16)


def rotary(heads_f32, positions):
    half_dim = HEAD_DIM // 2
    inv_freq = 10000.0 ** (-2.0 * jnp.arange(half_dim, dtype=jnp.float32) / HEAD_DIM)
    angles = positions.astype(jnp.float32)[..., None] * inv_freq
    cos_tab = jnp.cos(angles)[..., None, :]
    sin_tab = jnp.sin(angles)[..., None, :]
    lo_half = heads_f32[..., :half_dim]
    hi_half = heads_f32[..., half_dim:]
    return jnp.concatenate([lo_half * cos_tab - hi_half * sin_tab, hi_half * cos_tab + lo_half * sin_tab], axis=-1)


def attend(queries, keys, values, visible):
    scores = jnp.einsum('bqhd,bkhd->bhqk', queries, keys, preferred_element_type=jnp.float32) * (HEAD_DIM ** -0.5)
    scores = jnp.where(visible[:, None], scores, NEG_BIG)
    top = jnp.max(scores, axis=-1, keepdims=True)
    prob = jnp.exp(scores - top)
    total = jnp.sum(prob, axis=-1)
    out = jnp.einsum('bhqk,bkhd->bqhd', prob.astype(jnp.bfloat16), values, preferred_element_type=jnp.float32)
    return (out / jnp.moveaxis(total, 1, 2)[..., None]).reshape(*queries.shape[:2], -1).astype(jnp.bfloat16)


def solution(mesh):
    n_dev = mesh.shape['model']
    seq_spec = P('replica', 'model', None)
    col_spec = P(None, None, 'model')
    row_spec = P(None, 'model', None)
    gain_spec = P(None, None)
    tok_spec = P('replica', None)
    cache_spec = P(None, 'replica', None, 'model', None)
    in_specs = (seq_spec, P('replica'), tok_spec, gain_spec, col_spec, col_spec, col_spec, row_spec, gain_spec, col_spec, col_spec, row_spec)
    out_specs = (tok_spec, tok_spec, cache_spec, cache_spec)
    fours = [[0, 1, 2, 3], [4, 5, 6, 7]]
    across = [(i, i ^ 4) for i in range(n_dev)]

    def dot(a, b):
        return jnp.dot(a, b, preferred_element_type=jnp.float32)

    def per_device(prompt, lengths, new_tok, norm_attn, w_q, w_k, w_v, w_o, norm_mlp, w_gate, w_up, w_down):
        my_idx = lax.axis_index('model')
        n_batch, blk, d_model = prompt.shape
        n_tok = n_batch * blk
        seq_len = blk * n_dev
        heads = w_k.shape[2] // HEAD_DIM
        wq, wk, wv = w_q[0], w_k[0], w_v[0]
        key_pos = jnp.arange(seq_len)

        normed = lax.all_gather(rms_norm(prompt, norm_attn[0]), 'model', axis=0)
        rows = normed.reshape(n_dev * n_tok, d_model)
        pos = key_pos.reshape(n_dev, 1, blk)

        def project(w):
            return dot(rows, w).reshape(n_dev, n_batch, blk, heads, HEAD_DIM)

        def in_order(x):
            return jnp.moveaxis(x, 0, 1).reshape(n_batch, seq_len, heads, HEAD_DIM)

        q_all = in_order(rotary(project(wq), pos).astype(jnp.bfloat16))
        k_all = in_order(rotary(project(wk), pos).astype(jnp.bfloat16))
        v_all = in_order(project(wv).astype(jnp.bfloat16))
        outs = []
        for i in range(n_dev):
            seen = (i + 1) * blk
            q_pos = i * blk + jnp.arange(blk)
            visible = (key_pos[None, None, :seen] <= q_pos[None, :, None]) & (key_pos[None, None, :seen] < lengths[:, None, None])
            outs.append(attend(q_all[:, i * blk:seen], k_all[:, :seen], v_all[:, :seen], visible))
        heads_out = jnp.stack(outs)
        mine = lax.all_to_all(heads_out, 'model', split_axis=0, concat_axis=0)
        att = jnp.moveaxis(mine.reshape(n_dev, n_tok, -1), 0, 1).reshape(n_tok, -1)

        wo_full = lax.all_gather(w_o[0], 'model', axis=0, tiled=True)
        hidden = (prompt.astype(jnp.float32) + dot(att, wo_full).reshape(n_batch, blk, d_model)).astype(jnp.bfloat16)
        near = rms_norm(hidden, norm_mlp[0]).reshape(n_tok, d_model)
        pair = jnp.concatenate([near, lax.ppermute(near, 'model', across)], axis=0)
        wg, wu = (lax.all_gather(w[0], 'model', axis=1, tiled=True, axis_index_groups=fours) for w in (w_gate, w_up))
        wd = lax.all_gather(w_down[0], 'model', axis=0, tiled=True, axis_index_groups=fours)
        mid = (jax.nn.silu(dot(pair, wg)) * dot(pair, wu)).astype(jnp.bfloat16)
        other = lax.ppermute(dot(mid[n_tok:], wd), 'model', across)
        total = dot(mid[:n_tok], wd) + other
        hidden = (hidden.astype(jnp.float32) + total.reshape(n_batch, blk, d_model)).astype(jnp.bfloat16)
        seq_pos = my_idx * blk + jnp.arange(blk)
        last_sel = (seq_pos[None, :] == (lengths - 1)[:, None]).astype(jnp.bfloat16)
        last_hidden = lax.psum(jnp.einsum('bs,bsd->bd', last_sel, hidden, preferred_element_type=jnp.float32), 'model').astype(jnp.bfloat16)

        tok_norm = rms_norm(new_tok, norm_attn[0])
        q_new = rotary(dot(tok_norm, wq).reshape(n_batch, heads, HEAD_DIM), lengths).astype(jnp.bfloat16)
        k_new = rotary(dot(tok_norm, wk).reshape(n_batch, heads, HEAD_DIM), lengths).astype(jnp.bfloat16)
        v_new = dot(tok_norm, wv).astype(jnp.bfloat16).reshape(n_batch, heads, HEAD_DIM)
        k_cache = jnp.concatenate([k_all, k_new[:, None]], axis=1)
        v_cache = jnp.concatenate([v_all, v_new[:, None]], axis=1)
        cache_pos = jnp.arange(seq_len + 1)
        visible = (cache_pos[None, :] < lengths[:, None]) | (cache_pos[None, :] == seq_len)
        tok_attn = attend(q_new[:, None], k_cache, v_cache, visible[:, None])[:, 0]
        dec_hidden = (new_tok.astype(jnp.float32) + lax.psum(dot(tok_attn, w_o[0]), 'model')).astype(jnp.bfloat16)
        tok_norm = rms_norm(dec_hidden, norm_mlp[0])
        tok_mid = (jax.nn.silu(dot(tok_norm, w_gate[0])) * dot(tok_norm, w_up[0])).astype(jnp.bfloat16)
        dec_hidden = (dec_hidden.astype(jnp.float32) + lax.psum(dot(tok_mid, w_down[0]), 'model')).astype(jnp.bfloat16)
        return dec_hidden, last_hidden, k_cache[None], v_cache[None]

    return jax.shard_map(per_device, mesh=mesh, in_specs=in_specs, out_specs=out_specs, check_vma=False)
```

```python
import jax
import jax.numpy as jnp
from jax import lax
from jax.sharding import PartitionSpec as P

HEAD_DIM = 128
NEG_BIG = -1e30
PIECES = 4


def rms_norm(hidden, gain_vec):
    hid_f32 = hidden.astype(jnp.float32)
    inv_rms = lax.rsqrt(jnp.mean(hid_f32 * hid_f32, axis=-1, keepdims=True) + 1e-5)
    return (hid_f32 * inv_rms * gain_vec.astype(jnp.float32)).astype(jnp.bfloat16)


def rotary(heads_f32, positions):
    half_dim = HEAD_DIM // 2
    inv_freq = 10000.0 ** (-2.0 * jnp.arange(half_dim, dtype=jnp.float32) / HEAD_DIM)
    angles = positions.astype(jnp.float32)[..., None] * inv_freq
    cos_tab = jnp.cos(angles)[..., None, :]
    sin_tab = jnp.sin(angles)[..., None, :]
    lo_half = heads_f32[..., :half_dim]
    hi_half = heads_f32[..., half_dim:]
    return jnp.concatenate([lo_half * cos_tab - hi_half * sin_tab, hi_half * cos_tab + lo_half * sin_tab], axis=-1)


def attend(queries, keys, values, visible):
    scores = jnp.einsum('bqhd,bkhd->bhqk', queries, keys, preferred_element_type=jnp.float32) * (HEAD_DIM ** -0.5)
    scores = jnp.where(visible[:, None], scores, NEG_BIG)
    top = jnp.max(scores, axis=-1, keepdims=True)
    prob = jnp.exp(scores - top)
    total = jnp.sum(prob, axis=-1)
    out = jnp.einsum('bhqk,bkhd->bqhd', prob.astype(jnp.bfloat16), values, preferred_element_type=jnp.float32)
    return (out / jnp.moveaxis(total, 1, 2)[..., None]).reshape(*queries.shape[:2], -1).astype(jnp.bfloat16)


def solution(mesh):
    n_dev = mesh.shape['model']
    seq_spec = P('replica', 'model', None)
    col_spec = P(None, None, 'model')
    row_spec = P(None, 'model', None)
    gain_spec = P(None, None)
    tok_spec = P('replica', None)
    cache_spec = P(None, 'replica', None, 'model', None)
    in_specs = (seq_spec, P('replica'), tok_spec, gain_spec, col_spec, col_spec, col_spec, row_spec, gain_spec, col_spec, col_spec, row_spec)
    out_specs = (tok_spec, tok_spec, cache_spec, cache_spec)
    fours = [[0, 1, 2, 3], [4, 5, 6, 7]]
    across = [(i, i ^ 4) for i in range(n_dev)]

    def dot(a, b):
        return jnp.dot(a, b, preferred_element_type=jnp.float32)

    def per_device(prompt, lengths, new_tok, norm_attn, w_q, w_k, w_v, w_o, norm_mlp, w_gate, w_up, w_down):
        my_idx = lax.axis_index('model')
        n_batch, blk, d_model = prompt.shape
        n_tok = n_batch * blk
        seq_len = blk * n_dev
        heads = w_k.shape[2] // HEAD_DIM
        wq, wk, wv = w_q[0], w_k[0], w_v[0]
        key_pos = jnp.arange(seq_len)

        normed = lax.all_gather(rms_norm(prompt, norm_attn[0]), 'model', axis=0)
        rows = normed.reshape(n_dev * n_tok, d_model)
        pos = key_pos.reshape(n_dev, 1, blk)

        def project(w):
            return dot(rows, w).reshape(n_dev, n_batch, blk, heads, HEAD_DIM)

        def in_order(x):
            return jnp.moveaxis(x, 0, 1).reshape(n_batch, seq_len, heads, HEAD_DIM)

        q_all = in_order(rotary(project(wq), pos).astype(jnp.bfloat16))
        k_all = in_order(rotary(project(wk), pos).astype(jnp.bfloat16))
        v_all = in_order(project(wv).astype(jnp.bfloat16))
        outs = []
        for i in range(n_dev):
            seen = (i + 1) * blk
            q_pos = i * blk + jnp.arange(blk)
            visible = (key_pos[None, None, :seen] <= q_pos[None, :, None]) & (key_pos[None, None, :seen] < lengths[:, None, None])
            outs.append(attend(q_all[:, i * blk:seen], k_all[:, :seen], v_all[:, :seen], visible))
        heads_out = jnp.stack(outs)
        mine = lax.all_to_all(heads_out, 'model', split_axis=0, concat_axis=0)
        att = jnp.moveaxis(mine.reshape(n_dev, n_tok, -1), 0, 1).reshape(n_tok, -1)

        wo_full = lax.all_gather(w_o[0], 'model', axis=0, tiled=True)
        hidden = (prompt.astype(jnp.float32) + dot(att, wo_full).reshape(n_batch, blk, d_model)).astype(jnp.bfloat16)
        near = rms_norm(hidden, norm_mlp[0]).reshape(n_tok, d_model)
        wg, wu = (lax.all_gather(w[0], 'model', axis=1, tiled=True, axis_index_groups=fours) for w in (w_gate, w_up))
        wd = lax.all_gather(w_down[0], 'model', axis=0, tiled=True, axis_index_groups=fours)

        def mlp(rows):
            return dot((jax.nn.silu(dot(rows, wg)) * dot(rows, wu)).astype(jnp.bfloat16), wd)

        step = n_tok // PIECES
        theirs = [lax.ppermute(near[i:i + step], 'model', across) for i in range(0, n_tok, step)]
        other = []
        for piece in theirs:
            if other:
                piece, _ = lax.optimization_barrier((piece, other[-1][0]))
            partial = mlp(piece)
            other.append((partial, lax.ppermute(partial, 'model', across)))
        near, _ = lax.optimization_barrier((near, other[-1][0]))
        total = mlp(near) + jnp.concatenate([back for _, back in other], axis=0)
        hidden = (hidden.astype(jnp.float32) + total.reshape(n_batch, blk, d_model)).astype(jnp.bfloat16)
        seq_pos = my_idx * blk + jnp.arange(blk)
        last_sel = (seq_pos[None, :] == (lengths - 1)[:, None]).astype(jnp.bfloat16)
        last_hidden = lax.psum(jnp.einsum('bs,bsd->bd', last_sel, hidden, preferred_element_type=jnp.float32), 'model').astype(jnp.bfloat16)

        tok_norm = rms_norm(new_tok, norm_attn[0])
        q_new = rotary(dot(tok_norm, wq).reshape(n_batch, heads, HEAD_DIM), lengths).astype(jnp.bfloat16)
        k_new = rotary(dot(tok_norm, wk).reshape(n_batch, heads, HEAD_DIM), lengths).astype(jnp.bfloat16)
        v_new = dot(tok_norm, wv).astype(jnp.bfloat16).reshape(n_batch, heads, HEAD_DIM)
        k_cache = jnp.concatenate([k_all, k_new[:, None]], axis=1)
        v_cache = jnp.concatenate([v_all, v_new[:, None]], axis=1)
        cache_pos = jnp.arange(seq_len + 1)
        visible = (cache_pos[None, :] < lengths[:, None]) | (cache_pos[None, :] == seq_len)
        tok_attn = attend(q_new[:, None], k_cache, v_cache, visible[:, None])[:, 0]
        dec_hidden = (new_tok.astype(jnp.float32) + lax.psum(dot(tok_attn, w_o[0]), 'model')).astype(jnp.bfloat16)
        tok_norm = rms_norm(dec_hidden, norm_mlp[0])
        tok_mid = (jax.nn.silu(dot(tok_norm, w_gate[0])) * dot(tok_norm, w_up[0])).astype(jnp.bfloat16)
        dec_hidden = (dec_hidden.astype(jnp.float32) + lax.psum(dot(tok_mid, w_down[0]), 'model')).astype(jnp.bfloat16)
        return dec_hidden, last_hidden, k_cache[None], v_cache[None]

    return jax.shard_map(per_device, mesh=mesh, in_specs=in_specs, out_specs=out_specs, check_vma=False)
```

```python
import jax
import jax.numpy as jnp
from jax import lax
from jax.sharding import PartitionSpec as P

HEAD_DIM = 128
NEG_BIG = -1e30
PIECES = 2


def rms_norm(hidden, gain_vec):
    hid_f32 = hidden.astype(jnp.float32)
    inv_rms = lax.rsqrt(jnp.mean(hid_f32 * hid_f32, axis=-1, keepdims=True) + 1e-5)
    return (hid_f32 * inv_rms * gain_vec.astype(jnp.float32)).astype(jnp.bfloat16)


def rotary(heads_f32, positions):
    half_dim = HEAD_DIM // 2
    inv_freq = 10000.0 ** (-2.0 * jnp.arange(half_dim, dtype=jnp.float32) / HEAD_DIM)
    angles = positions.astype(jnp.float32)[..., None] * inv_freq
    cos_tab = jnp.cos(angles)[..., None, :]
    sin_tab = jnp.sin(angles)[..., None, :]
    lo_half = heads_f32[..., :half_dim]
    hi_half = heads_f32[..., half_dim:]
    return jnp.concatenate([lo_half * cos_tab - hi_half * sin_tab, hi_half * cos_tab + lo_half * sin_tab], axis=-1)


def attend(queries, keys, values, visible):
    scores = jnp.einsum('bqhd,bkhd->bhqk', queries, keys, preferred_element_type=jnp.float32) * (HEAD_DIM ** -0.5)
    scores = jnp.where(visible[:, None], scores, NEG_BIG)
    top = jnp.max(scores, axis=-1, keepdims=True)
    prob = jnp.exp(scores - top)
    total = jnp.sum(prob, axis=-1)
    out = jnp.einsum('bhqk,bkhd->bqhd', prob.astype(jnp.bfloat16), values, preferred_element_type=jnp.float32)
    return (out / jnp.moveaxis(total, 1, 2)[..., None]).reshape(*queries.shape[:2], -1).astype(jnp.bfloat16)


def solution(mesh):
    n_dev = mesh.shape['model']
    seq_spec = P('replica', 'model', None)
    col_spec = P(None, None, 'model')
    row_spec = P(None, 'model', None)
    gain_spec = P(None, None)
    tok_spec = P('replica', None)
    cache_spec = P(None, 'replica', None, 'model', None)
    in_specs = (seq_spec, P('replica'), tok_spec, gain_spec, col_spec, col_spec, col_spec, row_spec, gain_spec, col_spec, col_spec, row_spec)
    out_specs = (tok_spec, tok_spec, cache_spec, cache_spec)
    fours = [[0, 1, 2, 3], [4, 5, 6, 7]]
    across = [(i, i ^ 4) for i in range(n_dev)]

    def dot(a, b):
        return jnp.dot(a, b, preferred_element_type=jnp.float32)

    def per_device(prompt, lengths, new_tok, norm_attn, w_q, w_k, w_v, w_o, norm_mlp, w_gate, w_up, w_down):
        my_idx = lax.axis_index('model')
        n_batch, blk, d_model = prompt.shape
        n_tok = n_batch * blk
        seq_len = blk * n_dev
        heads = w_k.shape[2] // HEAD_DIM
        wq, wk, wv = w_q[0], w_k[0], w_v[0]
        key_pos = jnp.arange(seq_len)

        normed = lax.all_gather(rms_norm(prompt, norm_attn[0]), 'model', axis=0)
        rows = normed.reshape(n_dev * n_tok, d_model)
        pos = key_pos.reshape(n_dev, 1, blk)

        def project(w):
            return dot(rows, w).reshape(n_dev, n_batch, blk, heads, HEAD_DIM)

        def in_order(x):
            return jnp.moveaxis(x, 0, 1).reshape(n_batch, seq_len, heads, HEAD_DIM)

        q_all = in_order(rotary(project(wq), pos).astype(jnp.bfloat16))
        k_all = in_order(rotary(project(wk), pos).astype(jnp.bfloat16))
        v_all = in_order(project(wv).astype(jnp.bfloat16))
        outs = []
        for i in range(n_dev):
            seen = (i + 1) * blk
            q_pos = i * blk + jnp.arange(blk)
            visible = (key_pos[None, None, :seen] <= q_pos[None, :, None]) & (key_pos[None, None, :seen] < lengths[:, None, None])
            outs.append(attend(q_all[:, i * blk:seen], k_all[:, :seen], v_all[:, :seen], visible))
        heads_out = jnp.stack(outs)
        mine = lax.all_to_all(heads_out, 'model', split_axis=0, concat_axis=0)
        att = jnp.moveaxis(mine.reshape(n_dev, n_tok, -1), 0, 1).reshape(n_tok, -1)

        wo_full = lax.all_gather(w_o[0], 'model', axis=0, tiled=True)
        hidden = (prompt.astype(jnp.float32) + dot(att, wo_full).reshape(n_batch, blk, d_model)).astype(jnp.bfloat16)
        near = rms_norm(hidden, norm_mlp[0]).reshape(n_tok, d_model)
        near, new_tok = lax.optimization_barrier((near, new_tok))
        wg, wu = (lax.all_gather(w[0], 'model', axis=1, tiled=True, axis_index_groups=fours) for w in (w_gate, w_up))
        wd = lax.all_gather(w_down[0], 'model', axis=0, tiled=True, axis_index_groups=fours)

        def mlp(rows):
            return dot((jax.nn.silu(dot(rows, wg)) * dot(rows, wu)).astype(jnp.bfloat16), wd)

        step = n_tok // PIECES
        theirs = [lax.ppermute(near[i:i + step], 'model', across) for i in range(0, n_tok, step)]
        other = []
        for piece in theirs:
            partial = mlp(piece)
            other.append((partial, lax.ppermute(partial, 'model', across)))
        total = mlp(near) + jnp.concatenate([back for _, back in other], axis=0)
        hidden = (hidden.astype(jnp.float32) + total.reshape(n_batch, blk, d_model)).astype(jnp.bfloat16)
        seq_pos = my_idx * blk + jnp.arange(blk)
        last_sel = (seq_pos[None, :] == (lengths - 1)[:, None]).astype(jnp.bfloat16)
        last_hidden = lax.psum(jnp.einsum('bs,bsd->bd', last_sel, hidden, preferred_element_type=jnp.float32), 'model').astype(jnp.bfloat16)

        tok_norm = rms_norm(new_tok, norm_attn[0])
        q_new = rotary(dot(tok_norm, wq).reshape(n_batch, heads, HEAD_DIM), lengths).astype(jnp.bfloat16)
        k_new = rotary(dot(tok_norm, wk).reshape(n_batch, heads, HEAD_DIM), lengths).astype(jnp.bfloat16)
        v_new = dot(tok_norm, wv).astype(jnp.bfloat16).reshape(n_batch, heads, HEAD_DIM)
        k_cache = jnp.concatenate([k_all, k_new[:, None]], axis=1)
        v_cache = jnp.concatenate([v_all, v_new[:, None]], axis=1)
        cache_pos = jnp.arange(seq_len + 1)
        visible = (cache_pos[None, :] < lengths[:, None]) | (cache_pos[None, :] == seq_len)
        tok_attn = attend(q_new[:, None], k_cache, v_cache, visible[:, None])[:, 0]
        dec_hidden = (new_tok.astype(jnp.float32) + lax.psum(dot(tok_attn, w_o[0]), 'model')).astype(jnp.bfloat16)
        tok_norm = rms_norm(dec_hidden, norm_mlp[0])
        tok_mid = (jax.nn.silu(dot(tok_norm, w_gate[0])) * dot(tok_norm, w_up[0])).astype(jnp.bfloat16)
        dec_hidden = (dec_hidden.astype(jnp.float32) + lax.psum(dot(tok_mid, w_down[0]), 'model')).astype(jnp.bfloat16)
        return dec_hidden, last_hidden, k_cache[None], v_cache[None]

    return jax.shard_map(per_device, mesh=mesh, in_specs=in_specs, out_specs=out_specs, check_vma=False)
```

```python
import functools

import jax
import jax.numpy as jnp
from jax import lax
from jax.experimental import pallas as pl
from jax.experimental.pallas import tpu as pltpu
from jax.sharding import PartitionSpec as P


HEAD_DIM = 128
NEG_BIG = -1e30
STAT_ROWS = 8
NORM_ROWS = 32
COL_TILE = 256
N_MASKS = 8
MESH = pl.DeviceIdType.MESH


def rotary_tables(positions):
    half_dim = HEAD_DIM // 2
    inv_freq = 10000.0 ** (-2.0 * jnp.arange(half_dim, dtype=jnp.float32) / HEAD_DIM)
    angles = positions.astype(jnp.float32)[..., None] * inv_freq
    cos_tab = jnp.cos(angles)
    sin_tab = jnp.sin(angles)
    return jnp.concatenate([cos_tab, cos_tab], axis=-1), jnp.concatenate([-sin_tab, sin_tab], axis=-1)


def load_kernel(*refs):
    n = len(refs) // 2
    sem = refs[-1]
    copies = [pltpu.make_async_copy(refs[i], refs[n + i], sem.at[i]) for i in range(n)]
    for copy in copies:
        copy.start()
    for copy in copies:
        copy.wait()


def keep_in_vmem(*arrays):
    return pl.pallas_call(
        load_kernel,
        out_shape=[pltpu.VMEM(arr.shape, arr.dtype) for arr in arrays],
        in_specs=[pl.BlockSpec(memory_space=pl.ANY)] * len(arrays),
        out_specs=[pl.BlockSpec(memory_space=pltpu.VMEM)] * len(arrays),
        scratch_shapes=[pltpu.SemaphoreType.DMA((len(arrays),))],
        compiler_params=pltpu.CompilerParams(vmem_limit_bytes=24 * 2 ** 20),
        name="keep",
    )(*(pltpu.with_memory_space_constraint(arr, pltpu.HBM) for arr in arrays))


def turn_kernel(w_ref, out_ref):
    out_ref[...] = w_ref[...].T


def turn_call(w_t):
    n, d = w_t.shape
    cols = 512
    return pl.pallas_call(
        turn_kernel,
        grid=(d // cols,),
        in_specs=[pl.BlockSpec((n, cols), lambda g: (0, g))],
        out_specs=pl.BlockSpec((cols, n), lambda g: (g, 0)),
        out_shape=jax.ShapeDtypeStruct((d, n), w_t.dtype),
        compiler_params=pltpu.CompilerParams(vmem_limit_bytes=12 * 2 ** 20),
        cost_estimate=pl.CostEstimate(flops=2 * d * n * 128, bytes_accessed=4 * d * n, transcendentals=0),
        name="turn",
    )(pltpu.with_memory_space_constraint(w_t, pltpu.HBM))


def norm_kernel(outs_of, x_ref, gain_ref, *refs):
    n_out = len(refs) - 3
    out_refs = refs[:n_out]
    ss_buf, n_buf, sems = refs[n_out:]
    step = pl.program_id(0)
    blk, d_model = x_ref.shape[1:]
    lanes = [slice(c * HEAD_DIM, (c + 1) * HEAD_DIM) for c in range(d_model // HEAD_DIM)]

    def copies(at_step):
        return [pltpu.make_async_copy(n_buf.at[at_step % 2, pl.ds(lo, rows)], out_refs[o].at[i], sems.at[at_step % 2, k])
                for k, (o, i, lo, rows) in enumerate(outs_of[at_step])]

    for at_step in range(2, len(outs_of)):
        @pl.when(step == at_step)
        def _():
            for copy in copies(at_step - 2):
                copy.wait()

    def square_rows(r, carry):
        rows = pl.ds(pl.multiple_of(r * NORM_ROWS, NORM_ROWS), NORM_ROWS)
        acc = [jnp.zeros((NORM_ROWS, HEAD_DIM), jnp.float32) for _ in range(2)]
        for c, lane in enumerate(lanes):
            xf = x_ref[0, rows, lane].astype(jnp.float32)
            acc[c % 2] += xf * xf
        ss_buf[rows, :] = acc[0] + acc[1]
        return carry

    lax.fori_loop(0, blk // NORM_ROWS, square_rows, 0)
    total = jnp.sum(ss_buf[...], axis=-1, keepdims=True)
    ss_buf[...] = jnp.broadcast_to(lax.rsqrt(total / d_model + 1e-5), (blk, HEAD_DIM))
    slot = lax.rem(step, 2)

    def norm_rows(r, carry):
        rows = pl.ds(pl.multiple_of(r * NORM_ROWS, NORM_ROWS), NORM_ROWS)
        inv_rms = ss_buf[rows, :]
        for lane in lanes:
            xf = x_ref[0, rows, lane].astype(jnp.float32)
            n_buf[slot, rows, lane] = (xf * inv_rms * gain_ref[:, lane].astype(jnp.float32)).astype(jnp.bfloat16)
        return carry

    lax.fori_loop(0, blk // NORM_ROWS, norm_rows, 0)
    for at_step in range(len(outs_of)):
        @pl.when(step == at_step)
        def _():
            for copy in copies(at_step):
                copy.start()
            if at_step == len(outs_of) - 1:
                for copy in copies(at_step):
                    copy.wait()
                if at_step >= 1:
                    for copy in copies(at_step - 1):
                        copy.wait()


def first_kernel(places, rows, x_hbm, gain_hbm, *refs):
    n = len(places)
    out_refs = refs[:n]
    x_buf, gain_ref, sem = refs[n:]
    d_model = x_hbm.shape[2]
    loads = [pltpu.make_async_copy(x_hbm.at[bat, pl.ds(row0, rows)], x_buf.at[i], sem.at[i]) for i, (bat, row0) in enumerate(places)]
    loads.append(pltpu.make_async_copy(gain_hbm, gain_ref, sem.at[n]))
    for load in loads:
        load.start()
    loads[n].wait()
    lanes = [slice(c * HEAD_DIM, (c + 1) * HEAD_DIM) for c in range(d_model // HEAD_DIM)]
    for i in range(n):
        loads[i].wait()

        def norm_rows(r, carry):
            at = pl.ds(pl.multiple_of(r * NORM_ROWS, NORM_ROWS), NORM_ROWS)
            acc = [jnp.zeros((NORM_ROWS, HEAD_DIM), jnp.float32) for _ in range(2)]
            for c, lane in enumerate(lanes):
                xf = x_buf[i, at, lane].astype(jnp.float32)
                acc[c % 2] += xf * xf
            inv_rms = lax.rsqrt(jnp.sum(acc[0] + acc[1], axis=-1, keepdims=True) / d_model + 1e-5)
            for lane in lanes:
                xf = x_buf[i, at, lane].astype(jnp.float32)
                out_refs[i][0, at, lane] = (xf * inv_rms * gain_ref[:, lane].astype(jnp.float32)).astype(jnp.bfloat16)
            return carry

        lax.fori_loop(0, rows // NORM_ROWS, norm_rows, 0)


def first_call(x, gain, places, rows):
    d_model = x.shape[2]
    return pl.pallas_call(
        functools.partial(first_kernel, places, rows),
        out_shape=[pltpu.VMEM((1, rows, d_model), jnp.bfloat16)] * len(places),
        in_specs=[pl.BlockSpec(memory_space=pl.ANY)] * 2,
        out_specs=[pl.BlockSpec(memory_space=pltpu.VMEM)] * len(places),
        scratch_shapes=[
            pltpu.VMEM((len(places), rows, d_model), jnp.bfloat16),
            pltpu.VMEM(gain.shape, gain.dtype),
            pltpu.SemaphoreType.DMA((len(places) + 1,)),
        ],
        compiler_params=pltpu.CompilerParams(vmem_limit_bytes=8 * 2 ** 20),
        cost_estimate=pl.CostEstimate(flops=len(places) * rows * d_model * 8, bytes_accessed=len(places) * rows * d_model * 4, transcendentals=0),
        name="first_rows",
    )(*(pltpu.with_memory_space_constraint(a, pltpu.HBM) for a in (x, gain)))


def norm_call(x, gain, order, outs_of, shapes, blk=None, row_block=0):
    d_model = x.shape[2]
    blk = blk or x.shape[1]

    def prompt_of(g):
        idx = jnp.int32(order[-1])
        for k in range(len(order) - 1):
            idx = jnp.where(g == k, order[k], idx)
        return idx

    return pl.pallas_call(
        functools.partial(norm_kernel, outs_of),
        grid=(len(order),),
        in_specs=[pl.BlockSpec((1, blk, d_model), lambda g: (prompt_of(g), row_block, 0)),
                  pl.BlockSpec((1, d_model), lambda g: (0, 0))],
        out_specs=[pl.BlockSpec(memory_space=pl.ANY)] * len(shapes),
        out_shape=[jax.ShapeDtypeStruct((*shape, d_model), jnp.bfloat16) for shape in shapes],
        scratch_shapes=[
            pltpu.VMEM((blk, HEAD_DIM), jnp.float32),
            pltpu.VMEM((2, blk, d_model), jnp.bfloat16),
            pltpu.SemaphoreType.DMA((2, max(len(o) for o in outs_of))),
        ],
        compiler_params=pltpu.CompilerParams(vmem_limit_bytes=24 * 2 ** 20),
        cost_estimate=pl.CostEstimate(flops=len(order) * blk * d_model * 8, bytes_accessed=len(order) * blk * d_model * 6, transcendentals=0),
        name="norm_rows",
    )(pltpu.with_memory_space_constraint(x, pltpu.HBM), gain)


def rows_kernel(new_ref, last_ref, gain_ref, cos_ref, sin_ref, wq_hbm, wk, wv, q_ref, k_ref, v_ref, st_ref, wq, q_buf, sem):
    load = pltpu.make_async_copy(wq_hbm, wq, sem)
    load.start()
    n_batch = new_ref.shape[0]
    heads = wk.shape[1] // HEAD_DIM
    xf = jnp.concatenate([new_ref[...].astype(jnp.float32), last_ref[...].astype(jnp.float32)], axis=0)
    inv_rms = lax.rsqrt(jnp.mean(xf * xf, axis=-1, keepdims=True) + 1e-5)
    normed = (xf * inv_rms * gain_ref[...].astype(jnp.float32)).astype(jnp.bfloat16)
    k_all = jnp.dot(normed, wk[...], preferred_element_type=jnp.float32)[:n_batch]
    v_all = jnp.dot(normed, wv[...], preferred_element_type=jnp.float32)[:n_batch].astype(jnp.bfloat16)
    load.wait()
    q_all = jnp.dot(normed, wq[...], preferred_element_type=jnp.float32)
    q_buf[...] = jnp.zeros_like(q_buf)
    k_rot = []
    for h in range(heads):
        cols = slice(h * HEAD_DIM, (h + 1) * HEAD_DIM)
        qh = q_all[:, cols]
        qh = (qh * cos_ref[...] + pltpu.roll(qh, HEAD_DIM // 2, 1) * sin_ref[...]).astype(jnp.bfloat16).astype(jnp.float32)
        kh = k_all[:, cols]
        kh = (kh * cos_ref[:n_batch, :] + pltpu.roll(kh, HEAD_DIM // 2, 1) * sin_ref[:n_batch, :]).astype(jnp.bfloat16)
        k_rot.append(kh)
        score = jnp.sum(qh[:n_batch] * kh.astype(jnp.float32), axis=-1, keepdims=True) * (HEAD_DIM ** -0.5)
        zero = jnp.zeros((n_batch, HEAD_DIM), jnp.float32)
        for t in range(2):
            row = 2 * h + t
            q_buf[:, row, cols] = qh[t * n_batch:(t + 1) * n_batch]
            st_ref[0, :, row, :] = v_all[:, cols].astype(jnp.float32) if t == 0 else zero
            st_ref[1, :, row, :] = zero + score if t == 0 else zero + NEG_BIG
            st_ref[2, :, row, :] = zero + 1.0 if t == 0 else zero
    q_ref[...] = q_buf[...].astype(jnp.bfloat16)
    k_ref[...] = jnp.concatenate(k_rot, axis=1).reshape(n_batch, heads, HEAD_DIM)
    v_ref[...] = v_all.reshape(n_batch, heads, HEAD_DIM)


def rows_call(new_tok, last_x, gain, row_tabs, w_q, w_k, w_v):
    n_batch = new_tok.shape[0]
    width = w_q.shape[1]
    heads = width // HEAD_DIM
    vmem = pl.BlockSpec(memory_space=pltpu.VMEM)
    return pl.pallas_call(
        rows_kernel,
        out_shape=[
            jax.ShapeDtypeStruct((n_batch, STAT_ROWS, width), jnp.bfloat16),
            jax.ShapeDtypeStruct((n_batch, heads, HEAD_DIM), jnp.bfloat16),
            jax.ShapeDtypeStruct((n_batch, heads, HEAD_DIM), jnp.bfloat16),
            jax.ShapeDtypeStruct((3, n_batch, STAT_ROWS, HEAD_DIM), jnp.float32),
        ],
        in_specs=[vmem] * 5 + [pl.BlockSpec(memory_space=pl.ANY)] + [vmem] * 2,
        out_specs=[vmem] * 4,
        scratch_shapes=[
            pltpu.VMEM(w_q.shape, jnp.bfloat16),
            pltpu.VMEM((n_batch, STAT_ROWS, width), jnp.float32),
            pltpu.SemaphoreType.DMA,
        ],
        compiler_params=pltpu.CompilerParams(vmem_limit_bytes=24 * 2 ** 20),
        cost_estimate=pl.CostEstimate(flops=2 * 2 * n_batch * 3 * w_q.shape[0] * width, bytes_accessed=2 * w_q.size, transcendentals=0),
        name="query_rows",
    )(new_tok, last_x, gain, *row_tabs, pltpu.with_memory_space_constraint(w_q, pltpu.HBM), w_k, w_v)


def by_group(group, values):
    out = values[-1]
    for p in range(len(values) - 1):
        out = jnp.where(group == p, values[p], out)
    return out


def kv_kernel(n_in, masks, batches, firsts, row0, stat_of, with_new, sc_ref, *refs):
    n_groups = len(masks)
    n_arr = n_in * n_groups
    x_refs = refs[:n_arr]
    cos_ref, sin_ref, wk, wv, q_ref = refs[n_arr:n_arr + 5]
    rest = refs[n_arr + 5:]
    if with_new:
        new_refs = rest[:2]
        rest = rest[2:]
    else:
        rest = rest[3:]
    kc_ref, vc_ref, st_ref, x_buf, k_buf, v_buf, k_out, v_out, s_out, x_sem, sems, s_sem, new_sem = rest
    step = pl.program_id(0)
    n_steps = pl.num_programs(0)
    slot = lax.rem(step, 2)
    per_group = n_steps // n_groups
    blk = x_buf.shape[2]
    shard_rows = cos_ref.shape[1]
    width = wk.shape[1]
    heads = width // HEAD_DIM
    n_tok = n_in * blk

    def x_copies(at_step, which, group):
        local = at_step - group * per_group
        return [pltpu.make_async_copy(x_refs[group * n_in + i].at[firsts[group][i] + local],
                                      x_buf.at[which, i], x_sem.at[which, i]) for i in range(n_in)]

    def start_x(at_step, which):
        for group in range(n_groups):
            @pl.when(at_step // per_group == group)
            def _(group=group):
                for copy in x_copies(at_step, which, group):
                    copy.start()

    def place(i, at_step):
        group = at_step // per_group
        mask = by_group(group, [m[i] for m in masks])
        return sc_ref[mask], by_group(group, [b[i] for b in batches]) + lax.rem(at_step, per_group), mask

    def out_copies(which, at_step):
        copies = []
        for i in range(n_in):
            shard, bat, _ = place(i, at_step)
            rows = pl.ds(shard * shard_rows + row0, blk)
            copies.append(pltpu.make_async_copy(k_out.at[which, i], kc_ref.at[bat, rows], sems.at[which, i, 0]))
            copies.append(pltpu.make_async_copy(v_out.at[which, i], vc_ref.at[bat, rows], sems.at[which, i, 1]))
        return copies

    def new_copies():
        return [pltpu.make_async_copy(src.at[pl.ds(b, 1)], dst.at[b, pl.ds(dst.shape[1] - 1, 1)], new_sem.at[idx, b])
                for idx, (src, dst) in enumerate(zip(new_refs, (kc_ref, vc_ref))) for b in range(src.shape[0])]

    @pl.when(step == 0)
    def _():
        start_x(step, slot)
        if with_new:
            for copy in new_copies():
                copy.start()

    @pl.when(step + 1 < n_steps)
    def _():
        start_x(step + 1, 1 - slot)

    @pl.when(step >= 2)
    def _():
        for copy in out_copies(slot, step - 2):
            copy.wait()

    for copy in x_copies(0, slot, 0):
        copy.wait()
    x_rows = x_buf.at[slot]

    def col_tile(c, carry):
        cols = pl.ds(pl.multiple_of(c * COL_TILE, COL_TILE), COL_TILE)
        normed = x_rows[...].reshape(n_tok, x_buf.shape[3])
        kf = jnp.dot(normed, wk[:, cols], preferred_element_type=jnp.float32)
        vf = jnp.dot(normed, wv[:, cols], preferred_element_type=jnp.float32)
        v_buf[:, cols] = vf.astype(jnp.bfloat16)
        parts = []
        for i in range(n_in):
            shard = place(i, step)[0]
            cos_tab = cos_ref[shard, row0:row0 + blk]
            sin_tab = sin_ref[shard, row0:row0 + blk]
            halves = []
            for h in range(COL_TILE // HEAD_DIM):
                kh = kf[i * blk:(i + 1) * blk, h * HEAD_DIM:(h + 1) * HEAD_DIM]
                halves.append(kh * cos_tab + pltpu.roll(kh, HEAD_DIM // 2, 1) * sin_tab)
            parts.append(jnp.concatenate(halves, axis=1))
        k_buf[:, cols] = jnp.concatenate(parts, axis=0).astype(jnp.bfloat16)
        return carry

    lax.fori_loop(0, width // COL_TILE, col_tile, 0)

    for i in range(n_in):
        k_out[slot, i] = k_buf[i * blk:(i + 1) * blk, :].reshape(blk, heads, HEAD_DIM)
        v_out[slot, i] = v_buf[i * blk:(i + 1) * blk, :].reshape(blk, heads, HEAD_DIM)
    for copy in out_copies(slot, step):
        copy.start()

    head_of_row = lax.broadcasted_iota(jnp.int32, (STAT_ROWS, HEAD_DIM), 0) // (STAT_ROWS // heads)
    probs = []
    for i in range(n_in):
        shard, bat, _ = place(i, step)
        scores = lax.dot_general(q_ref[bat], k_buf[i * blk:(i + 1) * blk, :], (((1,), (1,)), ((), ())),
                                 preferred_element_type=jnp.float32) * (HEAD_DIM ** -0.5)
        pos = shard * shard_rows + row0 + lax.broadcasted_iota(jnp.int32, scores.shape, 1)
        visible = pos < sc_ref[N_MASKS + bat]
        scores = jnp.where(visible, scores, NEG_BIG)
        blk_max = jnp.max(scores, axis=-1, keepdims=True)
        prob = jnp.where(visible, jnp.exp(scores - blk_max), 0.0)
        probs.append((blk_max, prob))
    for i, (blk_max, prob) in enumerate(probs):
        full = jnp.dot(prob.astype(jnp.bfloat16), v_buf[i * blk:(i + 1) * blk, :], preferred_element_type=jnp.float32)
        acc = jnp.zeros((STAT_ROWS, HEAD_DIM), jnp.float32)
        for h in range(heads):
            acc = jnp.where(head_of_row == h, full[:, h * HEAD_DIM:(h + 1) * HEAD_DIM], acc)
        s_out[i, 0] = acc
        s_out[i, 1] = jnp.broadcast_to(blk_max, (STAT_ROWS, HEAD_DIM))
        s_out[i, 2] = jnp.broadcast_to(jnp.sum(prob, axis=-1, keepdims=True), (STAT_ROWS, HEAD_DIM))
    stat_copies = []
    for i in range(n_in):
        _, bat, mask = place(i, step)
        stat_copies.append(pltpu.make_async_copy(s_out.at[i], st_ref.at[mask + stat_of, bat], s_sem.at[i]))
        stat_copies[-1].start()
    for copy in stat_copies:
        copy.wait()

    @pl.when(step == n_steps - 1)
    def _():
        for copy in out_copies(slot, step):
            copy.wait()
        if with_new:
            for copy in new_copies():
                copy.wait()

    @pl.when((step == n_steps - 1) & (n_steps >= 2))
    def _():
        for copy in out_copies(1 - slot, step - 1):
            copy.wait()


def kv_call(groups, per_group, masks, batches, scalars, tabs, w_k, w_v, q_diag, caches, new_rows=None, row0=0, stat_of=0):
    n_groups = len(groups)
    n_in = len(groups[0])
    n_steps = n_groups * per_group
    cos_tab, sin_tab = tabs
    blk, d_model = groups[0][0][0].shape[1:]
    width = w_k.shape[1]
    heads = width // HEAD_DIM
    any_spec = pl.BlockSpec(memory_space=pl.ANY)
    operands = [arr for group in groups for arr, _ in group]
    in_specs = [any_spec] * len(operands) + [pl.BlockSpec(memory_space=pltpu.VMEM)] * 5
    operands += [cos_tab, sin_tab, w_k, w_v, q_diag]
    with_new = new_rows is not None
    if with_new:
        operands += new_rows
        in_specs += [any_spec] * 2
        aliases = {}
    else:
        operands += [*caches[:2], pltpu.with_memory_space_constraint(caches[2], pltpu.VMEM)]
        in_specs += [any_spec] * 3
        aliases = {len(operands) - 2: 0, len(operands) - 1: 1, len(operands): 2}
    tokens = n_in * blk
    n_batch = q_diag.shape[0]
    return pl.pallas_call(
        functools.partial(kv_kernel, n_in, masks, batches, [[first for _, first in group] for group in groups], row0, stat_of, with_new),
        grid_spec=pltpu.PrefetchScalarGridSpec(
            num_scalar_prefetch=1,
            grid=(n_steps,),
            in_specs=in_specs,
            out_specs=[any_spec] * 3,
            scratch_shapes=[
                pltpu.VMEM((2, n_in, blk, d_model), jnp.bfloat16),
                pltpu.VMEM((tokens, width), jnp.bfloat16),
                pltpu.VMEM((tokens, width), jnp.bfloat16),
                pltpu.VMEM((2, n_in, blk, heads, HEAD_DIM), jnp.bfloat16),
                pltpu.VMEM((2, n_in, blk, heads, HEAD_DIM), jnp.bfloat16),
                pltpu.VMEM((n_in, 3, STAT_ROWS, HEAD_DIM), jnp.float32),
                pltpu.SemaphoreType.DMA((2, n_in)),
                pltpu.SemaphoreType.DMA((2, n_in, 2)),
                pltpu.SemaphoreType.DMA((n_in,)),
                pltpu.SemaphoreType.DMA((2, n_batch)),
            ],
        ),
        out_shape=[*(jax.ShapeDtypeStruct(c.shape, c.dtype) for c in caches[:2]), pltpu.VMEM(caches[2].shape, caches[2].dtype)],
        input_output_aliases=aliases,
        compiler_params=pltpu.CompilerParams(vmem_limit_bytes=20 * 2 ** 20),
        cost_estimate=pl.CostEstimate(flops=4 * n_steps * tokens * d_model * width, bytes_accessed=2 * n_steps * tokens * (d_model + 2 * width), transcendentals=0),
        name="kv_chunk",
    )(scalars, *operands)


def tail_kernel(n_dev, parts_of, stv, self_ref, xs_ref, gain_ref, wo, wg_hbm, wu_hbm, wd_hbm, out_ref,
                wg, wu, wd, rows, a_buf, n_buf, ps1, pr1, ps2, pr2, xo1, xg1, xo2, xg2, w_sem, send_sem, recv_sem):
    me = lax.axis_index("model")
    n_batch = out_ref.shape[1]
    n_rows = 2 * n_batch
    d_model = out_ref.shape[2]
    cols = d_model // n_dev
    heads = STAT_ROWS // 2
    loads = [pltpu.make_async_copy(src, dst, w_sem.at[i]) for i, (src, dst) in enumerate(((wg_hbm, wg), (wu_hbm, wu), (wd_hbm, wd)))]
    for load in loads:
        load.start()
    barrier = pltpu.get_barrier_semaphore()

    def peer_of(mask):
        return sum(lax.rem(me // bit + mask // bit, 2) * bit for bit in (1, 2, 4))

    far_first = ((6, 7), (2, 3, 4, 5), (1,))
    for mask in sum(far_first, ()):
        pl.semaphore_signal(barrier, inc=1, device_id={"model": peer_of(mask)}, device_id_type=MESH)

    def send(phase, mask, src, dst):
        return pltpu.make_async_remote_copy(
            src_ref=src, dst_ref=dst, send_sem=send_sem.at[phase, mask - 1], recv_sem=recv_sem.at[phase, mask - 1],
            device_id={"model": peer_of(mask)}, device_id_type=MESH)

    for b in range(n_batch):
        top = self_ref[1, b]
        for j in range(parts_of[b]):
            top = jnp.maximum(top, stv[j, b, 1])
        scale = jnp.exp(self_ref[1, b] - top)
        den = scale * self_ref[2, b]
        num = scale * self_ref[0, b]
        for j in range(parts_of[b]):
            scale = jnp.exp(stv[j, b, 1] - top)
            den += scale * stv[j, b, 2]
            num += scale * stv[j, b, 0]
        rows[:, b, :] = num / den
    for h in range(heads):
        for t in range(2):
            a_buf[t * n_batch:(t + 1) * n_batch, h * HEAD_DIM:(h + 1) * HEAD_DIM] = rows[2 * h + t]
    att = a_buf[...].astype(jnp.bfloat16)

    def exchange(phase, base, copies, pr, xo, xg):
        total = base
        for copy, mask in reversed(copies):
            copy.wait_recv()
            total = total + pr[mask - 1]
        xo[...] = total.astype(jnp.bfloat16)
        xg[me] = xo[...]
        outs = []
        for mask in sum(far_first, ()):
            outs.append(send(phase + 1, mask, xo, xg.at[me]))
            outs[-1].start()
        for out in outs:
            out.wait_recv()
        return [copy for copy, _ in copies] + outs

    def col_block(p):
        return pl.ds(pl.multiple_of(p * cols, cols), cols)

    part = jnp.dot(att, wo[...], preferred_element_type=jnp.float32)
    for j in range(n_dev):
        ps1[j] = part[:, j * cols:(j + 1) * cols]
    pl.semaphore_wait(barrier, n_dev - 1)
    copies = []
    for mask in sum(far_first, ()):
        copies.append((send(0, mask, ps1.at[peer_of(mask)], pr1.at[mask - 1]), mask))
        copies[-1][0].start()
    sent = exchange(0, xs_ref[...].astype(jnp.float32) + ps1[me], copies, pr1, xo1, xg1)
    sq = jnp.zeros((n_rows, 1), jnp.float32)
    for j in range(n_dev):
        xf = xg1[j].astype(jnp.float32)
        sq += jnp.sum(xf * xf, axis=-1, keepdims=True)
    inv_rms = lax.rsqrt(sq / d_model + 1e-5)
    for j in range(n_dev):
        at = slice(j * cols, (j + 1) * cols)
        n_buf[:, at] = (xg1[j].astype(jnp.float32) * inv_rms * gain_ref[:, at].astype(jnp.float32)).astype(jnp.bfloat16)
    loads[0].wait()
    loads[1].wait()
    gate = jnp.dot(n_buf[...], wg[...], preferred_element_type=jnp.float32)
    up = jnp.dot(n_buf[...], wu[...], preferred_element_type=jnp.float32)
    mid = (gate * (1.0 / (1.0 + jnp.exp(-gate))) * up).astype(jnp.bfloat16)
    loads[2].wait()
    copies = []
    for group in far_first:
        for mask in group:
            ps2[mask] = jnp.dot(mid, wd[:, col_block(peer_of(mask))], preferred_element_type=jnp.float32)
        if group == far_first[-1]:
            ps2[0] = jnp.dot(mid, wd[:, col_block(me)], preferred_element_type=jnp.float32)
        for mask in group:
            copies.append((send(2, mask, ps2.at[mask], pr2.at[mask - 1]), mask))
            copies[-1][0].start()
    sent += exchange(2, xo1[...].astype(jnp.float32) + ps2[0], copies, pr2, xo2, xg2)
    for j in range(n_dev):
        at = slice(j * cols, (j + 1) * cols)
        out_ref[0, :, at] = xg2[j, :n_batch]
        out_ref[1, :, at] = xg2[j, n_batch:]
    for copy in sent:
        copy.wait_send()


def tail_call(n_dev, parts_of, stats, self_stat, x_mine, gain, w_o, w_gate, w_up, w_down, n_batch):
    n_rows, cols = x_mine.shape
    d_model = w_o.shape[1]
    vmem = pl.BlockSpec(memory_space=pltpu.VMEM)
    any_spec = pl.BlockSpec(memory_space=pl.ANY)
    exchanged = [pltpu.VMEM((n_dev, n_rows, cols), jnp.float32), pltpu.VMEM((n_dev - 1, n_rows, cols), jnp.float32)]
    summed = [pltpu.VMEM((n_rows, cols), jnp.bfloat16), pltpu.VMEM((n_dev, n_rows, cols), jnp.bfloat16)]
    return pl.pallas_call(
        functools.partial(tail_kernel, n_dev, parts_of),
        out_shape=jax.ShapeDtypeStruct((2, n_batch, d_model), jnp.bfloat16),
        in_specs=[vmem] * 5 + [any_spec] * 3,
        out_specs=vmem,
        scratch_shapes=[
            pltpu.VMEM(w_gate.shape, jnp.bfloat16),
            pltpu.VMEM(w_up.shape, jnp.bfloat16),
            pltpu.VMEM(w_down.shape, jnp.bfloat16),
            pltpu.VMEM((STAT_ROWS, n_batch, HEAD_DIM), jnp.float32),
            pltpu.VMEM((n_rows, w_o.shape[0]), jnp.float32),
            pltpu.VMEM((n_rows, d_model), jnp.bfloat16),
            *exchanged, *exchanged, *summed, *summed,
            pltpu.SemaphoreType.DMA((3,)),
            pltpu.SemaphoreType.DMA((4, n_dev - 1)),
            pltpu.SemaphoreType.DMA((4, n_dev - 1)),
        ],
        compiler_params=pltpu.CompilerParams(collective_id=0, has_side_effects=True, vmem_limit_bytes=46 * 2 ** 20),
        name="tail",
    )(pltpu.with_memory_space_constraint(stats, pltpu.VMEM), self_stat, x_mine, gain, w_o,
      *(pltpu.with_memory_space_constraint(w, pltpu.HBM) for w in (w_gate, w_up, w_down)))


def solution(mesh):
    n_dev = mesh.shape['model']
    seq_spec = P('replica', 'model', None)
    col_spec = P(None, None, 'model')
    row_spec = P(None, 'model', None)
    gain_spec = P(None, None)
    tok_spec = P('replica', None)
    cache_spec = P(None, 'replica', None, 'model', None)
    in_specs = (seq_spec, P('replica'), tok_spec, gain_spec, col_spec, col_spec, col_spec, row_spec, gain_spec, col_spec, col_spec, row_spec)
    out_specs = (tok_spec, tok_spec, cache_spec, cache_spec)

    def swap(arr, bit):
        return lax.ppermute(arr, 'model', [(i, i ^ bit) for i in range(n_dev)])

    def per_device(prompt, lengths, new_tok, norm_attn, w_q, w_k, w_v, w_o, norm_mlp, w_gate, w_up, w_down):
        my_idx = lax.axis_index('model')
        n_batch, blk, d_model = prompt.shape
        seq_len = blk * n_dev
        width = w_k.shape[2]
        heads = width // HEAD_DIM
        half = n_batch // 2
        wq = w_q[0]
        gain = norm_attn

        q1, q2, rows_h = 1, n_batch // 4, blk // 2
        a_parts, b_parts = {}, {}
        for h, name in enumerate(("0a", "0b")):
            a_parts[name], b_parts[name] = first_call(prompt, norm_attn, [(0, h * rows_h), (half, h * rows_h)], rows_h)
        from_y, from_x = {}, {}

        def send_part(step, along_y, along_x):
            from_y[step] = swap(along_y, 4)
            from_x[step] = swap(along_x, 2)

        send_part("0a", a_parts["0a"], b_parts["0a"])
        send_part("0b", a_parts["0b"], b_parts["0b"])
        order, outs_of = [], []
        for part, (lo, hi) in ((1, (q1, q2)), (2, (q2, half)), (0, (0, q1))):
            for k in range(lo, hi):
                for side in range(2):
                    order.append(side * half + k)
                    outs_of.append([(4, side * half + k, 0, blk)] + ([(2 * part - 2 + side, k - lo, 0, blk)] if part else []))
        a_parts["1"], b_parts["1"], a_parts["2"], b_parts["2"], normed = norm_call(
            prompt, gain, order, outs_of, [(q2 - q1, blk)] * 2 + [(half - q2, blk)] * 2 + [(n_batch, blk)])
        send_part("1", a_parts["1"], b_parts["1"])
        seq_pos = my_idx * blk + jnp.arange(blk)
        sel = (seq_pos[None, :] == (lengths - 1)[:, None]).astype(jnp.bfloat16)
        last_x = jnp.einsum('bs,bsd->bd', sel, prompt, preferred_element_type=jnp.float32).astype(jnp.bfloat16)
        core, cols_h = my_idx % 2, d_model // 2
        last_x = last_x + swap(last_x, 1)
        last_x = lax.dynamic_slice_in_dim(last_x, core * cols_h, cols_h, axis=1)
        last_x = (last_x + swap(last_x, 2)) + (swap(last_x, 4) + swap(last_x, 6))
        other_x = swap(last_x, 1)
        last_x = jnp.where(core == 0, jnp.concatenate([last_x, other_x], axis=1), jnp.concatenate([other_x, last_x], axis=1))
        send_part("2", a_parts["2"], b_parts["2"])
        send_part("3", b_parts["2"], a_parts["2"])
        send_part("4", normed[half:half + q2], normed[:q2])
        core_all = swap(normed, 1)

        bits = jnp.arange(N_MASKS)
        scalars = jnp.concatenate([sum(((my_idx // bit + bits // bit) % 2) * bit for bit in (1, 2, 4)), lengths]).astype(jnp.int32)
        row_tabs = rotary_tables(jnp.concatenate([lengths, lengths - 1]))
        tabs = tuple(tab.reshape(n_dev, blk, HEAD_DIM) for tab in rotary_tables(jnp.arange(seq_len)))
        x_rows = jnp.concatenate([new_tok, last_x], axis=0)
        x_mine = lax.dynamic_slice_in_dim(x_rows, my_idx * (d_model // n_dev), d_model // n_dev, axis=1)
        wk, wv, wo, last_x, scalars, row_tabs, tabs, x_mine = lax.optimization_barrier(
            (w_k[0], w_v[0], w_o[0], last_x, scalars, row_tabs, tabs, x_mine))
        wk, wv, wo = keep_in_vmem(wk, wv, wo)
        q_diag, k_new, v_new, self_stat = rows_call(new_tok, last_x, gain, row_tabs, wq, wk, wv)
        cache_shape = jax.ShapeDtypeStruct((n_batch, seq_len + 1, heads, HEAD_DIM), jnp.bfloat16)
        caches = [cache_shape, cache_shape, jax.ShapeDtypeStruct((2 * n_dev - 2, n_batch, 3, STAT_ROWS, HEAD_DIM), jnp.float32)]

        def run(groups, per_group, masks, batches, caches, **kw):
            return kv_call(groups, per_group, masks, batches, scalars, tabs, wk, wv, q_diag, caches, **kw)

        def half_rows(step):
            return {"row0": rows_h * (step == "0b"), "stat_of": (n_dev - 2) * (step == "0b")}

        def after(caches, *arrays):
            out = lax.optimization_barrier((caches[2], *arrays))
            return [caches[0], caches[1], out[0]], out[1:]

        caches = run([[(arr, 0), (arr, half)] for arr in (normed, core_all)], half,
                     [[0] * 2, [1] * 2], [[0, half]] * 2, caches, new_rows=[k_new, v_new])
        diag, turned = {}, {}
        starts = {"0a": (0, half), "0b": (0, half), "1": (q1, half + q1), "2": (q2, half + q2), "3": (half + q2, q2), "4": (half, 0)}
        for step, start in starts.items():
            caches, (got_y, got_x) = after(caches, from_y[step], from_x[step])
            other_y, other_x = swap(got_y, 1), swap(got_x, 1)
            if step not in "34":
                diag[step] = (swap(got_y, 2), swap(got_x, 4))
            streams = [[(got_y, 0), (got_x, 0)], [(other_y, 0), (other_x, 0)]]
            if step in ("0a", "0b"):
                caches = run([streams[0] + streams[1]], q1, [[4, 2, 5, 3]], [[*start, *start]], caches, **half_rows(step))
            else:
                caches = run(streams, got_y.shape[0], [[4, 2], [5, 3]], [list(start)] * 2, caches)
            if step in "34":
                caches, (w_t,) = after(caches, (w_gate if step == "3" else w_up)[0].T)
                turned[step] = turn_call(w_t)
                caches, (turned[step],) = after(caches, turned[step])
        for step in ("2", "1", "0a", "0b"):
            caches, (via_x, via_y) = after(caches, *diag[step])
            other_x, other_y = swap(via_x, 1), swap(via_y, 1)
            start = starts[step]
            streams = [[(via_x, 0), (via_y, 0)], [(other_x, 0), (other_y, 0)]]
            if step in ("0a", "0b"):
                caches = run([streams[0] + streams[1]], q1, [[6, 6, 7, 7]], [[*start, *start]], caches, **half_rows(step))
            else:
                caches = run(streams, via_x.shape[0], [[6] * 2, [7] * 2], [list(start)] * 2, caches)

        k_cache, v_cache, stats = caches
        parts_of = [2 * n_dev - 2 if b % half < q1 else n_dev for b in range(n_batch)]
        both = tail_call(n_dev, parts_of, stats, self_stat, x_mine, norm_mlp, wo, turned["3"], turned["4"], w_down[0], n_batch)
        return both[0], both[1], k_cache[None], v_cache[None]

    return jax.shard_map(per_device, mesh=mesh, in_specs=in_specs, out_specs=out_specs, check_vma=False)
```

```python
import functools

import jax
import jax.numpy as jnp
from jax import lax
from jax.experimental import pallas as pl
from jax.experimental.pallas import tpu as pltpu
from jax.sharding import PartitionSpec as P


HEAD_DIM = 128
NEG_BIG = -1e30
STAT_ROWS = 8
NORM_ROWS = 32
COL_TILE = 256
MESH = pl.DeviceIdType.MESH


def rotary_tables(positions):
    half_dim = HEAD_DIM // 2
    inv_freq = 10000.0 ** (-2.0 * jnp.arange(half_dim, dtype=jnp.float32) / HEAD_DIM)
    angles = positions.astype(jnp.float32)[..., None] * inv_freq
    cos_tab = jnp.cos(angles)
    sin_tab = jnp.sin(angles)
    return jnp.concatenate([cos_tab, cos_tab], axis=-1), jnp.concatenate([-sin_tab, sin_tab], axis=-1)


def load_kernel(*refs):
    n = len(refs) // 2
    sem = refs[-1]
    copies = [pltpu.make_async_copy(refs[i], refs[n + i], sem.at[i]) for i in range(n)]
    for copy in copies:
        copy.start()
    for copy in copies:
        copy.wait()


def keep_in_vmem(*arrays):
    return pl.pallas_call(
        load_kernel,
        out_shape=[pltpu.VMEM(arr.shape, arr.dtype) for arr in arrays],
        in_specs=[pl.BlockSpec(memory_space=pl.ANY)] * len(arrays),
        out_specs=[pl.BlockSpec(memory_space=pltpu.VMEM)] * len(arrays),
        scratch_shapes=[pltpu.SemaphoreType.DMA((len(arrays),))],
        compiler_params=pltpu.CompilerParams(vmem_limit_bytes=24 * 2 ** 20),
        name="keep",
    )(*(pltpu.with_memory_space_constraint(arr, pltpu.HBM) for arr in arrays))


def turn_kernel(w_ref, out_ref):
    out_ref[...] = w_ref[...].T


def turn_call(w_t):
    n, d = w_t.shape
    cols = 512
    return pl.pallas_call(
        turn_kernel,
        grid=(d // cols,),
        in_specs=[pl.BlockSpec((n, cols), lambda g: (0, g))],
        out_specs=pl.BlockSpec((cols, n), lambda g: (g, 0)),
        out_shape=jax.ShapeDtypeStruct((d, n), w_t.dtype),
        compiler_params=pltpu.CompilerParams(vmem_limit_bytes=12 * 2 ** 20),
        cost_estimate=pl.CostEstimate(flops=2 * d * n * 128, bytes_accessed=4 * d * n, transcendentals=0),
        name="turn",
    )(pltpu.with_memory_space_constraint(w_t, pltpu.HBM))


def norm_kernel(outs_of, x_ref, gain_ref, *refs):
    n_out = len(refs) - 3
    out_refs = refs[:n_out]
    ss_buf, n_buf, sems = refs[n_out:]
    step = pl.program_id(0)
    blk, d_model = x_ref.shape[1:]
    lanes = [slice(c * HEAD_DIM, (c + 1) * HEAD_DIM) for c in range(d_model // HEAD_DIM)]

    def copies(at_step):
        return [pltpu.make_async_copy(n_buf.at[at_step % 2, pl.ds(lo, rows)], out_refs[o].at[i], sems.at[at_step % 2, k])
                for k, (o, i, lo, rows) in enumerate(outs_of[at_step])]

    for at_step in range(2, len(outs_of)):
        @pl.when(step == at_step)
        def _():
            for copy in copies(at_step - 2):
                copy.wait()

    def square_rows(r, carry):
        rows = pl.ds(pl.multiple_of(r * NORM_ROWS, NORM_ROWS), NORM_ROWS)
        acc = [jnp.zeros((NORM_ROWS, HEAD_DIM), jnp.float32) for _ in range(2)]
        for c, lane in enumerate(lanes):
            xf = x_ref[0, rows, lane].astype(jnp.float32)
            acc[c % 2] += xf * xf
        ss_buf[rows, :] = acc[0] + acc[1]
        return carry

    lax.fori_loop(0, blk // NORM_ROWS, square_rows, 0)
    total = jnp.sum(ss_buf[...], axis=-1, keepdims=True)
    ss_buf[...] = jnp.broadcast_to(lax.rsqrt(total / d_model + 1e-5), (blk, HEAD_DIM))
    slot = lax.rem(step, 2)

    def norm_rows(r, carry):
        rows = pl.ds(pl.multiple_of(r * NORM_ROWS, NORM_ROWS), NORM_ROWS)
        inv_rms = ss_buf[rows, :]
        for lane in lanes:
            xf = x_ref[0, rows, lane].astype(jnp.float32)
            n_buf[slot, rows, lane] = (xf * inv_rms * gain_ref[:, lane].astype(jnp.float32)).astype(jnp.bfloat16)
        return carry

    lax.fori_loop(0, blk // NORM_ROWS, norm_rows, 0)
    for at_step in range(len(outs_of)):
        @pl.when(step == at_step)
        def _():
            for copy in copies(at_step):
                copy.start()
            if at_step == len(outs_of) - 1:
                for copy in copies(at_step):
                    copy.wait()
                if at_step >= 1:
                    for copy in copies(at_step - 1):
                        copy.wait()


def first_kernel(places, rows, x_hbm, gain_hbm, *refs):
    n = len(places)
    out_refs = refs[:n]
    x_buf, gain_ref, sem = refs[n:]
    d_model = x_hbm.shape[2]
    loads = [pltpu.make_async_copy(x_hbm.at[bat, pl.ds(row0, rows)], x_buf.at[i], sem.at[i]) for i, (bat, row0) in enumerate(places)]
    loads.append(pltpu.make_async_copy(gain_hbm, gain_ref, sem.at[n]))
    for load in loads:
        load.start()
    loads[n].wait()
    lanes = [slice(c * HEAD_DIM, (c + 1) * HEAD_DIM) for c in range(d_model // HEAD_DIM)]
    for i in range(n):
        loads[i].wait()

        def norm_rows(r, carry):
            at = pl.ds(pl.multiple_of(r * NORM_ROWS, NORM_ROWS), NORM_ROWS)
            acc = [jnp.zeros((NORM_ROWS, HEAD_DIM), jnp.float32) for _ in range(2)]
            for c, lane in enumerate(lanes):
                xf = x_buf[i, at, lane].astype(jnp.float32)
                acc[c % 2] += xf * xf
            inv_rms = lax.rsqrt(jnp.sum(acc[0] + acc[1], axis=-1, keepdims=True) / d_model + 1e-5)
            for lane in lanes:
                xf = x_buf[i, at, lane].astype(jnp.float32)
                out_refs[i][0, at, lane] = (xf * inv_rms * gain_ref[:, lane].astype(jnp.float32)).astype(jnp.bfloat16)
            return carry

        lax.fori_loop(0, rows // NORM_ROWS, norm_rows, 0)


def first_call(x, gain, places, rows):
    d_model = x.shape[2]
    return pl.pallas_call(
        functools.partial(first_kernel, places, rows),
        out_shape=[pltpu.VMEM((1, rows, d_model), jnp.bfloat16)] * len(places),
        in_specs=[pl.BlockSpec(memory_space=pl.ANY)] * 2,
        out_specs=[pl.BlockSpec(memory_space=pltpu.VMEM)] * len(places),
        scratch_shapes=[
            pltpu.VMEM((len(places), rows, d_model), jnp.bfloat16),
            pltpu.VMEM(gain.shape, gain.dtype),
            pltpu.SemaphoreType.DMA((len(places) + 1,)),
        ],
        compiler_params=pltpu.CompilerParams(vmem_limit_bytes=8 * 2 ** 20),
        cost_estimate=pl.CostEstimate(flops=len(places) * rows * d_model * 8, bytes_accessed=len(places) * rows * d_model * 4, transcendentals=0),
        name="first_rows",
    )(*(pltpu.with_memory_space_constraint(a, pltpu.HBM) for a in (x, gain)))


def norm_call(x, gain, order, outs_of, shapes, blk=None, row_block=0):
    d_model = x.shape[2]
    blk = blk or x.shape[1]

    def prompt_of(g):
        idx = jnp.int32(order[-1])
        for k in range(len(order) - 1):
            idx = jnp.where(g == k, order[k], idx)
        return idx

    return pl.pallas_call(
        functools.partial(norm_kernel, outs_of),
        grid=(len(order),),
        in_specs=[pl.BlockSpec((1, blk, d_model), lambda g: (prompt_of(g), row_block, 0)),
                  pl.BlockSpec((1, d_model), lambda g: (0, 0))],
        out_specs=[pl.BlockSpec(memory_space=pl.ANY)] * len(shapes),
        out_shape=[jax.ShapeDtypeStruct((*shape, d_model), jnp.bfloat16) for shape in shapes],
        scratch_shapes=[
            pltpu.VMEM((blk, HEAD_DIM), jnp.float32),
            pltpu.VMEM((2, blk, d_model), jnp.bfloat16),
            pltpu.SemaphoreType.DMA((2, max(len(o) for o in outs_of))),
        ],
        compiler_params=pltpu.CompilerParams(vmem_limit_bytes=24 * 2 ** 20),
        cost_estimate=pl.CostEstimate(flops=len(order) * blk * d_model * 8, bytes_accessed=len(order) * blk * d_model * 6, transcendentals=0),
        name="norm_rows",
    )(pltpu.with_memory_space_constraint(x, pltpu.HBM), gain)


def rows_kernel(new_ref, last_ref, gain_ref, cos_ref, sin_ref, wq_hbm, wk, wv, q_ref, k_ref, v_ref, st_ref, wq, q_buf, sem):
    load = pltpu.make_async_copy(wq_hbm, wq, sem)
    load.start()
    n_batch = new_ref.shape[0]
    heads = wk.shape[1] // HEAD_DIM
    xf = jnp.concatenate([new_ref[...].astype(jnp.float32), last_ref[...].astype(jnp.float32)], axis=0)
    inv_rms = lax.rsqrt(jnp.mean(xf * xf, axis=-1, keepdims=True) + 1e-5)
    normed = (xf * inv_rms * gain_ref[...].astype(jnp.float32)).astype(jnp.bfloat16)
    k_all = jnp.dot(normed, wk[...], preferred_element_type=jnp.float32)[:n_batch]
    v_all = jnp.dot(normed, wv[...], preferred_element_type=jnp.float32)[:n_batch].astype(jnp.bfloat16)
    load.wait()
    q_all = jnp.dot(normed, wq[...], preferred_element_type=jnp.float32)
    q_buf[...] = jnp.zeros_like(q_buf)
    k_rot = []
    for h in range(heads):
        cols = slice(h * HEAD_DIM, (h + 1) * HEAD_DIM)
        qh = q_all[:, cols]
        qh = (qh * cos_ref[...] + pltpu.roll(qh, HEAD_DIM // 2, 1) * sin_ref[...]).astype(jnp.bfloat16).astype(jnp.float32)
        kh = k_all[:, cols]
        kh = (kh * cos_ref[:n_batch, :] + pltpu.roll(kh, HEAD_DIM // 2, 1) * sin_ref[:n_batch, :]).astype(jnp.bfloat16)
        k_rot.append(kh)
        score = jnp.sum(qh[:n_batch] * kh.astype(jnp.float32), axis=-1, keepdims=True) * (HEAD_DIM ** -0.5)
        zero = jnp.zeros((n_batch, HEAD_DIM), jnp.float32)
        for t in range(2):
            row = 2 * h + t
            q_buf[:, row, cols] = qh[t * n_batch:(t + 1) * n_batch]
            st_ref[0, :, row, :] = v_all[:, cols].astype(jnp.float32) if t == 0 else zero
            st_ref[1, :, row, :] = zero + score if t == 0 else zero + NEG_BIG
            st_ref[2, :, row, :] = zero + 1.0 if t == 0 else zero
    q_ref[...] = q_buf[...].astype(jnp.bfloat16)
    k_ref[...] = jnp.concatenate(k_rot, axis=1).reshape(n_batch, heads, HEAD_DIM)
    v_ref[...] = v_all.reshape(n_batch, heads, HEAD_DIM)


def rows_call(new_tok, last_x, gain, row_tabs, w_q, w_k, w_v):
    n_batch = new_tok.shape[0]
    width = w_q.shape[1]
    heads = width // HEAD_DIM
    vmem = pl.BlockSpec(memory_space=pltpu.VMEM)
    return pl.pallas_call(
        rows_kernel,
        out_shape=[
            jax.ShapeDtypeStruct((n_batch, STAT_ROWS, width), jnp.bfloat16),
            jax.ShapeDtypeStruct((n_batch, heads, HEAD_DIM), jnp.bfloat16),
            jax.ShapeDtypeStruct((n_batch, heads, HEAD_DIM), jnp.bfloat16),
            jax.ShapeDtypeStruct((3, n_batch, STAT_ROWS, HEAD_DIM), jnp.float32),
        ],
        in_specs=[vmem] * 5 + [pl.BlockSpec(memory_space=pl.ANY)] + [vmem] * 2,
        out_specs=[vmem] * 4,
        scratch_shapes=[
            pltpu.VMEM(w_q.shape, jnp.bfloat16),
            pltpu.VMEM((n_batch, STAT_ROWS, width), jnp.float32),
            pltpu.SemaphoreType.DMA,
        ],
        compiler_params=pltpu.CompilerParams(vmem_limit_bytes=24 * 2 ** 20),
        cost_estimate=pl.CostEstimate(flops=2 * 2 * n_batch * 3 * w_q.shape[0] * width, bytes_accessed=2 * w_q.size, transcendentals=0),
        name="query_rows",
    )(new_tok, last_x, gain, *row_tabs, pltpu.with_memory_space_constraint(w_q, pltpu.HBM), w_k, w_v)


def when(condition):
    if isinstance(condition, bool):
        return lambda body: body() if condition else None
    return pl.when(condition)


def by_group(group, values):
    if isinstance(group, int):
        return values[group]
    out = values[-1]
    for p in range(len(values) - 1):
        out = jnp.where(group == p, values[p], out)
    return out


def kv_kernel(n_in, n_steps, masks, batches, firsts, row0, stat_of, with_new, *refs):
    n_groups = len(masks)
    n_arr = n_in * n_groups
    x_refs = refs[:n_arr]
    cos_ref, sin_ref, len_ref, wk, wv, q_ref = refs[n_arr:n_arr + 6]
    rest = refs[n_arr + 6:]
    if with_new:
        new_refs = rest[:2]
        rest = rest[2:]
    else:
        rest = rest[3:]
    kc_ref, vc_ref, st_ref, x_buf, k_buf, v_buf, k_out, v_out, s_out, x_sem, sems, s_sem = rest[:12]
    me = lax.axis_index("model")
    step = pl.program_id(0) if n_steps > 1 else 0
    slot = lax.rem(step, 2) if n_steps > 1 else 0
    per_group = n_steps // n_groups
    blk = x_buf.shape[2]
    shard_rows = cos_ref.shape[1]
    width = wk.shape[1]
    heads = width // HEAD_DIM
    n_tok = n_in * blk

    def x_copies(at_step, which, group):
        local = at_step - group * per_group
        return [pltpu.make_async_copy(x_refs[group * n_in + i].at[firsts[group][i] + local],
                                      x_buf.at[which, i], x_sem.at[which, i]) for i in range(n_in)]

    def start_x(at_step, which):
        for group in range(n_groups):
            @when(at_step // per_group == group)
            def _(group=group):
                for copy in x_copies(at_step, which, group):
                    copy.start()

    def place(i, at_step):
        group = at_step // per_group
        mask = by_group(group, [m[i] for m in masks])
        shard = sum(lax.rem(me // bit + mask // bit, 2) * bit for bit in (1, 2, 4))
        return shard, by_group(group, [b[i] for b in batches]) + at_step % per_group, mask

    def out_copies(which, at_step):
        copies = []
        for i in range(n_in):
            shard, bat, _ = place(i, at_step)
            rows = pl.ds(shard * shard_rows + row0, blk)
            copies.append(pltpu.make_async_copy(k_out.at[which, i], kc_ref.at[bat, rows], sems.at[which, i, 0]))
            copies.append(pltpu.make_async_copy(v_out.at[which, i], vc_ref.at[bat, rows], sems.at[which, i, 1]))
        return copies

    def new_copies():
        return [pltpu.make_async_copy(src.at[pl.ds(b, 1)], dst.at[b, pl.ds(dst.shape[1] - 1, 1)], rest[12].at[idx, b])
                for idx, (src, dst) in enumerate(zip(new_refs, (kc_ref, vc_ref))) for b in range(src.shape[0])]

    @when(step == 0)
    def _():
        start_x(step, slot)
        if with_new:
            for copy in new_copies():
                copy.start()

    @when(step + 1 < n_steps)
    def _():
        start_x(step + 1, 1 - slot)

    @when(step >= 2)
    def _():
        for copy in out_copies(slot, step - 2):
            copy.wait()

    for copy in x_copies(0, slot, 0):
        copy.wait()
    x_rows = x_buf.at[slot]

    def col_tile(c, carry):
        cols = pl.ds(pl.multiple_of(c * COL_TILE, COL_TILE), COL_TILE) if n_steps > 1 else slice(c * COL_TILE, (c + 1) * COL_TILE)
        normed = x_rows[...].reshape(n_tok, x_buf.shape[3])
        kf = jnp.dot(normed, wk[:, cols], preferred_element_type=jnp.float32)
        vf = jnp.dot(normed, wv[:, cols], preferred_element_type=jnp.float32)
        v_buf[:, cols] = vf.astype(jnp.bfloat16)
        parts = []
        for i in range(n_in):
            shard = place(i, step)[0]
            cos_tab = cos_ref[shard, row0:row0 + blk]
            sin_tab = sin_ref[shard, row0:row0 + blk]
            halves = []
            for h in range(COL_TILE // HEAD_DIM):
                kh = kf[i * blk:(i + 1) * blk, h * HEAD_DIM:(h + 1) * HEAD_DIM]
                halves.append(kh * cos_tab + pltpu.roll(kh, HEAD_DIM // 2, 1) * sin_tab)
            parts.append(jnp.concatenate(halves, axis=1))
        k_buf[:, cols] = jnp.concatenate(parts, axis=0).astype(jnp.bfloat16)
        return carry

    if n_steps > 1:
        lax.fori_loop(0, width // COL_TILE, col_tile, 0)
    else:
        for c in range(width // COL_TILE):
            col_tile(c, 0)

    for i in range(n_in):
        k_out[slot, i] = k_buf[i * blk:(i + 1) * blk, :].reshape(blk, heads, HEAD_DIM)
        v_out[slot, i] = v_buf[i * blk:(i + 1) * blk, :].reshape(blk, heads, HEAD_DIM)
    for copy in out_copies(slot, step):
        copy.start()

    head_of_row = lax.broadcasted_iota(jnp.int32, (STAT_ROWS, HEAD_DIM), 0) // (STAT_ROWS // heads)
    probs = []
    for i in range(n_in):
        shard, bat, _ = place(i, step)
        scores = lax.dot_general(q_ref[bat], k_buf[i * blk:(i + 1) * blk, :], (((1,), (1,)), ((), ())),
                                 preferred_element_type=jnp.float32) * (HEAD_DIM ** -0.5)
        pos = shard * shard_rows + row0 + lax.broadcasted_iota(jnp.int32, scores.shape, 1)
        visible = pos < len_ref[pl.ds(bat, 1), :blk]
        scores = jnp.where(visible, scores, NEG_BIG)
        blk_max = jnp.max(scores, axis=-1, keepdims=True)
        prob = jnp.where(visible, jnp.exp(scores - blk_max), 0.0)
        probs.append((blk_max, prob))
    for i, (blk_max, prob) in enumerate(probs):
        full = jnp.dot(prob.astype(jnp.bfloat16), v_buf[i * blk:(i + 1) * blk, :], preferred_element_type=jnp.float32)
        acc = jnp.zeros((STAT_ROWS, HEAD_DIM), jnp.float32)
        for h in range(heads):
            acc = jnp.where(head_of_row == h, full[:, h * HEAD_DIM:(h + 1) * HEAD_DIM], acc)
        s_out[i, 0] = acc
        s_out[i, 1] = jnp.broadcast_to(blk_max, (STAT_ROWS, HEAD_DIM))
        s_out[i, 2] = jnp.broadcast_to(jnp.sum(prob, axis=-1, keepdims=True), (STAT_ROWS, HEAD_DIM))
    stat_copies = []
    for i in range(n_in):
        _, bat, mask = place(i, step)
        stat_copies.append(pltpu.make_async_copy(s_out.at[i], st_ref.at[mask + stat_of, bat], s_sem.at[i]))
        stat_copies[-1].start()
    for copy in stat_copies:
        copy.wait()

    @when(step == n_steps - 1)
    def _():
        for copy in out_copies(slot, step):
            copy.wait()
        if with_new:
            for copy in new_copies():
                copy.wait()
        if n_steps > 1:
            for copy in out_copies(1 - slot, step - 1):
                copy.wait()


def kv_call(groups, per_group, masks, batches, lengths, tabs, w_k, w_v, q_diag, caches, new_rows=None, row0=0, stat_of=0):
    n_groups = len(groups)
    n_in = len(groups[0])
    n_steps = n_groups * per_group
    cos_tab, sin_tab = tabs
    blk, d_model = groups[0][0][0].shape[1:]
    width = w_k.shape[1]
    heads = width // HEAD_DIM
    any_spec = pl.BlockSpec(memory_space=pl.ANY)
    operands = [arr for group in groups for arr, _ in group]
    in_specs = [any_spec] * len(operands) + [pl.BlockSpec(memory_space=pltpu.VMEM)] * 6
    operands += [cos_tab, sin_tab, lengths, w_k, w_v, q_diag]
    with_new = new_rows is not None
    if with_new:
        operands += new_rows
        in_specs += [any_spec] * 2
        aliases = {}
    else:
        operands += [*caches[:2], pltpu.with_memory_space_constraint(caches[2], pltpu.VMEM)]
        in_specs += [any_spec] * 3
        aliases = {len(operands) - 3: 0, len(operands) - 2: 1, len(operands) - 1: 2}
    tokens = n_in * blk
    n_batch = q_diag.shape[0]
    slots = min(n_steps, 2)
    return pl.pallas_call(
        functools.partial(kv_kernel, n_in, n_steps, masks, batches, [[first for _, first in group] for group in groups], row0, stat_of, with_new),
        grid=(n_steps,) if n_steps > 1 else (),
        in_specs=in_specs,
        out_specs=[any_spec] * 3,
        scratch_shapes=[
            pltpu.VMEM((slots, n_in, blk, d_model), jnp.bfloat16),
            pltpu.VMEM((tokens, width), jnp.bfloat16),
            pltpu.VMEM((tokens, width), jnp.bfloat16),
            pltpu.VMEM((slots, n_in, blk, heads, HEAD_DIM), jnp.bfloat16),
            pltpu.VMEM((slots, n_in, blk, heads, HEAD_DIM), jnp.bfloat16),
            pltpu.VMEM((n_in, 3, STAT_ROWS, HEAD_DIM), jnp.float32),
            pltpu.SemaphoreType.DMA((slots, n_in)),
            pltpu.SemaphoreType.DMA((slots, n_in, 2)),
            pltpu.SemaphoreType.DMA((n_in,)),
        ] + [pltpu.SemaphoreType.DMA((2, n_batch))] * with_new,
        out_shape=[*(jax.ShapeDtypeStruct(c.shape, c.dtype) for c in caches[:2]), pltpu.VMEM(caches[2].shape, caches[2].dtype)],
        input_output_aliases=aliases,
        compiler_params=pltpu.CompilerParams(vmem_limit_bytes=20 * 2 ** 20),
        cost_estimate=pl.CostEstimate(flops=4 * n_steps * tokens * d_model * width, bytes_accessed=2 * n_steps * tokens * (d_model + 2 * width), transcendentals=0),
        name="kv_chunk",
    )(*operands)


def tail_kernel(n_dev, parts_of, stv, self_ref, xs_ref, gain_ref, wo, wg_hbm, wu_hbm, wd_hbm, out_ref,
                wg, wu, wd, rows, a_buf, n_buf, ps1, pr1, ps2, pr2, xo1, xg1, xo2, xg2, w_sem, send_sem, recv_sem):
    me = lax.axis_index("model")
    n_batch = out_ref.shape[1]
    n_rows = 2 * n_batch
    d_model = out_ref.shape[2]
    cols = d_model // n_dev
    heads = STAT_ROWS // 2
    loads = [pltpu.make_async_copy(src, dst, w_sem.at[i]) for i, (src, dst) in enumerate(((wg_hbm, wg), (wu_hbm, wu), (wd_hbm, wd)))]
    for load in loads:
        load.start()
    barrier = pltpu.get_barrier_semaphore()

    def peer_of(mask):
        return sum(lax.rem(me // bit + mask // bit, 2) * bit for bit in (1, 2, 4))

    far_first = ((6, 7), (2, 3, 4, 5), (1,))
    for mask in sum(far_first, ()):
        pl.semaphore_signal(barrier, inc=1, device_id={"model": peer_of(mask)}, device_id_type=MESH)

    def send(phase, mask, src, dst):
        return pltpu.make_async_remote_copy(
            src_ref=src, dst_ref=dst, send_sem=send_sem.at[phase, mask - 1], recv_sem=recv_sem.at[phase, mask - 1],
            device_id={"model": peer_of(mask)}, device_id_type=MESH)

    for b in range(n_batch):
        top = self_ref[1, b]
        for j in range(parts_of[b]):
            top = jnp.maximum(top, stv[j, b, 1])
        scale = jnp.exp(self_ref[1, b] - top)
        den = scale * self_ref[2, b]
        num = scale * self_ref[0, b]
        for j in range(parts_of[b]):
            scale = jnp.exp(stv[j, b, 1] - top)
            den += scale * stv[j, b, 2]
            num += scale * stv[j, b, 0]
        rows[:, b, :] = num / den
    for h in range(heads):
        for t in range(2):
            a_buf[t * n_batch:(t + 1) * n_batch, h * HEAD_DIM:(h + 1) * HEAD_DIM] = rows[2 * h + t]
    att = a_buf[...].astype(jnp.bfloat16)

    def exchange(phase, base, copies, pr, xo, xg):
        total = base
        for copy, mask in reversed(copies):
            copy.wait_recv()
            total = total + pr[mask - 1]
        xo[...] = total.astype(jnp.bfloat16)
        xg[me] = xo[...]
        outs = []
        for mask in sum(far_first, ()):
            outs.append(send(phase + 1, mask, xo, xg.at[me]))
            outs[-1].start()
        for out in outs:
            out.wait_recv()
        return [copy for copy, _ in copies] + outs

    def col_block(p):
        return pl.ds(pl.multiple_of(p * cols, cols), cols)

    part = jnp.dot(att, wo[...], preferred_element_type=jnp.float32)
    for j in range(n_dev):
        ps1[j] = part[:, j * cols:(j + 1) * cols]
    pl.semaphore_wait(barrier, n_dev - 1)
    copies = []
    for mask in sum(far_first, ()):
        copies.append((send(0, mask, ps1.at[peer_of(mask)], pr1.at[mask - 1]), mask))
        copies[-1][0].start()
    sent = exchange(0, xs_ref[...].astype(jnp.float32) + ps1[me], copies, pr1, xo1, xg1)
    sq = jnp.zeros((n_rows, 1), jnp.float32)
    for j in range(n_dev):
        xf = xg1[j].astype(jnp.float32)
        sq += jnp.sum(xf * xf, axis=-1, keepdims=True)
    inv_rms = lax.rsqrt(sq / d_model + 1e-5)
    for j in range(n_dev):
        at = slice(j * cols, (j + 1) * cols)
        n_buf[:, at] = (xg1[j].astype(jnp.float32) * inv_rms * gain_ref[:, at].astype(jnp.float32)).astype(jnp.bfloat16)
    loads[0].wait()
    loads[1].wait()
    gate = jnp.dot(n_buf[...], wg[...], preferred_element_type=jnp.float32)
    up = jnp.dot(n_buf[...], wu[...], preferred_element_type=jnp.float32)
    mid = (gate * (1.0 / (1.0 + jnp.exp(-gate))) * up).astype(jnp.bfloat16)
    loads[2].wait()
    copies = []
    for group in far_first:
        for mask in group:
            ps2[mask] = jnp.dot(mid, wd[:, col_block(peer_of(mask))], preferred_element_type=jnp.float32)
        if group == far_first[-1]:
            ps2[0] = jnp.dot(mid, wd[:, col_block(me)], preferred_element_type=jnp.float32)
        for mask in group:
            copies.append((send(2, mask, ps2.at[mask], pr2.at[mask - 1]), mask))
            copies[-1][0].start()
    sent += exchange(2, xo1[...].astype(jnp.float32) + ps2[0], copies, pr2, xo2, xg2)
    for j in range(n_dev):
        at = slice(j * cols, (j + 1) * cols)
        out_ref[0, :, at] = xg2[j, :n_batch]
        out_ref[1, :, at] = xg2[j, n_batch:]
    for copy in sent:
        copy.wait_send()


def tail_call(n_dev, parts_of, stats, self_stat, x_mine, gain, w_o, w_gate, w_up, w_down, n_batch):
    n_rows, cols = x_mine.shape
    d_model = w_o.shape[1]
    vmem = pl.BlockSpec(memory_space=pltpu.VMEM)
    any_spec = pl.BlockSpec(memory_space=pl.ANY)
    exchanged = [pltpu.VMEM((n_dev, n_rows, cols), jnp.float32), pltpu.VMEM((n_dev - 1, n_rows, cols), jnp.float32)]
    summed = [pltpu.VMEM((n_rows, cols), jnp.bfloat16), pltpu.VMEM((n_dev, n_rows, cols), jnp.bfloat16)]
    return pl.pallas_call(
        functools.partial(tail_kernel, n_dev, parts_of),
        out_shape=jax.ShapeDtypeStruct((2, n_batch, d_model), jnp.bfloat16),
        in_specs=[vmem] * 5 + [any_spec] * 3,
        out_specs=vmem,
        scratch_shapes=[
            pltpu.VMEM(w_gate.shape, jnp.bfloat16),
            pltpu.VMEM(w_up.shape, jnp.bfloat16),
            pltpu.VMEM(w_down.shape, jnp.bfloat16),
            pltpu.VMEM((STAT_ROWS, n_batch, HEAD_DIM), jnp.float32),
            pltpu.VMEM((n_rows, w_o.shape[0]), jnp.float32),
            pltpu.VMEM((n_rows, d_model), jnp.bfloat16),
            *exchanged, *exchanged, *summed, *summed,
            pltpu.SemaphoreType.DMA((3,)),
            pltpu.SemaphoreType.DMA((4, n_dev - 1)),
            pltpu.SemaphoreType.DMA((4, n_dev - 1)),
        ],
        compiler_params=pltpu.CompilerParams(collective_id=0, has_side_effects=True, vmem_limit_bytes=46 * 2 ** 20),
        name="tail",
    )(pltpu.with_memory_space_constraint(stats, pltpu.VMEM), self_stat, x_mine, gain, w_o,
      *(pltpu.with_memory_space_constraint(w, pltpu.HBM) for w in (w_gate, w_up, w_down)))


def solution(mesh):
    n_dev = mesh.shape['model']
    seq_spec = P('replica', 'model', None)
    col_spec = P(None, None, 'model')
    row_spec = P(None, 'model', None)
    gain_spec = P(None, None)
    tok_spec = P('replica', None)
    cache_spec = P(None, 'replica', None, 'model', None)
    in_specs = (seq_spec, P('replica'), tok_spec, gain_spec, col_spec, col_spec, col_spec, row_spec, gain_spec, col_spec, col_spec, row_spec)
    out_specs = (tok_spec, tok_spec, cache_spec, cache_spec)

    def swap(arr, bit):
        return lax.ppermute(arr, 'model', [(i, i ^ bit) for i in range(n_dev)])

    def per_device(prompt, lengths, new_tok, norm_attn, w_q, w_k, w_v, w_o, norm_mlp, w_gate, w_up, w_down):
        my_idx = lax.axis_index('model')
        n_batch, blk, d_model = prompt.shape
        seq_len = blk * n_dev
        width = w_k.shape[2]
        heads = width // HEAD_DIM
        half = n_batch // 2
        wq = w_q[0]
        gain = norm_attn

        q1, q2, rows_h = 1, n_batch // 4, blk // 2
        a_parts, b_parts = {}, {}
        for h, name in enumerate(("0a", "0b")):
            a_parts[name], b_parts[name] = first_call(prompt, norm_attn, [(0, h * rows_h), (half, h * rows_h)], rows_h)
        from_y, from_x = {}, {}

        def send_part(step, along_y, along_x):
            from_y[step] = swap(along_y, 4)
            from_x[step] = swap(along_x, 2)

        send_part("0a", a_parts["0a"], b_parts["0a"])
        send_part("0b", a_parts["0b"], b_parts["0b"])
        order, outs_of = [], []
        for part, (lo, hi) in ((1, (q1, q2)), (2, (q2, half)), (0, (0, q1))):
            for k in range(lo, hi):
                for side in range(2):
                    order.append(side * half + k)
                    outs_of.append([(4, side * half + k, 0, blk)] + ([(2 * part - 2 + side, k - lo, 0, blk)] if part else []))
        a_parts["1"], b_parts["1"], a_parts["2"], b_parts["2"], normed = norm_call(
            prompt, gain, order, outs_of, [(q2 - q1, blk)] * 2 + [(half - q2, blk)] * 2 + [(n_batch, blk)])
        send_part("1", a_parts["1"], b_parts["1"])
        seq_pos = my_idx * blk + jnp.arange(blk)
        sel = (seq_pos[None, :] == (lengths - 1)[:, None]).astype(jnp.bfloat16)
        last_x = jnp.einsum('bs,bsd->bd', sel, prompt, preferred_element_type=jnp.float32).astype(jnp.bfloat16)
        core, cols_h = my_idx % 2, d_model // 2
        last_x = last_x + swap(last_x, 1)
        last_x = lax.dynamic_slice_in_dim(last_x, core * cols_h, cols_h, axis=1)
        last_x = (last_x + swap(last_x, 2)) + (swap(last_x, 4) + swap(last_x, 6))
        other_x = swap(last_x, 1)
        last_x = jnp.where(core == 0, jnp.concatenate([last_x, other_x], axis=1), jnp.concatenate([other_x, last_x], axis=1))
        send_part("2", a_parts["2"], b_parts["2"])
        send_part("3", b_parts["2"], a_parts["2"])
        send_part("4", normed[half:half + q2], normed[:q2])
        core_all = swap(normed, 1)

        len_rows = jnp.broadcast_to(lengths.astype(jnp.int32)[:, None], (n_batch, HEAD_DIM))
        row_tabs = rotary_tables(jnp.concatenate([lengths, lengths - 1]))
        tabs = tuple(tab.reshape(n_dev, blk, HEAD_DIM) for tab in rotary_tables(jnp.arange(seq_len)))
        x_rows = jnp.concatenate([new_tok, last_x], axis=0)
        x_mine = lax.dynamic_slice_in_dim(x_rows, my_idx * (d_model // n_dev), d_model // n_dev, axis=1)
        wk, wv, wo, last_x, len_rows, row_tabs, tabs, x_mine = lax.optimization_barrier(
            (w_k[0], w_v[0], w_o[0], last_x, len_rows, row_tabs, tabs, x_mine))
        wk, wv, wo = keep_in_vmem(wk, wv, wo)
        q_diag, k_new, v_new, self_stat = rows_call(new_tok, last_x, gain, row_tabs, wq, wk, wv)
        cache_shape = jax.ShapeDtypeStruct((n_batch, seq_len + 1, heads, HEAD_DIM), jnp.bfloat16)
        caches = [cache_shape, cache_shape, jax.ShapeDtypeStruct((2 * n_dev - 2, n_batch, 3, STAT_ROWS, HEAD_DIM), jnp.float32)]

        def run(groups, per_group, masks, batches, caches, **kw):
            return kv_call(groups, per_group, masks, batches, len_rows, tabs, wk, wv, q_diag, caches, **kw)

        def half_rows(step):
            return {"row0": rows_h * (step == "0b"), "stat_of": (n_dev - 2) * (step == "0b")}

        def after(caches, *arrays):
            out = lax.optimization_barrier((caches[2], *arrays))
            return [caches[0], caches[1], out[0]], out[1:]

        caches = run([[(arr, 0), (arr, half)] for arr in (normed, core_all)], half,
                     [[0] * 2, [1] * 2], [[0, half]] * 2, caches, new_rows=[k_new, v_new])
        diag, turned = {}, {}
        starts = {"0a": (0, half), "0b": (0, half), "1": (q1, half + q1), "2": (q2, half + q2), "3": (half + q2, q2), "4": (half, 0)}
        for step, start in starts.items():
            caches, (got_y, got_x) = after(caches, from_y[step], from_x[step])
            other_y, other_x = swap(got_y, 1), swap(got_x, 1)
            if step not in "34":
                via_x = swap(got_y, 2)
                via_y = swap(got_x, 4)
                diag[step] = (via_x, via_y)
            streams = [[(got_y, 0), (got_x, 0)], [(other_y, 0), (other_x, 0)]]
            if step in ("0a", "0b"):
                caches = run([streams[0] + streams[1]], q1, [[4, 2, 5, 3]], [[*start, *start]], caches, **half_rows(step))
            else:
                caches = run(streams, got_y.shape[0], [[4, 2], [5, 3]], [list(start)] * 2, caches)
            if step in "34":
                caches, (w_t,) = after(caches, (w_gate if step == "3" else w_up)[0].T)
                turned[step] = turn_call(w_t)
                caches, (turned[step],) = after(caches, turned[step])
        for step in ("2", "1", "0a", "0b"):
            caches, (via_y,) = after(caches, diag[step][1])
            caches, (via_x,) = after(caches, diag[step][0])
            other_y = swap(via_y, 1)
            other_x = swap(via_x, 1)
            start = starts[step]
            streams = [[(via_x, 0), (via_y, 0)], [(other_x, 0), (other_y, 0)]]
            if step in ("0a", "0b"):
                caches = run([streams[0] + streams[1]], q1, [[6, 6, 7, 7]], [[*start, *start]], caches, **half_rows(step))
            else:
                caches = run(streams, via_x.shape[0], [[6] * 2, [7] * 2], [list(start)] * 2, caches)

        k_cache, v_cache, stats = caches
        parts_of = [2 * n_dev - 2 if b % half < q1 else n_dev for b in range(n_batch)]
        both = tail_call(n_dev, parts_of, stats, self_stat, x_mine, norm_mlp, wo, turned["3"], turned["4"], w_down[0], n_batch)
        return both[0], both[1], k_cache[None], v_cache[None]

    return jax.shard_map(per_device, mesh=mesh, in_specs=in_specs, out_specs=out_specs, check_vma=False)
```

```python
import functools

import jax
import jax.numpy as jnp
from jax import lax
from jax.experimental import pallas as pl
from jax.experimental.pallas import tpu as pltpu
from jax.sharding import PartitionSpec as P


HEAD_DIM = 128
NEG_BIG = -1e30
STAT_ROWS = 8
NORM_ROWS = 32
COL_TILE = 256
MESH = pl.DeviceIdType.MESH


def rotary_tables(positions):
    half_dim = HEAD_DIM // 2
    inv_freq = 10000.0 ** (-2.0 * jnp.arange(half_dim, dtype=jnp.float32) / HEAD_DIM)
    angles = positions.astype(jnp.float32)[..., None] * inv_freq
    cos_tab = jnp.cos(angles)
    sin_tab = jnp.sin(angles)
    return jnp.concatenate([cos_tab, cos_tab], axis=-1), jnp.concatenate([-sin_tab, sin_tab], axis=-1)


def load_kernel(*refs):
    n = len(refs) // 2
    sem = refs[-1]
    copies = [pltpu.make_async_copy(refs[i], refs[n + i], sem.at[i]) for i in range(n)]
    for copy in copies:
        copy.start()
    for copy in copies:
        copy.wait()


def keep_in_vmem(*arrays):
    return pl.pallas_call(
        load_kernel,
        out_shape=[pltpu.VMEM(arr.shape, arr.dtype) for arr in arrays],
        in_specs=[pl.BlockSpec(memory_space=pl.ANY)] * len(arrays),
        out_specs=[pl.BlockSpec(memory_space=pltpu.VMEM)] * len(arrays),
        scratch_shapes=[pltpu.SemaphoreType.DMA((len(arrays),))],
        compiler_params=pltpu.CompilerParams(vmem_limit_bytes=24 * 2 ** 20),
        name="keep",
    )(*(pltpu.with_memory_space_constraint(arr, pltpu.HBM) for arr in arrays))


def turn_kernel(w_ref, out_ref):
    out_ref[...] = w_ref[...].T


def turn_call(w_t):
    n, d = w_t.shape
    cols = 512
    return pl.pallas_call(
        turn_kernel,
        grid=(d // cols,),
        in_specs=[pl.BlockSpec((n, cols), lambda g: (0, g))],
        out_specs=pl.BlockSpec((cols, n), lambda g: (g, 0)),
        out_shape=jax.ShapeDtypeStruct((d, n), w_t.dtype),
        compiler_params=pltpu.CompilerParams(vmem_limit_bytes=12 * 2 ** 20),
        cost_estimate=pl.CostEstimate(flops=2 * d * n * 128, bytes_accessed=4 * d * n, transcendentals=0),
        name="turn",
    )(pltpu.with_memory_space_constraint(w_t, pltpu.HBM))


def norm_kernel(outs_of, x_ref, gain_ref, *refs):
    n_out = len(refs) - 3
    out_refs = refs[:n_out]
    ss_buf, n_buf, sems = refs[n_out:]
    step = pl.program_id(0)
    blk, d_model = x_ref.shape[1:]
    lanes = [slice(c * HEAD_DIM, (c + 1) * HEAD_DIM) for c in range(d_model // HEAD_DIM)]

    def copies(at_step):
        return [pltpu.make_async_copy(n_buf.at[at_step % 2, pl.ds(lo, rows)], out_refs[o].at[i], sems.at[at_step % 2, k])
                for k, (o, i, lo, rows) in enumerate(outs_of[at_step])]

    for at_step in range(2, len(outs_of)):
        @pl.when(step == at_step)
        def _():
            for copy in copies(at_step - 2):
                copy.wait()

    def square_rows(r, carry):
        rows = pl.ds(pl.multiple_of(r * NORM_ROWS, NORM_ROWS), NORM_ROWS)
        acc = [jnp.zeros((NORM_ROWS, HEAD_DIM), jnp.float32) for _ in range(2)]
        for c, lane in enumerate(lanes):
            xf = x_ref[0, rows, lane].astype(jnp.float32)
            acc[c % 2] += xf * xf
        ss_buf[rows, :] = acc[0] + acc[1]
        return carry

    lax.fori_loop(0, blk // NORM_ROWS, square_rows, 0)
    total = jnp.sum(ss_buf[...], axis=-1, keepdims=True)
    ss_buf[...] = jnp.broadcast_to(lax.rsqrt(total / d_model + 1e-5), (blk, HEAD_DIM))
    slot = lax.rem(step, 2)

    def norm_rows(r, carry):
        rows = pl.ds(pl.multiple_of(r * NORM_ROWS, NORM_ROWS), NORM_ROWS)
        inv_rms = ss_buf[rows, :]
        for lane in lanes:
            xf = x_ref[0, rows, lane].astype(jnp.float32)
            n_buf[slot, rows, lane] = (xf * inv_rms * gain_ref[:, lane].astype(jnp.float32)).astype(jnp.bfloat16)
        return carry

    lax.fori_loop(0, blk // NORM_ROWS, norm_rows, 0)
    for at_step in range(len(outs_of)):
        @pl.when(step == at_step)
        def _():
            for copy in copies(at_step):
                copy.start()
            if at_step == len(outs_of) - 1:
                for copy in copies(at_step):
                    copy.wait()
                if at_step >= 1:
                    for copy in copies(at_step - 1):
                        copy.wait()


def first_kernel(places, rows, x_hbm, gain_hbm, *refs):
    n = len(places)
    out_refs = refs[:n]
    x_buf, gain_ref, sem = refs[n:]
    d_model = x_hbm.shape[2]
    pieces = rows // NORM_ROWS
    gain_load = pltpu.make_async_copy(gain_hbm, gain_ref, sem.at[n * pieces])
    gain_load.start()
    loads = {}
    for k in range(pieces):
        for i, (bat, row0) in enumerate(places):
            loads[k, i] = pltpu.make_async_copy(x_hbm.at[bat, pl.ds(row0 + k * NORM_ROWS, NORM_ROWS)],
                                                x_buf.at[i, pl.ds(k * NORM_ROWS, NORM_ROWS)], sem.at[k * n + i])
            loads[k, i].start()
    gain_load.wait()
    lanes = [slice(c * HEAD_DIM, (c + 1) * HEAD_DIM) for c in range(d_model // HEAD_DIM)]
    for k in range(pieces):
        at = slice(k * NORM_ROWS, (k + 1) * NORM_ROWS)
        for i in range(n):
            loads[k, i].wait()
            acc = [jnp.zeros((NORM_ROWS, HEAD_DIM), jnp.float32) for _ in range(2)]
            for c, lane in enumerate(lanes):
                xf = x_buf[i, at, lane].astype(jnp.float32)
                acc[c % 2] += xf * xf
            inv_rms = lax.rsqrt(jnp.sum(acc[0] + acc[1], axis=-1, keepdims=True) / d_model + 1e-5)
            for lane in lanes:
                xf = x_buf[i, at, lane].astype(jnp.float32)
                out_refs[i][0, at, lane] = (xf * inv_rms * gain_ref[:, lane].astype(jnp.float32)).astype(jnp.bfloat16)


def first_call(x, gain, places, rows):
    d_model = x.shape[2]
    return pl.pallas_call(
        functools.partial(first_kernel, places, rows),
        out_shape=[pltpu.VMEM((1, rows, d_model), jnp.bfloat16)] * len(places),
        in_specs=[pl.BlockSpec(memory_space=pl.ANY)] * 2,
        out_specs=[pl.BlockSpec(memory_space=pltpu.VMEM)] * len(places),
        scratch_shapes=[
            pltpu.VMEM((len(places), rows, d_model), jnp.bfloat16),
            pltpu.VMEM(gain.shape, gain.dtype),
            pltpu.SemaphoreType.DMA((len(places) * rows // NORM_ROWS + 1,)),
        ],
        compiler_params=pltpu.CompilerParams(vmem_limit_bytes=8 * 2 ** 20),
        cost_estimate=pl.CostEstimate(flops=len(places) * rows * d_model * 8, bytes_accessed=len(places) * rows * d_model * 4, transcendentals=0),
        name="first_rows",
    )(*(pltpu.with_memory_space_constraint(a, pltpu.HBM) for a in (x, gain)))


def norm_call(x, gain, order, outs_of, shapes, blk=None, row_block=0):
    d_model = x.shape[2]
    blk = blk or x.shape[1]

    def prompt_of(g):
        idx = jnp.int32(order[-1])
        for k in range(len(order) - 1):
            idx = jnp.where(g == k, order[k], idx)
        return idx

    return pl.pallas_call(
        functools.partial(norm_kernel, outs_of),
        grid=(len(order),),
        in_specs=[pl.BlockSpec((1, blk, d_model), lambda g: (prompt_of(g), row_block, 0)),
                  pl.BlockSpec((1, d_model), lambda g: (0, 0))],
        out_specs=[pl.BlockSpec(memory_space=pl.ANY)] * len(shapes),
        out_shape=[jax.ShapeDtypeStruct((*shape, d_model), jnp.bfloat16) for shape in shapes],
        scratch_shapes=[
            pltpu.VMEM((blk, HEAD_DIM), jnp.float32),
            pltpu.VMEM((2, blk, d_model), jnp.bfloat16),
            pltpu.SemaphoreType.DMA((2, max(len(o) for o in outs_of))),
        ],
        compiler_params=pltpu.CompilerParams(vmem_limit_bytes=24 * 2 ** 20),
        cost_estimate=pl.CostEstimate(flops=len(order) * blk * d_model * 8, bytes_accessed=len(order) * blk * d_model * 6, transcendentals=0),
        name="norm_rows",
    )(pltpu.with_memory_space_constraint(x, pltpu.HBM), gain)


def rows_kernel(new_ref, last_ref, gain_ref, cos_ref, sin_ref, wq_hbm, wk, wv, q_ref, k_ref, v_ref, st_ref, wq, q_buf, sem):
    load = pltpu.make_async_copy(wq_hbm, wq, sem)
    load.start()
    n_batch = new_ref.shape[0]
    heads = wk.shape[1] // HEAD_DIM
    xf = jnp.concatenate([new_ref[...].astype(jnp.float32), last_ref[...].astype(jnp.float32)], axis=0)
    inv_rms = lax.rsqrt(jnp.mean(xf * xf, axis=-1, keepdims=True) + 1e-5)
    normed = (xf * inv_rms * gain_ref[...].astype(jnp.float32)).astype(jnp.bfloat16)
    k_all = jnp.dot(normed, wk[...], preferred_element_type=jnp.float32)[:n_batch]
    v_all = jnp.dot(normed, wv[...], preferred_element_type=jnp.float32)[:n_batch].astype(jnp.bfloat16)
    load.wait()
    q_all = jnp.dot(normed, wq[...], preferred_element_type=jnp.float32)
    q_buf[...] = jnp.zeros_like(q_buf)
    k_rot = []
    for h in range(heads):
        cols = slice(h * HEAD_DIM, (h + 1) * HEAD_DIM)
        qh = q_all[:, cols]
        qh = (qh * cos_ref[...] + pltpu.roll(qh, HEAD_DIM // 2, 1) * sin_ref[...]).astype(jnp.bfloat16).astype(jnp.float32)
        kh = k_all[:, cols]
        kh = (kh * cos_ref[:n_batch, :] + pltpu.roll(kh, HEAD_DIM // 2, 1) * sin_ref[:n_batch, :]).astype(jnp.bfloat16)
        k_rot.append(kh)
        score = jnp.sum(qh[:n_batch] * kh.astype(jnp.float32), axis=-1, keepdims=True) * (HEAD_DIM ** -0.5)
        zero = jnp.zeros((n_batch, HEAD_DIM), jnp.float32)
        for t in range(2):
            row = 2 * h + t
            q_buf[:, row, cols] = qh[t * n_batch:(t + 1) * n_batch]
            st_ref[0, :, row, :] = v_all[:, cols].astype(jnp.float32) if t == 0 else zero
            st_ref[1, :, row, :] = zero + score if t == 0 else zero + NEG_BIG
            st_ref[2, :, row, :] = zero + 1.0 if t == 0 else zero
    q_ref[...] = q_buf[...].astype(jnp.bfloat16)
    k_ref[...] = jnp.concatenate(k_rot, axis=1).reshape(n_batch, heads, HEAD_DIM)
    v_ref[...] = v_all.reshape(n_batch, heads, HEAD_DIM)


def rows_call(new_tok, last_x, gain, row_tabs, w_q, w_k, w_v):
    n_batch = new_tok.shape[0]
    width = w_q.shape[1]
    heads = width // HEAD_DIM
    vmem = pl.BlockSpec(memory_space=pltpu.VMEM)
    return pl.pallas_call(
        rows_kernel,
        out_shape=[
            jax.ShapeDtypeStruct((n_batch, STAT_ROWS, width), jnp.bfloat16),
            jax.ShapeDtypeStruct((n_batch, heads, HEAD_DIM), jnp.bfloat16),
            jax.ShapeDtypeStruct((n_batch, heads, HEAD_DIM), jnp.bfloat16),
            jax.ShapeDtypeStruct((3, n_batch, STAT_ROWS, HEAD_DIM), jnp.float32),
        ],
        in_specs=[vmem] * 5 + [pl.BlockSpec(memory_space=pl.ANY)] + [vmem] * 2,
        out_specs=[vmem] * 4,
        scratch_shapes=[
            pltpu.VMEM(w_q.shape, jnp.bfloat16),
            pltpu.VMEM((n_batch, STAT_ROWS, width), jnp.float32),
            pltpu.SemaphoreType.DMA,
        ],
        compiler_params=pltpu.CompilerParams(vmem_limit_bytes=24 * 2 ** 20),
        cost_estimate=pl.CostEstimate(flops=2 * 2 * n_batch * 3 * w_q.shape[0] * width, bytes_accessed=2 * w_q.size, transcendentals=0),
        name="query_rows",
    )(new_tok, last_x, gain, *row_tabs, pltpu.with_memory_space_constraint(w_q, pltpu.HBM), w_k, w_v)


def when(condition):
    if isinstance(condition, bool):
        return lambda body: body() if condition else None
    return pl.when(condition)


def by_group(group, values):
    if isinstance(group, int):
        return values[group]
    out = values[-1]
    for p in range(len(values) - 1):
        out = jnp.where(group == p, values[p], out)
    return out


def kv_kernel(n_in, n_steps, masks, batches, firsts, row0, stat_of, with_new, *refs):
    n_groups = len(masks)
    n_arr = n_in * n_groups
    x_refs = refs[:n_arr]
    cos_ref, sin_ref, len_ref, wk, wv, q_ref = refs[n_arr:n_arr + 6]
    rest = refs[n_arr + 6:]
    if with_new:
        new_refs = rest[:2]
        rest = rest[2:]
    else:
        rest = rest[3:]
    kc_ref, vc_ref, st_ref, x_buf, k_buf, v_buf, k_out, v_out, s_out, x_sem, sems, s_sem = rest[:12]
    me = lax.axis_index("model")
    step = pl.program_id(0) if n_steps > 1 else 0
    slot = lax.rem(step, 2) if n_steps > 1 else 0
    per_group = n_steps // n_groups
    blk = x_buf.shape[2]
    shard_rows = cos_ref.shape[1]
    width = wk.shape[1]
    heads = width // HEAD_DIM
    n_tok = n_in * blk

    def x_copies(at_step, which, group):
        local = at_step - group * per_group
        return [pltpu.make_async_copy(x_refs[group * n_in + i].at[firsts[group][i] + local],
                                      x_buf.at[which, i], x_sem.at[which, i]) for i in range(n_in)]

    def start_x(at_step, which):
        for group in range(n_groups):
            @when(at_step // per_group == group)
            def _(group=group):
                for copy in x_copies(at_step, which, group):
                    copy.start()

    def place(i, at_step):
        group = at_step // per_group
        mask = by_group(group, [m[i] for m in masks])
        shard = sum(lax.rem(me // bit + mask // bit, 2) * bit for bit in (1, 2, 4))
        return shard, by_group(group, [b[i] for b in batches]) + at_step % per_group, mask

    def out_copies(which, at_step):
        copies = []
        for i in range(n_in):
            shard, bat, _ = place(i, at_step)
            rows = pl.ds(shard * shard_rows + row0, blk)
            copies.append(pltpu.make_async_copy(k_out.at[which, i], kc_ref.at[bat, rows], sems.at[which, i, 0]))
            copies.append(pltpu.make_async_copy(v_out.at[which, i], vc_ref.at[bat, rows], sems.at[which, i, 1]))
        return copies

    def new_copies():
        return [pltpu.make_async_copy(src.at[pl.ds(b, 1)], dst.at[b, pl.ds(dst.shape[1] - 1, 1)], rest[12].at[idx, b])
                for idx, (src, dst) in enumerate(zip(new_refs, (kc_ref, vc_ref))) for b in range(src.shape[0])]

    @when(step == 0)
    def _():
        start_x(step, slot)
        if with_new:
            for copy in new_copies():
                copy.start()

    @when(step + 1 < n_steps)
    def _():
        start_x(step + 1, 1 - slot)

    @when(step >= 2)
    def _():
        for copy in out_copies(slot, step - 2):
            copy.wait()

    for copy in x_copies(0, slot, 0):
        copy.wait()
    x_rows = x_buf.at[slot]

    def col_tile(c, carry):
        cols = pl.ds(pl.multiple_of(c * COL_TILE, COL_TILE), COL_TILE) if n_steps > 1 else slice(c * COL_TILE, (c + 1) * COL_TILE)
        normed = x_rows[...].reshape(n_tok, x_buf.shape[3])
        kf = jnp.dot(normed, wk[:, cols], preferred_element_type=jnp.float32)
        vf = jnp.dot(normed, wv[:, cols], preferred_element_type=jnp.float32)
        v_buf[:, cols] = vf.astype(jnp.bfloat16)
        parts = []
        for i in range(n_in):
            shard = place(i, step)[0]
            cos_tab = cos_ref[shard, row0:row0 + blk]
            sin_tab = sin_ref[shard, row0:row0 + blk]
            halves = []
            for h in range(COL_TILE // HEAD_DIM):
                kh = kf[i * blk:(i + 1) * blk, h * HEAD_DIM:(h + 1) * HEAD_DIM]
                halves.append(kh * cos_tab + pltpu.roll(kh, HEAD_DIM // 2, 1) * sin_tab)
            parts.append(jnp.concatenate(halves, axis=1))
        k_buf[:, cols] = jnp.concatenate(parts, axis=0).astype(jnp.bfloat16)
        return carry

    if n_steps > 1:
        lax.fori_loop(0, width // COL_TILE, col_tile, 0)
    else:
        for c in range(width // COL_TILE):
            col_tile(c, 0)

    for i in range(n_in):
        k_out[slot, i] = k_buf[i * blk:(i + 1) * blk, :].reshape(blk, heads, HEAD_DIM)
        v_out[slot, i] = v_buf[i * blk:(i + 1) * blk, :].reshape(blk, heads, HEAD_DIM)
    for copy in out_copies(slot, step):
        copy.start()

    head_of_row = lax.broadcasted_iota(jnp.int32, (STAT_ROWS, HEAD_DIM), 0) // (STAT_ROWS // heads)
    probs = []
    for i in range(n_in):
        shard, bat, _ = place(i, step)
        scores = lax.dot_general(q_ref[bat], k_buf[i * blk:(i + 1) * blk, :], (((1,), (1,)), ((), ())),
                                 preferred_element_type=jnp.float32) * (HEAD_DIM ** -0.5)
        pos = shard * shard_rows + row0 + lax.broadcasted_iota(jnp.int32, scores.shape, 1)
        visible = pos < len_ref[pl.ds(bat, 1), :blk]
        scores = jnp.where(visible, scores, NEG_BIG)
        blk_max = jnp.max(scores, axis=-1, keepdims=True)
        prob = jnp.where(visible, jnp.exp(scores - blk_max), 0.0)
        probs.append((blk_max, prob))
    for i, (blk_max, prob) in enumerate(probs):
        full = jnp.dot(prob.astype(jnp.bfloat16), v_buf[i * blk:(i + 1) * blk, :], preferred_element_type=jnp.float32)
        acc = jnp.zeros((STAT_ROWS, HEAD_DIM), jnp.float32)
        for h in range(heads):
            acc = jnp.where(head_of_row == h, full[:, h * HEAD_DIM:(h + 1) * HEAD_DIM], acc)
        s_out[i, 0] = acc
        s_out[i, 1] = jnp.broadcast_to(blk_max, (STAT_ROWS, HEAD_DIM))
        s_out[i, 2] = jnp.broadcast_to(jnp.sum(prob, axis=-1, keepdims=True), (STAT_ROWS, HEAD_DIM))
    stat_copies = []
    for i in range(n_in):
        _, bat, mask = place(i, step)
        stat_copies.append(pltpu.make_async_copy(s_out.at[i], st_ref.at[mask + stat_of, bat], s_sem.at[i]))
        stat_copies[-1].start()
    for copy in stat_copies:
        copy.wait()

    @when(step == n_steps - 1)
    def _():
        for copy in out_copies(slot, step):
            copy.wait()
        if with_new:
            for copy in new_copies():
                copy.wait()
        if n_steps > 1:
            for copy in out_copies(1 - slot, step - 1):
                copy.wait()


def kv_call(groups, per_group, masks, batches, lengths, tabs, w_k, w_v, q_diag, caches, new_rows=None, row0=0, stat_of=0):
    n_groups = len(groups)
    n_in = len(groups[0])
    n_steps = n_groups * per_group
    cos_tab, sin_tab = tabs
    blk, d_model = groups[0][0][0].shape[1:]
    width = w_k.shape[1]
    heads = width // HEAD_DIM
    any_spec = pl.BlockSpec(memory_space=pl.ANY)
    operands = [arr for group in groups for arr, _ in group]
    in_specs = [any_spec] * len(operands) + [pl.BlockSpec(memory_space=pltpu.VMEM)] * 6
    operands += [cos_tab, sin_tab, lengths, w_k, w_v, q_diag]
    with_new = new_rows is not None
    if with_new:
        operands += new_rows
        in_specs += [any_spec] * 2
        aliases = {}
    else:
        operands += [*caches[:2], pltpu.with_memory_space_constraint(caches[2], pltpu.VMEM)]
        in_specs += [any_spec] * 3
        aliases = {len(operands) - 3: 0, len(operands) - 2: 1, len(operands) - 1: 2}
    tokens = n_in * blk
    n_batch = q_diag.shape[0]
    slots = min(n_steps, 2)
    return pl.pallas_call(
        functools.partial(kv_kernel, n_in, n_steps, masks, batches, [[first for _, first in group] for group in groups], row0, stat_of, with_new),
        grid=(n_steps,) if n_steps > 1 else (),
        in_specs=in_specs,
        out_specs=[any_spec] * 3,
        scratch_shapes=[
            pltpu.VMEM((slots, n_in, blk, d_model), jnp.bfloat16),
            pltpu.VMEM((tokens, width), jnp.bfloat16),
            pltpu.VMEM((tokens, width), jnp.bfloat16),
            pltpu.VMEM((slots, n_in, blk, heads, HEAD_DIM), jnp.bfloat16),
            pltpu.VMEM((slots, n_in, blk, heads, HEAD_DIM), jnp.bfloat16),
            pltpu.VMEM((n_in, 3, STAT_ROWS, HEAD_DIM), jnp.float32),
            pltpu.SemaphoreType.DMA((slots, n_in)),
            pltpu.SemaphoreType.DMA((slots, n_in, 2)),
            pltpu.SemaphoreType.DMA((n_in,)),
        ] + [pltpu.SemaphoreType.DMA((2, n_batch))] * with_new,
        out_shape=[*(jax.ShapeDtypeStruct(c.shape, c.dtype) for c in caches[:2]), pltpu.VMEM(caches[2].shape, caches[2].dtype)],
        input_output_aliases=aliases,
        compiler_params=pltpu.CompilerParams(vmem_limit_bytes=20 * 2 ** 20),
        cost_estimate=pl.CostEstimate(flops=4 * n_steps * tokens * d_model * width, bytes_accessed=2 * n_steps * tokens * (d_model + 2 * width), transcendentals=0),
        name="kv_chunk",
    )(*operands)


def tail_kernel(n_dev, parts_of, stv, self_ref, xs_ref, gain_ref, wo, wg_hbm, wu_hbm, wd_hbm, out_ref,
                wg, wu, wd, rows, a_buf, n_buf, ps1, pr1, ps2, pr2, xo1, xg1, xo2, xg2, w_sem, send_sem, recv_sem):
    me = lax.axis_index("model")
    n_batch = out_ref.shape[1]
    n_rows = 2 * n_batch
    d_model = out_ref.shape[2]
    cols = d_model // n_dev
    heads = STAT_ROWS // 2
    loads = [pltpu.make_async_copy(src, dst, w_sem.at[i]) for i, (src, dst) in enumerate(((wg_hbm, wg), (wu_hbm, wu), (wd_hbm, wd)))]
    loads[0].start()
    loads[1].start()
    barrier = pltpu.get_barrier_semaphore()

    def peer_of(mask):
        return sum(lax.rem(me // bit + mask // bit, 2) * bit for bit in (1, 2, 4))

    far_first = ((6,), (7, 2), (4, 5, 3), (1,))
    for mask in sum(far_first, ()):
        pl.semaphore_signal(barrier, inc=1, device_id={"model": peer_of(mask)}, device_id_type=MESH)

    def send(phase, mask, src, dst):
        return pltpu.make_async_remote_copy(
            src_ref=src, dst_ref=dst, send_sem=send_sem.at[phase, mask - 1], recv_sem=recv_sem.at[phase, mask - 1],
            device_id={"model": peer_of(mask)}, device_id_type=MESH)

    for b in range(n_batch):
        top = self_ref[1, b]
        for j in range(parts_of[b]):
            top = jnp.maximum(top, stv[j, b, 1])
        scale = jnp.exp(self_ref[1, b] - top)
        den = scale * self_ref[2, b]
        num = scale * self_ref[0, b]
        for j in range(parts_of[b]):
            scale = jnp.exp(stv[j, b, 1] - top)
            den += scale * stv[j, b, 2]
            num += scale * stv[j, b, 0]
        rows[:, b, :] = num / den
    for h in range(heads):
        for t in range(2):
            a_buf[t * n_batch:(t + 1) * n_batch, h * HEAD_DIM:(h + 1) * HEAD_DIM] = rows[2 * h + t]
    att = a_buf[...].astype(jnp.bfloat16)

    def exchange(phase, base, copies, pr, xo, xg):
        total = base
        for copy, mask in reversed(copies):
            copy.wait_recv()
            total = total + pr[mask - 1]
        xo[...] = total.astype(jnp.bfloat16)
        xg[me] = xo[...]
        outs = []
        for mask in sum(far_first, ()):
            outs.append(send(phase + 1, mask, xo, xg.at[me]))
            outs[-1].start()
        if phase == 0:
            loads[2].start()
        for out in outs:
            out.wait_recv()
        return [copy for copy, _ in copies] + outs

    def col_block(p):
        return pl.ds(pl.multiple_of(p * cols, cols), cols)

    part = jnp.dot(att, wo[...], preferred_element_type=jnp.float32)
    for j in range(n_dev):
        ps1[j] = part[:, j * cols:(j + 1) * cols]
    pl.semaphore_wait(barrier, n_dev - 1)
    copies = []
    for mask in sum(far_first, ()):
        copies.append((send(0, mask, ps1.at[peer_of(mask)], pr1.at[mask - 1]), mask))
        copies[-1][0].start()
    sent = exchange(0, xs_ref[...].astype(jnp.float32) + ps1[me], copies, pr1, xo1, xg1)
    sq = jnp.zeros((n_rows, 1), jnp.float32)
    for j in range(n_dev):
        xf = xg1[j].astype(jnp.float32)
        sq += jnp.sum(xf * xf, axis=-1, keepdims=True)
    inv_rms = lax.rsqrt(sq / d_model + 1e-5)
    for j in range(n_dev):
        at = slice(j * cols, (j + 1) * cols)
        n_buf[:, at] = (xg1[j].astype(jnp.float32) * inv_rms * gain_ref[:, at].astype(jnp.float32)).astype(jnp.bfloat16)
    loads[0].wait()
    loads[1].wait()
    gate = jnp.dot(n_buf[...], wg[...], preferred_element_type=jnp.float32)
    up = jnp.dot(n_buf[...], wu[...], preferred_element_type=jnp.float32)
    mid = (gate * (1.0 / (1.0 + jnp.exp(-gate))) * up).astype(jnp.bfloat16)
    loads[2].wait()
    copies = []
    for group in far_first:
        for mask in group:
            ps2[mask] = jnp.dot(mid, wd[:, col_block(peer_of(mask))], preferred_element_type=jnp.float32)
        if group == far_first[-1]:
            ps2[0] = jnp.dot(mid, wd[:, col_block(me)], preferred_element_type=jnp.float32)
        for mask in group:
            copies.append((send(2, mask, ps2.at[mask], pr2.at[mask - 1]), mask))
            copies[-1][0].start()
    sent += exchange(2, xo1[...].astype(jnp.float32) + ps2[0], copies, pr2, xo2, xg2)
    for j in range(n_dev):
        at = slice(j * cols, (j + 1) * cols)
        out_ref[0, :, at] = xg2[j, :n_batch]
        out_ref[1, :, at] = xg2[j, n_batch:]
    for copy in sent:
        copy.wait_send()


def tail_call(n_dev, parts_of, stats, self_stat, x_mine, gain, w_o, w_gate, w_up, w_down, n_batch):
    n_rows, cols = x_mine.shape
    d_model = w_o.shape[1]
    vmem = pl.BlockSpec(memory_space=pltpu.VMEM)
    any_spec = pl.BlockSpec(memory_space=pl.ANY)
    exchanged = [pltpu.VMEM((n_dev, n_rows, cols), jnp.float32), pltpu.VMEM((n_dev - 1, n_rows, cols), jnp.float32)]
    summed = [pltpu.VMEM((n_rows, cols), jnp.bfloat16), pltpu.VMEM((n_dev, n_rows, cols), jnp.bfloat16)]
    return pl.pallas_call(
        functools.partial(tail_kernel, n_dev, parts_of),
        out_shape=jax.ShapeDtypeStruct((2, n_batch, d_model), jnp.bfloat16),
        in_specs=[vmem] * 5 + [any_spec] * 3,
        out_specs=vmem,
        scratch_shapes=[
            pltpu.VMEM(w_gate.shape, jnp.bfloat16),
            pltpu.VMEM(w_up.shape, jnp.bfloat16),
            pltpu.VMEM(w_down.shape, jnp.bfloat16),
            pltpu.VMEM((STAT_ROWS, n_batch, HEAD_DIM), jnp.float32),
            pltpu.VMEM((n_rows, w_o.shape[0]), jnp.float32),
            pltpu.VMEM((n_rows, d_model), jnp.bfloat16),
            *exchanged, *exchanged, *summed, *summed,
            pltpu.SemaphoreType.DMA((3,)),
            pltpu.SemaphoreType.DMA((4, n_dev - 1)),
            pltpu.SemaphoreType.DMA((4, n_dev - 1)),
        ],
        compiler_params=pltpu.CompilerParams(collective_id=0, has_side_effects=True, vmem_limit_bytes=46 * 2 ** 20),
        name="tail",
    )(pltpu.with_memory_space_constraint(stats, pltpu.VMEM), self_stat, x_mine, gain, w_o,
      *(pltpu.with_memory_space_constraint(w, pltpu.HBM) for w in (w_gate, w_up, w_down)))


def solution(mesh):
    n_dev = mesh.shape['model']
    seq_spec = P('replica', 'model', None)
    col_spec = P(None, None, 'model')
    row_spec = P(None, 'model', None)
    gain_spec = P(None, None)
    tok_spec = P('replica', None)
    cache_spec = P(None, 'replica', None, 'model', None)
    in_specs = (seq_spec, P('replica'), tok_spec, gain_spec, col_spec, col_spec, col_spec, row_spec, gain_spec, col_spec, col_spec, row_spec)
    out_specs = (tok_spec, tok_spec, cache_spec, cache_spec)

    def swap(arr, bit):
        return lax.ppermute(arr, 'model', [(i, i ^ bit) for i in range(n_dev)])

    def per_device(prompt, lengths, new_tok, norm_attn, w_q, w_k, w_v, w_o, norm_mlp, w_gate, w_up, w_down):
        my_idx = lax.axis_index('model')
        n_batch, blk, d_model = prompt.shape
        seq_len = blk * n_dev
        width = w_k.shape[2]
        heads = width // HEAD_DIM
        half = n_batch // 2
        wq = w_q[0]
        gain = norm_attn

        q1, q2, rows_h = 1, n_batch // 4, blk // 2
        a_parts, b_parts = {}, {}
        for h, name in enumerate(("0a", "0b")):
            a_parts[name], b_parts[name] = first_call(prompt, norm_attn, [(0, h * rows_h), (half, h * rows_h)], rows_h)
        from_y, from_x = {}, {}

        def send_part(step, along_y, along_x):
            from_y[step] = swap(along_y, 4)
            from_x[step] = swap(along_x, 2)

        send_part("0a", a_parts["0a"], b_parts["0a"])
        send_part("0b", a_parts["0b"], b_parts["0b"])
        order, outs_of = [], []
        for part, (lo, hi) in ((1, (q1, q2)), (2, (q2, half)), (0, (0, q1))):
            for k in range(lo, hi):
                for side in range(2):
                    order.append(side * half + k)
                    outs_of.append([(4, side * half + k, 0, blk)] + ([(2 * part - 2 + side, k - lo, 0, blk)] if part else []))
        a_parts["1"], b_parts["1"], a_parts["2"], b_parts["2"], normed = norm_call(
            prompt, gain, order, outs_of, [(q2 - q1, blk)] * 2 + [(half - q2, blk)] * 2 + [(n_batch, blk)])
        send_part("1", a_parts["1"], b_parts["1"])
        seq_pos = my_idx * blk + jnp.arange(blk)
        sel = (seq_pos[None, :] == (lengths - 1)[:, None]).astype(jnp.bfloat16)
        last_x = jnp.einsum('bs,bsd->bd', sel, prompt, preferred_element_type=jnp.float32).astype(jnp.bfloat16)
        core, cols_h = my_idx % 2, d_model // 2
        last_x = last_x + swap(last_x, 1)
        last_x = lax.dynamic_slice_in_dim(last_x, core * cols_h, cols_h, axis=1)
        last_x = (last_x + swap(last_x, 2)) + (swap(last_x, 4) + swap(last_x, 6))
        other_x = swap(last_x, 1)
        last_x = jnp.where(core == 0, jnp.concatenate([last_x, other_x], axis=1), jnp.concatenate([other_x, last_x], axis=1))
        send_part("2", a_parts["2"], b_parts["2"])
        send_part("3", b_parts["2"], a_parts["2"])
        send_part("4", normed[half:half + q2], normed[:q2])
        core_all = swap(normed, 1)

        len_rows = jnp.broadcast_to(lengths.astype(jnp.int32)[:, None], (n_batch, HEAD_DIM))
        row_tabs = rotary_tables(jnp.concatenate([lengths, lengths - 1]))
        tabs = tuple(tab.reshape(n_dev, blk, HEAD_DIM) for tab in rotary_tables(jnp.arange(seq_len)))
        x_rows = jnp.concatenate([new_tok, last_x], axis=0)
        x_mine = lax.dynamic_slice_in_dim(x_rows, my_idx * (d_model // n_dev), d_model // n_dev, axis=1)
        wk, wv, wo, last_x, len_rows, row_tabs, tabs, x_mine = lax.optimization_barrier(
            (w_k[0], w_v[0], w_o[0], last_x, len_rows, row_tabs, tabs, x_mine))
        wk, wv, wo = keep_in_vmem(wk, wv, wo)
        q_diag, k_new, v_new, self_stat = rows_call(new_tok, last_x, gain, row_tabs, wq, wk, wv)
        cache_shape = jax.ShapeDtypeStruct((n_batch, seq_len + 1, heads, HEAD_DIM), jnp.bfloat16)
        caches = [cache_shape, cache_shape, jax.ShapeDtypeStruct((2 * n_dev - 2, n_batch, 3, STAT_ROWS, HEAD_DIM), jnp.float32)]

        def run(groups, per_group, masks, batches, caches, **kw):
            return kv_call(groups, per_group, masks, batches, len_rows, tabs, wk, wv, q_diag, caches, **kw)

        def half_rows(step):
            return {"row0": rows_h * (step == "0b"), "stat_of": (n_dev - 2) * (step == "0b")}

        def after(caches, *arrays):
            out = lax.optimization_barrier((caches[2], *arrays))
            return [caches[0], caches[1], out[0]], out[1:]

        caches = run([[(arr, 0), (arr, half)] for arr in (normed, core_all)], half,
                     [[0] * 2, [1] * 2], [[0, half]] * 2, caches, new_rows=[k_new, v_new])
        diag, turned = {}, {}
        starts = {"0a": (0, half), "0b": (0, half), "1": (q1, half + q1), "2": (q2, half + q2), "3": (half + q2, q2), "4": (half, 0)}
        for step, start in starts.items():
            caches, (got_y, got_x) = after(caches, from_y[step], from_x[step])
            other_y, other_x = swap(got_y, 1), swap(got_x, 1)
            if step not in "34":
                via_x = swap(got_y, 2)
                via_y = swap(got_x, 4)
                diag[step] = (via_x, via_y)
            streams = [[(got_y, 0), (got_x, 0)], [(other_y, 0), (other_x, 0)]]
            if step in ("0a", "0b"):
                caches = run([streams[0] + streams[1]], q1, [[4, 2, 5, 3]], [[*start, *start]], caches, **half_rows(step))
            else:
                caches = run(streams, got_y.shape[0], [[4, 2], [5, 3]], [list(start)] * 2, caches)
            if step in "34":
                caches, (w_t,) = after(caches, (w_gate if step == "3" else w_up)[0].T)
                turned[step] = turn_call(w_t)
                caches, (turned[step],) = after(caches, turned[step])
        for step in ("2", "1", "0a", "0b"):
            caches, (via_y,) = after(caches, diag[step][1])
            caches, (via_x,) = after(caches, diag[step][0])
            other_y = swap(via_y, 1)
            if step == "0b":
                via_x, other_y = lax.optimization_barrier((via_x, other_y))
            other_x = swap(via_x, 1)
            start = starts[step]
            streams = [[(via_x, 0), (via_y, 0)], [(other_x, 0), (other_y, 0)]]
            if step in ("0a", "0b"):
                caches = run([streams[0] + streams[1]], q1, [[6, 6, 7, 7]], [[*start, *start]], caches, **half_rows(step))
            else:
                caches = run(streams, via_x.shape[0], [[6] * 2, [7] * 2], [list(start)] * 2, caches)

        k_cache, v_cache, stats = caches
        parts_of = [2 * n_dev - 2 if b % half < q1 else n_dev for b in range(n_batch)]
        both = tail_call(n_dev, parts_of, stats, self_stat, x_mine, norm_mlp, wo, turned["3"], turned["4"], w_down[0], n_batch)
        return both[0], both[1], k_cache[None], v_cache[None]

    return jax.shard_map(per_device, mesh=mesh, in_specs=in_specs, out_specs=out_specs, check_vma=False)
```

```python
import functools

import jax
import jax.numpy as jnp
from jax import lax
from jax.experimental import pallas as pl
from jax.experimental.pallas import tpu as pltpu
from jax.sharding import PartitionSpec as P


HEAD_DIM = 128
NEG_BIG = -1e30
STAT_ROWS = 8
NORM_ROWS = 32
COL_TILE = 256
FIRST_ROWS = 16
MESH = pl.DeviceIdType.MESH


def rotary_tables(positions):
    half_dim = HEAD_DIM // 2
    inv_freq = 10000.0 ** (-2.0 * jnp.arange(half_dim, dtype=jnp.float32) / HEAD_DIM)
    angles = positions.astype(jnp.float32)[..., None] * inv_freq
    cos_tab = jnp.cos(angles)
    sin_tab = jnp.sin(angles)
    return jnp.concatenate([cos_tab, cos_tab], axis=-1), jnp.concatenate([-sin_tab, sin_tab], axis=-1)


def load_kernel(*refs):
    n = len(refs) // 2
    sem = refs[-1]
    copies = [pltpu.make_async_copy(refs[i], refs[n + i], sem.at[i]) for i in range(n)]
    for copy in copies:
        copy.start()
    for copy in copies:
        copy.wait()


def keep_in_vmem(*arrays):
    return pl.pallas_call(
        load_kernel,
        out_shape=[pltpu.VMEM(arr.shape, arr.dtype) for arr in arrays],
        in_specs=[pl.BlockSpec(memory_space=pl.ANY)] * len(arrays),
        out_specs=[pl.BlockSpec(memory_space=pltpu.VMEM)] * len(arrays),
        scratch_shapes=[pltpu.SemaphoreType.DMA((len(arrays),))],
        compiler_params=pltpu.CompilerParams(vmem_limit_bytes=24 * 2 ** 20),
        name="keep",
    )(*(pltpu.with_memory_space_constraint(arr, pltpu.HBM) for arr in arrays))


def turn_kernel(w_ref, out_ref):
    out_ref[...] = w_ref[...].T


def turn_call(w_t):
    n, d = w_t.shape
    cols = 512
    return pl.pallas_call(
        turn_kernel,
        grid=(d // cols,),
        in_specs=[pl.BlockSpec((n, cols), lambda g: (0, g))],
        out_specs=pl.BlockSpec((cols, n), lambda g: (g, 0)),
        out_shape=jax.ShapeDtypeStruct((d, n), w_t.dtype),
        compiler_params=pltpu.CompilerParams(vmem_limit_bytes=12 * 2 ** 20),
        cost_estimate=pl.CostEstimate(flops=2 * d * n * 128, bytes_accessed=4 * d * n, transcendentals=0),
        name="turn",
    )(pltpu.with_memory_space_constraint(w_t, pltpu.HBM))


def norm_kernel(outs_of, x_ref, gain_ref, *refs):
    n_out = len(refs) - 3
    out_refs = refs[:n_out]
    ss_buf, n_buf, sems = refs[n_out:]
    step = pl.program_id(0)
    blk, d_model = x_ref.shape[1:]
    lanes = [slice(c * HEAD_DIM, (c + 1) * HEAD_DIM) for c in range(d_model // HEAD_DIM)]

    def copies(at_step):
        return [pltpu.make_async_copy(n_buf.at[at_step % 2, pl.ds(lo, rows)], out_refs[o].at[i], sems.at[at_step % 2, k])
                for k, (o, i, lo, rows) in enumerate(outs_of[at_step])]

    for at_step in range(2, len(outs_of)):
        @pl.when(step == at_step)
        def _():
            for copy in copies(at_step - 2):
                copy.wait()

    def square_rows(r, carry):
        rows = pl.ds(pl.multiple_of(r * NORM_ROWS, NORM_ROWS), NORM_ROWS)
        acc = [jnp.zeros((NORM_ROWS, HEAD_DIM), jnp.float32) for _ in range(2)]
        for c, lane in enumerate(lanes):
            xf = x_ref[0, rows, lane].astype(jnp.float32)
            acc[c % 2] += xf * xf
        ss_buf[rows, :] = acc[0] + acc[1]
        return carry

    lax.fori_loop(0, blk // NORM_ROWS, square_rows, 0)
    total = jnp.sum(ss_buf[...], axis=-1, keepdims=True)
    ss_buf[...] = jnp.broadcast_to(lax.rsqrt(total / d_model + 1e-5), (blk, HEAD_DIM))
    slot = lax.rem(step, 2)

    def norm_rows(r, carry):
        rows = pl.ds(pl.multiple_of(r * NORM_ROWS, NORM_ROWS), NORM_ROWS)
        inv_rms = ss_buf[rows, :]
        for lane in lanes:
            xf = x_ref[0, rows, lane].astype(jnp.float32)
            n_buf[slot, rows, lane] = (xf * inv_rms * gain_ref[:, lane].astype(jnp.float32)).astype(jnp.bfloat16)
        return carry

    lax.fori_loop(0, blk // NORM_ROWS, norm_rows, 0)
    for at_step in range(len(outs_of)):
        @pl.when(step == at_step)
        def _():
            for copy in copies(at_step):
                copy.start()
            if at_step == len(outs_of) - 1:
                for copy in copies(at_step):
                    copy.wait()
                if at_step >= 1:
                    for copy in copies(at_step - 1):
                        copy.wait()


def first_kernel(places, rows, x_hbm, gain_hbm, *refs):
    n = len(places)
    out_refs = refs[:n]
    x_buf, gain_ref, sem = refs[n:]
    d_model = x_hbm.shape[2]
    loads = [pltpu.make_async_copy(x_hbm.at[bat, pl.ds(row0, rows)], x_buf.at[i], sem.at[i]) for i, (bat, row0) in enumerate(places)]
    loads.append(pltpu.make_async_copy(gain_hbm, gain_ref, sem.at[n]))
    for load in loads:
        load.start()
    loads[n].wait()
    lanes = [slice(c * HEAD_DIM, (c + 1) * HEAD_DIM) for c in range(d_model // HEAD_DIM)]
    for i in range(n):
        loads[i].wait()

        def norm_rows(r, carry):
            at = pl.ds(pl.multiple_of(r * FIRST_ROWS, FIRST_ROWS), FIRST_ROWS)
            acc = [jnp.zeros((FIRST_ROWS, HEAD_DIM), jnp.float32) for _ in range(2)]
            for c, lane in enumerate(lanes):
                xf = x_buf[i, at, lane].astype(jnp.float32)
                acc[c % 2] += xf * xf
            inv_rms = lax.rsqrt(jnp.sum(acc[0] + acc[1], axis=-1, keepdims=True) / d_model + 1e-5)
            for lane in lanes:
                xf = x_buf[i, at, lane].astype(jnp.float32)
                out_refs[i][0, at, lane] = (xf * inv_rms * gain_ref[:, lane].astype(jnp.float32)).astype(jnp.bfloat16)
            return carry

        lax.fori_loop(0, rows // FIRST_ROWS, norm_rows, 0, unroll=True)


def first_call(x, gain, places, rows):
    d_model = x.shape[2]
    return pl.pallas_call(
        functools.partial(first_kernel, places, rows),
        out_shape=[pltpu.VMEM((1, rows, d_model), jnp.bfloat16)] * len(places),
        in_specs=[pl.BlockSpec(memory_space=pl.ANY)] * 2,
        out_specs=[pl.BlockSpec(memory_space=pltpu.VMEM)] * len(places),
        scratch_shapes=[
            pltpu.VMEM((len(places), rows, d_model), jnp.bfloat16),
            pltpu.VMEM(gain.shape, gain.dtype),
            pltpu.SemaphoreType.DMA((len(places) + 1,)),
        ],
        compiler_params=pltpu.CompilerParams(vmem_limit_bytes=8 * 2 ** 20),
        cost_estimate=pl.CostEstimate(flops=len(places) * rows * d_model * 8, bytes_accessed=len(places) * rows * d_model * 4, transcendentals=0),
        name="first_rows",
    )(*(pltpu.with_memory_space_constraint(a, pltpu.HBM) for a in (x, gain)))


def norm_call(x, gain, order, outs_of, shapes, blk=None, row_block=0):
    d_model = x.shape[2]
    blk = blk or x.shape[1]

    def prompt_of(g):
        idx = jnp.int32(order[-1])
        for k in range(len(order) - 1):
            idx = jnp.where(g == k, order[k], idx)
        return idx

    return pl.pallas_call(
        functools.partial(norm_kernel, outs_of),
        grid=(len(order),),
        in_specs=[pl.BlockSpec((1, blk, d_model), lambda g: (prompt_of(g), row_block, 0)),
                  pl.BlockSpec((1, d_model), lambda g: (0, 0))],
        out_specs=[pl.BlockSpec(memory_space=pl.ANY)] * len(shapes),
        out_shape=[jax.ShapeDtypeStruct((*shape, d_model), jnp.bfloat16) for shape in shapes],
        scratch_shapes=[
            pltpu.VMEM((blk, HEAD_DIM), jnp.float32),
            pltpu.VMEM((2, blk, d_model), jnp.bfloat16),
            pltpu.SemaphoreType.DMA((2, max(len(o) for o in outs_of))),
        ],
        compiler_params=pltpu.CompilerParams(vmem_limit_bytes=24 * 2 ** 20),
        cost_estimate=pl.CostEstimate(flops=len(order) * blk * d_model * 8, bytes_accessed=len(order) * blk * d_model * 6, transcendentals=0),
        name="norm_rows",
    )(pltpu.with_memory_space_constraint(x, pltpu.HBM), gain)


def rows_kernel(new_ref, last_ref, gain_ref, cos_ref, sin_ref, wq_hbm, wk, wv, q_ref, k_ref, v_ref, st_ref, wq, q_buf, sem):
    load = pltpu.make_async_copy(wq_hbm, wq, sem)
    load.start()
    n_batch = new_ref.shape[0]
    heads = wk.shape[1] // HEAD_DIM
    xf = jnp.concatenate([new_ref[...].astype(jnp.float32), last_ref[...].astype(jnp.float32)], axis=0)
    inv_rms = lax.rsqrt(jnp.mean(xf * xf, axis=-1, keepdims=True) + 1e-5)
    normed = (xf * inv_rms * gain_ref[...].astype(jnp.float32)).astype(jnp.bfloat16)
    k_all = jnp.dot(normed, wk[...], preferred_element_type=jnp.float32)[:n_batch]
    v_all = jnp.dot(normed, wv[...], preferred_element_type=jnp.float32)[:n_batch].astype(jnp.bfloat16)
    load.wait()
    q_all = jnp.dot(normed, wq[...], preferred_element_type=jnp.float32)
    q_buf[...] = jnp.zeros_like(q_buf)
    k_rot = []
    for h in range(heads):
        cols = slice(h * HEAD_DIM, (h + 1) * HEAD_DIM)
        qh = q_all[:, cols]
        qh = (qh * cos_ref[...] + pltpu.roll(qh, HEAD_DIM // 2, 1) * sin_ref[...]).astype(jnp.bfloat16).astype(jnp.float32)
        kh = k_all[:, cols]
        kh = (kh * cos_ref[:n_batch, :] + pltpu.roll(kh, HEAD_DIM // 2, 1) * sin_ref[:n_batch, :]).astype(jnp.bfloat16)
        k_rot.append(kh)
        score = jnp.sum(qh[:n_batch] * kh.astype(jnp.float32), axis=-1, keepdims=True) * (HEAD_DIM ** -0.5)
        zero = jnp.zeros((n_batch, HEAD_DIM), jnp.float32)
        for t in range(2):
            row = 2 * h + t
            q_buf[:, row, cols] = qh[t * n_batch:(t + 1) * n_batch]
            st_ref[0, :, row, :] = v_all[:, cols].astype(jnp.float32) if t == 0 else zero
            st_ref[1, :, row, :] = zero + score if t == 0 else zero + NEG_BIG
            st_ref[2, :, row, :] = zero + 1.0 if t == 0 else zero
    q_ref[...] = q_buf[...].astype(jnp.bfloat16)
    k_ref[...] = jnp.concatenate(k_rot, axis=1).reshape(n_batch, heads, HEAD_DIM)
    v_ref[...] = v_all.reshape(n_batch, heads, HEAD_DIM)


def rows_call(new_tok, last_x, gain, row_tabs, w_q, w_k, w_v):
    n_batch = new_tok.shape[0]
    width = w_q.shape[1]
    heads = width // HEAD_DIM
    vmem = pl.BlockSpec(memory_space=pltpu.VMEM)
    return pl.pallas_call(
        rows_kernel,
        out_shape=[
            jax.ShapeDtypeStruct((n_batch, STAT_ROWS, width), jnp.bfloat16),
            jax.ShapeDtypeStruct((n_batch, heads, HEAD_DIM), jnp.bfloat16),
            jax.ShapeDtypeStruct((n_batch, heads, HEAD_DIM), jnp.bfloat16),
            jax.ShapeDtypeStruct((3, n_batch, STAT_ROWS, HEAD_DIM), jnp.float32),
        ],
        in_specs=[vmem] * 5 + [pl.BlockSpec(memory_space=pl.ANY)] + [vmem] * 2,
        out_specs=[vmem] * 4,
        scratch_shapes=[
            pltpu.VMEM(w_q.shape, jnp.bfloat16),
            pltpu.VMEM((n_batch, STAT_ROWS, width), jnp.float32),
            pltpu.SemaphoreType.DMA,
        ],
        compiler_params=pltpu.CompilerParams(vmem_limit_bytes=24 * 2 ** 20),
        cost_estimate=pl.CostEstimate(flops=2 * 2 * n_batch * 3 * w_q.shape[0] * width, bytes_accessed=2 * w_q.size, transcendentals=0),
        name="query_rows",
    )(new_tok, last_x, gain, *row_tabs, pltpu.with_memory_space_constraint(w_q, pltpu.HBM), w_k, w_v)


def when(condition):
    if isinstance(condition, bool):
        return lambda body: body() if condition else None
    return pl.when(condition)


def by_group(group, values):
    if isinstance(group, int):
        return values[group]
    out = values[-1]
    for p in range(len(values) - 1):
        out = jnp.where(group == p, values[p], out)
    return out


def kv_kernel(n_in, n_steps, masks, batches, firsts, row0, stat_of, with_new, *refs):
    n_groups = len(masks)
    n_arr = n_in * n_groups
    x_refs = refs[:n_arr]
    cos_ref, sin_ref, len_ref, wk, wv, q_ref = refs[n_arr:n_arr + 6]
    rest = refs[n_arr + 6:]
    if with_new:
        new_refs = rest[:2]
        rest = rest[2:]
    else:
        rest = rest[3:]
    kc_ref, vc_ref, st_ref, x_buf, k_buf, v_buf, k_out, v_out, s_out, x_sem, sems, s_sem = rest[:12]
    me = lax.axis_index("model")
    step = pl.program_id(0) if n_steps > 1 else 0
    slot = lax.rem(step, 2) if n_steps > 1 else 0
    per_group = n_steps // n_groups
    blk = x_buf.shape[2]
    shard_rows = cos_ref.shape[1]
    width = wk.shape[1]
    heads = width // HEAD_DIM
    n_tok = n_in * blk

    def x_copies(at_step, which, group):
        local = at_step - group * per_group
        return [pltpu.make_async_copy(x_refs[group * n_in + i].at[firsts[group][i] + local],
                                      x_buf.at[which, i], x_sem.at[which, i]) for i in range(n_in)]

    def start_x(at_step, which):
        for group in range(n_groups):
            @when(at_step // per_group == group)
            def _(group=group):
                for copy in x_copies(at_step, which, group):
                    copy.start()

    def place(i, at_step):
        group = at_step // per_group
        mask = by_group(group, [m[i] for m in masks])
        shard = sum(lax.rem(me // bit + mask // bit, 2) * bit for bit in (1, 2, 4))
        return shard, by_group(group, [b[i] for b in batches]) + at_step % per_group, mask

    def out_copies(which, at_step):
        copies = []
        for i in range(n_in):
            shard, bat, _ = place(i, at_step)
            rows = pl.ds(shard * shard_rows + row0, blk)
            copies.append(pltpu.make_async_copy(k_out.at[which, i], kc_ref.at[bat, rows], sems.at[which, i, 0]))
            copies.append(pltpu.make_async_copy(v_out.at[which, i], vc_ref.at[bat, rows], sems.at[which, i, 1]))
        return copies

    def new_copies():
        return [pltpu.make_async_copy(src.at[pl.ds(b, 1)], dst.at[b, pl.ds(dst.shape[1] - 1, 1)], rest[12].at[idx, b])
                for idx, (src, dst) in enumerate(zip(new_refs, (kc_ref, vc_ref))) for b in range(src.shape[0])]

    @when(step == 0)
    def _():
        start_x(step, slot)
        if with_new:
            for copy in new_copies():
                copy.start()

    @when(step + 1 < n_steps)
    def _():
        start_x(step + 1, 1 - slot)

    @when(step >= 2)
    def _():
        for copy in out_copies(slot, step - 2):
            copy.wait()

    for copy in x_copies(0, slot, 0):
        copy.wait()
    x_rows = x_buf.at[slot]

    def col_tile(c, carry):
        cols = pl.ds(pl.multiple_of(c * COL_TILE, COL_TILE), COL_TILE) if n_steps > 1 else slice(c * COL_TILE, (c + 1) * COL_TILE)
        normed = x_rows[...].reshape(n_tok, x_buf.shape[3])
        kf = jnp.dot(normed, wk[:, cols], preferred_element_type=jnp.float32)
        vf = jnp.dot(normed, wv[:, cols], preferred_element_type=jnp.float32)
        v_buf[:, cols] = vf.astype(jnp.bfloat16)
        parts = []
        for i in range(n_in):
            shard = place(i, step)[0]
            cos_tab = cos_ref[shard, row0:row0 + blk]
            sin_tab = sin_ref[shard, row0:row0 + blk]
            halves = []
            for h in range(COL_TILE // HEAD_DIM):
                kh = kf[i * blk:(i + 1) * blk, h * HEAD_DIM:(h + 1) * HEAD_DIM]
                halves.append(kh * cos_tab + pltpu.roll(kh, HEAD_DIM // 2, 1) * sin_tab)
            parts.append(jnp.concatenate(halves, axis=1))
        k_buf[:, cols] = jnp.concatenate(parts, axis=0).astype(jnp.bfloat16)
        return carry

    if n_steps > 1:
        lax.fori_loop(0, width // COL_TILE, col_tile, 0)
    else:
        for c in range(width // COL_TILE):
            col_tile(c, 0)

    for i in range(n_in):
        k_out[slot, i] = k_buf[i * blk:(i + 1) * blk, :].reshape(blk, heads, HEAD_DIM)
        v_out[slot, i] = v_buf[i * blk:(i + 1) * blk, :].reshape(blk, heads, HEAD_DIM)
    for copy in out_copies(slot, step):
        copy.start()

    head_of_row = lax.broadcasted_iota(jnp.int32, (STAT_ROWS, HEAD_DIM), 0) // (STAT_ROWS // heads)
    probs = []
    for i in range(n_in):
        shard, bat, _ = place(i, step)
        scores = lax.dot_general(q_ref[bat], k_buf[i * blk:(i + 1) * blk, :], (((1,), (1,)), ((), ())),
                                 preferred_element_type=jnp.float32) * (HEAD_DIM ** -0.5)
        pos = shard * shard_rows + row0 + lax.broadcasted_iota(jnp.int32, scores.shape, 1)
        visible = pos < len_ref[pl.ds(bat, 1), :blk]
        scores = jnp.where(visible, scores, NEG_BIG)
        blk_max = jnp.max(scores, axis=-1, keepdims=True)
        prob = jnp.where(visible, jnp.exp(scores - blk_max), 0.0)
        probs.append((blk_max, prob))
    for i, (blk_max, prob) in enumerate(probs):
        full = jnp.dot(prob.astype(jnp.bfloat16), v_buf[i * blk:(i + 1) * blk, :], preferred_element_type=jnp.float32)
        acc = jnp.zeros((STAT_ROWS, HEAD_DIM), jnp.float32)
        for h in range(heads):
            acc = jnp.where(head_of_row == h, full[:, h * HEAD_DIM:(h + 1) * HEAD_DIM], acc)
        s_out[i, 0] = acc
        s_out[i, 1] = jnp.broadcast_to(blk_max, (STAT_ROWS, HEAD_DIM))
        s_out[i, 2] = jnp.broadcast_to(jnp.sum(prob, axis=-1, keepdims=True), (STAT_ROWS, HEAD_DIM))
    stat_copies = []
    for i in range(n_in):
        _, bat, mask = place(i, step)
        stat_copies.append(pltpu.make_async_copy(s_out.at[i], st_ref.at[mask + stat_of, bat], s_sem.at[i]))
        stat_copies[-1].start()
    for copy in stat_copies:
        copy.wait()

    @when(step == n_steps - 1)
    def _():
        for copy in out_copies(slot, step):
            copy.wait()
        if with_new:
            for copy in new_copies():
                copy.wait()
        if n_steps > 1:
            for copy in out_copies(1 - slot, step - 1):
                copy.wait()


def kv_call(groups, per_group, masks, batches, lengths, tabs, w_k, w_v, q_diag, caches, new_rows=None, row0=0, stat_of=0):
    n_groups = len(groups)
    n_in = len(groups[0])
    n_steps = n_groups * per_group
    cos_tab, sin_tab = tabs
    blk, d_model = groups[0][0][0].shape[1:]
    width = w_k.shape[1]
    heads = width // HEAD_DIM
    any_spec = pl.BlockSpec(memory_space=pl.ANY)
    operands = [arr for group in groups for arr, _ in group]
    in_specs = [any_spec] * len(operands) + [pl.BlockSpec(memory_space=pltpu.VMEM)] * 6
    operands += [cos_tab, sin_tab, lengths, w_k, w_v, q_diag]
    with_new = new_rows is not None
    if with_new:
        operands += new_rows
        in_specs += [any_spec] * 2
        aliases = {}
    else:
        operands += [*caches[:2], pltpu.with_memory_space_constraint(caches[2], pltpu.VMEM)]
        in_specs += [any_spec] * 3
        aliases = {len(operands) - 3: 0, len(operands) - 2: 1, len(operands) - 1: 2}
    tokens = n_in * blk
    n_batch = q_diag.shape[0]
    slots = min(n_steps, 2)
    return pl.pallas_call(
        functools.partial(kv_kernel, n_in, n_steps, masks, batches, [[first for _, first in group] for group in groups], row0, stat_of, with_new),
        grid=(n_steps,) if n_steps > 1 else (),
        in_specs=in_specs,
        out_specs=[any_spec] * 3,
        scratch_shapes=[
            pltpu.VMEM((slots, n_in, blk, d_model), jnp.bfloat16),
            pltpu.VMEM((tokens, width), jnp.bfloat16),
            pltpu.VMEM((tokens, width), jnp.bfloat16),
            pltpu.VMEM((slots, n_in, blk, heads, HEAD_DIM), jnp.bfloat16),
            pltpu.VMEM((slots, n_in, blk, heads, HEAD_DIM), jnp.bfloat16),
            pltpu.VMEM((n_in, 3, STAT_ROWS, HEAD_DIM), jnp.float32),
            pltpu.SemaphoreType.DMA((slots, n_in)),
            pltpu.SemaphoreType.DMA((slots, n_in, 2)),
            pltpu.SemaphoreType.DMA((n_in,)),
        ] + [pltpu.SemaphoreType.DMA((2, n_batch))] * with_new,
        out_shape=[*(jax.ShapeDtypeStruct(c.shape, c.dtype) for c in caches[:2]), pltpu.VMEM(caches[2].shape, caches[2].dtype)],
        input_output_aliases=aliases,
        compiler_params=pltpu.CompilerParams(vmem_limit_bytes=20 * 2 ** 20),
        cost_estimate=pl.CostEstimate(flops=4 * n_steps * tokens * d_model * width, bytes_accessed=2 * n_steps * tokens * (d_model + 2 * width), transcendentals=0),
        name="kv_chunk",
    )(*operands)


def tail_kernel(n_dev, parts_of, stv, self_ref, xs_ref, gain_ref, wo, wg_hbm, wu_hbm, wd_hbm, out_ref,
                wg, wu, wd, rows, a_buf, n_buf, ps1, pr1, ps2, pr2, xo1, xg1, xo2, xg2, w_sem, send_sem, recv_sem):
    me = lax.axis_index("model")
    n_batch = out_ref.shape[1]
    n_rows = 2 * n_batch
    d_model = out_ref.shape[2]
    cols = d_model // n_dev
    heads = STAT_ROWS // 2
    loads = [pltpu.make_async_copy(src, dst, w_sem.at[i]) for i, (src, dst) in enumerate(((wg_hbm, wg), (wu_hbm, wu), (wd_hbm, wd)))]
    for load in loads:
        load.start()
    barrier = pltpu.get_barrier_semaphore()

    def peer_of(mask):
        return sum(lax.rem(me // bit + mask // bit, 2) * bit for bit in (1, 2, 4))

    far_first = ((6, 7), (2, 3, 4, 5), (1,))
    for mask in sum(far_first, ()):
        pl.semaphore_signal(barrier, inc=1, device_id={"model": peer_of(mask)}, device_id_type=MESH)

    def send(phase, mask, src, dst):
        return pltpu.make_async_remote_copy(
            src_ref=src, dst_ref=dst, send_sem=send_sem.at[phase, mask - 1], recv_sem=recv_sem.at[phase, mask - 1],
            device_id={"model": peer_of(mask)}, device_id_type=MESH)

    for b in range(n_batch):
        top = self_ref[1, b]
        for j in range(parts_of[b]):
            top = jnp.maximum(top, stv[j, b, 1])
        scale = jnp.exp(self_ref[1, b] - top)
        den = scale * self_ref[2, b]
        num = scale * self_ref[0, b]
        for j in range(parts_of[b]):
            scale = jnp.exp(stv[j, b, 1] - top)
            den += scale * stv[j, b, 2]
            num += scale * stv[j, b, 0]
        rows[:, b, :] = num / den
    for h in range(heads):
        for t in range(2):
            a_buf[t * n_batch:(t + 1) * n_batch, h * HEAD_DIM:(h + 1) * HEAD_DIM] = rows[2 * h + t]
    att = a_buf[...].astype(jnp.bfloat16)

    def exchange(phase, base, copies, pr, xo, xg):
        total = base
        for copy, mask in reversed(copies):
            copy.wait_recv()
            total = total + pr[mask - 1]
        xo[...] = total.astype(jnp.bfloat16)
        xg[me] = xo[...]
        outs = []
        for mask in sum(far_first, ()):
            outs.append(send(phase + 1, mask, xo, xg.at[me]))
            outs[-1].start()
        for out in outs:
            out.wait_recv()
        return [copy for copy, _ in copies] + outs

    def col_block(p):
        return pl.ds(pl.multiple_of(p * cols, cols), cols)

    part = jnp.dot(att, wo[...], preferred_element_type=jnp.float32)
    for j in range(n_dev):
        ps1[j] = part[:, j * cols:(j + 1) * cols]
    pl.semaphore_wait(barrier, n_dev - 1)
    copies = []
    for mask in sum(far_first, ()):
        copies.append((send(0, mask, ps1.at[peer_of(mask)], pr1.at[mask - 1]), mask))
        copies[-1][0].start()
    sent = exchange(0, xs_ref[...].astype(jnp.float32) + ps1[me], copies, pr1, xo1, xg1)
    sq = jnp.zeros((n_rows, 1), jnp.float32)
    for j in range(n_dev):
        xf = xg1[j].astype(jnp.float32)
        sq += jnp.sum(xf * xf, axis=-1, keepdims=True)
    inv_rms = lax.rsqrt(sq / d_model + 1e-5)
    for j in range(n_dev):
        at = slice(j * cols, (j + 1) * cols)
        n_buf[:, at] = (xg1[j].astype(jnp.float32) * inv_rms * gain_ref[:, at].astype(jnp.float32)).astype(jnp.bfloat16)
    loads[0].wait()
    loads[1].wait()
    gate = jnp.dot(n_buf[...], wg[...], preferred_element_type=jnp.float32)
    up = jnp.dot(n_buf[...], wu[...], preferred_element_type=jnp.float32)
    mid = (gate * (1.0 / (1.0 + jnp.exp(-gate))) * up).astype(jnp.bfloat16)
    loads[2].wait()
    copies = []
    for group in far_first:
        for mask in group:
            ps2[mask] = jnp.dot(mid, wd[:, col_block(peer_of(mask))], preferred_element_type=jnp.float32)
        if group == far_first[-1]:
            ps2[0] = jnp.dot(mid, wd[:, col_block(me)], preferred_element_type=jnp.float32)
        for mask in group:
            copies.append((send(2, mask, ps2.at[mask], pr2.at[mask - 1]), mask))
            copies[-1][0].start()
    sent += exchange(2, xo1[...].astype(jnp.float32) + ps2[0], copies, pr2, xo2, xg2)
    for j in range(n_dev):
        at = slice(j * cols, (j + 1) * cols)
        out_ref[0, :, at] = xg2[j, :n_batch]
        out_ref[1, :, at] = xg2[j, n_batch:]
    for copy in sent:
        copy.wait_send()


def tail_call(n_dev, parts_of, stats, self_stat, x_mine, gain, w_o, w_gate, w_up, w_down, n_batch):
    n_rows, cols = x_mine.shape
    d_model = w_o.shape[1]
    vmem = pl.BlockSpec(memory_space=pltpu.VMEM)
    any_spec = pl.BlockSpec(memory_space=pl.ANY)
    exchanged = [pltpu.VMEM((n_dev, n_rows, cols), jnp.float32), pltpu.VMEM((n_dev - 1, n_rows, cols), jnp.float32)]
    summed = [pltpu.VMEM((n_rows, cols), jnp.bfloat16), pltpu.VMEM((n_dev, n_rows, cols), jnp.bfloat16)]
    return pl.pallas_call(
        functools.partial(tail_kernel, n_dev, parts_of),
        out_shape=jax.ShapeDtypeStruct((2, n_batch, d_model), jnp.bfloat16),
        in_specs=[vmem] * 5 + [any_spec] * 3,
        out_specs=vmem,
        scratch_shapes=[
            pltpu.VMEM(w_gate.shape, jnp.bfloat16),
            pltpu.VMEM(w_up.shape, jnp.bfloat16),
            pltpu.VMEM(w_down.shape, jnp.bfloat16),
            pltpu.VMEM((STAT_ROWS, n_batch, HEAD_DIM), jnp.float32),
            pltpu.VMEM((n_rows, w_o.shape[0]), jnp.float32),
            pltpu.VMEM((n_rows, d_model), jnp.bfloat16),
            *exchanged, *exchanged, *summed, *summed,
            pltpu.SemaphoreType.DMA((3,)),
            pltpu.SemaphoreType.DMA((4, n_dev - 1)),
            pltpu.SemaphoreType.DMA((4, n_dev - 1)),
        ],
        compiler_params=pltpu.CompilerParams(collective_id=0, has_side_effects=True, vmem_limit_bytes=46 * 2 ** 20),
        name="tail",
    )(pltpu.with_memory_space_constraint(stats, pltpu.VMEM), self_stat, x_mine, gain, w_o,
      *(pltpu.with_memory_space_constraint(w, pltpu.HBM) for w in (w_gate, w_up, w_down)))


def solution(mesh):
    n_dev = mesh.shape['model']
    seq_spec = P('replica', 'model', None)
    col_spec = P(None, None, 'model')
    row_spec = P(None, 'model', None)
    gain_spec = P(None, None)
    tok_spec = P('replica', None)
    cache_spec = P(None, 'replica', None, 'model', None)
    in_specs = (seq_spec, P('replica'), tok_spec, gain_spec, col_spec, col_spec, col_spec, row_spec, gain_spec, col_spec, col_spec, row_spec)
    out_specs = (tok_spec, tok_spec, cache_spec, cache_spec)

    def swap(arr, bit):
        return lax.ppermute(arr, 'model', [(i, i ^ bit) for i in range(n_dev)])

    def per_device(prompt, lengths, new_tok, norm_attn, w_q, w_k, w_v, w_o, norm_mlp, w_gate, w_up, w_down):
        my_idx = lax.axis_index('model')
        n_batch, blk, d_model = prompt.shape
        seq_len = blk * n_dev
        width = w_k.shape[2]
        heads = width // HEAD_DIM
        half = n_batch // 2
        wq = w_q[0]
        gain = norm_attn

        q1, q2 = 1, n_batch // 4
        pieces = {"0b": (blk - 3 * blk // 8, 3 * blk // 8), "0a": (0, blk - 3 * blk // 8)}
        a_parts, b_parts = {}, {}
        for name, (lo, rows) in pieces.items():
            a_parts[name], b_parts[name] = first_call(prompt, norm_attn, [(0, lo), (half, lo)], rows)
        from_y, from_x = {}, {}

        def send_part(step, along_y, along_x):
            from_y[step] = swap(along_y, 4)
            from_x[step] = swap(along_x, 2)

        for name in pieces:
            send_part(name, a_parts[name], b_parts[name])
        order, outs_of = [], []
        for part, (lo, hi) in ((1, (q1, q2)), (2, (q2, half)), (0, (0, q1))):
            for k in range(lo, hi):
                for side in range(2):
                    order.append(side * half + k)
                    outs_of.append([(4, side * half + k, 0, blk)] + ([(2 * part - 2 + side, k - lo, 0, blk)] if part else []))
        a_parts["1"], b_parts["1"], a_parts["2"], b_parts["2"], normed = norm_call(
            prompt, gain, order, outs_of, [(q2 - q1, blk)] * 2 + [(half - q2, blk)] * 2 + [(n_batch, blk)])
        send_part("1", a_parts["1"], b_parts["1"])
        seq_pos = my_idx * blk + jnp.arange(blk)
        sel = (seq_pos[None, :] == (lengths - 1)[:, None]).astype(jnp.bfloat16)
        last_x = jnp.einsum('bs,bsd->bd', sel, prompt, preferred_element_type=jnp.float32).astype(jnp.bfloat16)
        core, cols_h = my_idx % 2, d_model // 2
        last_x = last_x + swap(last_x, 1)
        last_x = lax.dynamic_slice_in_dim(last_x, core * cols_h, cols_h, axis=1)
        last_x = (last_x + swap(last_x, 2)) + (swap(last_x, 4) + swap(last_x, 6))
        other_x = swap(last_x, 1)
        last_x = jnp.where(core == 0, jnp.concatenate([last_x, other_x], axis=1), jnp.concatenate([other_x, last_x], axis=1))
        send_part("2", a_parts["2"], b_parts["2"])
        send_part("3", b_parts["2"], a_parts["2"])
        send_part("4", normed[half:half + q2], normed[:q2])
        core_all = swap(normed, 1)

        len_rows = jnp.broadcast_to(lengths.astype(jnp.int32)[:, None], (n_batch, HEAD_DIM))
        row_tabs = rotary_tables(jnp.concatenate([lengths, lengths - 1]))
        tabs = tuple(tab.reshape(n_dev, blk, HEAD_DIM) for tab in rotary_tables(jnp.arange(seq_len)))
        x_rows = jnp.concatenate([new_tok, last_x], axis=0)
        x_mine = lax.dynamic_slice_in_dim(x_rows, my_idx * (d_model // n_dev), d_model // n_dev, axis=1)
        wk, wv, wo, last_x, len_rows, row_tabs, tabs, x_mine = lax.optimization_barrier(
            (w_k[0], w_v[0], w_o[0], last_x, len_rows, row_tabs, tabs, x_mine))
        wk, wv, wo = keep_in_vmem(wk, wv, wo)
        q_diag, k_new, v_new, self_stat = rows_call(new_tok, last_x, gain, row_tabs, wq, wk, wv)
        cache_shape = jax.ShapeDtypeStruct((n_batch, seq_len + 1, heads, HEAD_DIM), jnp.bfloat16)
        caches = [cache_shape, cache_shape, jax.ShapeDtypeStruct((2 * n_dev - 2, n_batch, 3, STAT_ROWS, HEAD_DIM), jnp.float32)]

        def run(groups, per_group, masks, batches, caches, **kw):
            return kv_call(groups, per_group, masks, batches, len_rows, tabs, wk, wv, q_diag, caches, **kw)

        def piece_of(step):
            return {"row0": pieces[step][0], "stat_of": (n_dev - 2) * (step == "0b")}

        def after(caches, *arrays):
            out = lax.optimization_barrier((caches[2], *arrays))
            return [caches[0], caches[1], out[0]], out[1:]

        caches = run([[(arr, 0), (arr, half)] for arr in (normed, core_all)], half,
                     [[0] * 2, [1] * 2], [[0, half]] * 2, caches, new_rows=[k_new, v_new])
        diag, turned = {}, {}
        starts = {"0b": (0, half), "0a": (0, half), "1": (q1, half + q1), "2": (q2, half + q2), "3": (half + q2, q2), "4": (half, 0)}
        for step, start in starts.items():
            caches, (got_y, got_x) = after(caches, from_y[step], from_x[step])
            other_y, other_x = swap(got_y, 1), swap(got_x, 1)
            if step not in "34":
                via_x = swap(got_y, 2)
                via_y = swap(got_x, 4)
                diag[step] = (via_x, via_y)
            streams = [[(got_y, 0), (got_x, 0)], [(other_y, 0), (other_x, 0)]]
            if step in ("0a", "0b"):
                caches = run([streams[0] + streams[1]], q1, [[4, 2, 5, 3]], [[*start, *start]], caches, **piece_of(step))
            else:
                caches = run(streams, got_y.shape[0], [[4, 2], [5, 3]], [list(start)] * 2, caches)
            if step in "34":
                caches, (w_t,) = after(caches, (w_gate if step == "3" else w_up)[0].T)
                turned[step] = turn_call(w_t)
                caches, (turned[step],) = after(caches, turned[step])
        for step in ("2", "1", "0a", "0b"):
            caches, (via_y,) = after(caches, diag[step][1])
            caches, (via_x,) = after(caches, diag[step][0])
            other_y = swap(via_y, 1)
            other_x = swap(via_x, 1)
            start = starts[step]
            streams = [[(via_x, 0), (via_y, 0)], [(other_x, 0), (other_y, 0)]]
            if step in ("0a", "0b"):
                caches = run([streams[0] + streams[1]], q1, [[6, 6, 7, 7]], [[*start, *start]], caches, **piece_of(step))
            else:
                caches = run(streams, via_x.shape[0], [[6] * 2, [7] * 2], [list(start)] * 2, caches)

        k_cache, v_cache, stats = caches
        parts_of = [2 * n_dev - 2 if b % half < q1 else n_dev for b in range(n_batch)]
        both = tail_call(n_dev, parts_of, stats, self_stat, x_mine, norm_mlp, wo, turned["3"], turned["4"], w_down[0], n_batch)
        return both[0], both[1], k_cache[None], v_cache[None]

    return jax.shard_map(per_device, mesh=mesh, in_specs=in_specs, out_specs=out_specs, check_vma=False)
```

```python
import functools

import jax
import jax.numpy as jnp
from jax import lax
from jax.experimental import pallas as pl
from jax.experimental.pallas import tpu as pltpu
from jax.sharding import PartitionSpec as P


HEAD_DIM = 128
NEG_BIG = -1e30
STAT_ROWS = 8
NORM_ROWS = 32
COL_TILE = 256
MESH = pl.DeviceIdType.MESH


def rotary_tables(positions):
    half_dim = HEAD_DIM // 2
    inv_freq = 10000.0 ** (-2.0 * jnp.arange(half_dim, dtype=jnp.float32) / HEAD_DIM)
    angles = positions.astype(jnp.float32)[..., None] * inv_freq
    cos_tab = jnp.cos(angles)
    sin_tab = jnp.sin(angles)
    return jnp.concatenate([cos_tab, cos_tab], axis=-1), jnp.concatenate([-sin_tab, sin_tab], axis=-1)


def load_kernel(*refs):
    n = len(refs) // 2
    sem = refs[-1]
    copies = [pltpu.make_async_copy(refs[i], refs[n + i], sem.at[i]) for i in range(n)]
    for copy in copies:
        copy.start()
    for copy in copies:
        copy.wait()


def keep_in_vmem(*arrays):
    return pl.pallas_call(
        load_kernel,
        out_shape=[pltpu.VMEM(arr.shape, arr.dtype) for arr in arrays],
        in_specs=[pl.BlockSpec(memory_space=pl.ANY)] * len(arrays),
        out_specs=[pl.BlockSpec(memory_space=pltpu.VMEM)] * len(arrays),
        scratch_shapes=[pltpu.SemaphoreType.DMA((len(arrays),))],
        compiler_params=pltpu.CompilerParams(vmem_limit_bytes=24 * 2 ** 20),
        name="keep",
    )(*(pltpu.with_memory_space_constraint(arr, pltpu.HBM) for arr in arrays))


def turn_kernel(w_ref, out_ref):
    out_ref[...] = w_ref[...].T


def turn_call(w_t):
    n, d = w_t.shape
    cols = 512
    return pl.pallas_call(
        turn_kernel,
        grid=(d // cols,),
        in_specs=[pl.BlockSpec((n, cols), lambda g: (0, g))],
        out_specs=pl.BlockSpec((cols, n), lambda g: (g, 0)),
        out_shape=jax.ShapeDtypeStruct((d, n), w_t.dtype),
        compiler_params=pltpu.CompilerParams(vmem_limit_bytes=12 * 2 ** 20),
        cost_estimate=pl.CostEstimate(flops=2 * d * n * 128, bytes_accessed=4 * d * n, transcendentals=0),
        name="turn",
    )(pltpu.with_memory_space_constraint(w_t, pltpu.HBM))


def norm_kernel(outs_of, x_ref, gain_ref, *refs):
    n_out = len(refs) - 3
    out_refs = refs[:n_out]
    ss_buf, n_buf, sems = refs[n_out:]
    step = pl.program_id(0)
    blk, d_model = x_ref.shape[1:]
    lanes = [slice(c * HEAD_DIM, (c + 1) * HEAD_DIM) for c in range(d_model // HEAD_DIM)]

    def copies(at_step):
        return [pltpu.make_async_copy(n_buf.at[at_step % 2, pl.ds(lo, rows)], out_refs[o].at[i], sems.at[at_step % 2, k])
                for k, (o, i, lo, rows) in enumerate(outs_of[at_step])]

    for at_step in range(2, len(outs_of)):
        @pl.when(step == at_step)
        def _():
            for copy in copies(at_step - 2):
                copy.wait()

    def square_rows(r, carry):
        rows = pl.ds(pl.multiple_of(r * NORM_ROWS, NORM_ROWS), NORM_ROWS)
        acc = [jnp.zeros((NORM_ROWS, HEAD_DIM), jnp.float32) for _ in range(2)]
        for c, lane in enumerate(lanes):
            xf = x_ref[0, rows, lane].astype(jnp.float32)
            acc[c % 2] += xf * xf
        ss_buf[rows, :] = acc[0] + acc[1]
        return carry

    lax.fori_loop(0, blk // NORM_ROWS, square_rows, 0)
    total = jnp.sum(ss_buf[...], axis=-1, keepdims=True)
    ss_buf[...] = jnp.broadcast_to(lax.rsqrt(total / d_model + 1e-5), (blk, HEAD_DIM))
    slot = lax.rem(step, 2)

    def norm_rows(r, carry):
        rows = pl.ds(pl.multiple_of(r * NORM_ROWS, NORM_ROWS), NORM_ROWS)
        inv_rms = ss_buf[rows, :]
        for lane in lanes:
            xf = x_ref[0, rows, lane].astype(jnp.float32)
            n_buf[slot, rows, lane] = (xf * inv_rms * gain_ref[:, lane].astype(jnp.float32)).astype(jnp.bfloat16)
        return carry

    lax.fori_loop(0, blk // NORM_ROWS, norm_rows, 0)
    for at_step in range(len(outs_of)):
        @pl.when(step == at_step)
        def _():
            for copy in copies(at_step):
                copy.start()
            if at_step == len(outs_of) - 1:
                for copy in copies(at_step):
                    copy.wait()
                if at_step >= 1:
                    for copy in copies(at_step - 1):
                        copy.wait()


def first_kernel(places, rows, x_hbm, gain_hbm, *refs):
    n = len(places)
    out_refs = refs[:n]
    x_buf, gain_ref, sem = refs[n:]
    d_model = x_hbm.shape[2]
    loads = [pltpu.make_async_copy(x_hbm.at[bat, pl.ds(row0, rows)], x_buf.at[i], sem.at[i]) for i, (bat, row0) in enumerate(places)]
    loads.append(pltpu.make_async_copy(gain_hbm, gain_ref, sem.at[n]))
    for load in loads:
        load.start()
    loads[n].wait()
    lanes = [slice(c * HEAD_DIM, (c + 1) * HEAD_DIM) for c in range(d_model // HEAD_DIM)]
    for i in range(n):
        loads[i].wait()

        def norm_rows(r, carry):
            at = pl.ds(pl.multiple_of(r * NORM_ROWS, NORM_ROWS), NORM_ROWS)
            acc = [jnp.zeros((NORM_ROWS, HEAD_DIM), jnp.float32) for _ in range(2)]
            for c, lane in enumerate(lanes):
                xf = x_buf[i, at, lane].astype(jnp.float32)
                acc[c % 2] += xf * xf
            inv_rms = lax.rsqrt(jnp.sum(acc[0] + acc[1], axis=-1, keepdims=True) / d_model + 1e-5)
            for lane in lanes:
                xf = x_buf[i, at, lane].astype(jnp.float32)
                out_refs[i][0, at, lane] = (xf * inv_rms * gain_ref[:, lane].astype(jnp.float32)).astype(jnp.bfloat16)
            return carry

        lax.fori_loop(0, rows // NORM_ROWS, norm_rows, 0)


def raw_kernel(places, rows, x_hbm, *refs):
    n = len(places)
    copies = [pltpu.make_async_copy(x_hbm.at[bat, pl.ds(row0, rows)], refs[i].at[0], refs[n].at[i]) for i, (bat, row0) in enumerate(places)]
    for copy in copies:
        copy.start()
    for copy in copies:
        copy.wait()


def raw_call(x, places, rows):
    d_model = x.shape[2]
    return pl.pallas_call(
        functools.partial(raw_kernel, places, rows),
        out_shape=[pltpu.VMEM((1, rows, d_model), jnp.bfloat16)] * len(places),
        in_specs=[pl.BlockSpec(memory_space=pl.ANY)],
        out_specs=[pl.BlockSpec(memory_space=pltpu.VMEM)] * len(places),
        scratch_shapes=[pltpu.SemaphoreType.DMA((len(places),))],
        compiler_params=pltpu.CompilerParams(vmem_limit_bytes=8 * 2 ** 20),
        name="raw_rows",
    )(pltpu.with_memory_space_constraint(x, pltpu.HBM))


def first_call(x, gain, places, rows):
    d_model = x.shape[2]
    return pl.pallas_call(
        functools.partial(first_kernel, places, rows),
        out_shape=[pltpu.VMEM((1, rows, d_model), jnp.bfloat16)] * len(places),
        in_specs=[pl.BlockSpec(memory_space=pl.ANY)] * 2,
        out_specs=[pl.BlockSpec(memory_space=pltpu.VMEM)] * len(places),
        scratch_shapes=[
            pltpu.VMEM((len(places), rows, d_model), jnp.bfloat16),
            pltpu.VMEM(gain.shape, gain.dtype),
            pltpu.SemaphoreType.DMA((len(places) + 1,)),
        ],
        compiler_params=pltpu.CompilerParams(vmem_limit_bytes=8 * 2 ** 20),
        cost_estimate=pl.CostEstimate(flops=len(places) * rows * d_model * 8, bytes_accessed=len(places) * rows * d_model * 4, transcendentals=0),
        name="first_rows",
    )(*(pltpu.with_memory_space_constraint(a, pltpu.HBM) for a in (x, gain)))


def norm_call(x, gain, order, outs_of, shapes, blk=None, row_block=0):
    d_model = x.shape[2]
    blk = blk or x.shape[1]

    def prompt_of(g):
        idx = jnp.int32(order[-1])
        for k in range(len(order) - 1):
            idx = jnp.where(g == k, order[k], idx)
        return idx

    return pl.pallas_call(
        functools.partial(norm_kernel, outs_of),
        grid=(len(order),),
        in_specs=[pl.BlockSpec((1, blk, d_model), lambda g: (prompt_of(g), row_block, 0)),
                  pl.BlockSpec((1, d_model), lambda g: (0, 0))],
        out_specs=[pl.BlockSpec(memory_space=pl.ANY)] * len(shapes),
        out_shape=[jax.ShapeDtypeStruct((*shape, d_model), jnp.bfloat16) for shape in shapes],
        scratch_shapes=[
            pltpu.VMEM((blk, HEAD_DIM), jnp.float32),
            pltpu.VMEM((2, blk, d_model), jnp.bfloat16),
            pltpu.SemaphoreType.DMA((2, max(len(o) for o in outs_of))),
        ],
        compiler_params=pltpu.CompilerParams(vmem_limit_bytes=24 * 2 ** 20),
        cost_estimate=pl.CostEstimate(flops=len(order) * blk * d_model * 8, bytes_accessed=len(order) * blk * d_model * 6, transcendentals=0),
        name="norm_rows",
    )(pltpu.with_memory_space_constraint(x, pltpu.HBM), gain)


def rows_kernel(new_ref, last_ref, gain_ref, cos_ref, sin_ref, wq_hbm, wk, wv, q_ref, k_ref, v_ref, st_ref, wq, q_buf, sem):
    load = pltpu.make_async_copy(wq_hbm, wq, sem)
    load.start()
    n_batch = new_ref.shape[0]
    heads = wk.shape[1] // HEAD_DIM
    xf = jnp.concatenate([new_ref[...].astype(jnp.float32), last_ref[...].astype(jnp.float32)], axis=0)
    inv_rms = lax.rsqrt(jnp.mean(xf * xf, axis=-1, keepdims=True) + 1e-5)
    normed = (xf * inv_rms * gain_ref[...].astype(jnp.float32)).astype(jnp.bfloat16)
    k_all = jnp.dot(normed, wk[...], preferred_element_type=jnp.float32)[:n_batch]
    v_all = jnp.dot(normed, wv[...], preferred_element_type=jnp.float32)[:n_batch].astype(jnp.bfloat16)
    load.wait()
    q_all = jnp.dot(normed, wq[...], preferred_element_type=jnp.float32)
    q_buf[...] = jnp.zeros_like(q_buf)
    k_rot = []
    for h in range(heads):
        cols = slice(h * HEAD_DIM, (h + 1) * HEAD_DIM)
        qh = q_all[:, cols]
        qh = (qh * cos_ref[...] + pltpu.roll(qh, HEAD_DIM // 2, 1) * sin_ref[...]).astype(jnp.bfloat16).astype(jnp.float32)
        kh = k_all[:, cols]
        kh = (kh * cos_ref[:n_batch, :] + pltpu.roll(kh, HEAD_DIM // 2, 1) * sin_ref[:n_batch, :]).astype(jnp.bfloat16)
        k_rot.append(kh)
        score = jnp.sum(qh[:n_batch] * kh.astype(jnp.float32), axis=-1, keepdims=True) * (HEAD_DIM ** -0.5)
        zero = jnp.zeros((n_batch, HEAD_DIM), jnp.float32)
        for t in range(2):
            row = 2 * h + t
            q_buf[:, row, cols] = qh[t * n_batch:(t + 1) * n_batch]
            st_ref[0, :, row, :] = v_all[:, cols].astype(jnp.float32) if t == 0 else zero
            st_ref[1, :, row, :] = zero + score if t == 0 else zero + NEG_BIG
            st_ref[2, :, row, :] = zero + 1.0 if t == 0 else zero
    q_ref[...] = q_buf[...].astype(jnp.bfloat16)
    k_ref[...] = jnp.concatenate(k_rot, axis=1).reshape(n_batch, heads, HEAD_DIM)
    v_ref[...] = v_all.reshape(n_batch, heads, HEAD_DIM)


def rows_call(new_tok, last_x, gain, row_tabs, w_q, w_k, w_v):
    n_batch = new_tok.shape[0]
    width = w_q.shape[1]
    heads = width // HEAD_DIM
    vmem = pl.BlockSpec(memory_space=pltpu.VMEM)
    return pl.pallas_call(
        rows_kernel,
        out_shape=[
            jax.ShapeDtypeStruct((n_batch, STAT_ROWS, width), jnp.bfloat16),
            jax.ShapeDtypeStruct((n_batch, heads, HEAD_DIM), jnp.bfloat16),
            jax.ShapeDtypeStruct((n_batch, heads, HEAD_DIM), jnp.bfloat16),
            jax.ShapeDtypeStruct((3, n_batch, STAT_ROWS, HEAD_DIM), jnp.float32),
        ],
        in_specs=[vmem] * 5 + [pl.BlockSpec(memory_space=pl.ANY)] + [vmem] * 2,
        out_specs=[vmem] * 4,
        scratch_shapes=[
            pltpu.VMEM(w_q.shape, jnp.bfloat16),
            pltpu.VMEM((n_batch, STAT_ROWS, width), jnp.float32),
            pltpu.SemaphoreType.DMA,
        ],
        compiler_params=pltpu.CompilerParams(vmem_limit_bytes=24 * 2 ** 20),
        cost_estimate=pl.CostEstimate(flops=2 * 2 * n_batch * 3 * w_q.shape[0] * width, bytes_accessed=2 * w_q.size, transcendentals=0),
        name="query_rows",
    )(new_tok, last_x, gain, *row_tabs, pltpu.with_memory_space_constraint(w_q, pltpu.HBM), w_k, w_v)


def when(condition):
    if isinstance(condition, bool):
        return lambda body: body() if condition else None
    return pl.when(condition)


def by_group(group, values):
    if isinstance(group, int):
        return values[group]
    out = values[-1]
    for p in range(len(values) - 1):
        out = jnp.where(group == p, values[p], out)
    return out


def kv_kernel(n_in, n_steps, masks, batches, firsts, row0, stat_of, with_new, raw, *refs):
    n_groups = len(masks)
    n_arr = n_in * n_groups
    x_refs = refs[:n_arr]
    cos_ref, sin_ref, len_ref, wk, wv, q_ref = refs[n_arr:n_arr + 6]
    rest = refs[n_arr + 6:]
    if raw:
        gain_ref, *rest = rest
    if with_new:
        new_refs = rest[:2]
        rest = rest[2:]
    else:
        rest = rest[3:]
    kc_ref, vc_ref, st_ref, x_buf, k_buf, v_buf, k_out, v_out, s_out, x_sem, sems, s_sem = rest[:12]
    me = lax.axis_index("model")
    step = pl.program_id(0) if n_steps > 1 else 0
    slot = lax.rem(step, 2) if n_steps > 1 else 0
    per_group = n_steps // n_groups
    blk = x_buf.shape[2]
    shard_rows = cos_ref.shape[1]
    width = wk.shape[1]
    heads = width // HEAD_DIM
    n_tok = n_in * blk

    def x_copies(at_step, which, group):
        local = at_step - group * per_group
        return [pltpu.make_async_copy(x_refs[group * n_in + i].at[firsts[group][i] + local],
                                      x_buf.at[which, i], x_sem.at[which, i]) for i in range(n_in)]

    def start_x(at_step, which):
        for group in range(n_groups):
            @when(at_step // per_group == group)
            def _(group=group):
                for copy in x_copies(at_step, which, group):
                    copy.start()

    def place(i, at_step):
        group = at_step // per_group
        mask = by_group(group, [m[i] for m in masks])
        shard = sum(lax.rem(me // bit + mask // bit, 2) * bit for bit in (1, 2, 4))
        return shard, by_group(group, [b[i] for b in batches]) + at_step % per_group, mask

    def out_copies(which, at_step):
        copies = []
        for i in range(n_in):
            shard, bat, _ = place(i, at_step)
            rows = pl.ds(shard * shard_rows + row0, blk)
            copies.append(pltpu.make_async_copy(k_out.at[which, i], kc_ref.at[bat, rows], sems.at[which, i, 0]))
            copies.append(pltpu.make_async_copy(v_out.at[which, i], vc_ref.at[bat, rows], sems.at[which, i, 1]))
        return copies

    def new_copies():
        return [pltpu.make_async_copy(src.at[pl.ds(b, 1)], dst.at[b, pl.ds(dst.shape[1] - 1, 1)], rest[12].at[idx, b])
                for idx, (src, dst) in enumerate(zip(new_refs, (kc_ref, vc_ref))) for b in range(src.shape[0])]

    @when(step == 0)
    def _():
        start_x(step, slot)
        if with_new:
            for copy in new_copies():
                copy.start()

    @when(step + 1 < n_steps)
    def _():
        start_x(step + 1, 1 - slot)

    @when(step >= 2)
    def _():
        for copy in out_copies(slot, step - 2):
            copy.wait()

    for copy in x_copies(0, slot, 0):
        copy.wait()
    x_rows = x_buf.at[slot]
    if raw:
        lanes = [slice(c * HEAD_DIM, (c + 1) * HEAD_DIM) for c in range(x_buf.shape[3] // HEAD_DIM)]
        for i in range(n_in):
            def norm_rows(r, carry, i=i):
                at = pl.ds(pl.multiple_of(r * NORM_ROWS, NORM_ROWS), NORM_ROWS)
                acc = [jnp.zeros((NORM_ROWS, HEAD_DIM), jnp.float32) for _ in range(2)]
                for c, lane in enumerate(lanes):
                    xf = x_rows[i, at, lane].astype(jnp.float32)
                    acc[c % 2] += xf * xf
                inv_rms = lax.rsqrt(jnp.sum(acc[0] + acc[1], axis=-1, keepdims=True) / x_buf.shape[3] + 1e-5)
                for lane in lanes:
                    xf = x_rows[i, at, lane].astype(jnp.float32)
                    x_rows[i, at, lane] = (xf * inv_rms * gain_ref[:, lane].astype(jnp.float32)).astype(jnp.bfloat16)
                return carry

            lax.fori_loop(0, blk // NORM_ROWS, norm_rows, 0)

    def col_tile(c, carry):
        cols = pl.ds(pl.multiple_of(c * COL_TILE, COL_TILE), COL_TILE) if n_steps > 1 else slice(c * COL_TILE, (c + 1) * COL_TILE)
        normed = x_rows[...].reshape(n_tok, x_buf.shape[3])
        kf = jnp.dot(normed, wk[:, cols], preferred_element_type=jnp.float32)
        vf = jnp.dot(normed, wv[:, cols], preferred_element_type=jnp.float32)
        v_buf[:, cols] = vf.astype(jnp.bfloat16)
        parts = []
        for i in range(n_in):
            shard = place(i, step)[0]
            cos_tab = cos_ref[shard, row0:row0 + blk]
            sin_tab = sin_ref[shard, row0:row0 + blk]
            halves = []
            for h in range(COL_TILE // HEAD_DIM):
                kh = kf[i * blk:(i + 1) * blk, h * HEAD_DIM:(h + 1) * HEAD_DIM]
                halves.append(kh * cos_tab + pltpu.roll(kh, HEAD_DIM // 2, 1) * sin_tab)
            parts.append(jnp.concatenate(halves, axis=1))
        k_buf[:, cols] = jnp.concatenate(parts, axis=0).astype(jnp.bfloat16)
        return carry

    if n_steps > 1:
        lax.fori_loop(0, width // COL_TILE, col_tile, 0)
    else:
        for c in range(width // COL_TILE):
            col_tile(c, 0)

    for i in range(n_in):
        k_out[slot, i] = k_buf[i * blk:(i + 1) * blk, :].reshape(blk, heads, HEAD_DIM)
        v_out[slot, i] = v_buf[i * blk:(i + 1) * blk, :].reshape(blk, heads, HEAD_DIM)
    for copy in out_copies(slot, step):
        copy.start()

    head_of_row = lax.broadcasted_iota(jnp.int32, (STAT_ROWS, HEAD_DIM), 0) // (STAT_ROWS // heads)
    probs = []
    for i in range(n_in):
        shard, bat, _ = place(i, step)
        scores = lax.dot_general(q_ref[bat], k_buf[i * blk:(i + 1) * blk, :], (((1,), (1,)), ((), ())),
                                 preferred_element_type=jnp.float32) * (HEAD_DIM ** -0.5)
        pos = shard * shard_rows + row0 + lax.broadcasted_iota(jnp.int32, scores.shape, 1)
        visible = pos < len_ref[pl.ds(bat, 1), :blk]
        scores = jnp.where(visible, scores, NEG_BIG)
        blk_max = jnp.max(scores, axis=-1, keepdims=True)
        prob = jnp.where(visible, jnp.exp(scores - blk_max), 0.0)
        probs.append((blk_max, prob))
    for i, (blk_max, prob) in enumerate(probs):
        full = jnp.dot(prob.astype(jnp.bfloat16), v_buf[i * blk:(i + 1) * blk, :], preferred_element_type=jnp.float32)
        acc = jnp.zeros((STAT_ROWS, HEAD_DIM), jnp.float32)
        for h in range(heads):
            acc = jnp.where(head_of_row == h, full[:, h * HEAD_DIM:(h + 1) * HEAD_DIM], acc)
        s_out[i, 0] = acc
        s_out[i, 1] = jnp.broadcast_to(blk_max, (STAT_ROWS, HEAD_DIM))
        s_out[i, 2] = jnp.broadcast_to(jnp.sum(prob, axis=-1, keepdims=True), (STAT_ROWS, HEAD_DIM))
    stat_copies = []
    for i in range(n_in):
        _, bat, mask = place(i, step)
        stat_copies.append(pltpu.make_async_copy(s_out.at[i], st_ref.at[mask + stat_of, bat], s_sem.at[i]))
        stat_copies[-1].start()
    for copy in stat_copies:
        copy.wait()

    @when(step == n_steps - 1)
    def _():
        for copy in out_copies(slot, step):
            copy.wait()
        if with_new:
            for copy in new_copies():
                copy.wait()
        if n_steps > 1:
            for copy in out_copies(1 - slot, step - 1):
                copy.wait()


def kv_call(groups, per_group, masks, batches, lengths, tabs, w_k, w_v, q_diag, caches, new_rows=None, row0=0, stat_of=0, gain=None):
    n_groups = len(groups)
    n_in = len(groups[0])
    n_steps = n_groups * per_group
    cos_tab, sin_tab = tabs
    blk, d_model = groups[0][0][0].shape[1:]
    width = w_k.shape[1]
    heads = width // HEAD_DIM
    any_spec = pl.BlockSpec(memory_space=pl.ANY)
    operands = [arr for group in groups for arr, _ in group]
    in_specs = [any_spec] * len(operands) + [pl.BlockSpec(memory_space=pltpu.VMEM)] * 6
    operands += [cos_tab, sin_tab, lengths, w_k, w_v, q_diag]
    if gain is not None:
        in_specs.append(pl.BlockSpec(memory_space=pltpu.VMEM))
        operands.append(gain)
    with_new = new_rows is not None
    if with_new:
        operands += new_rows
        in_specs += [any_spec] * 2
        aliases = {}
    else:
        operands += [*caches[:2], pltpu.with_memory_space_constraint(caches[2], pltpu.VMEM)]
        in_specs += [any_spec] * 3
        aliases = {len(operands) - 3: 0, len(operands) - 2: 1, len(operands) - 1: 2}
    tokens = n_in * blk
    n_batch = q_diag.shape[0]
    slots = min(n_steps, 2)
    return pl.pallas_call(
        functools.partial(kv_kernel, n_in, n_steps, masks, batches, [[first for _, first in group] for group in groups], row0, stat_of, with_new, gain is not None),
        grid=(n_steps,) if n_steps > 1 else (),
        in_specs=in_specs,
        out_specs=[any_spec] * 3,
        scratch_shapes=[
            pltpu.VMEM((slots, n_in, blk, d_model), jnp.bfloat16),
            pltpu.VMEM((tokens, width), jnp.bfloat16),
            pltpu.VMEM((tokens, width), jnp.bfloat16),
            pltpu.VMEM((slots, n_in, blk, heads, HEAD_DIM), jnp.bfloat16),
            pltpu.VMEM((slots, n_in, blk, heads, HEAD_DIM), jnp.bfloat16),
            pltpu.VMEM((n_in, 3, STAT_ROWS, HEAD_DIM), jnp.float32),
            pltpu.SemaphoreType.DMA((slots, n_in)),
            pltpu.SemaphoreType.DMA((slots, n_in, 2)),
            pltpu.SemaphoreType.DMA((n_in,)),
        ] + [pltpu.SemaphoreType.DMA((2, n_batch))] * with_new,
        out_shape=[*(jax.ShapeDtypeStruct(c.shape, c.dtype) for c in caches[:2]), pltpu.VMEM(caches[2].shape, caches[2].dtype)],
        input_output_aliases=aliases,
        compiler_params=pltpu.CompilerParams(vmem_limit_bytes=20 * 2 ** 20),
        cost_estimate=pl.CostEstimate(flops=4 * n_steps * tokens * d_model * width, bytes_accessed=2 * n_steps * tokens * (d_model + 2 * width), transcendentals=0),
        name="kv_chunk",
    )(*operands)


def tail_kernel(n_dev, parts_of, stv, self_ref, xs_ref, gain_ref, wo, wg_hbm, wu_hbm, wd_hbm, out_ref,
                wg, wu, wd, rows, a_buf, n_buf, ps1, pr1, ps2, pr2, xo1, xg1, xo2, xg2, w_sem, send_sem, recv_sem):
    me = lax.axis_index("model")
    n_batch = out_ref.shape[1]
    n_rows = 2 * n_batch
    d_model = out_ref.shape[2]
    cols = d_model // n_dev
    heads = STAT_ROWS // 2
    loads = [pltpu.make_async_copy(src, dst, w_sem.at[i]) for i, (src, dst) in enumerate(((wg_hbm, wg), (wu_hbm, wu), (wd_hbm, wd)))]
    for load in loads:
        load.start()
    barrier = pltpu.get_barrier_semaphore()

    def peer_of(mask):
        return sum(lax.rem(me // bit + mask // bit, 2) * bit for bit in (1, 2, 4))

    far_first = ((6, 7), (2, 3, 4, 5), (1,))
    for mask in sum(far_first, ()):
        pl.semaphore_signal(barrier, inc=1, device_id={"model": peer_of(mask)}, device_id_type=MESH)

    def send(phase, mask, src, dst):
        return pltpu.make_async_remote_copy(
            src_ref=src, dst_ref=dst, send_sem=send_sem.at[phase, mask - 1], recv_sem=recv_sem.at[phase, mask - 1],
            device_id={"model": peer_of(mask)}, device_id_type=MESH)

    for b in range(n_batch):
        top = self_ref[1, b]
        for j in range(parts_of[b]):
            top = jnp.maximum(top, stv[j, b, 1])
        scale = jnp.exp(self_ref[1, b] - top)
        den = scale * self_ref[2, b]
        num = scale * self_ref[0, b]
        for j in range(parts_of[b]):
            scale = jnp.exp(stv[j, b, 1] - top)
            den += scale * stv[j, b, 2]
            num += scale * stv[j, b, 0]
        rows[:, b, :] = num / den
    for h in range(heads):
        for t in range(2):
            a_buf[t * n_batch:(t + 1) * n_batch, h * HEAD_DIM:(h + 1) * HEAD_DIM] = rows[2 * h + t]
    att = a_buf[...].astype(jnp.bfloat16)

    def exchange(phase, base, copies, pr, xo, xg):
        total = base
        for copy, mask in reversed(copies):
            copy.wait_recv()
            total = total + pr[mask - 1]
        xo[...] = total.astype(jnp.bfloat16)
        xg[me] = xo[...]
        outs = []
        for mask in sum(far_first, ()):
            outs.append(send(phase + 1, mask, xo, xg.at[me]))
            outs[-1].start()
        for out in outs:
            out.wait_recv()
        return [copy for copy, _ in copies] + outs

    def col_block(p):
        return pl.ds(pl.multiple_of(p * cols, cols), cols)

    part = jnp.dot(att, wo[...], preferred_element_type=jnp.float32)
    for j in range(n_dev):
        ps1[j] = part[:, j * cols:(j + 1) * cols]
    pl.semaphore_wait(barrier, n_dev - 1)
    copies = []
    for mask in sum(far_first, ()):
        copies.append((send(0, mask, ps1.at[peer_of(mask)], pr1.at[mask - 1]), mask))
        copies[-1][0].start()
    sent = exchange(0, xs_ref[...].astype(jnp.float32) + ps1[me], copies, pr1, xo1, xg1)
    sq = jnp.zeros((n_rows, 1), jnp.float32)
    for j in range(n_dev):
        xf = xg1[j].astype(jnp.float32)
        sq += jnp.sum(xf * xf, axis=-1, keepdims=True)
    inv_rms = lax.rsqrt(sq / d_model + 1e-5)
    for j in range(n_dev):
        at = slice(j * cols, (j + 1) * cols)
        n_buf[:, at] = (xg1[j].astype(jnp.float32) * inv_rms * gain_ref[:, at].astype(jnp.float32)).astype(jnp.bfloat16)
    loads[0].wait()
    loads[1].wait()
    gate = jnp.dot(n_buf[...], wg[...], preferred_element_type=jnp.float32)
    up = jnp.dot(n_buf[...], wu[...], preferred_element_type=jnp.float32)
    mid = (gate * (1.0 / (1.0 + jnp.exp(-gate))) * up).astype(jnp.bfloat16)
    loads[2].wait()
    copies = []
    for group in far_first:
        for mask in group:
            ps2[mask] = jnp.dot(mid, wd[:, col_block(peer_of(mask))], preferred_element_type=jnp.float32)
        if group == far_first[-1]:
            ps2[0] = jnp.dot(mid, wd[:, col_block(me)], preferred_element_type=jnp.float32)
        for mask in group:
            copies.append((send(2, mask, ps2.at[mask], pr2.at[mask - 1]), mask))
            copies[-1][0].start()
    sent += exchange(2, xo1[...].astype(jnp.float32) + ps2[0], copies, pr2, xo2, xg2)
    for j in range(n_dev):
        at = slice(j * cols, (j + 1) * cols)
        out_ref[0, :, at] = xg2[j, :n_batch]
        out_ref[1, :, at] = xg2[j, n_batch:]
    for copy in sent:
        copy.wait_send()


def tail_call(n_dev, parts_of, stats, self_stat, x_mine, gain, w_o, w_gate, w_up, w_down, n_batch):
    n_rows, cols = x_mine.shape
    d_model = w_o.shape[1]
    vmem = pl.BlockSpec(memory_space=pltpu.VMEM)
    any_spec = pl.BlockSpec(memory_space=pl.ANY)
    exchanged = [pltpu.VMEM((n_dev, n_rows, cols), jnp.float32), pltpu.VMEM((n_dev - 1, n_rows, cols), jnp.float32)]
    summed = [pltpu.VMEM((n_rows, cols), jnp.bfloat16), pltpu.VMEM((n_dev, n_rows, cols), jnp.bfloat16)]
    return pl.pallas_call(
        functools.partial(tail_kernel, n_dev, parts_of),
        out_shape=jax.ShapeDtypeStruct((2, n_batch, d_model), jnp.bfloat16),
        in_specs=[vmem] * 5 + [any_spec] * 3,
        out_specs=vmem,
        scratch_shapes=[
            pltpu.VMEM(w_gate.shape, jnp.bfloat16),
            pltpu.VMEM(w_up.shape, jnp.bfloat16),
            pltpu.VMEM(w_down.shape, jnp.bfloat16),
            pltpu.VMEM((STAT_ROWS, n_batch, HEAD_DIM), jnp.float32),
            pltpu.VMEM((n_rows, w_o.shape[0]), jnp.float32),
            pltpu.VMEM((n_rows, d_model), jnp.bfloat16),
            *exchanged, *exchanged, *summed, *summed,
            pltpu.SemaphoreType.DMA((3,)),
            pltpu.SemaphoreType.DMA((4, n_dev - 1)),
            pltpu.SemaphoreType.DMA((4, n_dev - 1)),
        ],
        compiler_params=pltpu.CompilerParams(collective_id=0, has_side_effects=True, vmem_limit_bytes=46 * 2 ** 20),
        name="tail",
    )(pltpu.with_memory_space_constraint(stats, pltpu.VMEM), self_stat, x_mine, gain, w_o,
      *(pltpu.with_memory_space_constraint(w, pltpu.HBM) for w in (w_gate, w_up, w_down)))


def solution(mesh):
    n_dev = mesh.shape['model']
    seq_spec = P('replica', 'model', None)
    col_spec = P(None, None, 'model')
    row_spec = P(None, 'model', None)
    gain_spec = P(None, None)
    tok_spec = P('replica', None)
    cache_spec = P(None, 'replica', None, 'model', None)
    in_specs = (seq_spec, P('replica'), tok_spec, gain_spec, col_spec, col_spec, col_spec, row_spec, gain_spec, col_spec, col_spec, row_spec)
    out_specs = (tok_spec, tok_spec, cache_spec, cache_spec)

    def swap(arr, bit):
        return lax.ppermute(arr, 'model', [(i, i ^ bit) for i in range(n_dev)])

    def per_device(prompt, lengths, new_tok, norm_attn, w_q, w_k, w_v, w_o, norm_mlp, w_gate, w_up, w_down):
        my_idx = lax.axis_index('model')
        n_batch, blk, d_model = prompt.shape
        seq_len = blk * n_dev
        width = w_k.shape[2]
        heads = width // HEAD_DIM
        half = n_batch // 2
        wq = w_q[0]
        gain = norm_attn

        q1, q2, rows_h = 1, n_batch // 4, blk // 2
        a_parts, b_parts = {}, {}
        a_parts["0a"], b_parts["0a"] = raw_call(prompt, [(0, 0), (half, 0)], rows_h)
        a_parts["0b"], b_parts["0b"] = first_call(prompt, norm_attn, [(0, rows_h), (half, rows_h)], rows_h)
        from_y, from_x = {}, {}

        def send_part(step, along_y, along_x):
            from_y[step] = swap(along_y, 4)
            from_x[step] = swap(along_x, 2)

        send_part("0a", a_parts["0a"], b_parts["0a"])
        send_part("0b", a_parts["0b"], b_parts["0b"])
        order, outs_of = [], []
        for part, (lo, hi) in ((1, (q1, q2)), (2, (q2, half)), (0, (0, q1))):
            for k in range(lo, hi):
                for side in range(2):
                    order.append(side * half + k)
                    outs_of.append([(4, side * half + k, 0, blk)] + ([(2 * part - 2 + side, k - lo, 0, blk)] if part else []))
        a_parts["1"], b_parts["1"], a_parts["2"], b_parts["2"], normed = norm_call(
            prompt, gain, order, outs_of, [(q2 - q1, blk)] * 2 + [(half - q2, blk)] * 2 + [(n_batch, blk)])
        send_part("1", a_parts["1"], b_parts["1"])
        seq_pos = my_idx * blk + jnp.arange(blk)
        sel = (seq_pos[None, :] == (lengths - 1)[:, None]).astype(jnp.bfloat16)
        last_x = jnp.einsum('bs,bsd->bd', sel, prompt, preferred_element_type=jnp.float32).astype(jnp.bfloat16)
        core, cols_h = my_idx % 2, d_model // 2
        last_x = last_x + swap(last_x, 1)
        last_x = lax.dynamic_slice_in_dim(last_x, core * cols_h, cols_h, axis=1)
        last_x = last_x + swap(last_x, 2)
        last_x = last_x + swap(last_x, 4)
        other_x = swap(last_x, 1)
        last_x = jnp.where(core == 0, jnp.concatenate([last_x, other_x], axis=1), jnp.concatenate([other_x, last_x], axis=1))
        send_part("2", a_parts["2"], b_parts["2"])
        send_part("3", b_parts["2"], a_parts["2"])
        send_part("4", normed[half:half + q2], normed[:q2])
        core_all = swap(normed, 1)

        len_rows = jnp.broadcast_to(lengths.astype(jnp.int32)[:, None], (n_batch, HEAD_DIM))
        row_tabs = rotary_tables(jnp.concatenate([lengths, lengths - 1]))
        tabs = tuple(tab.reshape(n_dev, blk, HEAD_DIM) for tab in rotary_tables(jnp.arange(seq_len)))
        x_rows = jnp.concatenate([new_tok, last_x], axis=0)
        x_mine = lax.dynamic_slice_in_dim(x_rows, my_idx * (d_model // n_dev), d_model // n_dev, axis=1)
        wk, wv, wo, last_x, len_rows, row_tabs, tabs, x_mine = lax.optimization_barrier(
            (w_k[0], w_v[0], w_o[0], last_x, len_rows, row_tabs, tabs, x_mine))
        wk, wv, wo = keep_in_vmem(wk, wv, wo)
        q_diag, k_new, v_new, self_stat = rows_call(new_tok, last_x, gain, row_tabs, wq, wk, wv)
        cache_shape = jax.ShapeDtypeStruct((n_batch, seq_len + 1, heads, HEAD_DIM), jnp.bfloat16)
        caches = [cache_shape, cache_shape, jax.ShapeDtypeStruct((2 * n_dev - 2, n_batch, 3, STAT_ROWS, HEAD_DIM), jnp.float32)]

        def run(groups, per_group, masks, batches, caches, **kw):
            return kv_call(groups, per_group, masks, batches, len_rows, tabs, wk, wv, q_diag, caches, **kw)

        def half_rows(step):
            return {"row0": rows_h * (step == "0b"), "stat_of": (n_dev - 2) * (step == "0b"), "gain": norm_attn if step == "0a" else None}

        def after(caches, *arrays):
            out = lax.optimization_barrier((caches[2], *arrays))
            return [caches[0], caches[1], out[0]], out[1:]

        caches = run([[(arr, 0), (arr, half)] for arr in (normed, core_all)], half,
                     [[0] * 2, [1] * 2], [[0, half]] * 2, caches, new_rows=[k_new, v_new])
        diag, turned = {}, {}
        starts = {"0a": (0, half), "0b": (0, half), "1": (q1, half + q1), "2": (q2, half + q2), "3": (half + q2, q2), "4": (half, 0)}
        for step, start in starts.items():
            caches, (got_y, got_x) = after(caches, from_y[step], from_x[step])
            other_y, other_x = swap(got_y, 1), swap(got_x, 1)
            if step not in "34":
                via_x = swap(got_y, 2)
                via_y = swap(got_x, 4)
                diag[step] = (via_x, via_y)
            streams = [[(got_y, 0), (got_x, 0)], [(other_y, 0), (other_x, 0)]]
            if step in ("0a", "0b"):
                caches = run([streams[0] + streams[1]], q1, [[4, 2, 5, 3]], [[*start, *start]], caches, **half_rows(step))
            else:
                caches = run(streams, got_y.shape[0], [[4, 2], [5, 3]], [list(start)] * 2, caches)
            if step in "34":
                caches, (w_t,) = after(caches, (w_gate if step == "3" else w_up)[0].T)
                turned[step] = turn_call(w_t)
                caches, (turned[step],) = after(caches, turned[step])
        for step in ("2", "1", "0a", "0b"):
            caches, (via_y,) = after(caches, diag[step][1])
            caches, (via_x,) = after(caches, diag[step][0])
            other_y = swap(via_y, 1)
            other_x = swap(via_x, 1)
            start = starts[step]
            streams = [[(via_x, 0), (via_y, 0)], [(other_x, 0), (other_y, 0)]]
            if step in ("0a", "0b"):
                caches = run([streams[0] + streams[1]], q1, [[6, 6, 7, 7]], [[*start, *start]], caches, **half_rows(step))
            else:
                caches = run(streams, via_x.shape[0], [[6] * 2, [7] * 2], [list(start)] * 2, caches)

        k_cache, v_cache, stats = caches
        parts_of = [2 * n_dev - 2 if b % half < q1 else n_dev for b in range(n_batch)]
        both = tail_call(n_dev, parts_of, stats, self_stat, x_mine, norm_mlp, wo, turned["3"], turned["4"], w_down[0], n_batch)
        return both[0], both[1], k_cache[None], v_cache[None]

    return jax.shard_map(per_device, mesh=mesh, in_specs=in_specs, out_specs=out_specs, check_vma=False)
```

```python
import jax
import jax.numpy as jnp
from jax import lax
from jax.sharding import PartitionSpec as P


HEAD_DIM = 128
NEG_BIG = -1e30
PIECES = 2


def rms_norm(hidden, gain_vec):
    hid_f32 = hidden.astype(jnp.float32)
    inv_rms = lax.rsqrt(jnp.mean(hid_f32 * hid_f32, axis=-1, keepdims=True) + 1e-5)
    return (hid_f32 * inv_rms * gain_vec.astype(jnp.float32)).astype(jnp.bfloat16)


def rotary(heads_f32, positions):
    half_dim = HEAD_DIM // 2
    inv_freq = 10000.0 ** (-2.0 * jnp.arange(half_dim, dtype=jnp.float32) / HEAD_DIM)
    angles = positions.astype(jnp.float32)[..., None] * inv_freq
    cos_tab = jnp.cos(angles)[..., None, :]
    sin_tab = jnp.sin(angles)[..., None, :]
    lo_half = heads_f32[..., :half_dim]
    hi_half = heads_f32[..., half_dim:]
    return jnp.concatenate([lo_half * cos_tab - hi_half * sin_tab, hi_half * cos_tab + lo_half * sin_tab], axis=-1)


def attend(queries, keys, values, visible):
    scores = jnp.einsum('bqhd,bkhd->bhqk', queries, keys, preferred_element_type=jnp.float32) * (HEAD_DIM ** -0.5)
    scores = jnp.where(visible[:, None], scores, NEG_BIG)
    top = jnp.max(scores, axis=-1, keepdims=True)
    prob = jnp.exp(scores - top)
    total = jnp.sum(prob, axis=-1)
    out = jnp.einsum('bhqk,bkhd->bqhd', prob.astype(jnp.bfloat16), values, preferred_element_type=jnp.float32)
    return (out / jnp.moveaxis(total, 1, 2)[..., None]).reshape(*queries.shape[:2], -1).astype(jnp.bfloat16)


def solution(mesh):
    n_dev = mesh.shape['model']
    seq_spec = P('replica', 'model', None)
    col_spec = P(None, None, 'model')
    row_spec = P(None, 'model', None)
    gain_spec = P(None, None)
    tok_spec = P('replica', None)
    cache_spec = P(None, 'replica', None, 'model', None)
    in_specs = (seq_spec, P('replica'), tok_spec, gain_spec, col_spec, col_spec, col_spec, row_spec, gain_spec, col_spec, col_spec, row_spec)
    out_specs = (tok_spec, tok_spec, cache_spec, cache_spec)
    fours = [[0, 1, 2, 3], [4, 5, 6, 7]]
    across = [(i, i ^ 4) for i in range(n_dev)]

    def dot(a, b):
        return jnp.dot(a, b, preferred_element_type=jnp.float32)

    def per_device(prompt, lengths, new_tok, norm_attn, w_q, w_k, w_v, w_o, norm_mlp, w_gate, w_up, w_down):
        my_idx = lax.axis_index('model')
        n_batch, blk, d_model = prompt.shape
        n_tok = n_batch * blk
        seq_len = blk * n_dev
        heads = w_k.shape[2] // HEAD_DIM
        wq, wk, wv = w_q[0], w_k[0], w_v[0]
        key_pos = jnp.arange(seq_len)

        normed = lax.all_gather(rms_norm(prompt, norm_attn[0]), 'model', axis=0)
        rows = normed.reshape(n_dev * n_tok, d_model)
        pos = key_pos.reshape(n_dev, 1, blk)

        def project(w):
            return dot(rows, w).reshape(n_dev, n_batch, blk, heads, HEAD_DIM)

        def in_order(x):
            return jnp.moveaxis(x, 0, 1).reshape(n_batch, seq_len, heads, HEAD_DIM)

        q_all = in_order(rotary(project(wq), pos).astype(jnp.bfloat16))
        k_all = in_order(rotary(project(wk), pos).astype(jnp.bfloat16))
        v_all = in_order(project(wv).astype(jnp.bfloat16))
        outs = []
        for i in range(n_dev):
            seen = (i + 1) * blk
            q_pos = i * blk + jnp.arange(blk)
            visible = (key_pos[None, None, :seen] <= q_pos[None, :, None]) & (key_pos[None, None, :seen] < lengths[:, None, None])
            outs.append(attend(q_all[:, i * blk:seen], k_all[:, :seen], v_all[:, :seen], visible))
        heads_out = jnp.stack(outs)
        mine = lax.all_to_all(heads_out, 'model', split_axis=0, concat_axis=0)
        att = jnp.moveaxis(mine.reshape(n_dev, n_tok, -1), 0, 1).reshape(n_tok, -1)

        wo_full = lax.all_gather(w_o[0], 'model', axis=0, tiled=True)
        hidden = (prompt.astype(jnp.float32) + dot(att, wo_full).reshape(n_batch, blk, d_model)).astype(jnp.bfloat16)
        near = rms_norm(hidden, norm_mlp[0]).reshape(n_tok, d_model)
        near, new_tok = lax.optimization_barrier((near, new_tok))
        wg = lax.all_gather(w_gate[0], 'model', axis=1, tiled=True, axis_index_groups=fours)
        wu = lax.all_gather(w_up[0], 'model', axis=1, tiled=True, axis_index_groups=fours)
        wd = lax.all_gather(w_down[0], 'model', axis=0, tiled=True)
        n_four = wg.shape[1]

        def units(rows):
            return (jax.nn.silu(dot(rows, wg)) * dot(rows, wu)).astype(jnp.bfloat16)

        step = n_tok // PIECES
        theirs = [lax.ppermute(near[i:i + step], 'model', across) for i in range(0, n_tok, step)]
        back = jnp.concatenate([lax.ppermute(units(piece), 'model', across) for piece in theirs], axis=0)
        own = units(near)
        low = my_idx < 4
        total = dot(jnp.where(low, own, back), wd[:n_four]) + dot(jnp.where(low, back, own), wd[n_four:])
        hidden = (hidden.astype(jnp.float32) + total.reshape(n_batch, blk, d_model)).astype(jnp.bfloat16)
        seq_pos = my_idx * blk + jnp.arange(blk)
        last_sel = (seq_pos[None, :] == (lengths - 1)[:, None]).astype(jnp.bfloat16)
        last_hidden = lax.psum(jnp.einsum('bs,bsd->bd', last_sel, hidden, preferred_element_type=jnp.float32), 'model').astype(jnp.bfloat16)

        tok_norm = rms_norm(new_tok, norm_attn[0])
        q_new = rotary(dot(tok_norm, wq).reshape(n_batch, heads, HEAD_DIM), lengths).astype(jnp.bfloat16)
        k_new = rotary(dot(tok_norm, wk).reshape(n_batch, heads, HEAD_DIM), lengths).astype(jnp.bfloat16)
        v_new = dot(tok_norm, wv).astype(jnp.bfloat16).reshape(n_batch, heads, HEAD_DIM)
        k_cache = jnp.concatenate([k_all, k_new[:, None]], axis=1)
        v_cache = jnp.concatenate([v_all, v_new[:, None]], axis=1)
        cache_pos = jnp.arange(seq_len + 1)
        visible = (cache_pos[None, :] < lengths[:, None]) | (cache_pos[None, :] == seq_len)
        tok_attn = attend(q_new[:, None], k_cache, v_cache, visible[:, None])[:, 0]
        dec_hidden = (new_tok.astype(jnp.float32) + lax.psum(dot(tok_attn, w_o[0]), 'model')).astype(jnp.bfloat16)
        tok_norm = rms_norm(dec_hidden, norm_mlp[0])
        tok_mid = (jax.nn.silu(dot(tok_norm, w_gate[0])) * dot(tok_norm, w_up[0])).astype(jnp.bfloat16)
        dec_hidden = (dec_hidden.astype(jnp.float32) + lax.psum(dot(tok_mid, w_down[0]), 'model')).astype(jnp.bfloat16)
        return dec_hidden, last_hidden, k_cache[None], v_cache[None]

    return jax.shard_map(per_device, mesh=mesh, in_specs=in_specs, out_specs=out_specs, check_vma=False)
```

```python
import functools

import jax
import jax.numpy as jnp
from jax import lax
from jax.experimental import pallas as pl
from jax.experimental.pallas import tpu as pltpu
from jax.sharding import PartitionSpec as P


HEAD_DIM = 128
NEG_BIG = -1e30
STAT_ROWS = 8
NORM_ROWS = 32
COL_TILE = 256
MESH = pl.DeviceIdType.MESH


def rotary_tables(positions):
    half_dim = HEAD_DIM // 2
    inv_freq = 10000.0 ** (-2.0 * jnp.arange(half_dim, dtype=jnp.float32) / HEAD_DIM)
    angles = positions.astype(jnp.float32)[..., None] * inv_freq
    cos_tab = jnp.cos(angles)
    sin_tab = jnp.sin(angles)
    return jnp.concatenate([cos_tab, cos_tab], axis=-1), jnp.concatenate([-sin_tab, sin_tab], axis=-1)


def load_kernel(*refs):
    n = len(refs) // 2
    sem = refs[-1]
    copies = [pltpu.make_async_copy(refs[i], refs[n + i], sem.at[i]) for i in range(n)]
    for copy in copies:
        copy.start()
    for copy in copies:
        copy.wait()


def keep_in_vmem(*arrays):
    return pl.pallas_call(
        load_kernel,
        out_shape=[pltpu.VMEM(arr.shape, arr.dtype) for arr in arrays],
        in_specs=[pl.BlockSpec(memory_space=pl.ANY)] * len(arrays),
        out_specs=[pl.BlockSpec(memory_space=pltpu.VMEM)] * len(arrays),
        scratch_shapes=[pltpu.SemaphoreType.DMA((len(arrays),))],
        compiler_params=pltpu.CompilerParams(vmem_limit_bytes=24 * 2 ** 20),
        name="keep",
    )(*(pltpu.with_memory_space_constraint(arr, pltpu.HBM) for arr in arrays))


def turn_kernel(w_ref, out_ref):
    out_ref[...] = w_ref[...].T


def turn_call(w_t):
    n, d = w_t.shape
    cols = 512
    return pl.pallas_call(
        turn_kernel,
        grid=(d // cols,),
        in_specs=[pl.BlockSpec((n, cols), lambda g: (0, g))],
        out_specs=pl.BlockSpec((cols, n), lambda g: (g, 0)),
        out_shape=jax.ShapeDtypeStruct((d, n), w_t.dtype),
        compiler_params=pltpu.CompilerParams(vmem_limit_bytes=12 * 2 ** 20),
        cost_estimate=pl.CostEstimate(flops=2 * d * n * 128, bytes_accessed=4 * d * n, transcendentals=0),
        name="turn",
    )(pltpu.with_memory_space_constraint(w_t, pltpu.HBM))


def norm_kernel(outs_of, x_ref, gain_ref, *refs):
    n_out = len(refs) - 3
    out_refs = refs[:n_out]
    ss_buf, n_buf, sems = refs[n_out:]
    step = pl.program_id(0)
    blk, d_model = x_ref.shape[1:]
    lanes = [slice(c * HEAD_DIM, (c + 1) * HEAD_DIM) for c in range(d_model // HEAD_DIM)]

    def copies(at_step):
        return [pltpu.make_async_copy(n_buf.at[at_step % 2, pl.ds(lo, rows)], out_refs[o].at[i], sems.at[at_step % 2, k])
                for k, (o, i, lo, rows) in enumerate(outs_of[at_step])]

    for at_step in range(2, len(outs_of)):
        @pl.when(step == at_step)
        def _():
            for copy in copies(at_step - 2):
                copy.wait()

    def square_rows(r, carry):
        rows = pl.ds(pl.multiple_of(r * NORM_ROWS, NORM_ROWS), NORM_ROWS)
        acc = [jnp.zeros((NORM_ROWS, HEAD_DIM), jnp.float32) for _ in range(2)]
        for c, lane in enumerate(lanes):
            xf = x_ref[0, rows, lane].astype(jnp.float32)
            acc[c % 2] += xf * xf
        ss_buf[rows, :] = acc[0] + acc[1]
        return carry

    lax.fori_loop(0, blk // NORM_ROWS, square_rows, 0)
    total = jnp.sum(ss_buf[...], axis=-1, keepdims=True)
    ss_buf[...] = jnp.broadcast_to(lax.rsqrt(total / d_model + 1e-5), (blk, HEAD_DIM))
    slot = lax.rem(step, 2)

    def norm_rows(r, carry):
        rows = pl.ds(pl.multiple_of(r * NORM_ROWS, NORM_ROWS), NORM_ROWS)
        inv_rms = ss_buf[rows, :]
        for lane in lanes:
            xf = x_ref[0, rows, lane].astype(jnp.float32)
            n_buf[slot, rows, lane] = (xf * inv_rms * gain_ref[:, lane].astype(jnp.float32)).astype(jnp.bfloat16)
        return carry

    lax.fori_loop(0, blk // NORM_ROWS, norm_rows, 0)
    for at_step in range(len(outs_of)):
        @pl.when(step == at_step)
        def _():
            for copy in copies(at_step):
                copy.start()
            if at_step == len(outs_of) - 1:
                for copy in copies(at_step):
                    copy.wait()
                if at_step >= 1:
                    for copy in copies(at_step - 1):
                        copy.wait()


def first_kernel(places, rows, x_hbm, gain_hbm, *refs):
    n = len(places)
    out_refs = refs[:n]
    x_buf, gain_ref, sem = refs[n:]
    d_model = x_hbm.shape[2]
    loads = [pltpu.make_async_copy(x_hbm.at[bat, pl.ds(row0, rows)], x_buf.at[i], sem.at[i]) for i, (bat, row0) in enumerate(places)]
    loads.append(pltpu.make_async_copy(gain_hbm, gain_ref, sem.at[n]))
    for load in loads:
        load.start()
    loads[n].wait()
    lanes = [slice(c * HEAD_DIM, (c + 1) * HEAD_DIM) for c in range(d_model // HEAD_DIM)]
    for i in range(n):
        loads[i].wait()

        def norm_rows(r, carry):
            at = pl.ds(pl.multiple_of(r * NORM_ROWS, NORM_ROWS), NORM_ROWS)
            acc = [jnp.zeros((NORM_ROWS, HEAD_DIM), jnp.float32) for _ in range(2)]
            for c, lane in enumerate(lanes):
                xf = x_buf[i, at, lane].astype(jnp.float32)
                acc[c % 2] += xf * xf
            inv_rms = lax.rsqrt(jnp.sum(acc[0] + acc[1], axis=-1, keepdims=True) / d_model + 1e-5)
            for lane in lanes:
                xf = x_buf[i, at, lane].astype(jnp.float32)
                out_refs[i][0, at, lane] = (xf * inv_rms * gain_ref[:, lane].astype(jnp.float32)).astype(jnp.bfloat16)
            return carry

        lax.fori_loop(0, rows // NORM_ROWS, norm_rows, 0)


def first_call(x, gain, places, rows):
    d_model = x.shape[2]
    return pl.pallas_call(
        functools.partial(first_kernel, places, rows),
        out_shape=[pltpu.VMEM((1, rows, d_model), jnp.bfloat16)] * len(places),
        in_specs=[pl.BlockSpec(memory_space=pl.ANY)] * 2,
        out_specs=[pl.BlockSpec(memory_space=pltpu.VMEM)] * len(places),
        scratch_shapes=[
            pltpu.VMEM((len(places), rows, d_model), jnp.bfloat16),
            pltpu.VMEM(gain.shape, gain.dtype),
            pltpu.SemaphoreType.DMA((len(places) + 1,)),
        ],
        compiler_params=pltpu.CompilerParams(vmem_limit_bytes=8 * 2 ** 20),
        cost_estimate=pl.CostEstimate(flops=len(places) * rows * d_model * 8, bytes_accessed=len(places) * rows * d_model * 4, transcendentals=0),
        name="first_rows",
    )(*(pltpu.with_memory_space_constraint(a, pltpu.HBM) for a in (x, gain)))


def norm_call(x, gain, order, outs_of, shapes, blk=None, row_block=0):
    d_model = x.shape[2]
    blk = blk or x.shape[1]

    def prompt_of(g):
        idx = jnp.int32(order[-1])
        for k in range(len(order) - 1):
            idx = jnp.where(g == k, order[k], idx)
        return idx

    return pl.pallas_call(
        functools.partial(norm_kernel, outs_of),
        grid=(len(order),),
        in_specs=[pl.BlockSpec((1, blk, d_model), lambda g: (prompt_of(g), row_block, 0)),
                  pl.BlockSpec((1, d_model), lambda g: (0, 0))],
        out_specs=[pl.BlockSpec(memory_space=pl.ANY)] * len(shapes),
        out_shape=[jax.ShapeDtypeStruct((*shape, d_model), jnp.bfloat16) for shape in shapes],
        scratch_shapes=[
            pltpu.VMEM((blk, HEAD_DIM), jnp.float32),
            pltpu.VMEM((2, blk, d_model), jnp.bfloat16),
            pltpu.SemaphoreType.DMA((2, max(len(o) for o in outs_of))),
        ],
        compiler_params=pltpu.CompilerParams(vmem_limit_bytes=24 * 2 ** 20),
        cost_estimate=pl.CostEstimate(flops=len(order) * blk * d_model * 8, bytes_accessed=len(order) * blk * d_model * 6, transcendentals=0),
        name="norm_rows",
    )(pltpu.with_memory_space_constraint(x, pltpu.HBM), gain)


def rows_kernel(new_ref, last_ref, gain_ref, cos_ref, sin_ref, wq_hbm, wk, wv, q_ref, k_ref, v_ref, st_ref, wq, q_buf, sem):
    load = pltpu.make_async_copy(wq_hbm, wq, sem)
    load.start()
    n_batch = new_ref.shape[0]
    heads = wk.shape[1] // HEAD_DIM
    xf = jnp.concatenate([new_ref[...].astype(jnp.float32), last_ref[...].astype(jnp.float32)], axis=0)
    inv_rms = lax.rsqrt(jnp.mean(xf * xf, axis=-1, keepdims=True) + 1e-5)
    normed = (xf * inv_rms * gain_ref[...].astype(jnp.float32)).astype(jnp.bfloat16)
    k_all = jnp.dot(normed, wk[...], preferred_element_type=jnp.float32)[:n_batch]
    v_all = jnp.dot(normed, wv[...], preferred_element_type=jnp.float32)[:n_batch].astype(jnp.bfloat16)
    load.wait()
    q_all = jnp.dot(normed, wq[...], preferred_element_type=jnp.float32)
    q_buf[...] = jnp.zeros_like(q_buf)
    k_rot = []
    for h in range(heads):
        cols = slice(h * HEAD_DIM, (h + 1) * HEAD_DIM)
        qh = q_all[:, cols]
        qh = (qh * cos_ref[...] + pltpu.roll(qh, HEAD_DIM // 2, 1) * sin_ref[...]).astype(jnp.bfloat16).astype(jnp.float32)
        kh = k_all[:, cols]
        kh = (kh * cos_ref[:n_batch, :] + pltpu.roll(kh, HEAD_DIM // 2, 1) * sin_ref[:n_batch, :]).astype(jnp.bfloat16)
        k_rot.append(kh)
        score = jnp.sum(qh[:n_batch] * kh.astype(jnp.float32), axis=-1, keepdims=True) * (HEAD_DIM ** -0.5)
        zero = jnp.zeros((n_batch, HEAD_DIM), jnp.float32)
        for t in range(2):
            row = 2 * h + t
            q_buf[:, row, cols] = qh[t * n_batch:(t + 1) * n_batch]
            st_ref[0, :, row, :] = v_all[:, cols].astype(jnp.float32) if t == 0 else zero
            st_ref[1, :, row, :] = zero + score if t == 0 else zero + NEG_BIG
            st_ref[2, :, row, :] = zero + 1.0 if t == 0 else zero
    q_ref[...] = q_buf[...].astype(jnp.bfloat16)
    k_ref[...] = jnp.concatenate(k_rot, axis=1).reshape(n_batch, heads, HEAD_DIM)
    v_ref[...] = v_all.reshape(n_batch, heads, HEAD_DIM)


def rows_call(new_tok, last_x, gain, row_tabs, w_q, w_k, w_v):
    n_batch = new_tok.shape[0]
    width = w_q.shape[1]
    heads = width // HEAD_DIM
    vmem = pl.BlockSpec(memory_space=pltpu.VMEM)
    return pl.pallas_call(
        rows_kernel,
        out_shape=[
            jax.ShapeDtypeStruct((n_batch, STAT_ROWS, width), jnp.bfloat16),
            jax.ShapeDtypeStruct((n_batch, heads, HEAD_DIM), jnp.bfloat16),
            jax.ShapeDtypeStruct((n_batch, heads, HEAD_DIM), jnp.bfloat16),
            jax.ShapeDtypeStruct((3, n_batch, STAT_ROWS, HEAD_DIM), jnp.float32),
        ],
        in_specs=[vmem] * 5 + [pl.BlockSpec(memory_space=pl.ANY)] + [vmem] * 2,
        out_specs=[vmem] * 4,
        scratch_shapes=[
            pltpu.VMEM(w_q.shape, jnp.bfloat16),
            pltpu.VMEM((n_batch, STAT_ROWS, width), jnp.float32),
            pltpu.SemaphoreType.DMA,
        ],
        compiler_params=pltpu.CompilerParams(vmem_limit_bytes=24 * 2 ** 20),
        cost_estimate=pl.CostEstimate(flops=2 * 2 * n_batch * 3 * w_q.shape[0] * width, bytes_accessed=2 * w_q.size, transcendentals=0),
        name="query_rows",
    )(new_tok, last_x, gain, *row_tabs, pltpu.with_memory_space_constraint(w_q, pltpu.HBM), w_k, w_v)


def when(condition):
    if isinstance(condition, bool):
        return lambda body: body() if condition else None
    return pl.when(condition)


def by_group(group, values):
    if isinstance(group, int):
        return values[group]
    out = values[-1]
    for p in range(len(values) - 1):
        out = jnp.where(group == p, values[p], out)
    return out


def kv_kernel(n_in, n_steps, masks, batches, firsts, row0, stat_of, with_new, raw, *refs):
    n_groups = len(masks)
    n_arr = n_in * n_groups
    x_refs = refs[:n_arr]
    cos_ref, sin_ref, len_ref, wk, wv, q_ref = refs[n_arr:n_arr + 6]
    rest = refs[n_arr + 6:]
    if raw:
        gain_ref, *rest = rest
    if with_new:
        new_refs = rest[:2]
        rest = rest[2:]
    else:
        rest = rest[3:]
    kc_ref, vc_ref, st_ref, x_buf, k_buf, v_buf, k_out, v_out, s_out, x_sem, sems, s_sem = rest[:12]
    me = lax.axis_index("model")
    step = pl.program_id(0) if n_steps > 1 else 0
    slot = lax.rem(step, 2) if n_steps > 1 else 0
    per_group = n_steps // n_groups
    blk = x_buf.shape[2]
    shard_rows = cos_ref.shape[1]
    width = wk.shape[1]
    heads = width // HEAD_DIM
    n_tok = n_in * blk

    def x_copies(at_step, which, group):
        local = at_step - group * per_group
        return [pltpu.make_async_copy(x_refs[group * n_in + i].at[firsts[group][i] + local],
                                      x_buf.at[which, i], x_sem.at[which, i]) for i in range(n_in)]

    def start_x(at_step, which):
        for group in range(n_groups):
            @when(at_step // per_group == group)
            def _(group=group):
                for copy in x_copies(at_step, which, group):
                    copy.start()

    def place(i, at_step):
        group = at_step // per_group
        mask = by_group(group, [m[i] for m in masks])
        shard = sum(lax.rem(me // bit + mask // bit, 2) * bit for bit in (1, 2, 4))
        return shard, by_group(group, [b[i] for b in batches]) + at_step % per_group, mask

    def out_copies(which, at_step):
        copies = []
        for i in range(n_in):
            shard, bat, _ = place(i, at_step)
            rows = pl.ds(shard * shard_rows + row0, blk)
            copies.append(pltpu.make_async_copy(k_out.at[which, i], kc_ref.at[bat, rows], sems.at[which, i, 0]))
            copies.append(pltpu.make_async_copy(v_out.at[which, i], vc_ref.at[bat, rows], sems.at[which, i, 1]))
        return copies

    def new_copies():
        return [pltpu.make_async_copy(src.at[pl.ds(b, 1)], dst.at[b, pl.ds(dst.shape[1] - 1, 1)], rest[12].at[idx, b])
                for idx, (src, dst) in enumerate(zip(new_refs, (kc_ref, vc_ref))) for b in range(src.shape[0])]

    @when(step == 0)
    def _():
        start_x(step, slot)
        if with_new:
            for copy in new_copies():
                copy.start()

    @when(step + 1 < n_steps)
    def _():
        start_x(step + 1, 1 - slot)

    @when(step >= 2)
    def _():
        for copy in out_copies(slot, step - 2):
            copy.wait()

    for copy in x_copies(0, slot, 0):
        copy.wait()
    x_rows = x_buf.at[slot]
    if raw:
        lanes = [slice(c * HEAD_DIM, (c + 1) * HEAD_DIM) for c in range(x_buf.shape[3] // HEAD_DIM)]
        for i in range(n_in):
            def norm_rows(r, carry, i=i):
                at = pl.ds(pl.multiple_of(r * NORM_ROWS, NORM_ROWS), NORM_ROWS)
                acc = [jnp.zeros((NORM_ROWS, HEAD_DIM), jnp.float32) for _ in range(2)]
                for c, lane in enumerate(lanes):
                    xf = x_rows[i, at, lane].astype(jnp.float32)
                    acc[c % 2] += xf * xf
                inv_rms = lax.rsqrt(jnp.sum(acc[0] + acc[1], axis=-1, keepdims=True) / x_buf.shape[3] + 1e-5)
                for lane in lanes:
                    xf = x_rows[i, at, lane].astype(jnp.float32)
                    x_rows[i, at, lane] = (xf * inv_rms * gain_ref[:, lane].astype(jnp.float32)).astype(jnp.bfloat16)
                return carry

            lax.fori_loop(0, blk // NORM_ROWS, norm_rows, 0)

    def col_tile(c, carry):
        cols = pl.ds(pl.multiple_of(c * COL_TILE, COL_TILE), COL_TILE) if n_steps > 1 else slice(c * COL_TILE, (c + 1) * COL_TILE)
        normed = x_rows[...].reshape(n_tok, x_buf.shape[3])
        kf = jnp.dot(normed, wk[:, cols], preferred_element_type=jnp.float32)
        vf = jnp.dot(normed, wv[:, cols], preferred_element_type=jnp.float32)
        v_buf[:, cols] = vf.astype(jnp.bfloat16)
        parts = []
        for i in range(n_in):
            shard = place(i, step)[0]
            cos_tab = cos_ref[shard, row0:row0 + blk]
            sin_tab = sin_ref[shard, row0:row0 + blk]
            halves = []
            for h in range(COL_TILE // HEAD_DIM):
                kh = kf[i * blk:(i + 1) * blk, h * HEAD_DIM:(h + 1) * HEAD_DIM]
                halves.append(kh * cos_tab + pltpu.roll(kh, HEAD_DIM // 2, 1) * sin_tab)
            parts.append(jnp.concatenate(halves, axis=1))
        k_buf[:, cols] = jnp.concatenate(parts, axis=0).astype(jnp.bfloat16)
        return carry

    if n_steps > 1:
        lax.fori_loop(0, width // COL_TILE, col_tile, 0)
    else:
        for c in range(width // COL_TILE):
            col_tile(c, 0)

    for i in range(n_in):
        k_out[slot, i] = k_buf[i * blk:(i + 1) * blk, :].reshape(blk, heads, HEAD_DIM)
        v_out[slot, i] = v_buf[i * blk:(i + 1) * blk, :].reshape(blk, heads, HEAD_DIM)
    for copy in out_copies(slot, step):
        copy.start()

    head_of_row = lax.broadcasted_iota(jnp.int32, (STAT_ROWS, HEAD_DIM), 0) // (STAT_ROWS // heads)
    probs = []
    for i in range(n_in):
        shard, bat, _ = place(i, step)
        scores = lax.dot_general(q_ref[bat], k_buf[i * blk:(i + 1) * blk, :], (((1,), (1,)), ((), ())),
                                 preferred_element_type=jnp.float32) * (HEAD_DIM ** -0.5)
        pos = shard * shard_rows + row0 + lax.broadcasted_iota(jnp.int32, scores.shape, 1)
        visible = pos < len_ref[pl.ds(bat, 1), :blk]
        scores = jnp.where(visible, scores, NEG_BIG)
        blk_max = jnp.max(scores, axis=-1, keepdims=True)
        prob = jnp.where(visible, jnp.exp(scores - blk_max), 0.0)
        probs.append((blk_max, prob))
    for i, (blk_max, prob) in enumerate(probs):
        full = jnp.dot(prob.astype(jnp.bfloat16), v_buf[i * blk:(i + 1) * blk, :], preferred_element_type=jnp.float32)
        acc = jnp.zeros((STAT_ROWS, HEAD_DIM), jnp.float32)
        for h in range(heads):
            acc = jnp.where(head_of_row == h, full[:, h * HEAD_DIM:(h + 1) * HEAD_DIM], acc)
        s_out[i, 0] = acc
        s_out[i, 1] = jnp.broadcast_to(blk_max, (STAT_ROWS, HEAD_DIM))
        s_out[i, 2] = jnp.broadcast_to(jnp.sum(prob, axis=-1, keepdims=True), (STAT_ROWS, HEAD_DIM))
    stat_copies = []
    for i in range(n_in):
        _, bat, mask = place(i, step)
        stat_copies.append(pltpu.make_async_copy(s_out.at[i], st_ref.at[mask + stat_of, bat], s_sem.at[i]))
        stat_copies[-1].start()
    for copy in stat_copies:
        copy.wait()

    @when(step == n_steps - 1)
    def _():
        for copy in out_copies(slot, step):
            copy.wait()
        if with_new:
            for copy in new_copies():
                copy.wait()
        if n_steps > 1:
            for copy in out_copies(1 - slot, step - 1):
                copy.wait()


def kv_call(groups, per_group, masks, batches, lengths, tabs, w_k, w_v, q_diag, caches, new_rows=None, row0=0, stat_of=0, gain=None):
    n_groups = len(groups)
    n_in = len(groups[0])
    n_steps = n_groups * per_group
    cos_tab, sin_tab = tabs
    blk, d_model = groups[0][0][0].shape[1:]
    width = w_k.shape[1]
    heads = width // HEAD_DIM
    any_spec = pl.BlockSpec(memory_space=pl.ANY)
    operands = [arr for group in groups for arr, _ in group]
    in_specs = [any_spec] * len(operands) + [pl.BlockSpec(memory_space=pltpu.VMEM)] * 6
    operands += [cos_tab, sin_tab, lengths, w_k, w_v, q_diag]
    if gain is not None:
        in_specs.append(pl.BlockSpec(memory_space=pltpu.VMEM))
        operands.append(gain)
    with_new = new_rows is not None
    if with_new:
        operands += new_rows
        in_specs += [any_spec] * 2
        aliases = {}
    else:
        operands += [*caches[:2], pltpu.with_memory_space_constraint(caches[2], pltpu.VMEM)]
        in_specs += [any_spec] * 3
        aliases = {len(operands) - 3: 0, len(operands) - 2: 1, len(operands) - 1: 2}
    tokens = n_in * blk
    n_batch = q_diag.shape[0]
    slots = min(n_steps, 2)
    return pl.pallas_call(
        functools.partial(kv_kernel, n_in, n_steps, masks, batches, [[first for _, first in group] for group in groups], row0, stat_of, with_new, gain is not None),
        grid=(n_steps,) if n_steps > 1 else (),
        in_specs=in_specs,
        out_specs=[any_spec] * 3,
        scratch_shapes=[
            pltpu.VMEM((slots, n_in, blk, d_model), jnp.bfloat16),
            pltpu.VMEM((tokens, width), jnp.bfloat16),
            pltpu.VMEM((tokens, width), jnp.bfloat16),
            pltpu.VMEM((slots, n_in, blk, heads, HEAD_DIM), jnp.bfloat16),
            pltpu.VMEM((slots, n_in, blk, heads, HEAD_DIM), jnp.bfloat16),
            pltpu.VMEM((n_in, 3, STAT_ROWS, HEAD_DIM), jnp.float32),
            pltpu.SemaphoreType.DMA((slots, n_in)),
            pltpu.SemaphoreType.DMA((slots, n_in, 2)),
            pltpu.SemaphoreType.DMA((n_in,)),
        ] + [pltpu.SemaphoreType.DMA((2, n_batch))] * with_new,
        out_shape=[*(jax.ShapeDtypeStruct(c.shape, c.dtype) for c in caches[:2]), pltpu.VMEM(caches[2].shape, caches[2].dtype)],
        input_output_aliases=aliases,
        compiler_params=pltpu.CompilerParams(vmem_limit_bytes=20 * 2 ** 20),
        cost_estimate=pl.CostEstimate(flops=4 * n_steps * tokens * d_model * width, bytes_accessed=2 * n_steps * tokens * (d_model + 2 * width), transcendentals=0),
        name="kv_chunk",
    )(*operands)


def tail_kernel(n_dev, parts_of, stv, self_ref, xs_ref, gain_ref, wo, wg_hbm, wu_hbm, wd_hbm, out_ref,
                wg, wu, wd, rows, a_buf, n_buf, ps1, pr1, ps2, pr2, xo1, xg1, xo2, xg2, w_sem, send_sem, recv_sem):
    me = lax.axis_index("model")
    n_batch = out_ref.shape[1]
    n_rows = 2 * n_batch
    d_model = out_ref.shape[2]
    cols = d_model // n_dev
    heads = STAT_ROWS // 2
    loads = [pltpu.make_async_copy(src, dst, w_sem.at[i]) for i, (src, dst) in enumerate(((wg_hbm, wg), (wu_hbm, wu), (wd_hbm, wd)))]
    for load in loads:
        load.start()
    barrier = pltpu.get_barrier_semaphore()

    def peer_of(mask):
        return sum(lax.rem(me // bit + mask // bit, 2) * bit for bit in (1, 2, 4))

    far_first = ((6, 7), (2, 3, 4, 5), (1,))
    for mask in sum(far_first, ()):
        pl.semaphore_signal(barrier, inc=1, device_id={"model": peer_of(mask)}, device_id_type=MESH)

    def send(phase, mask, src, dst):
        return pltpu.make_async_remote_copy(
            src_ref=src, dst_ref=dst, send_sem=send_sem.at[phase, mask - 1], recv_sem=recv_sem.at[phase, mask - 1],
            device_id={"model": peer_of(mask)}, device_id_type=MESH)

    for b in range(n_batch):
        top = self_ref[1, b]
        for j in range(parts_of[b]):
            top = jnp.maximum(top, stv[j, b, 1])
        scale = jnp.exp(self_ref[1, b] - top)
        den = scale * self_ref[2, b]
        num = scale * self_ref[0, b]
        for j in range(parts_of[b]):
            scale = jnp.exp(stv[j, b, 1] - top)
            den += scale * stv[j, b, 2]
            num += scale * stv[j, b, 0]
        rows[:, b, :] = num / den
    for h in range(heads):
        for t in range(2):
            a_buf[t * n_batch:(t + 1) * n_batch, h * HEAD_DIM:(h + 1) * HEAD_DIM] = rows[2 * h + t]
    att = a_buf[...].astype(jnp.bfloat16)

    def exchange(phase, base, copies, pr, xo, xg):
        total = base
        for copy, mask in reversed(copies):
            copy.wait_recv()
            total = total + pr[mask - 1]
        xo[...] = total.astype(jnp.bfloat16)
        xg[me] = xo[...]
        outs = []
        for mask in sum(far_first, ()):
            outs.append(send(phase + 1, mask, xo, xg.at[me]))
            outs[-1].start()
        for out in outs:
            out.wait_recv()
        return [copy for copy, _ in copies] + outs

    def col_block(p):
        return pl.ds(pl.multiple_of(p * cols, cols), cols)

    part = jnp.dot(att, wo[...], preferred_element_type=jnp.float32)
    for j in range(n_dev):
        ps1[j] = part[:, j * cols:(j + 1) * cols]
    pl.semaphore_wait(barrier, n_dev - 1)
    copies = []
    for mask in sum(far_first, ()):
        copies.append((send(0, mask, ps1.at[peer_of(mask)], pr1.at[mask - 1]), mask))
        copies[-1][0].start()
    sent = exchange(0, xs_ref[...].astype(jnp.float32) + ps1[me], copies, pr1, xo1, xg1)
    sq = jnp.zeros((n_rows, 1), jnp.float32)
    for j in range(n_dev):
        xf = xg1[j].astype(jnp.float32)
        sq += jnp.sum(xf * xf, axis=-1, keepdims=True)
    inv_rms = lax.rsqrt(sq / d_model + 1e-5)
    for j in range(n_dev):
        at = slice(j * cols, (j + 1) * cols)
        n_buf[:, at] = (xg1[j].astype(jnp.float32) * inv_rms * gain_ref[:, at].astype(jnp.float32)).astype(jnp.bfloat16)
    loads[0].wait()
    loads[1].wait()
    gate = jnp.dot(n_buf[...], wg[...], preferred_element_type=jnp.float32)
    up = jnp.dot(n_buf[...], wu[...], preferred_element_type=jnp.float32)
    mid = (gate * (1.0 / (1.0 + jnp.exp(-gate))) * up).astype(jnp.bfloat16)
    loads[2].wait()
    copies = []
    for group in far_first:
        for mask in group:
            ps2[mask] = jnp.dot(mid, wd[:, col_block(peer_of(mask))], preferred_element_type=jnp.float32)
        if group == far_first[-1]:
            ps2[0] = jnp.dot(mid, wd[:, col_block(me)], preferred_element_type=jnp.float32)
        for mask in group:
            copies.append((send(2, mask, ps2.at[mask], pr2.at[mask - 1]), mask))
            copies[-1][0].start()
    sent += exchange(2, xo1[...].astype(jnp.float32) + ps2[0], copies, pr2, xo2, xg2)
    for j in range(n_dev):
        at = slice(j * cols, (j + 1) * cols)
        out_ref[0, :, at] = xg2[j, :n_batch]
        out_ref[1, :, at] = xg2[j, n_batch:]
    for copy in sent:
        copy.wait_send()


def tail_call(n_dev, parts_of, stats, self_stat, x_mine, gain, w_o, w_gate, w_up, w_down, n_batch):
    n_rows, cols = x_mine.shape
    d_model = w_o.shape[1]
    vmem = pl.BlockSpec(memory_space=pltpu.VMEM)
    any_spec = pl.BlockSpec(memory_space=pl.ANY)
    exchanged = [pltpu.VMEM((n_dev, n_rows, cols), jnp.float32), pltpu.VMEM((n_dev - 1, n_rows, cols), jnp.float32)]
    summed = [pltpu.VMEM((n_rows, cols), jnp.bfloat16), pltpu.VMEM((n_dev, n_rows, cols), jnp.bfloat16)]
    return pl.pallas_call(
        functools.partial(tail_kernel, n_dev, parts_of),
        out_shape=jax.ShapeDtypeStruct((2, n_batch, d_model), jnp.bfloat16),
        in_specs=[vmem] * 5 + [any_spec] * 3,
        out_specs=vmem,
        scratch_shapes=[
            pltpu.VMEM(w_gate.shape, jnp.bfloat16),
            pltpu.VMEM(w_up.shape, jnp.bfloat16),
            pltpu.VMEM(w_down.shape, jnp.bfloat16),
            pltpu.VMEM((STAT_ROWS, n_batch, HEAD_DIM), jnp.float32),
            pltpu.VMEM((n_rows, w_o.shape[0]), jnp.float32),
            pltpu.VMEM((n_rows, d_model), jnp.bfloat16),
            *exchanged, *exchanged, *summed, *summed,
            pltpu.SemaphoreType.DMA((3,)),
            pltpu.SemaphoreType.DMA((4, n_dev - 1)),
            pltpu.SemaphoreType.DMA((4, n_dev - 1)),
        ],
        compiler_params=pltpu.CompilerParams(collective_id=0, has_side_effects=True, vmem_limit_bytes=46 * 2 ** 20),
        name="tail",
    )(pltpu.with_memory_space_constraint(stats, pltpu.VMEM), self_stat, x_mine, gain, w_o,
      *(pltpu.with_memory_space_constraint(w, pltpu.HBM) for w in (w_gate, w_up, w_down)))


def solution(mesh):
    n_dev = mesh.shape['model']
    seq_spec = P('replica', 'model', None)
    col_spec = P(None, None, 'model')
    row_spec = P(None, 'model', None)
    gain_spec = P(None, None)
    tok_spec = P('replica', None)
    cache_spec = P(None, 'replica', None, 'model', None)
    in_specs = (seq_spec, P('replica'), tok_spec, gain_spec, col_spec, col_spec, col_spec, row_spec, gain_spec, col_spec, col_spec, row_spec)
    out_specs = (tok_spec, tok_spec, cache_spec, cache_spec)

    def swap(arr, bit):
        return lax.ppermute(arr, 'model', [(i, i ^ bit) for i in range(n_dev)])

    def per_device(prompt, lengths, new_tok, norm_attn, w_q, w_k, w_v, w_o, norm_mlp, w_gate, w_up, w_down):
        my_idx = lax.axis_index('model')
        n_batch, blk, d_model = prompt.shape
        seq_len = blk * n_dev
        width = w_k.shape[2]
        heads = width // HEAD_DIM
        half = n_batch // 2
        wq = w_q[0]
        gain = norm_attn

        q1, q2, rows_h = 1, n_batch // 4, blk // 2
        a_parts, b_parts = {}, {}
        a_parts["0a"], b_parts["0a"] = prompt[:1, :rows_h], prompt[half:half + 1, :rows_h]
        a_parts["0b"], b_parts["0b"] = first_call(prompt, norm_attn, [(0, rows_h), (half, rows_h)], rows_h)
        from_y, from_x = {}, {}

        def send_part(step, along_y, along_x):
            from_y[step] = swap(along_y, 4)
            from_x[step] = swap(along_x, 2)

        send_part("0a", a_parts["0a"], b_parts["0a"])
        send_part("0b", a_parts["0b"], b_parts["0b"])
        order, outs_of = [], []
        for part, (lo, hi) in ((1, (q1, q2)), (2, (q2, half)), (0, (0, q1))):
            for k in range(lo, hi):
                for side in range(2):
                    order.append(side * half + k)
                    outs_of.append([(4, side * half + k, 0, blk)] + ([(2 * part - 2 + side, k - lo, 0, blk)] if part else []))
        a_parts["1"], b_parts["1"], a_parts["2"], b_parts["2"], normed = norm_call(
            prompt, gain, order, outs_of, [(q2 - q1, blk)] * 2 + [(half - q2, blk)] * 2 + [(n_batch, blk)])
        send_part("1", a_parts["1"], b_parts["1"])
        seq_pos = my_idx * blk + jnp.arange(blk)
        sel = (seq_pos[None, :] == (lengths - 1)[:, None]).astype(jnp.bfloat16)
        last_x = jnp.einsum('bs,bsd->bd', sel, prompt, preferred_element_type=jnp.float32).astype(jnp.bfloat16)
        core, cols_h = my_idx % 2, d_model // 2
        last_x = last_x + swap(last_x, 1)
        last_x = lax.dynamic_slice_in_dim(last_x, core * cols_h, cols_h, axis=1)
        last_x = (last_x + swap(last_x, 2)) + (swap(last_x, 4) + swap(last_x, 6))
        other_x = swap(last_x, 1)
        last_x = jnp.where(core == 0, jnp.concatenate([last_x, other_x], axis=1), jnp.concatenate([other_x, last_x], axis=1))
        send_part("2", a_parts["2"], b_parts["2"])
        send_part("3", b_parts["2"], a_parts["2"])
        send_part("4", normed[half:half + q2], normed[:q2])
        core_all = swap(normed, 1)

        len_rows = jnp.broadcast_to(lengths.astype(jnp.int32)[:, None], (n_batch, HEAD_DIM))
        row_tabs = rotary_tables(jnp.concatenate([lengths, lengths - 1]))
        tabs = tuple(tab.reshape(n_dev, blk, HEAD_DIM) for tab in rotary_tables(jnp.arange(seq_len)))
        x_rows = jnp.concatenate([new_tok, last_x], axis=0)
        x_mine = lax.dynamic_slice_in_dim(x_rows, my_idx * (d_model // n_dev), d_model // n_dev, axis=1)
        wk, wv, wo, last_x, len_rows, row_tabs, tabs, x_mine = lax.optimization_barrier(
            (w_k[0], w_v[0], w_o[0], last_x, len_rows, row_tabs, tabs, x_mine))
        wk, wv, wo = keep_in_vmem(wk, wv, wo)
        q_diag, k_new, v_new, self_stat = rows_call(new_tok, last_x, gain, row_tabs, wq, wk, wv)
        cache_shape = jax.ShapeDtypeStruct((n_batch, seq_len + 1, heads, HEAD_DIM), jnp.bfloat16)
        caches = [cache_shape, cache_shape, jax.ShapeDtypeStruct((2 * n_dev - 2, n_batch, 3, STAT_ROWS, HEAD_DIM), jnp.float32)]

        def run(groups, per_group, masks, batches, caches, **kw):
            return kv_call(groups, per_group, masks, batches, len_rows, tabs, wk, wv, q_diag, caches, **kw)

        def half_rows(step):
            return {"row0": rows_h * (step == "0b"), "stat_of": (n_dev - 2) * (step == "0b"), "gain": norm_attn if step == "0a" else None}

        def after(caches, *arrays):
            out = lax.optimization_barrier((caches[2], *arrays))
            return [caches[0], caches[1], out[0]], out[1:]

        caches = run([[(arr, 0), (arr, half)] for arr in (normed, core_all)], half,
                     [[0] * 2, [1] * 2], [[0, half]] * 2, caches, new_rows=[k_new, v_new])
        diag, turned = {}, {}
        starts = {"0a": (0, half), "0b": (0, half), "1": (q1, half + q1), "2": (q2, half + q2), "3": (half + q2, q2), "4": (half, 0)}
        for step, start in starts.items():
            caches, (got_y, got_x) = after(caches, from_y[step], from_x[step])
            other_y, other_x = swap(got_y, 1), swap(got_x, 1)
            if step not in "34":
                via_x = swap(got_y, 2)
                via_y = swap(got_x, 4)
                diag[step] = (via_x, via_y)
            streams = [[(got_y, 0), (got_x, 0)], [(other_y, 0), (other_x, 0)]]
            if step in ("0a", "0b"):
                caches = run([streams[0] + streams[1]], q1, [[4, 2, 5, 3]], [[*start, *start]], caches, **half_rows(step))
            else:
                caches = run(streams, got_y.shape[0], [[4, 2], [5, 3]], [list(start)] * 2, caches)
            if step in "34":
                caches, (w_t,) = after(caches, (w_gate if step == "3" else w_up)[0].T)
                turned[step] = turn_call(w_t)
                caches, (turned[step],) = after(caches, turned[step])
        for step in ("2", "1", "0a", "0b"):
            caches, (via_y,) = after(caches, diag[step][1])
            caches, (via_x,) = after(caches, diag[step][0])
            other_y = swap(via_y, 1)
            other_x = swap(via_x, 1)
            start = starts[step]
            streams = [[(via_x, 0), (via_y, 0)], [(other_x, 0), (other_y, 0)]]
            if step in ("0a", "0b"):
                caches = run([streams[0] + streams[1]], q1, [[6, 6, 7, 7]], [[*start, *start]], caches, **half_rows(step))
            else:
                caches = run(streams, via_x.shape[0], [[6] * 2, [7] * 2], [list(start)] * 2, caches)

        k_cache, v_cache, stats = caches
        parts_of = [2 * n_dev - 2 if b % half < q1 else n_dev for b in range(n_batch)]
        both = tail_call(n_dev, parts_of, stats, self_stat, x_mine, norm_mlp, wo, turned["3"], turned["4"], w_down[0], n_batch)
        return both[0], both[1], k_cache[None], v_cache[None]

    return jax.shard_map(per_device, mesh=mesh, in_specs=in_specs, out_specs=out_specs, check_vma=False)
```

```python
import functools

import jax
import jax.numpy as jnp
from jax import lax
from jax.experimental import pallas as pl
from jax.experimental.pallas import tpu as pltpu
from jax.sharding import PartitionSpec as P


HEAD_DIM = 128
NEG_BIG = -1e30
STAT_ROWS = 8
NORM_ROWS = 32
COL_TILE = 256
MESH = pl.DeviceIdType.MESH


def rotary_tables(positions):
    half_dim = HEAD_DIM // 2
    inv_freq = 10000.0 ** (-2.0 * jnp.arange(half_dim, dtype=jnp.float32) / HEAD_DIM)
    angles = positions.astype(jnp.float32)[..., None] * inv_freq
    cos_tab = jnp.cos(angles)
    sin_tab = jnp.sin(angles)
    return jnp.concatenate([cos_tab, cos_tab], axis=-1), jnp.concatenate([-sin_tab, sin_tab], axis=-1)


def load_kernel(*refs):
    n = len(refs) // 2
    sem = refs[-1]
    copies = [pltpu.make_async_copy(refs[i], refs[n + i], sem.at[i]) for i in range(n)]
    for copy in copies:
        copy.start()
    for copy in copies:
        copy.wait()


def keep_in_vmem(*arrays):
    return pl.pallas_call(
        load_kernel,
        out_shape=[pltpu.VMEM(arr.shape, arr.dtype) for arr in arrays],
        in_specs=[pl.BlockSpec(memory_space=pl.ANY)] * len(arrays),
        out_specs=[pl.BlockSpec(memory_space=pltpu.VMEM)] * len(arrays),
        scratch_shapes=[pltpu.SemaphoreType.DMA((len(arrays),))],
        compiler_params=pltpu.CompilerParams(vmem_limit_bytes=24 * 2 ** 20),
        name="keep",
    )(*(pltpu.with_memory_space_constraint(arr, pltpu.HBM) for arr in arrays))


def turn_kernel(w_ref, out_ref):
    out_ref[...] = w_ref[...].T


def turn_call(w_t):
    n, d = w_t.shape
    cols = 512
    return pl.pallas_call(
        turn_kernel,
        grid=(d // cols,),
        in_specs=[pl.BlockSpec((n, cols), lambda g: (0, g))],
        out_specs=pl.BlockSpec((cols, n), lambda g: (g, 0)),
        out_shape=jax.ShapeDtypeStruct((d, n), w_t.dtype),
        compiler_params=pltpu.CompilerParams(vmem_limit_bytes=12 * 2 ** 20),
        cost_estimate=pl.CostEstimate(flops=2 * d * n * 128, bytes_accessed=4 * d * n, transcendentals=0),
        name="turn",
    )(pltpu.with_memory_space_constraint(w_t, pltpu.HBM))


def norm_kernel(outs_of, x_ref, gain_ref, *refs):
    n_out = len(refs) - 3
    out_refs = refs[:n_out]
    ss_buf, n_buf, sems = refs[n_out:]
    step = pl.program_id(0)
    blk, d_model = x_ref.shape[1:]
    lanes = [slice(c * HEAD_DIM, (c + 1) * HEAD_DIM) for c in range(d_model // HEAD_DIM)]

    def copies(at_step):
        return [pltpu.make_async_copy(n_buf.at[at_step % 2, pl.ds(lo, rows)], out_refs[o].at[i], sems.at[at_step % 2, k])
                for k, (o, i, lo, rows) in enumerate(outs_of[at_step])]

    for at_step in range(2, len(outs_of)):
        @pl.when(step == at_step)
        def _():
            for copy in copies(at_step - 2):
                copy.wait()

    def square_rows(r, carry):
        rows = pl.ds(pl.multiple_of(r * NORM_ROWS, NORM_ROWS), NORM_ROWS)
        acc = [jnp.zeros((NORM_ROWS, HEAD_DIM), jnp.float32) for _ in range(2)]
        for c, lane in enumerate(lanes):
            xf = x_ref[0, rows, lane].astype(jnp.float32)
            acc[c % 2] += xf * xf
        ss_buf[rows, :] = acc[0] + acc[1]
        return carry

    lax.fori_loop(0, blk // NORM_ROWS, square_rows, 0)
    total = jnp.sum(ss_buf[...], axis=-1, keepdims=True)
    ss_buf[...] = jnp.broadcast_to(lax.rsqrt(total / d_model + 1e-5), (blk, HEAD_DIM))
    slot = lax.rem(step, 2)

    def norm_rows(r, carry):
        rows = pl.ds(pl.multiple_of(r * NORM_ROWS, NORM_ROWS), NORM_ROWS)
        inv_rms = ss_buf[rows, :]
        for lane in lanes:
            xf = x_ref[0, rows, lane].astype(jnp.float32)
            n_buf[slot, rows, lane] = (xf * inv_rms * gain_ref[:, lane].astype(jnp.float32)).astype(jnp.bfloat16)
        return carry

    lax.fori_loop(0, blk // NORM_ROWS, norm_rows, 0)
    for at_step in range(len(outs_of)):
        @pl.when(step == at_step)
        def _():
            for copy in copies(at_step):
                copy.start()
            if at_step == len(outs_of) - 1:
                for copy in copies(at_step):
                    copy.wait()
                if at_step >= 1:
                    for copy in copies(at_step - 1):
                        copy.wait()


def first_kernel(places, rows, x_hbm, gain_hbm, *refs):
    n = len(places)
    out_refs = refs[:n]
    x_buf, gain_ref, sem = refs[n:]
    d_model = x_hbm.shape[2]
    loads = [pltpu.make_async_copy(x_hbm.at[bat, pl.ds(row0, rows)], x_buf.at[i], sem.at[i]) for i, (bat, row0) in enumerate(places)]
    loads.append(pltpu.make_async_copy(gain_hbm, gain_ref, sem.at[n]))
    for load in loads:
        load.start()
    loads[n].wait()
    lanes = [slice(c * HEAD_DIM, (c + 1) * HEAD_DIM) for c in range(d_model // HEAD_DIM)]
    for i in range(n):
        loads[i].wait()

        def norm_rows(r, carry):
            at = pl.ds(pl.multiple_of(r * NORM_ROWS, NORM_ROWS), NORM_ROWS)
            acc = [jnp.zeros((NORM_ROWS, HEAD_DIM), jnp.float32) for _ in range(2)]
            for c, lane in enumerate(lanes):
                xf = x_buf[i, at, lane].astype(jnp.float32)
                acc[c % 2] += xf * xf
            inv_rms = lax.rsqrt(jnp.sum(acc[0] + acc[1], axis=-1, keepdims=True) / d_model + 1e-5)
            for lane in lanes:
                xf = x_buf[i, at, lane].astype(jnp.float32)
                out_refs[i][0, at, lane] = (xf * inv_rms * gain_ref[:, lane].astype(jnp.float32)).astype(jnp.bfloat16)
            return carry

        lax.fori_loop(0, rows // NORM_ROWS, norm_rows, 0)


def first_call(x, gain, places, rows):
    d_model = x.shape[2]
    return pl.pallas_call(
        functools.partial(first_kernel, places, rows),
        out_shape=[pltpu.VMEM((1, rows, d_model), jnp.bfloat16)] * len(places),
        in_specs=[pl.BlockSpec(memory_space=pl.ANY)] * 2,
        out_specs=[pl.BlockSpec(memory_space=pltpu.VMEM)] * len(places),
        scratch_shapes=[
            pltpu.VMEM((len(places), rows, d_model), jnp.bfloat16),
            pltpu.VMEM(gain.shape, gain.dtype),
            pltpu.SemaphoreType.DMA((len(places) + 1,)),
        ],
        compiler_params=pltpu.CompilerParams(vmem_limit_bytes=8 * 2 ** 20),
        cost_estimate=pl.CostEstimate(flops=len(places) * rows * d_model * 8, bytes_accessed=len(places) * rows * d_model * 4, transcendentals=0),
        name="first_rows",
    )(*(pltpu.with_memory_space_constraint(a, pltpu.HBM) for a in (x, gain)))


def norm_call(x, gain, order, outs_of, shapes, blk=None, row_block=0):
    d_model = x.shape[2]
    blk = blk or x.shape[1]

    def prompt_of(g):
        idx = jnp.int32(order[-1])
        for k in range(len(order) - 1):
            idx = jnp.where(g == k, order[k], idx)
        return idx

    return pl.pallas_call(
        functools.partial(norm_kernel, outs_of),
        grid=(len(order),),
        in_specs=[pl.BlockSpec((1, blk, d_model), lambda g: (prompt_of(g), row_block, 0)),
                  pl.BlockSpec((1, d_model), lambda g: (0, 0))],
        out_specs=[pl.BlockSpec(memory_space=pl.ANY)] * len(shapes),
        out_shape=[jax.ShapeDtypeStruct((*shape, d_model), jnp.bfloat16) for shape in shapes],
        scratch_shapes=[
            pltpu.VMEM((blk, HEAD_DIM), jnp.float32),
            pltpu.VMEM((2, blk, d_model), jnp.bfloat16),
            pltpu.SemaphoreType.DMA((2, max(len(o) for o in outs_of))),
        ],
        compiler_params=pltpu.CompilerParams(vmem_limit_bytes=24 * 2 ** 20),
        cost_estimate=pl.CostEstimate(flops=len(order) * blk * d_model * 8, bytes_accessed=len(order) * blk * d_model * 6, transcendentals=0),
        name="norm_rows",
    )(pltpu.with_memory_space_constraint(x, pltpu.HBM), gain)


def rows_kernel(new_ref, last_ref, gain_ref, cos_ref, sin_ref, wq_hbm, wk, wv, q_ref, k_ref, v_ref, st_ref, wq, q_buf, sem):
    load = pltpu.make_async_copy(wq_hbm, wq, sem)
    load.start()
    n_batch = new_ref.shape[0]
    heads = wk.shape[1] // HEAD_DIM
    xf = jnp.concatenate([new_ref[...].astype(jnp.float32), last_ref[...].astype(jnp.float32)], axis=0)
    inv_rms = lax.rsqrt(jnp.mean(xf * xf, axis=-1, keepdims=True) + 1e-5)
    normed = (xf * inv_rms * gain_ref[...].astype(jnp.float32)).astype(jnp.bfloat16)
    k_all = jnp.dot(normed, wk[...], preferred_element_type=jnp.float32)[:n_batch]
    v_all = jnp.dot(normed, wv[...], preferred_element_type=jnp.float32)[:n_batch].astype(jnp.bfloat16)
    load.wait()
    q_all = jnp.dot(normed, wq[...], preferred_element_type=jnp.float32)
    q_buf[...] = jnp.zeros_like(q_buf)
    k_rot = []
    for h in range(heads):
        cols = slice(h * HEAD_DIM, (h + 1) * HEAD_DIM)
        qh = q_all[:, cols]
        qh = (qh * cos_ref[...] + pltpu.roll(qh, HEAD_DIM // 2, 1) * sin_ref[...]).astype(jnp.bfloat16).astype(jnp.float32)
        kh = k_all[:, cols]
        kh = (kh * cos_ref[:n_batch, :] + pltpu.roll(kh, HEAD_DIM // 2, 1) * sin_ref[:n_batch, :]).astype(jnp.bfloat16)
        k_rot.append(kh)
        score = jnp.sum(qh[:n_batch] * kh.astype(jnp.float32), axis=-1, keepdims=True) * (HEAD_DIM ** -0.5)
        zero = jnp.zeros((n_batch, HEAD_DIM), jnp.float32)
        for t in range(2):
            row = 2 * h + t
            q_buf[:, row, cols] = qh[t * n_batch:(t + 1) * n_batch]
            st_ref[0, :, row, :] = v_all[:, cols].astype(jnp.float32) if t == 0 else zero
            st_ref[1, :, row, :] = zero + score if t == 0 else zero + NEG_BIG
            st_ref[2, :, row, :] = zero + 1.0 if t == 0 else zero
    q_ref[...] = q_buf[...].astype(jnp.bfloat16)
    k_ref[...] = jnp.concatenate(k_rot, axis=1).reshape(n_batch, heads, HEAD_DIM)
    v_ref[...] = v_all.reshape(n_batch, heads, HEAD_DIM)


def rows_call(new_tok, last_x, gain, row_tabs, w_q, w_k, w_v):
    n_batch = new_tok.shape[0]
    width = w_q.shape[1]
    heads = width // HEAD_DIM
    vmem = pl.BlockSpec(memory_space=pltpu.VMEM)
    return pl.pallas_call(
        rows_kernel,
        out_shape=[
            jax.ShapeDtypeStruct((n_batch, STAT_ROWS, width), jnp.bfloat16),
            jax.ShapeDtypeStruct((n_batch, heads, HEAD_DIM), jnp.bfloat16),
            jax.ShapeDtypeStruct((n_batch, heads, HEAD_DIM), jnp.bfloat16),
            jax.ShapeDtypeStruct((3, n_batch, STAT_ROWS, HEAD_DIM), jnp.float32),
        ],
        in_specs=[vmem] * 5 + [pl.BlockSpec(memory_space=pl.ANY)] + [vmem] * 2,
        out_specs=[vmem] * 4,
        scratch_shapes=[
            pltpu.VMEM(w_q.shape, jnp.bfloat16),
            pltpu.VMEM((n_batch, STAT_ROWS, width), jnp.float32),
            pltpu.SemaphoreType.DMA,
        ],
        compiler_params=pltpu.CompilerParams(vmem_limit_bytes=24 * 2 ** 20),
        cost_estimate=pl.CostEstimate(flops=2 * 2 * n_batch * 3 * w_q.shape[0] * width, bytes_accessed=2 * w_q.size, transcendentals=0),
        name="query_rows",
    )(new_tok, last_x, gain, *row_tabs, pltpu.with_memory_space_constraint(w_q, pltpu.HBM), w_k, w_v)


def when(condition):
    if isinstance(condition, bool):
        return lambda body: body() if condition else None
    return pl.when(condition)


def by_group(group, values):
    if isinstance(group, int):
        return values[group]
    out = values[-1]
    for p in range(len(values) - 1):
        out = jnp.where(group == p, values[p], out)
    return out


def kv_kernel(n_in, n_steps, masks, batches, firsts, row0, stat_of, with_new, raw, *refs):
    n_groups = len(masks)
    n_arr = n_in * n_groups
    x_refs = refs[:n_arr]
    cos_ref, sin_ref, len_ref, wk, wv, q_ref = refs[n_arr:n_arr + 6]
    rest = refs[n_arr + 6:]
    if raw:
        gain_ref, *rest = rest
    if with_new:
        new_refs = rest[:2]
        rest = rest[2:]
    else:
        rest = rest[3:]
    kc_ref, vc_ref, st_ref, x_buf, k_buf, v_buf, k_out, v_out, s_out, x_sem, sems, s_sem = rest[:12]
    me = lax.axis_index("model")
    step = pl.program_id(0) if n_steps > 1 else 0
    slot = lax.rem(step, 2) if n_steps > 1 else 0
    per_group = n_steps // n_groups
    blk = x_buf.shape[2]
    shard_rows = cos_ref.shape[1]
    width = wk.shape[1]
    heads = width // HEAD_DIM
    n_tok = n_in * blk

    def x_copies(at_step, which, group):
        local = at_step - group * per_group
        return [pltpu.make_async_copy(x_refs[group * n_in + i].at[firsts[group][i] + local],
                                      x_buf.at[which, i], x_sem.at[which, i]) for i in range(n_in)]

    def start_x(at_step, which):
        for group in range(n_groups):
            @when(at_step // per_group == group)
            def _(group=group):
                for copy in x_copies(at_step, which, group):
                    copy.start()

    def place(i, at_step):
        group = at_step // per_group
        mask = by_group(group, [m[i] for m in masks])
        shard = sum(lax.rem(me // bit + mask // bit, 2) * bit for bit in (1, 2, 4))
        return shard, by_group(group, [b[i] for b in batches]) + at_step % per_group, mask

    def out_copies(which, at_step):
        copies = []
        for i in range(n_in):
            shard, bat, _ = place(i, at_step)
            rows = pl.ds(shard * shard_rows + row0, blk)
            copies.append(pltpu.make_async_copy(k_out.at[which, i], kc_ref.at[bat, rows], sems.at[which, i, 0]))
            copies.append(pltpu.make_async_copy(v_out.at[which, i], vc_ref.at[bat, rows], sems.at[which, i, 1]))
        return copies

    def new_copies():
        return [pltpu.make_async_copy(src.at[pl.ds(b, 1)], dst.at[b, pl.ds(dst.shape[1] - 1, 1)], rest[12].at[idx, b])
                for idx, (src, dst) in enumerate(zip(new_refs, (kc_ref, vc_ref))) for b in range(src.shape[0])]

    in_place = n_steps == 1

    @when(step == 0)
    def _():
        if not in_place:
            start_x(step, slot)
        if with_new:
            for copy in new_copies():
                copy.start()

    @when(step + 1 < n_steps)
    def _():
        start_x(step + 1, 1 - slot)

    @when(step >= 2)
    def _():
        for copy in out_copies(slot, step - 2):
            copy.wait()

    if not in_place:
        for copy in x_copies(0, slot, 0):
            copy.wait()
    x_rows = x_buf.at[slot]
    if raw:
        lanes = [slice(c * HEAD_DIM, (c + 1) * HEAD_DIM) for c in range(x_buf.shape[3] // HEAD_DIM)]
        for i in range(n_in):
            def norm_rows(r, carry, i=i):
                at = pl.ds(pl.multiple_of(r * NORM_ROWS, NORM_ROWS), NORM_ROWS)
                acc = [jnp.zeros((NORM_ROWS, HEAD_DIM), jnp.float32) for _ in range(2)]
                for c, lane in enumerate(lanes):
                    xf = x_refs[i][0, at, lane].astype(jnp.float32)
                    acc[c % 2] += xf * xf
                inv_rms = lax.rsqrt(jnp.sum(acc[0] + acc[1], axis=-1, keepdims=True) / x_buf.shape[3] + 1e-5)
                for lane in lanes:
                    xf = x_refs[i][0, at, lane].astype(jnp.float32)
                    x_rows[i, at, lane] = (xf * inv_rms * gain_ref[:, lane].astype(jnp.float32)).astype(jnp.bfloat16)
                return carry

            lax.fori_loop(0, blk // NORM_ROWS, norm_rows, 0)

    def col_tile(c, carry):
        cols = pl.ds(pl.multiple_of(c * COL_TILE, COL_TILE), COL_TILE) if n_steps > 1 else slice(c * COL_TILE, (c + 1) * COL_TILE)
        if in_place and not raw:
            normed = jnp.concatenate([x_ref[0] for x_ref in x_refs], axis=0)
        else:
            normed = x_rows[...].reshape(n_tok, x_buf.shape[3])
        kf = jnp.dot(normed, wk[:, cols], preferred_element_type=jnp.float32)
        vf = jnp.dot(normed, wv[:, cols], preferred_element_type=jnp.float32)
        v_buf[:, cols] = vf.astype(jnp.bfloat16)
        parts = []
        for i in range(n_in):
            shard = place(i, step)[0]
            cos_tab = cos_ref[shard, row0:row0 + blk]
            sin_tab = sin_ref[shard, row0:row0 + blk]
            halves = []
            for h in range(COL_TILE // HEAD_DIM):
                kh = kf[i * blk:(i + 1) * blk, h * HEAD_DIM:(h + 1) * HEAD_DIM]
                halves.append(kh * cos_tab + pltpu.roll(kh, HEAD_DIM // 2, 1) * sin_tab)
            parts.append(jnp.concatenate(halves, axis=1))
        k_buf[:, cols] = jnp.concatenate(parts, axis=0).astype(jnp.bfloat16)
        return carry

    if n_steps > 1:
        lax.fori_loop(0, width // COL_TILE, col_tile, 0)
    else:
        for c in range(width // COL_TILE):
            col_tile(c, 0)

    for i in range(n_in):
        k_out[slot, i] = k_buf[i * blk:(i + 1) * blk, :].reshape(blk, heads, HEAD_DIM)
        v_out[slot, i] = v_buf[i * blk:(i + 1) * blk, :].reshape(blk, heads, HEAD_DIM)
    for copy in out_copies(slot, step):
        copy.start()

    head_of_row = lax.broadcasted_iota(jnp.int32, (STAT_ROWS, HEAD_DIM), 0) // (STAT_ROWS // heads)
    probs = []
    for i in range(n_in):
        shard, bat, _ = place(i, step)
        scores = lax.dot_general(q_ref[bat], k_buf[i * blk:(i + 1) * blk, :], (((1,), (1,)), ((), ())),
                                 preferred_element_type=jnp.float32) * (HEAD_DIM ** -0.5)
        pos = shard * shard_rows + row0 + lax.broadcasted_iota(jnp.int32, scores.shape, 1)
        visible = pos < len_ref[pl.ds(bat, 1), :blk]
        scores = jnp.where(visible, scores, NEG_BIG)
        blk_max = jnp.max(scores, axis=-1, keepdims=True)
        prob = jnp.where(visible, jnp.exp(scores - blk_max), 0.0)
        probs.append((blk_max, prob))
    for i, (blk_max, prob) in enumerate(probs):
        full = jnp.dot(prob.astype(jnp.bfloat16), v_buf[i * blk:(i + 1) * blk, :], preferred_element_type=jnp.float32)
        acc = jnp.zeros((STAT_ROWS, HEAD_DIM), jnp.float32)
        for h in range(heads):
            acc = jnp.where(head_of_row == h, full[:, h * HEAD_DIM:(h + 1) * HEAD_DIM], acc)
        s_out[i, 0] = acc
        s_out[i, 1] = jnp.broadcast_to(blk_max, (STAT_ROWS, HEAD_DIM))
        s_out[i, 2] = jnp.broadcast_to(jnp.sum(prob, axis=-1, keepdims=True), (STAT_ROWS, HEAD_DIM))
    stat_copies = []
    for i in range(n_in):
        _, bat, mask = place(i, step)
        stat_copies.append(pltpu.make_async_copy(s_out.at[i], st_ref.at[mask + stat_of, bat], s_sem.at[i]))
        stat_copies[-1].start()
    for copy in stat_copies:
        copy.wait()

    @when(step == n_steps - 1)
    def _():
        for copy in out_copies(slot, step):
            copy.wait()
        if with_new:
            for copy in new_copies():
                copy.wait()
        if n_steps > 1:
            for copy in out_copies(1 - slot, step - 1):
                copy.wait()


def kv_call(groups, per_group, masks, batches, lengths, tabs, w_k, w_v, q_diag, caches, new_rows=None, row0=0, stat_of=0, gain=None):
    n_groups = len(groups)
    n_in = len(groups[0])
    n_steps = n_groups * per_group
    cos_tab, sin_tab = tabs
    blk, d_model = groups[0][0][0].shape[1:]
    width = w_k.shape[1]
    heads = width // HEAD_DIM
    any_spec = pl.BlockSpec(memory_space=pl.ANY)
    operands = [arr for group in groups for arr, _ in group]
    x_spec = any_spec
    if n_steps == 1:
        x_spec = pl.BlockSpec(memory_space=pltpu.VMEM)
        operands = [pltpu.with_memory_space_constraint(arr, pltpu.VMEM) for arr in operands]
    in_specs = [x_spec] * len(operands) + [pl.BlockSpec(memory_space=pltpu.VMEM)] * 6
    operands += [cos_tab, sin_tab, lengths, w_k, w_v, q_diag]
    if gain is not None:
        in_specs.append(pl.BlockSpec(memory_space=pltpu.VMEM))
        operands.append(gain)
    with_new = new_rows is not None
    if with_new:
        operands += new_rows
        in_specs += [any_spec] * 2
        aliases = {}
    else:
        operands += [*caches[:2], pltpu.with_memory_space_constraint(caches[2], pltpu.VMEM)]
        in_specs += [any_spec] * 3
        aliases = {len(operands) - 3: 0, len(operands) - 2: 1, len(operands) - 1: 2}
    tokens = n_in * blk
    n_batch = q_diag.shape[0]
    slots = min(n_steps, 2)
    return pl.pallas_call(
        functools.partial(kv_kernel, n_in, n_steps, masks, batches, [[first for _, first in group] for group in groups], row0, stat_of, with_new, gain is not None),
        grid=(n_steps,) if n_steps > 1 else (),
        in_specs=in_specs,
        out_specs=[any_spec] * 3,
        scratch_shapes=[
            pltpu.VMEM((slots, n_in, blk, d_model), jnp.bfloat16),
            pltpu.VMEM((tokens, width), jnp.bfloat16),
            pltpu.VMEM((tokens, width), jnp.bfloat16),
            pltpu.VMEM((slots, n_in, blk, heads, HEAD_DIM), jnp.bfloat16),
            pltpu.VMEM((slots, n_in, blk, heads, HEAD_DIM), jnp.bfloat16),
            pltpu.VMEM((n_in, 3, STAT_ROWS, HEAD_DIM), jnp.float32),
            pltpu.SemaphoreType.DMA((slots, n_in)),
            pltpu.SemaphoreType.DMA((slots, n_in, 2)),
            pltpu.SemaphoreType.DMA((n_in,)),
        ] + [pltpu.SemaphoreType.DMA((2, n_batch))] * with_new,
        out_shape=[*(jax.ShapeDtypeStruct(c.shape, c.dtype) for c in caches[:2]), pltpu.VMEM(caches[2].shape, caches[2].dtype)],
        input_output_aliases=aliases,
        compiler_params=pltpu.CompilerParams(vmem_limit_bytes=20 * 2 ** 20),
        cost_estimate=pl.CostEstimate(flops=4 * n_steps * tokens * d_model * width, bytes_accessed=2 * n_steps * tokens * (d_model + 2 * width), transcendentals=0),
        name="kv_chunk",
    )(*operands)


def tail_kernel(n_dev, parts_of, stv, self_ref, xs_ref, gain_ref, wo, wg_hbm, wu_hbm, wd_hbm, out_ref,
                wg, wu, wd, rows, a_buf, n_buf, ps1, pr1, ps2, pr2, xo1, xg1, xo2, xg2, w_sem, send_sem, recv_sem):
    me = lax.axis_index("model")
    n_batch = out_ref.shape[1]
    n_rows = 2 * n_batch
    d_model = out_ref.shape[2]
    cols = d_model // n_dev
    heads = STAT_ROWS // 2
    loads = [pltpu.make_async_copy(src, dst, w_sem.at[i]) for i, (src, dst) in enumerate(((wg_hbm, wg), (wu_hbm, wu), (wd_hbm, wd)))]
    for load in loads:
        load.start()
    barrier = pltpu.get_barrier_semaphore()

    def peer_of(mask):
        return sum(lax.rem(me // bit + mask // bit, 2) * bit for bit in (1, 2, 4))

    far_first = ((6,), (7, 2), (4, 5, 3), (1,))
    for mask in sum(far_first, ()):
        pl.semaphore_signal(barrier, inc=1, device_id={"model": peer_of(mask)}, device_id_type=MESH)

    def send(phase, mask, src, dst):
        return pltpu.make_async_remote_copy(
            src_ref=src, dst_ref=dst, send_sem=send_sem.at[phase, mask - 1], recv_sem=recv_sem.at[phase, mask - 1],
            device_id={"model": peer_of(mask)}, device_id_type=MESH)

    for b in range(n_batch):
        top = self_ref[1, b]
        for j in range(parts_of[b]):
            top = jnp.maximum(top, stv[j, b, 1])
        scale = jnp.exp(self_ref[1, b] - top)
        den = scale * self_ref[2, b]
        num = scale * self_ref[0, b]
        for j in range(parts_of[b]):
            scale = jnp.exp(stv[j, b, 1] - top)
            den += scale * stv[j, b, 2]
            num += scale * stv[j, b, 0]
        rows[:, b, :] = num / den
    for h in range(heads):
        for t in range(2):
            a_buf[t * n_batch:(t + 1) * n_batch, h * HEAD_DIM:(h + 1) * HEAD_DIM] = rows[2 * h + t]
    att = a_buf[...].astype(jnp.bfloat16)

    def exchange(phase, base, copies, pr, xo, xg):
        total = base
        for copy, mask in reversed(copies):
            copy.wait_recv()
            total = total + pr[mask - 1]
        xo[...] = total.astype(jnp.bfloat16)
        xg[me] = xo[...]
        outs = []
        for mask in sum(far_first, ()):
            outs.append(send(phase + 1, mask, xo, xg.at[me]))
            outs[-1].start()
        for out in outs:
            out.wait_recv()
        return [copy for copy, _ in copies] + outs

    def col_block(p):
        return pl.ds(pl.multiple_of(p * cols, cols), cols)

    part = jnp.dot(att, wo[...], preferred_element_type=jnp.float32)
    for j in range(n_dev):
        ps1[j] = part[:, j * cols:(j + 1) * cols]
    pl.semaphore_wait(barrier, n_dev - 1)
    copies = []
    for mask in sum(far_first, ()):
        copies.append((send(0, mask, ps1.at[peer_of(mask)], pr1.at[mask - 1]), mask))
        copies[-1][0].start()
    sent = exchange(0, xs_ref[...].astype(jnp.float32) + ps1[me], copies, pr1, xo1, xg1)
    sq = jnp.zeros((n_rows, 1), jnp.float32)
    for j in range(n_dev):
        xf = xg1[j].astype(jnp.float32)
        sq += jnp.sum(xf * xf, axis=-1, keepdims=True)
    inv_rms = lax.rsqrt(sq / d_model + 1e-5)
    for j in range(n_dev):
        at = slice(j * cols, (j + 1) * cols)
        n_buf[:, at] = (xg1[j].astype(jnp.float32) * inv_rms * gain_ref[:, at].astype(jnp.float32)).astype(jnp.bfloat16)
    loads[0].wait()
    loads[1].wait()
    gate = jnp.dot(n_buf[...], wg[...], preferred_element_type=jnp.float32)
    up = jnp.dot(n_buf[...], wu[...], preferred_element_type=jnp.float32)
    mid = (gate * (1.0 / (1.0 + jnp.exp(-gate))) * up).astype(jnp.bfloat16)
    loads[2].wait()
    copies = []
    for group in far_first:
        for mask in group:
            ps2[mask] = jnp.dot(mid, wd[:, col_block(peer_of(mask))], preferred_element_type=jnp.float32)
        if group == far_first[-1]:
            ps2[0] = jnp.dot(mid, wd[:, col_block(me)], preferred_element_type=jnp.float32)
        for mask in group:
            copies.append((send(2, mask, ps2.at[mask], pr2.at[mask - 1]), mask))
            copies[-1][0].start()
    sent += exchange(2, xo1[...].astype(jnp.float32) + ps2[0], copies, pr2, xo2, xg2)
    for j in range(n_dev):
        at = slice(j * cols, (j + 1) * cols)
        out_ref[0, :, at] = xg2[j, :n_batch]
        out_ref[1, :, at] = xg2[j, n_batch:]
    for copy in sent:
        copy.wait_send()


def tail_call(n_dev, parts_of, stats, self_stat, x_mine, gain, w_o, w_gate, w_up, w_down, n_batch):
    n_rows, cols = x_mine.shape
    d_model = w_o.shape[1]
    vmem = pl.BlockSpec(memory_space=pltpu.VMEM)
    any_spec = pl.BlockSpec(memory_space=pl.ANY)
    exchanged = [pltpu.VMEM((n_dev, n_rows, cols), jnp.float32), pltpu.VMEM((n_dev - 1, n_rows, cols), jnp.float32)]
    summed = [pltpu.VMEM((n_rows, cols), jnp.bfloat16), pltpu.VMEM((n_dev, n_rows, cols), jnp.bfloat16)]
    return pl.pallas_call(
        functools.partial(tail_kernel, n_dev, parts_of),
        out_shape=jax.ShapeDtypeStruct((2, n_batch, d_model), jnp.bfloat16),
        in_specs=[vmem] * 5 + [any_spec] * 3,
        out_specs=vmem,
        scratch_shapes=[
            pltpu.VMEM(w_gate.shape, jnp.bfloat16),
            pltpu.VMEM(w_up.shape, jnp.bfloat16),
            pltpu.VMEM(w_down.shape, jnp.bfloat16),
            pltpu.VMEM((STAT_ROWS, n_batch, HEAD_DIM), jnp.float32),
            pltpu.VMEM((n_rows, w_o.shape[0]), jnp.float32),
            pltpu.VMEM((n_rows, d_model), jnp.bfloat16),
            *exchanged, *exchanged, *summed, *summed,
            pltpu.SemaphoreType.DMA((3,)),
            pltpu.SemaphoreType.DMA((4, n_dev - 1)),
            pltpu.SemaphoreType.DMA((4, n_dev - 1)),
        ],
        compiler_params=pltpu.CompilerParams(collective_id=0, has_side_effects=True, vmem_limit_bytes=46 * 2 ** 20),
        name="tail",
    )(pltpu.with_memory_space_constraint(stats, pltpu.VMEM), self_stat, x_mine, gain, w_o,
      *(pltpu.with_memory_space_constraint(w, pltpu.HBM) for w in (w_gate, w_up, w_down)))


def solution(mesh):
    n_dev = mesh.shape['model']
    seq_spec = P('replica', 'model', None)
    col_spec = P(None, None, 'model')
    row_spec = P(None, 'model', None)
    gain_spec = P(None, None)
    tok_spec = P('replica', None)
    cache_spec = P(None, 'replica', None, 'model', None)
    in_specs = (seq_spec, P('replica'), tok_spec, gain_spec, col_spec, col_spec, col_spec, row_spec, gain_spec, col_spec, col_spec, row_spec)
    out_specs = (tok_spec, tok_spec, cache_spec, cache_spec)

    def swap(arr, bit):
        return lax.ppermute(arr, 'model', [(i, i ^ bit) for i in range(n_dev)])

    def per_device(prompt, lengths, new_tok, norm_attn, w_q, w_k, w_v, w_o, norm_mlp, w_gate, w_up, w_down):
        my_idx = lax.axis_index('model')
        n_batch, blk, d_model = prompt.shape
        seq_len = blk * n_dev
        width = w_k.shape[2]
        heads = width // HEAD_DIM
        half = n_batch // 2
        wq = w_q[0]
        gain = norm_attn

        q1, q2, rows_h = 1, n_batch // 4, blk // 2
        a_parts, b_parts = {}, {}
        a_parts["0a"], b_parts["0a"] = prompt[:1, :rows_h], prompt[half:half + 1, :rows_h]
        a_parts["0b"], b_parts["0b"] = first_call(prompt, norm_attn, [(0, rows_h), (half, rows_h)], rows_h)
        from_y, from_x = {}, {}

        def send_part(step, along_y, along_x):
            from_y[step] = swap(along_y, 4)
            from_x[step] = swap(along_x, 2)

        send_part("0a", a_parts["0a"], b_parts["0a"])
        send_part("0b", a_parts["0b"], b_parts["0b"])
        order, outs_of = [], []
        for part, (lo, hi) in ((1, (q1, q2)), (2, (q2, half)), (0, (0, q1))):
            for k in range(lo, hi):
                for side in range(2):
                    order.append(side * half + k)
                    outs_of.append([(4, side * half + k, 0, blk)] + ([(2 * part - 2 + side, k - lo, 0, blk)] if part else []))
        a_parts["1"], b_parts["1"], a_parts["2"], b_parts["2"], normed = norm_call(
            prompt, gain, order, outs_of, [(q2 - q1, blk)] * 2 + [(half - q2, blk)] * 2 + [(n_batch, blk)])
        send_part("1", a_parts["1"], b_parts["1"])
        seq_pos = my_idx * blk + jnp.arange(blk)
        sel = (seq_pos[None, :] == (lengths - 1)[:, None]).astype(jnp.bfloat16)
        last_x = jnp.einsum('bs,bsd->bd', sel, prompt, preferred_element_type=jnp.float32).astype(jnp.bfloat16)
        core, cols_h = my_idx % 2, d_model // 2
        last_x = last_x + swap(last_x, 1)
        last_x = lax.dynamic_slice_in_dim(last_x, core * cols_h, cols_h, axis=1)
        last_x = (last_x + swap(last_x, 2)) + (swap(last_x, 4) + swap(last_x, 6))
        other_x = swap(last_x, 1)
        last_x = jnp.where(core == 0, jnp.concatenate([last_x, other_x], axis=1), jnp.concatenate([other_x, last_x], axis=1))
        send_part("2", a_parts["2"], b_parts["2"])
        send_part("3", b_parts["2"], a_parts["2"])
        send_part("4", normed[half:half + q2], normed[:q2])
        core_all = swap(normed, 1)

        len_rows = jnp.broadcast_to(lengths.astype(jnp.int32)[:, None], (n_batch, HEAD_DIM))
        row_tabs = rotary_tables(jnp.concatenate([lengths, lengths - 1]))
        tabs = tuple(tab.reshape(n_dev, blk, HEAD_DIM) for tab in rotary_tables(jnp.arange(seq_len)))
        x_rows = jnp.concatenate([new_tok, last_x], axis=0)
        x_mine = lax.dynamic_slice_in_dim(x_rows, my_idx * (d_model // n_dev), d_model // n_dev, axis=1)
        wk, wv, wo, last_x, len_rows, row_tabs, tabs, x_mine = lax.optimization_barrier(
            (w_k[0], w_v[0], w_o[0], last_x, len_rows, row_tabs, tabs, x_mine))
        wk, wv, wo = keep_in_vmem(wk, wv, wo)
        q_diag, k_new, v_new, self_stat = rows_call(new_tok, last_x, gain, row_tabs, wq, wk, wv)
        cache_shape = jax.ShapeDtypeStruct((n_batch, seq_len + 1, heads, HEAD_DIM), jnp.bfloat16)
        caches = [cache_shape, cache_shape, jax.ShapeDtypeStruct((2 * n_dev - 2, n_batch, 3, STAT_ROWS, HEAD_DIM), jnp.float32)]

        def run(groups, per_group, masks, batches, caches, **kw):
            return kv_call(groups, per_group, masks, batches, len_rows, tabs, wk, wv, q_diag, caches, **kw)

        def half_rows(step):
            return {"row0": rows_h * (step == "0b"), "stat_of": (n_dev - 2) * (step == "0b"), "gain": norm_attn if step == "0a" else None}

        def after(caches, *arrays):
            out = lax.optimization_barrier((caches[2], *arrays))
            return [caches[0], caches[1], out[0]], out[1:]

        caches = run([[(arr, 0), (arr, half)] for arr in (normed, core_all)], half,
                     [[0] * 2, [1] * 2], [[0, half]] * 2, caches, new_rows=[k_new, v_new])
        diag, turned = {}, {}
        starts = {"0a": (0, half), "0b": (0, half), "1": (q1, half + q1), "2": (q2, half + q2), "3": (half + q2, q2), "4": (half, 0)}
        for step, start in starts.items():
            caches, (got_y, got_x) = after(caches, from_y[step], from_x[step])
            other_y, other_x = swap(got_y, 1), swap(got_x, 1)
            if step not in "34":
                via_x = swap(got_y, 2)
                via_y = swap(got_x, 4)
                diag[step] = (via_x, via_y)
            streams = [[(got_y, 0), (got_x, 0)], [(other_y, 0), (other_x, 0)]]
            if step in ("0a", "0b"):
                caches = run([streams[0] + streams[1]], q1, [[4, 2, 5, 3]], [[*start, *start]], caches, **half_rows(step))
            else:
                caches = run(streams, got_y.shape[0], [[4, 2], [5, 3]], [list(start)] * 2, caches)
            if step in "34":
                caches, (w_t,) = after(caches, (w_gate if step == "3" else w_up)[0].T)
                turned[step] = turn_call(w_t)
                caches, (turned[step],) = after(caches, turned[step])
        for step in ("2", "1", "0a", "0b"):
            caches, (via_y,) = after(caches, diag[step][1])
            caches, (via_x,) = after(caches, diag[step][0])
            other_y = swap(via_y, 1)
            other_x = swap(via_x, 1)
            start = starts[step]
            streams = [[(via_x, 0), (via_y, 0)], [(other_x, 0), (other_y, 0)]]
            if step in ("0a", "0b"):
                caches = run([streams[0] + streams[1]], q1, [[6, 6, 7, 7]], [[*start, *start]], caches, **half_rows(step))
            else:
                caches = run(streams, via_x.shape[0], [[6] * 2, [7] * 2], [list(start)] * 2, caches)

        k_cache, v_cache, stats = caches
        parts_of = [2 * n_dev - 2 if b % half < q1 else n_dev for b in range(n_batch)]
        both = tail_call(n_dev, parts_of, stats, self_stat, x_mine, norm_mlp, wo, turned["3"], turned["4"], w_down[0], n_batch)
        return both[0], both[1], k_cache[None], v_cache[None]

    return jax.shard_map(per_device, mesh=mesh, in_specs=in_specs, out_specs=out_specs, check_vma=False)
```

```python
import functools

import jax
import jax.numpy as jnp
from jax import lax
from jax.experimental import pallas as pl
from jax.experimental.pallas import tpu as pltpu
from jax.sharding import PartitionSpec as P


HEAD_DIM = 128
NEG_BIG = -1e30
STAT_ROWS = 8
NORM_ROWS = 32
COL_TILE = 256
MESH = pl.DeviceIdType.MESH


def rotary_tables(positions):
    half_dim = HEAD_DIM // 2
    inv_freq = 10000.0 ** (-2.0 * jnp.arange(half_dim, dtype=jnp.float32) / HEAD_DIM)
    angles = positions.astype(jnp.float32)[..., None] * inv_freq
    cos_tab = jnp.cos(angles)
    sin_tab = jnp.sin(angles)
    return jnp.concatenate([cos_tab, cos_tab], axis=-1), jnp.concatenate([-sin_tab, sin_tab], axis=-1)


def load_kernel(*refs):
    n = len(refs) // 2
    sem = refs[-1]
    copies = [pltpu.make_async_copy(refs[i], refs[n + i], sem.at[i]) for i in range(n)]
    for copy in copies:
        copy.start()
    for copy in copies:
        copy.wait()


def keep_in_vmem(*arrays):
    return pl.pallas_call(
        load_kernel,
        out_shape=[pltpu.VMEM(arr.shape, arr.dtype) for arr in arrays],
        in_specs=[pl.BlockSpec(memory_space=pl.ANY)] * len(arrays),
        out_specs=[pl.BlockSpec(memory_space=pltpu.VMEM)] * len(arrays),
        scratch_shapes=[pltpu.SemaphoreType.DMA((len(arrays),))],
        compiler_params=pltpu.CompilerParams(vmem_limit_bytes=24 * 2 ** 20),
        name="keep",
    )(*(pltpu.with_memory_space_constraint(arr, pltpu.HBM) for arr in arrays))


def turn_kernel(w_ref, out_ref):
    out_ref[...] = w_ref[...].T


def turn_call(w_t):
    n, d = w_t.shape
    cols = 512
    return pl.pallas_call(
        turn_kernel,
        grid=(d // cols,),
        in_specs=[pl.BlockSpec((n, cols), lambda g: (0, g))],
        out_specs=pl.BlockSpec((cols, n), lambda g: (g, 0)),
        out_shape=jax.ShapeDtypeStruct((d, n), w_t.dtype),
        compiler_params=pltpu.CompilerParams(vmem_limit_bytes=12 * 2 ** 20),
        cost_estimate=pl.CostEstimate(flops=2 * d * n * 128, bytes_accessed=4 * d * n, transcendentals=0),
        name="turn",
    )(pltpu.with_memory_space_constraint(w_t, pltpu.HBM))


def norm_kernel(outs_of, x_ref, gain_ref, *refs):
    n_out = len(refs) - 3
    out_refs = refs[:n_out]
    ss_buf, n_buf, sems = refs[n_out:]
    step = pl.program_id(0)
    blk, d_model = x_ref.shape[1:]
    lanes = [slice(c * HEAD_DIM, (c + 1) * HEAD_DIM) for c in range(d_model // HEAD_DIM)]

    def copies(at_step):
        return [pltpu.make_async_copy(n_buf.at[at_step % 2, pl.ds(lo, rows)], out_refs[o].at[i], sems.at[at_step % 2, k])
                for k, (o, i, lo, rows) in enumerate(outs_of[at_step])]

    for at_step in range(2, len(outs_of)):
        @pl.when(step == at_step)
        def _():
            for copy in copies(at_step - 2):
                copy.wait()

    def square_rows(r, carry):
        rows = pl.ds(pl.multiple_of(r * NORM_ROWS, NORM_ROWS), NORM_ROWS)
        acc = [jnp.zeros((NORM_ROWS, HEAD_DIM), jnp.float32) for _ in range(2)]
        for c, lane in enumerate(lanes):
            xf = x_ref[0, rows, lane].astype(jnp.float32)
            acc[c % 2] += xf * xf
        ss_buf[rows, :] = acc[0] + acc[1]
        return carry

    lax.fori_loop(0, blk // NORM_ROWS, square_rows, 0)
    total = jnp.sum(ss_buf[...], axis=-1, keepdims=True)
    ss_buf[...] = jnp.broadcast_to(lax.rsqrt(total / d_model + 1e-5), (blk, HEAD_DIM))
    slot = lax.rem(step, 2)

    def norm_rows(r, carry):
        rows = pl.ds(pl.multiple_of(r * NORM_ROWS, NORM_ROWS), NORM_ROWS)
        inv_rms = ss_buf[rows, :]
        for lane in lanes:
            xf = x_ref[0, rows, lane].astype(jnp.float32)
            n_buf[slot, rows, lane] = (xf * inv_rms * gain_ref[:, lane].astype(jnp.float32)).astype(jnp.bfloat16)
        return carry

    lax.fori_loop(0, blk // NORM_ROWS, norm_rows, 0)
    for at_step in range(len(outs_of)):
        @pl.when(step == at_step)
        def _():
            for copy in copies(at_step):
                copy.start()
            if at_step == len(outs_of) - 1:
                for copy in copies(at_step):
                    copy.wait()
                if at_step >= 1:
                    for copy in copies(at_step - 1):
                        copy.wait()


def first_kernel(places, rows, x_hbm, gain_hbm, *refs):
    n = len(places)
    out_refs = refs[:n]
    x_buf, gain_ref, sem = refs[n:]
    d_model = x_hbm.shape[2]
    loads = [pltpu.make_async_copy(x_hbm.at[bat, pl.ds(row0, rows)], x_buf.at[i], sem.at[i]) for i, (bat, row0) in enumerate(places)]
    loads.append(pltpu.make_async_copy(gain_hbm, gain_ref, sem.at[n]))
    for load in loads:
        load.start()
    loads[n].wait()
    lanes = [slice(c * HEAD_DIM, (c + 1) * HEAD_DIM) for c in range(d_model // HEAD_DIM)]
    for i in range(n):
        loads[i].wait()

        def norm_rows(r, carry):
            at = pl.ds(pl.multiple_of(r * NORM_ROWS, NORM_ROWS), NORM_ROWS)
            acc = [jnp.zeros((NORM_ROWS, HEAD_DIM), jnp.float32) for _ in range(2)]
            for c, lane in enumerate(lanes):
                xf = x_buf[i, at, lane].astype(jnp.float32)
                acc[c % 2] += xf * xf
            inv_rms = lax.rsqrt(jnp.sum(acc[0] + acc[1], axis=-1, keepdims=True) / d_model + 1e-5)
            for lane in lanes:
                xf = x_buf[i, at, lane].astype(jnp.float32)
                out_refs[i][0, at, lane] = (xf * inv_rms * gain_ref[:, lane].astype(jnp.float32)).astype(jnp.bfloat16)
            return carry

        lax.fori_loop(0, rows // NORM_ROWS, norm_rows, 0)


def first_call(x, gain, places, rows):
    d_model = x.shape[2]
    return pl.pallas_call(
        functools.partial(first_kernel, places, rows),
        out_shape=[pltpu.VMEM((1, rows, d_model), jnp.bfloat16)] * len(places),
        in_specs=[pl.BlockSpec(memory_space=pl.ANY)] * 2,
        out_specs=[pl.BlockSpec(memory_space=pltpu.VMEM)] * len(places),
        scratch_shapes=[
            pltpu.VMEM((len(places), rows, d_model), jnp.bfloat16),
            pltpu.VMEM(gain.shape, gain.dtype),
            pltpu.SemaphoreType.DMA((len(places) + 1,)),
        ],
        compiler_params=pltpu.CompilerParams(vmem_limit_bytes=8 * 2 ** 20),
        cost_estimate=pl.CostEstimate(flops=len(places) * rows * d_model * 8, bytes_accessed=len(places) * rows * d_model * 4, transcendentals=0),
        name="first_rows",
    )(*(pltpu.with_memory_space_constraint(a, pltpu.HBM) for a in (x, gain)))


def norm_call(x, gain, order, outs_of, shapes, blk=None, row_block=0):
    d_model = x.shape[2]
    blk = blk or x.shape[1]

    def prompt_of(g):
        idx = jnp.int32(order[-1])
        for k in range(len(order) - 1):
            idx = jnp.where(g == k, order[k], idx)
        return idx

    return pl.pallas_call(
        functools.partial(norm_kernel, outs_of),
        grid=(len(order),),
        in_specs=[pl.BlockSpec((1, blk, d_model), lambda g: (prompt_of(g), row_block, 0)),
                  pl.BlockSpec((1, d_model), lambda g: (0, 0))],
        out_specs=[pl.BlockSpec(memory_space=pl.ANY)] * len(shapes),
        out_shape=[jax.ShapeDtypeStruct((*shape, d_model), jnp.bfloat16) for shape in shapes],
        scratch_shapes=[
            pltpu.VMEM((blk, HEAD_DIM), jnp.float32),
            pltpu.VMEM((2, blk, d_model), jnp.bfloat16),
            pltpu.SemaphoreType.DMA((2, max(len(o) for o in outs_of))),
        ],
        compiler_params=pltpu.CompilerParams(vmem_limit_bytes=24 * 2 ** 20),
        cost_estimate=pl.CostEstimate(flops=len(order) * blk * d_model * 8, bytes_accessed=len(order) * blk * d_model * 6, transcendentals=0),
        name="norm_rows",
    )(pltpu.with_memory_space_constraint(x, pltpu.HBM), gain)


def rows_kernel(new_ref, last_ref, gain_ref, cos_ref, sin_ref, wq_hbm, wk, wv, q_ref, k_ref, v_ref, st_ref, wq, q_buf, sem):
    load = pltpu.make_async_copy(wq_hbm, wq, sem)
    load.start()
    n_batch = new_ref.shape[0]
    heads = wk.shape[1] // HEAD_DIM
    xf = jnp.concatenate([new_ref[...].astype(jnp.float32), last_ref[...].astype(jnp.float32)], axis=0)
    inv_rms = lax.rsqrt(jnp.mean(xf * xf, axis=-1, keepdims=True) + 1e-5)
    normed = (xf * inv_rms * gain_ref[...].astype(jnp.float32)).astype(jnp.bfloat16)
    k_all = jnp.dot(normed, wk[...], preferred_element_type=jnp.float32)[:n_batch]
    v_all = jnp.dot(normed, wv[...], preferred_element_type=jnp.float32)[:n_batch].astype(jnp.bfloat16)
    load.wait()
    q_all = jnp.dot(normed, wq[...], preferred_element_type=jnp.float32)
    q_buf[...] = jnp.zeros_like(q_buf)
    k_rot = []
    for h in range(heads):
        cols = slice(h * HEAD_DIM, (h + 1) * HEAD_DIM)
        qh = q_all[:, cols]
        qh = (qh * cos_ref[...] + pltpu.roll(qh, HEAD_DIM // 2, 1) * sin_ref[...]).astype(jnp.bfloat16).astype(jnp.float32)
        kh = k_all[:, cols]
        kh = (kh * cos_ref[:n_batch, :] + pltpu.roll(kh, HEAD_DIM // 2, 1) * sin_ref[:n_batch, :]).astype(jnp.bfloat16)
        k_rot.append(kh)
        score = jnp.sum(qh[:n_batch] * kh.astype(jnp.float32), axis=-1, keepdims=True) * (HEAD_DIM ** -0.5)
        zero = jnp.zeros((n_batch, HEAD_DIM), jnp.float32)
        for t in range(2):
            row = 2 * h + t
            q_buf[:, row, cols] = qh[t * n_batch:(t + 1) * n_batch]
            st_ref[0, :, row, :] = v_all[:, cols].astype(jnp.float32) if t == 0 else zero
            st_ref[1, :, row, :] = zero + score if t == 0 else zero + NEG_BIG
            st_ref[2, :, row, :] = zero + 1.0 if t == 0 else zero
    q_ref[...] = q_buf[...].astype(jnp.bfloat16)
    k_ref[...] = jnp.concatenate(k_rot, axis=1).reshape(n_batch, heads, HEAD_DIM)
    v_ref[...] = v_all.reshape(n_batch, heads, HEAD_DIM)


def rows_call(new_tok, last_x, gain, row_tabs, w_q, w_k, w_v):
    n_batch = new_tok.shape[0]
    width = w_q.shape[1]
    heads = width // HEAD_DIM
    vmem = pl.BlockSpec(memory_space=pltpu.VMEM)
    return pl.pallas_call(
        rows_kernel,
        out_shape=[
            jax.ShapeDtypeStruct((n_batch, STAT_ROWS, width), jnp.bfloat16),
            jax.ShapeDtypeStruct((n_batch, heads, HEAD_DIM), jnp.bfloat16),
            jax.ShapeDtypeStruct((n_batch, heads, HEAD_DIM), jnp.bfloat16),
            jax.ShapeDtypeStruct((3, n_batch, STAT_ROWS, HEAD_DIM), jnp.float32),
        ],
        in_specs=[vmem] * 5 + [pl.BlockSpec(memory_space=pl.ANY)] + [vmem] * 2,
        out_specs=[vmem] * 4,
        scratch_shapes=[
            pltpu.VMEM(w_q.shape, jnp.bfloat16),
            pltpu.VMEM((n_batch, STAT_ROWS, width), jnp.float32),
            pltpu.SemaphoreType.DMA,
        ],
        compiler_params=pltpu.CompilerParams(vmem_limit_bytes=24 * 2 ** 20),
        cost_estimate=pl.CostEstimate(flops=2 * 2 * n_batch * 3 * w_q.shape[0] * width, bytes_accessed=2 * w_q.size, transcendentals=0),
        name="query_rows",
    )(new_tok, last_x, gain, *row_tabs, pltpu.with_memory_space_constraint(w_q, pltpu.HBM), w_k, w_v)


def when(condition):
    if isinstance(condition, bool):
        return lambda body: body() if condition else None
    return pl.when(condition)


def by_group(group, values):
    if isinstance(group, int):
        return values[group]
    out = values[-1]
    for p in range(len(values) - 1):
        out = jnp.where(group == p, values[p], out)
    return out


def kv_kernel(n_in, n_steps, masks, batches, firsts, row0, stat_of, with_new, raw, *refs):
    n_groups = len(masks)
    n_arr = n_in * n_groups
    x_refs = refs[:n_arr]
    cos_ref, sin_ref, len_ref, wk, wv, q_ref = refs[n_arr:n_arr + 6]
    rest = refs[n_arr + 6:]
    if raw:
        gain_ref, *rest = rest
    if with_new:
        new_refs = rest[:2]
        rest = rest[2:]
    else:
        rest = rest[3:]
    kc_ref, vc_ref, st_ref, x_buf, k_buf, v_buf, k_out, v_out, s_out, x_sem, sems, s_sem = rest[:12]
    me = lax.axis_index("model")
    step = pl.program_id(0) if n_steps > 1 else 0
    slot = lax.rem(step, 2) if n_steps > 1 else 0
    per_group = n_steps // n_groups
    blk = x_buf.shape[2]
    shard_rows = cos_ref.shape[1]
    width = wk.shape[1]
    heads = width // HEAD_DIM
    n_tok = n_in * blk

    def x_copies(at_step, which, group):
        local = at_step - group * per_group
        return [pltpu.make_async_copy(x_refs[group * n_in + i].at[firsts[group][i] + local],
                                      x_buf.at[which, i], x_sem.at[which, i]) for i in range(n_in)]

    def start_x(at_step, which):
        for group in range(n_groups):
            @when(at_step // per_group == group)
            def _(group=group):
                for copy in x_copies(at_step, which, group):
                    copy.start()

    def place(i, at_step):
        group = at_step // per_group
        mask = by_group(group, [m[i] for m in masks])
        shard = sum(lax.rem(me // bit + mask // bit, 2) * bit for bit in (1, 2, 4))
        return shard, by_group(group, [b[i] for b in batches]) + at_step % per_group, mask

    def out_copies(which, at_step):
        copies = []
        for i in range(n_in):
            shard, bat, _ = place(i, at_step)
            rows = pl.ds(shard * shard_rows + row0, blk)
            copies.append(pltpu.make_async_copy(k_out.at[which, i], kc_ref.at[bat, rows], sems.at[which, i, 0]))
            copies.append(pltpu.make_async_copy(v_out.at[which, i], vc_ref.at[bat, rows], sems.at[which, i, 1]))
        return copies

    def new_copies():
        return [pltpu.make_async_copy(src.at[pl.ds(b, 1)], dst.at[b, pl.ds(dst.shape[1] - 1, 1)], rest[12].at[idx, b])
                for idx, (src, dst) in enumerate(zip(new_refs, (kc_ref, vc_ref))) for b in range(src.shape[0])]

    in_place = n_steps == 1

    @when(step == 0)
    def _():
        if not in_place:
            start_x(step, slot)
        if with_new:
            for copy in new_copies():
                copy.start()

    @when(step + 1 < n_steps)
    def _():
        start_x(step + 1, 1 - slot)

    @when(step >= 2)
    def _():
        for copy in out_copies(slot, step - 2):
            copy.wait()

    if not in_place:
        for copy in x_copies(0, slot, 0):
            copy.wait()
    x_rows = x_buf.at[slot]
    if raw:
        lanes = [slice(c * HEAD_DIM, (c + 1) * HEAD_DIM) for c in range(x_buf.shape[3] // HEAD_DIM)]
        for i in range(n_in):
            def norm_rows(r, carry, i=i):
                at = pl.ds(pl.multiple_of(r * NORM_ROWS, NORM_ROWS), NORM_ROWS)
                acc = [jnp.zeros((NORM_ROWS, HEAD_DIM), jnp.float32) for _ in range(2)]
                for c, lane in enumerate(lanes):
                    xf = x_refs[i][0, at, lane].astype(jnp.float32)
                    acc[c % 2] += xf * xf
                inv_rms = lax.rsqrt(jnp.sum(acc[0] + acc[1], axis=-1, keepdims=True) / x_buf.shape[3] + 1e-5)
                for lane in lanes:
                    xf = x_refs[i][0, at, lane].astype(jnp.float32)
                    x_rows[i, at, lane] = (xf * inv_rms * gain_ref[:, lane].astype(jnp.float32)).astype(jnp.bfloat16)
                return carry

            lax.fori_loop(0, blk // NORM_ROWS, norm_rows, 0)

    def col_tile(c, carry):
        cols = pl.ds(pl.multiple_of(c * COL_TILE, COL_TILE), COL_TILE) if n_steps > 1 else slice(c * COL_TILE, (c + 1) * COL_TILE)
        if in_place and not raw:
            normed = jnp.concatenate([x_ref[0] for x_ref in x_refs], axis=0)
        else:
            normed = x_rows[...].reshape(n_tok, x_buf.shape[3])
        kf = jnp.dot(normed, wk[:, cols], preferred_element_type=jnp.float32)
        vf = jnp.dot(normed, wv[:, cols], preferred_element_type=jnp.float32)
        v_buf[:, cols] = vf.astype(jnp.bfloat16)
        parts = []
        for i in range(n_in):
            shard = place(i, step)[0]
            cos_tab = cos_ref[shard, row0:row0 + blk]
            sin_tab = sin_ref[shard, row0:row0 + blk]
            halves = []
            for h in range(COL_TILE // HEAD_DIM):
                kh = kf[i * blk:(i + 1) * blk, h * HEAD_DIM:(h + 1) * HEAD_DIM]
                halves.append(kh * cos_tab + pltpu.roll(kh, HEAD_DIM // 2, 1) * sin_tab)
            parts.append(jnp.concatenate(halves, axis=1))
        k_buf[:, cols] = jnp.concatenate(parts, axis=0).astype(jnp.bfloat16)
        return carry

    if n_steps > 1:
        lax.fori_loop(0, width // COL_TILE, col_tile, 0)
    else:
        for c in range(width // COL_TILE):
            col_tile(c, 0)

    for i in range(n_in):
        k_out[slot, i] = k_buf[i * blk:(i + 1) * blk, :].reshape(blk, heads, HEAD_DIM)
        v_out[slot, i] = v_buf[i * blk:(i + 1) * blk, :].reshape(blk, heads, HEAD_DIM)
    for copy in out_copies(slot, step):
        copy.start()

    head_of_row = lax.broadcasted_iota(jnp.int32, (STAT_ROWS, HEAD_DIM), 0) // (STAT_ROWS // heads)
    probs = []
    for i in range(n_in):
        shard, bat, _ = place(i, step)
        scores = lax.dot_general(q_ref[bat], k_buf[i * blk:(i + 1) * blk, :], (((1,), (1,)), ((), ())),
                                 preferred_element_type=jnp.float32) * (HEAD_DIM ** -0.5)
        pos = shard * shard_rows + row0 + lax.broadcasted_iota(jnp.int32, scores.shape, 1)
        visible = pos < len_ref[pl.ds(bat, 1), :blk]
        scores = jnp.where(visible, scores, NEG_BIG)
        blk_max = jnp.max(scores, axis=-1, keepdims=True)
        prob = jnp.where(visible, jnp.exp(scores - blk_max), 0.0)
        probs.append((blk_max, prob))
    for i, (blk_max, prob) in enumerate(probs):
        full = jnp.dot(prob.astype(jnp.bfloat16), v_buf[i * blk:(i + 1) * blk, :], preferred_element_type=jnp.float32)
        acc = jnp.zeros((STAT_ROWS, HEAD_DIM), jnp.float32)
        for h in range(heads):
            acc = jnp.where(head_of_row == h, full[:, h * HEAD_DIM:(h + 1) * HEAD_DIM], acc)
        s_out[i, 0] = acc
        s_out[i, 1] = jnp.broadcast_to(blk_max, (STAT_ROWS, HEAD_DIM))
        s_out[i, 2] = jnp.broadcast_to(jnp.sum(prob, axis=-1, keepdims=True), (STAT_ROWS, HEAD_DIM))
    stat_copies = []
    for i in range(n_in):
        _, bat, mask = place(i, step)
        stat_copies.append(pltpu.make_async_copy(s_out.at[i], st_ref.at[mask + stat_of, bat], s_sem.at[i]))
        stat_copies[-1].start()
    for copy in stat_copies:
        copy.wait()

    @when(step == n_steps - 1)
    def _():
        for copy in out_copies(slot, step):
            copy.wait()
        if with_new:
            for copy in new_copies():
                copy.wait()
        if n_steps > 1:
            for copy in out_copies(1 - slot, step - 1):
                copy.wait()


def kv_call(groups, per_group, masks, batches, lengths, tabs, w_k, w_v, q_diag, caches, new_rows=None, row0=0, stat_of=0, gain=None):
    n_groups = len(groups)
    n_in = len(groups[0])
    n_steps = n_groups * per_group
    cos_tab, sin_tab = tabs
    blk, d_model = groups[0][0][0].shape[1:]
    width = w_k.shape[1]
    heads = width // HEAD_DIM
    any_spec = pl.BlockSpec(memory_space=pl.ANY)
    operands = [arr for group in groups for arr, _ in group]
    x_spec = any_spec
    if n_steps == 1:
        x_spec = pl.BlockSpec(memory_space=pltpu.VMEM)
        operands = [pltpu.with_memory_space_constraint(arr, pltpu.VMEM) for arr in operands]
    in_specs = [x_spec] * len(operands) + [pl.BlockSpec(memory_space=pltpu.VMEM)] * 6
    operands += [cos_tab, sin_tab, lengths, w_k, w_v, q_diag]
    if gain is not None:
        in_specs.append(pl.BlockSpec(memory_space=pltpu.VMEM))
        operands.append(gain)
    with_new = new_rows is not None
    if with_new:
        operands += new_rows
        in_specs += [any_spec] * 2
        aliases = {}
    else:
        operands += [*caches[:2], pltpu.with_memory_space_constraint(caches[2], pltpu.VMEM)]
        in_specs += [any_spec] * 3
        aliases = {len(operands) - 3: 0, len(operands) - 2: 1, len(operands) - 1: 2}
    tokens = n_in * blk
    n_batch = q_diag.shape[0]
    slots = min(n_steps, 2)
    return pl.pallas_call(
        functools.partial(kv_kernel, n_in, n_steps, masks, batches, [[first for _, first in group] for group in groups], row0, stat_of, with_new, gain is not None),
        grid=(n_steps,) if n_steps > 1 else (),
        in_specs=in_specs,
        out_specs=[any_spec] * 3,
        scratch_shapes=[
            pltpu.VMEM((slots, n_in, blk, d_model), jnp.bfloat16),
            pltpu.VMEM((tokens, width), jnp.bfloat16),
            pltpu.VMEM((tokens, width), jnp.bfloat16),
            pltpu.VMEM((slots, n_in, blk, heads, HEAD_DIM), jnp.bfloat16),
            pltpu.VMEM((slots, n_in, blk, heads, HEAD_DIM), jnp.bfloat16),
            pltpu.VMEM((n_in, 3, STAT_ROWS, HEAD_DIM), jnp.float32),
            pltpu.SemaphoreType.DMA((slots, n_in)),
            pltpu.SemaphoreType.DMA((slots, n_in, 2)),
            pltpu.SemaphoreType.DMA((n_in,)),
        ] + [pltpu.SemaphoreType.DMA((2, n_batch))] * with_new,
        out_shape=[*(jax.ShapeDtypeStruct(c.shape, c.dtype) for c in caches[:2]), pltpu.VMEM(caches[2].shape, caches[2].dtype)],
        input_output_aliases=aliases,
        compiler_params=pltpu.CompilerParams(vmem_limit_bytes=20 * 2 ** 20),
        cost_estimate=pl.CostEstimate(flops=4 * n_steps * tokens * d_model * width, bytes_accessed=2 * n_steps * tokens * (d_model + 2 * width), transcendentals=0),
        name="kv_chunk",
    )(*operands)


def tail_kernel(n_dev, parts_of, stv, self_ref, xs_ref, gain_ref, wo, wg_hbm, wu_hbm, wd_hbm, out_ref,
                wg, wu, wd, rows, a_buf, n_buf, ps1, pr1, ps2, pr2, xo1, xg1, xo2, xg2, w_sem, send_sem, recv_sem):
    me = lax.axis_index("model")
    n_batch = out_ref.shape[1]
    n_rows = 2 * n_batch
    d_model = out_ref.shape[2]
    cols = d_model // n_dev
    heads = STAT_ROWS // 2
    loads = [pltpu.make_async_copy(src, dst, w_sem.at[i]) for i, (src, dst) in enumerate(((wg_hbm, wg), (wu_hbm, wu), (wd_hbm, wd)))]
    for load in loads:
        load.start()
    barrier = pltpu.get_barrier_semaphore()

    def peer_of(mask):
        return sum(lax.rem(me // bit + mask // bit, 2) * bit for bit in (1, 2, 4))

    far_first = ((6, 7), (2, 3, 4, 5), (1,))
    for mask in sum(far_first, ()):
        pl.semaphore_signal(barrier, inc=1, device_id={"model": peer_of(mask)}, device_id_type=MESH)

    def send(phase, mask, src, dst):
        return pltpu.make_async_remote_copy(
            src_ref=src, dst_ref=dst, send_sem=send_sem.at[phase, mask - 1], recv_sem=recv_sem.at[phase, mask - 1],
            device_id={"model": peer_of(mask)}, device_id_type=MESH)

    for b in range(n_batch):
        top = self_ref[1, b]
        for j in range(parts_of[b]):
            top = jnp.maximum(top, stv[j, b, 1])
        scale = jnp.exp(self_ref[1, b] - top)
        den = scale * self_ref[2, b]
        num = scale * self_ref[0, b]
        for j in range(parts_of[b]):
            scale = jnp.exp(stv[j, b, 1] - top)
            den += scale * stv[j, b, 2]
            num += scale * stv[j, b, 0]
        rows[:, b, :] = num / den
    for h in range(heads):
        for t in range(2):
            a_buf[t * n_batch:(t + 1) * n_batch, h * HEAD_DIM:(h + 1) * HEAD_DIM] = rows[2 * h + t]
    att = a_buf[...].astype(jnp.bfloat16)

    def exchange(phase, base, copies, pr, xo, xg):
        total = base
        for copy, mask in reversed(copies):
            copy.wait_recv()
            total = total + pr[mask - 1]
        xo[...] = total.astype(jnp.bfloat16)
        xg[me] = xo[...]
        outs = []
        for mask in sum(far_first, ()):
            outs.append(send(phase + 1, mask, xo, xg.at[me]))
            outs[-1].start()
        for out in outs:
            out.wait_recv()
        return [copy for copy, _ in copies] + outs

    def col_block(p):
        return pl.ds(pl.multiple_of(p * cols, cols), cols)

    part = jnp.dot(att, wo[...], preferred_element_type=jnp.float32)
    for j in range(n_dev):
        ps1[j] = part[:, j * cols:(j + 1) * cols]
    pl.semaphore_wait(barrier, n_dev - 1)
    copies = []
    for mask in sum(far_first, ()):
        copies.append((send(0, mask, ps1.at[peer_of(mask)], pr1.at[mask - 1]), mask))
        copies[-1][0].start()
    sent = exchange(0, xs_ref[...].astype(jnp.float32) + ps1[me], copies, pr1, xo1, xg1)
    squares = jnp.zeros((n_rows, cols), jnp.float32)
    for j in range(n_dev):
        xf = xg1[j].astype(jnp.float32)
        squares += xf * xf
    inv_rms = lax.rsqrt(jnp.sum(squares, axis=-1, keepdims=True) / d_model + 1e-5)
    for j in range(n_dev):
        at = slice(j * cols, (j + 1) * cols)
        n_buf[:, at] = (xg1[j].astype(jnp.float32) * inv_rms * gain_ref[:, at].astype(jnp.float32)).astype(jnp.bfloat16)
    loads[0].wait()
    loads[1].wait()
    gate = jnp.dot(n_buf[...], wg[...], preferred_element_type=jnp.float32)
    up = jnp.dot(n_buf[...], wu[...], preferred_element_type=jnp.float32)
    mid = (gate * (1.0 / (1.0 + jnp.exp(-gate))) * up).astype(jnp.bfloat16)
    loads[2].wait()
    copies = []
    for group in far_first:
        for mask in group:
            ps2[mask] = jnp.dot(mid, wd[:, col_block(peer_of(mask))], preferred_element_type=jnp.float32)
        if group == far_first[-1]:
            ps2[0] = jnp.dot(mid, wd[:, col_block(me)], preferred_element_type=jnp.float32)
        for mask in group:
            copies.append((send(2, mask, ps2.at[mask], pr2.at[mask - 1]), mask))
            copies[-1][0].start()
    sent += exchange(2, xo1[...].astype(jnp.float32) + ps2[0], copies, pr2, xo2, xg2)
    for j in range(n_dev):
        at = slice(j * cols, (j + 1) * cols)
        out_ref[0, :, at] = xg2[j, :n_batch]
        out_ref[1, :, at] = xg2[j, n_batch:]
    for copy in sent:
        copy.wait_send()


def tail_call(n_dev, parts_of, stats, self_stat, x_mine, gain, w_o, w_gate, w_up, w_down, n_batch):
    n_rows, cols = x_mine.shape
    d_model = w_o.shape[1]
    vmem = pl.BlockSpec(memory_space=pltpu.VMEM)
    any_spec = pl.BlockSpec(memory_space=pl.ANY)
    exchanged = [pltpu.VMEM((n_dev, n_rows, cols), jnp.float32), pltpu.VMEM((n_dev - 1, n_rows, cols), jnp.float32)]
    summed = [pltpu.VMEM((n_rows, cols), jnp.bfloat16), pltpu.VMEM((n_dev, n_rows, cols), jnp.bfloat16)]
    return pl.pallas_call(
        functools.partial(tail_kernel, n_dev, parts_of),
        out_shape=jax.ShapeDtypeStruct((2, n_batch, d_model), jnp.bfloat16),
        in_specs=[vmem] * 5 + [any_spec] * 3,
        out_specs=vmem,
        scratch_shapes=[
            pltpu.VMEM(w_gate.shape, jnp.bfloat16),
            pltpu.VMEM(w_up.shape, jnp.bfloat16),
            pltpu.VMEM(w_down.shape, jnp.bfloat16),
            pltpu.VMEM((STAT_ROWS, n_batch, HEAD_DIM), jnp.float32),
            pltpu.VMEM((n_rows, w_o.shape[0]), jnp.float32),
            pltpu.VMEM((n_rows, d_model), jnp.bfloat16),
            *exchanged, *exchanged, *summed, *summed,
            pltpu.SemaphoreType.DMA((3,)),
            pltpu.SemaphoreType.DMA((4, n_dev - 1)),
            pltpu.SemaphoreType.DMA((4, n_dev - 1)),
        ],
        compiler_params=pltpu.CompilerParams(collective_id=0, has_side_effects=True, vmem_limit_bytes=46 * 2 ** 20),
        name="tail",
    )(pltpu.with_memory_space_constraint(stats, pltpu.VMEM), self_stat, x_mine, gain, w_o,
      *(pltpu.with_memory_space_constraint(w, pltpu.HBM) for w in (w_gate, w_up, w_down)))


def solution(mesh):
    n_dev = mesh.shape['model']
    seq_spec = P('replica', 'model', None)
    col_spec = P(None, None, 'model')
    row_spec = P(None, 'model', None)
    gain_spec = P(None, None)
    tok_spec = P('replica', None)
    cache_spec = P(None, 'replica', None, 'model', None)
    in_specs = (seq_spec, P('replica'), tok_spec, gain_spec, col_spec, col_spec, col_spec, row_spec, gain_spec, col_spec, col_spec, row_spec)
    out_specs = (tok_spec, tok_spec, cache_spec, cache_spec)

    def swap(arr, bit):
        return lax.ppermute(arr, 'model', [(i, i ^ bit) for i in range(n_dev)])

    def per_device(prompt, lengths, new_tok, norm_attn, w_q, w_k, w_v, w_o, norm_mlp, w_gate, w_up, w_down):
        my_idx = lax.axis_index('model')
        n_batch, blk, d_model = prompt.shape
        seq_len = blk * n_dev
        width = w_k.shape[2]
        heads = width // HEAD_DIM
        half = n_batch // 2
        wq = w_q[0]
        gain = norm_attn

        q1, q2, rows_h = 1, n_batch // 4, blk // 2
        a_parts, b_parts = {}, {}
        a_parts["0a"], b_parts["0a"] = prompt[:1, :rows_h], prompt[half:half + 1, :rows_h]
        a_parts["0b"], b_parts["0b"] = first_call(prompt, norm_attn, [(0, rows_h), (half, rows_h)], rows_h)
        from_y, from_x = {}, {}

        def send_part(step, along_y, along_x):
            from_y[step] = swap(along_y, 4)
            from_x[step] = swap(along_x, 2)

        send_part("0a", a_parts["0a"], b_parts["0a"])
        send_part("0b", a_parts["0b"], b_parts["0b"])
        order, outs_of = [], []
        for part, (lo, hi) in ((1, (q1, q2)), (2, (q2, half)), (0, (0, q1))):
            for k in range(lo, hi):
                for side in range(2):
                    order.append(side * half + k)
                    outs_of.append([(4, side * half + k, 0, blk)] + ([(2 * part - 2 + side, k - lo, 0, blk)] if part else []))
        a_parts["1"], b_parts["1"], a_parts["2"], b_parts["2"], normed = norm_call(
            prompt, gain, order, outs_of, [(q2 - q1, blk)] * 2 + [(half - q2, blk)] * 2 + [(n_batch, blk)])
        send_part("1", a_parts["1"], b_parts["1"])
        seq_pos = my_idx * blk + jnp.arange(blk)
        sel = (seq_pos[None, :] == (lengths - 1)[:, None]).astype(jnp.bfloat16)
        last_x = jnp.einsum('bs,bsd->bd', sel, prompt, preferred_element_type=jnp.float32).astype(jnp.bfloat16)
        core, cols_h = my_idx % 2, d_model // 2
        last_x = last_x + swap(last_x, 1)
        last_x = lax.dynamic_slice_in_dim(last_x, core * cols_h, cols_h, axis=1)
        last_x = (last_x + swap(last_x, 2)) + (swap(last_x, 4) + swap(last_x, 6))
        other_x = swap(last_x, 1)
        last_x = jnp.where(core == 0, jnp.concatenate([last_x, other_x], axis=1), jnp.concatenate([other_x, last_x], axis=1))
        send_part("2", a_parts["2"], b_parts["2"])
        send_part("3", b_parts["2"], a_parts["2"])
        send_part("4", normed[half:half + q2], normed[:q2])
        core_all = swap(normed, 1)

        len_rows = jnp.broadcast_to(lengths.astype(jnp.int32)[:, None], (n_batch, HEAD_DIM))
        row_tabs = rotary_tables(jnp.concatenate([lengths, lengths - 1]))
        tabs = tuple(tab.reshape(n_dev, blk, HEAD_DIM) for tab in rotary_tables(jnp.arange(seq_len)))
        x_rows = jnp.concatenate([new_tok, last_x], axis=0)
        x_mine = lax.dynamic_slice_in_dim(x_rows, my_idx * (d_model // n_dev), d_model // n_dev, axis=1)
        wk, wv, wo, last_x, len_rows, row_tabs, tabs, x_mine = lax.optimization_barrier(
            (w_k[0], w_v[0], w_o[0], last_x, len_rows, row_tabs, tabs, x_mine))
        wk, wv, wo = keep_in_vmem(wk, wv, wo)
        q_diag, k_new, v_new, self_stat = rows_call(new_tok, last_x, gain, row_tabs, wq, wk, wv)
        cache_shape = jax.ShapeDtypeStruct((n_batch, seq_len + 1, heads, HEAD_DIM), jnp.bfloat16)
        caches = [cache_shape, cache_shape, jax.ShapeDtypeStruct((2 * n_dev - 2, n_batch, 3, STAT_ROWS, HEAD_DIM), jnp.float32)]

        def run(groups, per_group, masks, batches, caches, **kw):
            return kv_call(groups, per_group, masks, batches, len_rows, tabs, wk, wv, q_diag, caches, **kw)

        def half_rows(step):
            return {"row0": rows_h * (step == "0b"), "stat_of": (n_dev - 2) * (step == "0b"), "gain": norm_attn if step == "0a" else None}

        def after(caches, *arrays):
            out = lax.optimization_barrier((caches[2], *arrays))
            return [caches[0], caches[1], out[0]], out[1:]

        caches = run([[(arr, 0), (arr, half)] for arr in (normed, core_all)], half,
                     [[0] * 2, [1] * 2], [[0, half]] * 2, caches, new_rows=[k_new, v_new])
        diag, turned = {}, {}
        starts = {"0a": (0, half), "0b": (0, half), "1": (q1, half + q1), "2": (q2, half + q2), "3": (half + q2, q2), "4": (half, 0)}
        for step, start in starts.items():
            caches, (got_y, got_x) = after(caches, from_y[step], from_x[step])
            other_y, other_x = swap(got_y, 1), swap(got_x, 1)
            if step not in "34":
                via_x = swap(got_y, 2)
                via_y = swap(got_x, 4)
                diag[step] = (via_x, via_y)
            streams = [[(got_y, 0), (got_x, 0)], [(other_y, 0), (other_x, 0)]]
            if step in ("0a", "0b"):
                caches = run([streams[0] + streams[1]], q1, [[4, 2, 5, 3]], [[*start, *start]], caches, **half_rows(step))
            else:
                caches = run(streams, got_y.shape[0], [[4, 2], [5, 3]], [list(start)] * 2, caches)
            if step in "34":
                caches, (w_t,) = after(caches, (w_gate if step == "3" else w_up)[0].T)
                turned[step] = turn_call(w_t)
                caches, (turned[step],) = after(caches, turned[step])
        for step in ("2", "1", "0a", "0b"):
            caches, (via_y,) = after(caches, diag[step][1])
            caches, (via_x,) = after(caches, diag[step][0])
            other_y = swap(via_y, 1)
            other_x = swap(via_x, 1)
            start = starts[step]
            streams = [[(via_x, 0), (via_y, 0)], [(other_x, 0), (other_y, 0)]]
            if step in ("0a", "0b"):
                caches = run([streams[0] + streams[1]], q1, [[6, 6, 7, 7]], [[*start, *start]], caches, **half_rows(step))
            else:
                caches = run(streams, via_x.shape[0], [[6] * 2, [7] * 2], [list(start)] * 2, caches)

        k_cache, v_cache, stats = caches
        parts_of = [2 * n_dev - 2 if b % half < q1 else n_dev for b in range(n_batch)]
        both = tail_call(n_dev, parts_of, stats, self_stat, x_mine, norm_mlp, wo, turned["3"], turned["4"], w_down[0], n_batch)
        return both[0], both[1], k_cache[None], v_cache[None]

    return jax.shard_map(per_device, mesh=mesh, in_specs=in_specs, out_specs=out_specs, check_vma=False)
```
